16 devices in a mesh: ep: 2 (over z), dp: 8 (over y, x, core).
Axes of the slice: x: 2, y: 2, z: 2, core: 2. Of those that a mesh axis runs over, the one named last changes fastest.
Arguments:
- tokens: bfloat16 [16384, 512], P(('dp', 'ep'))
- d_out: bfloat16 [16384, 512], P(('dp', 'ep'))
- expert_ids: int32 [2, 16384, 8], P(None, ('dp', 'ep'))
- gate_vals: float32 [2, 16384, 8], P(None, ('dp', 'ep'))
- w_mix: bfloat16 [2, 512, 512], replicated
- w_gate: bfloat16 [2, 128, 512, 192], P(None, 'ep')
- w_up: bfloat16 [2, 128, 512, 192], P(None, 'ep')
- w_down: bfloat16 [2, 128, 192, 512], P(None, 'ep')
Outputs:
- output 1: bfloat16 [16384, 512], P(('dp', 'ep'))
- output 2: bfloat16 [16384, 512], P(('dp', 'ep'))
- output 3: bfloat16 [2, 512, 512], replicated
- output 4: bfloat16 [2, 128, 512, 192], P(None, 'ep')
- output 5: bfloat16 [2, 128, 512, 192], P(None, 'ep')
- output 6: bfloat16 [2, 128, 192, 512], P(None, 'ep')
All inputs are finite; a program needn't handle non-finite values.
Results may differ from the reference program's by a relative error of at most 0.0179442.
Values are sent between devices in bfloat16 or wider.
A program may use at most 1 GiB of HBM per device.

```python
import jax
import jax.numpy as jnp

D = 512
FF = 192
EXPERTS = 128
TOP = 8
TOK = 1024
NDEV = 16
LAYERS = 2
CAP = 192
HOT = 16

N_TOK = TOK * NDEV
CAP_ALL = CAP * NDEV


def route_device(hot_mask, dev_key):
    key_rest, key_run, key_tok = jax.random.split(dev_key, 3)
    rest_copies = TOK * TOP - HOT * CAP
    base_count = rest_copies // (EXPERTS - HOT)
    extra_count = rest_copies % (EXPERTS - HOT)
    shuffled = jax.random.permutation(key_rest, EXPERTS)
    cold_sorted = 1 - hot_mask[shuffled]
    cold_rank = jnp.cumsum(cold_sorted) - 1
    bonus_sorted = cold_sorted * (cold_rank < extra_count).astype(jnp.int32)
    bonus = jnp.zeros((EXPERTS,), jnp.int32).at[shuffled].set(bonus_sorted)
    counts = jnp.where(hot_mask == 1, CAP, base_count + bonus)
    run_order = jax.random.permutation(key_run, EXPERTS)
    flat_ids = jnp.repeat(run_order, counts[run_order], total_repeat_length=TOK * TOP)
    table = flat_ids.reshape(TOP, TOK).T
    return table[jax.random.permutation(key_tok, TOK)]


def route_layer(layer_key):
    key_hot, key_dev = jax.random.split(layer_key)
    hot_ids = jax.random.permutation(key_hot, EXPERTS)[:HOT]
    hot_mask = jnp.zeros((EXPERTS,), jnp.int32).at[hot_ids].set(1)
    per_device = jax.vmap(route_device, in_axes=(None, 0))(hot_mask, jax.random.split(key_dev, NDEV))
    return per_device.reshape(N_TOK, TOP)


def setup_inputs(seed: int = 0) -> dict:
    keys = jax.random.split(jax.random.key(seed), 8)
    tokens = jax.random.normal(keys[0], (N_TOK, D), jnp.float32).astype(jnp.bfloat16)
    d_out = jax.random.normal(keys[1], (N_TOK, D), jnp.float32).astype(jnp.bfloat16)
    expert_ids = jax.vmap(route_layer)(jax.random.split(keys[2], LAYERS))
    gate_vals = jax.random.uniform(keys[3], (LAYERS, N_TOK, TOP), jnp.float32, 0.5, 1.5) * TOP ** -0.5
    w_mix = (jax.random.normal(keys[4], (LAYERS, D, D), jnp.float32) * D ** -0.5).astype(jnp.bfloat16)
    w_gate = (jax.random.normal(keys[5], (LAYERS, EXPERTS, D, FF), jnp.float32) * D ** -0.5).astype(jnp.bfloat16)
    w_up = (jax.random.normal(keys[6], (LAYERS, EXPERTS, D, FF), jnp.float32) * D ** -0.5).astype(jnp.bfloat16)
    w_down = (jax.random.normal(keys[7], (LAYERS, EXPERTS, FF, D), jnp.float32) * FF ** -0.5).astype(jnp.bfloat16)
    return {'tokens': tokens, 'd_out': d_out, 'expert_ids': expert_ids, 'gate_vals': gate_vals,
            'w_mix': w_mix, 'w_gate': w_gate, 'w_up': w_up, 'w_down': w_down}


def silu_parts(pre_gate):
    sig_val = jax.nn.sigmoid(pre_gate)
    return pre_gate * sig_val, sig_val * (1.0 + pre_gate * (1.0 - sig_val))


def copy_slots(expert_ids):
    flat_ids = expert_ids.reshape(-1)
    sort_order = jnp.argsort(flat_ids, stable=True)
    sorted_ids = flat_ids[sort_order]
    counts = jnp.bincount(flat_ids, length=EXPERTS)
    starts = jnp.cumsum(counts) - counts
    rows_sorted = sorted_ids * CAP_ALL + jnp.arange(flat_ids.shape[0]) - starts[sorted_ids]
    return jnp.zeros_like(flat_ids).at[sort_order].set(rows_sorted)


def layer_forward(x_in, expert_ids, gate_vals, w_mix, w_gate, w_up, w_down):
    mixed = x_in.astype(jnp.float32) + jnp.dot(x_in, w_mix, preferred_element_type=jnp.float32)
    u_act = mixed.astype(jnp.bfloat16)
    copy_rows = copy_slots(expert_ids)
    copy_tok = jnp.arange(N_TOK * TOP) // TOP
    expert_in = jnp.zeros((EXPERTS * CAP_ALL, D), jnp.bfloat16).at[copy_rows].set(u_act[copy_tok])
    expert_in = expert_in.reshape(EXPERTS, CAP_ALL, D)
    expert_f = expert_in.astype(jnp.float32)
    pre_gate = jnp.einsum('ecd,edf->ecf', expert_f, w_gate.astype(jnp.float32))
    pre_up = jnp.einsum('ecd,edf->ecf', expert_f, w_up.astype(jnp.float32))
    act, _ = silu_parts(pre_gate)
    hidden = (act * pre_up).astype(jnp.bfloat16)
    expert_out = jnp.einsum('ecf,efd->ecd', hidden.astype(jnp.float32), w_down.astype(jnp.float32)).astype(jnp.bfloat16)
    out_copy = expert_out.reshape(EXPERTS * CAP_ALL, D)[copy_rows].reshape(N_TOK, TOP, D)
    y_out = u_act.astype(jnp.float32) + jnp.sum(gate_vals[:, :, None] * out_copy.astype(jnp.float32), axis=1)
    return y_out.astype(jnp.bfloat16), (x_in, copy_rows, expert_in, pre_gate, pre_up, hidden)


def layer_backward(saved, d_y, gate_vals, w_mix, w_gate, w_up, w_down):
    x_in, copy_rows, expert_in, pre_gate, pre_up, hidden = saved
    g_dy = (gate_vals[:, :, None] * d_y.astype(jnp.float32)[:, None, :]).astype(jnp.bfloat16).reshape(N_TOK * TOP, D)
    d_buf = jnp.zeros((EXPERTS * CAP_ALL, D), jnp.bfloat16).at[copy_rows].set(g_dy).reshape(EXPERTS, CAP_ALL, D)
    d_buf_f = d_buf.astype(jnp.float32)
    d_hidden = jnp.einsum('ecd,efd->ecf', d_buf_f, w_down.astype(jnp.float32))
    act, act_slope = silu_parts(pre_gate)
    d_pre_gate = (d_hidden * pre_up * act_slope).astype(jnp.bfloat16).astype(jnp.float32)
    d_pre_up = (d_hidden * act).astype(jnp.bfloat16).astype(jnp.float32)
    d_expert_in = (jnp.einsum('ecf,edf->ecd', d_pre_gate, w_gate.astype(jnp.float32))
                   + jnp.einsum('ecf,edf->ecd', d_pre_up, w_up.astype(jnp.float32))).astype(jnp.bfloat16)
    expert_f = expert_in.astype(jnp.float32)
    g_gate = jnp.einsum('ecd,ecf->edf', expert_f, d_pre_gate).astype(jnp.bfloat16)
    g_up = jnp.einsum('ecd,ecf->edf', expert_f, d_pre_up).astype(jnp.bfloat16)
    g_down = jnp.einsum('ecf,ecd->efd', hidden.astype(jnp.float32), d_buf_f).astype(jnp.bfloat16)
    d_copy = d_expert_in.reshape(EXPERTS * CAP_ALL, D)[copy_rows].reshape(N_TOK, TOP, D)
    d_u = (d_y.astype(jnp.float32) + jnp.sum(gate_vals[:, :, None] * d_copy.astype(jnp.float32), axis=1)).astype(jnp.bfloat16)
    g_mix = jnp.dot(x_in.T, d_u, preferred_element_type=jnp.float32).astype(jnp.bfloat16)
    d_x = (d_u.astype(jnp.float32) + jnp.dot(d_u, w_mix.T, preferred_element_type=jnp.float32)).astype(jnp.bfloat16)
    return d_x, (g_mix, g_gate, g_up, g_down)


def reference(tokens, d_out, expert_ids, gate_vals, w_mix, w_gate, w_up, w_down):
    layer_in = tokens
    saved_all = []
    for layer in range(LAYERS):
        layer_in, saved = layer_forward(layer_in, expert_ids[layer], gate_vals[layer], w_mix[layer],
                                        w_gate[layer], w_up[layer], w_down[layer])
        saved_all.append(saved)
    d_y = d_out
    grads = []
    for layer in reversed(range(LAYERS)):
        d_y, grad_set = layer_backward(saved_all[layer], d_y, gate_vals[layer], w_mix[layer],
                                       w_gate[layer], w_up[layer], w_down[layer])
        grads.insert(0, grad_set)
    return (layer_in, d_y,
            jnp.stack([entry[0] for entry in grads]),
            jnp.stack([entry[1] for entry in grads]),
            jnp.stack([entry[2] for entry in grads]),
            jnp.stack([entry[3] for entry in grads]))
```

```python
import functools

import jax
import jax.numpy as jnp
from jax import lax
from jax.experimental import pallas as pl
from jax.experimental.pallas import tpu as pltpu
from jax.sharding import PartitionSpec as P

CAP_FACTOR = 3
LANES = 128
TILE = 128
WTILE = 256
BATCH = 16
UNROLL = 16
PAGE = 1024
VMEM_LIMIT = 62 * 2**20


def cdiv(a, b):
    return (a + b - 1) // b


def nt_dot(a, b):
    return lax.dot_general(a, b, (((1,), (1,)), ((), ())), preferred_element_type=jnp.float32)


def tn_dot(a, b):
    return lax.dot_general(a, b, (((0,), (0,)), ((), ())), preferred_element_type=jnp.float32)


def nn_dot(a, b):
    return lax.dot_general(a, b, (((1,), (0,)), ((), ())), preferred_element_type=jnp.float32)


def load_rows(ref, start, rows, parts):
    cols = [ref[pl.ds(start * parts + k, rows, stride=parts), :] for k in range(parts)]
    return jnp.concatenate(cols, axis=1).astype(jnp.bfloat16)


def store_rows(ref, start, vals, parts):
    rows = vals.shape[0]
    for k in range(parts):
        ref[pl.ds(start * parts + k, rows, stride=parts), :] = vals[:, k * LANES:(k + 1) * LANES]


def fetch_pair(first, other, dst, sem, ep, tok):
    copies = (pltpu.make_async_copy(first, dst.at[pl.ds(ep * tok, tok)], sem.at[0]),
              pltpu.make_async_copy(other, dst.at[pl.ds((1 - ep) * tok, tok)], sem.at[1]))
    return copies


def add_rows(acc, vals_ref, idx, gat, row, parts):
    for b in range(0, TILE, BATCH):
        toks = [idx[row + b + r] for r in range(BATCH)]
        gates = [gat[row + b + r] for r in range(BATCH)]
        vals = [acc[pl.ds(toks[r] * parts, parts), :] + gates[r] * vals_ref[pl.ds((b + r) * parts, parts), :]
                for r in range(BATCH)]
        for r in reversed(range(BATCH)):
            acc[pl.ds(toks[r] * parts, parts), :] = vals[r]


def write_sums(acc, own_ref, other_ref, ep, tok, parts):
    step = min(32, tok)

    def copy_out(q, carry):
        r0 = pl.multiple_of(q * step, step)
        for k in range(parts):
            cols = slice(k * LANES, (k + 1) * LANES)
            own_ref[pl.ds(r0, step), cols] = acc[pl.ds((ep * tok + r0) * parts + k, step, stride=parts), :]
            other_ref[pl.ds(r0, step), cols] = acc[pl.ds(((1 - ep) * tok + r0) * parts + k, step, stride=parts), :]
        return carry

    lax.fori_loop(0, tok // step, copy_out, 0)


def expert_copies(weights, buf, sem, layer, e):
    slot = lax.rem(e, 2)
    ff = weights[0].shape[2]
    return [pltpu.make_async_copy(w.at[layer, e], buf.at[slot, pl.ds(k * ff, ff)], sem.at[slot])
            for k, w in enumerate(weights)]


def run_tiles(step, weights, wbuf, wsem, tile_e, tile_first, n_steps, layer, copies):
    n_local = weights[0].shape[1]
    ahead = list(copies) + expert_copies(weights, wbuf, wsem, layer, 0)
    for c in ahead:
        c.start()
    for c in expert_copies(weights, wbuf, wsem, layer, 1):
        c.start()
    for c in ahead:
        c.wait()

    def one(i, carry):
        e = tile_e[i + 1]

        @pl.when(tile_first[i + 1] == 1)
        def _():
            for c in expert_copies(weights, wbuf, wsem, layer, e):
                c.wait()

            @pl.when(e + 1 < n_local)
            def _():
                for c in expert_copies(weights, wbuf, wsem, layer, e + 1):
                    c.start()

        step(i, lax.rem(e, 2))
        return carry

    lax.fori_loop(0, n_steps, one, 0)


def forward_body(te, tf, tr, tn, nt, idx, gat, epr, u_own, u_oth, g_ref, up_ref, w_ref, own_ref, other_ref,
                 usc, ut, ot, acc, wbuf, sem, wsem, *, layer, tok, parts):
    ff = g_ref.shape[2]
    ep = epr[0]
    acc[...] = jnp.zeros_like(acc)
    ot[...] = jnp.zeros_like(ot)
    ut[...] = jnp.zeros_like(ut)

    def step(i, slot):
        u = load_rows(ut, 0, TILE, parts)
        ab = nt_dot(wbuf[slot, :2 * ff], u)
        add_rows(acc, ot, idx, gat, tr[i], parts)
        row = tr[i + 2]
        for r in range(TILE):
            ut[pl.ds(parts * r, parts), :] = usc[idx[row + r]].astype(jnp.float32)
        a, b = ab[:ff], ab[ff:]
        h = (a * jax.nn.sigmoid(a) * b).astype(jnp.bfloat16)
        o = tn_dot(h, wbuf[slot, 2 * ff:]).astype(jnp.bfloat16).astype(jnp.float32)
        live = lax.broadcasted_iota(jnp.int32, o.shape, 0) < tn[i + 1]
        store_rows(ot, 0, jnp.where(live, o, 0.0), parts)

    run_tiles(step, (g_ref, up_ref, w_ref), wbuf, wsem, te, tf, nt[0] + 2, layer,
              fetch_pair(u_own, u_oth, usc, sem, ep, tok))
    write_sums(acc, own_ref, other_ref, ep, tok, parts)


def backward_body(te, tf, tr, tn, nt, idx, gat, epr, u_own, u_oth, d_own, d_oth, g_ref, up_ref, w_ref, own_ref, other_ref,
                  usc, dsc, ut, ct, vt, acc, wbuf, sem, wsem, *, layer, tok, parts):
    ff = g_ref.shape[2]
    ep = epr[0]
    acc[...] = jnp.zeros_like(acc)
    vt[...] = jnp.zeros_like(vt)
    ut[...] = jnp.zeros_like(ut)
    ct[...] = jnp.zeros_like(ct)

    def step(i, slot):
        u = load_rows(ut, 0, TILE, parts)
        c = load_rows(ct, 0, TILE, parts)
        gu = wbuf[slot, :2 * ff]
        ab = nt_dot(gu, u)
        dh = nt_dot(wbuf[slot, 2 * ff:], c)
        add_rows(acc, vt, idx, gat, tr[i], parts)
        row = tr[i + 2]
        for r in range(TILE):
            t = idx[row + r]
            ut[pl.ds(parts * r, parts), :] = usc[t].astype(jnp.float32)
            ct[pl.ds(parts * r, parts), :] = gat[row + r] * dsc[t].astype(jnp.float32)
        a, b = ab[:ff], ab[ff:]
        s = jax.nn.sigmoid(a)
        da = (dh * b * (s * (1.0 + a * (1.0 - s)))).astype(jnp.bfloat16)
        db = (dh * (a * s)).astype(jnp.bfloat16)
        v = tn_dot(jnp.concatenate([da, db], axis=0), gu).astype(jnp.bfloat16).astype(jnp.float32)
        live = lax.broadcasted_iota(jnp.int32, v.shape, 0) < tn[i + 1]
        store_rows(vt, 0, jnp.where(live, v, 0.0), parts)

    run_tiles(step, (g_ref, up_ref, w_ref), wbuf, wsem, te, tf, nt[0] + 2, layer,
              fetch_pair(u_own, u_oth, usc, sem.at[0], ep, tok) + fetch_pair(d_own, d_oth, dsc, sem.at[1], ep, tok))
    write_sums(acc, own_ref, other_ref, ep, tok, parts)


def token_kernel(body, name, layer, tables, ep, slabs, weights):
    tok, parts, _ = slabs[0].shape
    n_layers, n_local, ff, d_model = weights[0].shape
    n_pairs = len(slabs) // 2
    rows_spec = pl.BlockSpec((tok, d_model), lambda i, *_: (0, 0))
    any_spec = pl.BlockSpec(memory_space=pl.ANY)
    sem_shape = (2,) if n_pairs == 1 else (2, 2)
    copies = 8 * tok
    return pl.pallas_call(
        functools.partial(body, layer=layer, tok=tok, parts=parts),
        grid_spec=pltpu.PrefetchScalarGridSpec(
            num_scalar_prefetch=len(tables) + 1,
            grid=(1,),
            in_specs=[any_spec] * (len(slabs) + 3),
            out_specs=[rows_spec] * 2,
            scratch_shapes=[pltpu.VMEM((2 * tok, parts, LANES), jnp.bfloat16)] * n_pairs
            + [pltpu.VMEM((TILE * parts, LANES), jnp.float32)] * (n_pairs + 1)
            + [pltpu.VMEM((2 * tok * parts, LANES), jnp.float32), pltpu.VMEM((2, 3 * ff, d_model), jnp.bfloat16),
               pltpu.SemaphoreType.DMA(sem_shape), pltpu.SemaphoreType.DMA((2,))],
        ),
        out_shape=[jax.ShapeDtypeStruct((tok, d_model), jnp.float32)] * 2,
        compiler_params=pltpu.CompilerParams(dimension_semantics=("arbitrary",), vmem_limit_bytes=VMEM_LIMIT),
        cost_estimate=pl.CostEstimate(flops=(3 + 3 * (n_pairs - 1)) * 2 * copies * d_model * ff * 4,
                                      bytes_accessed=3 * n_local * ff * d_model * 2, transcendentals=0),
        name=name,
    )(*tables, ep, *slabs, *weights)


def weight_grad_body(st, core, u_all, d_all, idx_all, gat_all, *refs, rows, src, page_rows, parts, n_exp, n_alias, max_rows):
    g_ref, up_ref, w_ref = refs[:3]
    dg_ref, du_ref, dw_ref, og_ref, ou_ref, ow_ref, usc, dsc, ut, ct, gacc, wacc, idx_s, gat_s, sem, tsem = refs[3 + n_alias:]
    e = pl.program_id(0)
    ff = g_ref.shape[2]
    base = core[0] * n_exp
    per_slot = src * page_rows

    def table_copies(exp, slot):
        out = []
        for d in range(src):
            first = st[d * LANES + base + exp]
            at = pl.multiple_of(lax.div(first, PAGE) * PAGE + d * rows, PAGE)
            to = pl.multiple_of(slot * per_slot + d * page_rows, PAGE)
            out.append(pltpu.make_async_copy(idx_all.at[pl.ds(at, page_rows)], idx_s.at[pl.ds(to, page_rows)], tsem.at[0]))
            out.append(pltpu.make_async_copy(gat_all.at[pl.ds(at, page_rows)], gat_s.at[pl.ds(to, page_rows)], tsem.at[1]))
        return out

    slot = lax.rem(e, 2)

    @pl.when(e == 0)
    def _():
        cu = pltpu.make_async_copy(u_all, usc, sem.at[0])
        cd = pltpu.make_async_copy(d_all, dsc, sem.at[1])
        cu.start()
        cd.start()
        for c in table_copies(0, 0):
            c.start()

        def clear(q, carry):
            ut[pl.ds(pl.multiple_of(q * 256, 256), 256), :] = jnp.zeros((256, LANES), jnp.float32)
            return carry

        lax.fori_loop(0, ut.shape[0] // 256, clear, 0)
        cu.wait()
        cd.wait()

    for c in table_copies(e, slot):
        c.wait()

    @pl.when(e + 1 < n_exp)
    def _():
        for c in table_copies(e + 1, 1 - slot):
            c.start()

    off = 0
    for d in range(src):
        first = st[d * LANES + base + e]
        count = st[d * LANES + base + e + 1] - first
        p0 = slot * per_slot + d * page_rows + lax.rem(first, PAGE)

        def gather(q, carry, p0=p0, off=off):
            p = p0 + q * UNROLL
            o = (off + q * UNROLL) * parts
            for r in range(UNROLL):
                t = idx_s[p + r]
                ut[pl.ds(o + r * parts, parts), :] = usc[t].astype(jnp.float32)
                ct[pl.ds(o + r * parts, parts), :] = gat_s[p + r] * dsc[t].astype(jnp.float32)
            return carry

        lax.fori_loop(0, lax.div(count + UNROLL - 1, UNROLL), gather, 0)
        off = off + count
    tiles = lax.div(off + WTILE - 1, WTILE)

    def clear_tail(q, carry):
        ct[pl.ds((off + q * 8) * parts, 8 * parts), :] = jnp.zeros((8 * parts, LANES), jnp.float32)
        return carry

    lax.fori_loop(0, lax.div(tiles * WTILE - off + 7, 8), clear_tail, 0)
    gacc[...] = jnp.zeros_like(gacc)
    wacc[...] = jnp.zeros_like(wacc)

    def tile(j, carry):
        u = load_rows(ut, j * WTILE, WTILE, parts)
        c = load_rows(ct, j * WTILE, WTILE, parts)
        ab = nt_dot(jnp.concatenate([g_ref[0, 0], up_ref[0, 0]], axis=0), u)
        dh = nt_dot(w_ref[0, 0], c)
        a, b = ab[:ff], ab[ff:]
        s = jax.nn.sigmoid(a)
        act = a * s
        h = (act * b).astype(jnp.bfloat16)
        da = (dh * b * (s * (1.0 + a * (1.0 - s)))).astype(jnp.bfloat16)
        db = (dh * act).astype(jnp.bfloat16)
        gacc[...] += nn_dot(jnp.concatenate([da, db], axis=0), u)
        wacc[...] += nn_dot(h, c)
        return carry

    lax.fori_loop(0, tiles, tile, 0)
    dg = gacc[:ff].astype(jnp.bfloat16)
    du = gacc[ff:].astype(jnp.bfloat16)
    dw = wacc[...].astype(jnp.bfloat16)
    dg_ref[0, 0], du_ref[0, 0], dw_ref[0, 0] = dg, du, dw
    og_ref[0], ou_ref[0], ow_ref[0] = dg, du, dw


def weight_grads(layer, starts, core, u_all, d_all, idx_all, gat_all, weights, full, cap):
    n_tok, parts, _ = u_all.shape
    n_layers, n_local, ff, d_model = weights[0].shape
    n_exp = n_local // 2
    src = starts.shape[0] // LANES
    rows = idx_all.shape[0] // src
    page_rows = cdiv(PAGE - 1 + 2 * cap + UNROLL, PAGE) * PAGE
    max_rows = cdiv(src * 2 * cap, WTILE) * WTILE + max(UNROLL, 8)
    max_rows = cdiv(max_rows, 64) * 64
    any_spec = pl.BlockSpec(memory_space=pl.ANY)
    mine = pl.BlockSpec((1, 1, ff, d_model), lambda e, st, core: (layer, core[0] * n_exp + e, 0, 0))
    half = pl.BlockSpec((1, ff, d_model), lambda e, st, core: (e, 0, 0))
    aliased = list(full) if full is not None else []
    outs = pl.pallas_call(
        functools.partial(weight_grad_body, rows=rows, src=src, page_rows=page_rows, parts=parts, n_exp=n_exp,
                          n_alias=len(aliased), max_rows=max_rows),
        grid_spec=pltpu.PrefetchScalarGridSpec(
            num_scalar_prefetch=2,
            grid=(n_exp,),
            in_specs=[any_spec] * 4 + [mine] * 3 + [any_spec] * len(aliased),
            out_specs=[mine] * 3 + [half] * 3,
            scratch_shapes=[pltpu.VMEM((n_tok, parts, LANES), jnp.bfloat16)] * 2
            + [pltpu.VMEM((max_rows * parts, LANES), jnp.float32)] * 2
            + [pltpu.VMEM((2 * ff, d_model), jnp.float32), pltpu.VMEM((ff, d_model), jnp.float32),
               pltpu.SMEM((2 * src * page_rows,), jnp.int32), pltpu.SMEM((2 * src * page_rows,), jnp.float32),
               pltpu.SemaphoreType.DMA((2,)), pltpu.SemaphoreType.DMA((2,))],
        ),
        out_shape=[jax.ShapeDtypeStruct((n_layers, n_local, ff, d_model), jnp.bfloat16)] * 3
        + [jax.ShapeDtypeStruct((n_exp, ff, d_model), jnp.bfloat16)] * 3,
        input_output_aliases={9 + k: k for k in range(len(aliased))},
        compiler_params=pltpu.CompilerParams(dimension_semantics=("arbitrary",), vmem_limit_bytes=VMEM_LIMIT),
        cost_estimate=pl.CostEstimate(flops=6 * 2 * n_tok * 2 * d_model * ff * 4,
                                      bytes_accessed=n_tok * d_model * 4 + 9 * n_exp * ff * d_model * 2, transcendentals=0),
        name="weight_grads",
    )(starts, core, u_all, d_all, idx_all, gat_all, *weights, *aliased)
    return outs[:3], outs[3:]


def merge_body(core, a, b, c, f0, f1, f2, o0, o1, o2):
    o0[0, 0], o1[0, 0], o2[0, 0] = a[0], b[0], c[0]


def merge_half(layer, core, half, full):
    n_layers, n_local, ff, d_model = full[0].shape
    n_exp = n_local // 2
    any_spec = pl.BlockSpec(memory_space=pl.ANY)
    part = pl.BlockSpec((1, ff, d_model), lambda e, core: (e, 0, 0))
    place = pl.BlockSpec((1, 1, ff, d_model), lambda e, core: (layer, (1 - core[0]) * n_exp + e, 0, 0))
    return pl.pallas_call(
        merge_body,
        grid_spec=pltpu.PrefetchScalarGridSpec(
            num_scalar_prefetch=1, grid=(n_exp,), in_specs=[part] * 3 + [any_spec] * 3, out_specs=[place] * 3),
        out_shape=[jax.ShapeDtypeStruct(x.shape, x.dtype) for x in full],
        input_output_aliases={4: 0, 5: 1, 6: 2},
        compiler_params=pltpu.CompilerParams(dimension_semantics=("arbitrary",)),
        cost_estimate=pl.CostEstimate(flops=0, bytes_accessed=6 * n_exp * ff * d_model * 2, transcendentals=0),
        name="merge_half",
    )(core, *half, *full)


def route_tables(ids, gates, ep, n_local):
    n_src, top_k, tok = ids.shape
    n = n_src * top_k * tok
    local = ids - ep * n_local
    here = (local >= 0) & (local < n_local)
    group = jnp.where(here, local, n_local).reshape(-1)
    key, gate = lax.sort((group * n + jnp.arange(n, dtype=jnp.int32), gates.reshape(-1)), num_keys=1, is_stable=False)
    copy = key % n
    token = copy // (top_k * tok) * tok + copy % tok
    counts = jnp.sum((group[:, None] == jnp.arange(n_local)[None, :]).astype(jnp.int32), axis=0)
    ends = jnp.cumsum(counts)
    starts = ends - counts
    n_tiles = jnp.maximum((counts + TILE - 1) // TILE, 1)
    tile_end = jnp.cumsum(n_tiles)
    tile_id = jnp.arange(n // TILE + n_local + 4, dtype=jnp.int32) - 2
    tile_e = jnp.minimum(jnp.sum((tile_end[None, :] <= tile_id[:, None]).astype(jnp.int32), axis=1), n_local - 1)
    pick = (tile_e[:, None] == jnp.arange(n_local)[None, :]).astype(jnp.int32)
    inside = (tile_id - jnp.sum(pick * (tile_end - n_tiles)[None, :], axis=1)) * TILE
    real = (tile_id >= 0) & (tile_id < tile_end[-1])
    tile_row = jnp.where(real, jnp.sum(pick * starts[None, :], axis=1) + inside, 0)
    tile_first = (real & (inside == 0) & (tile_e > 0)).astype(jnp.int32)
    tile_n = jnp.where(real, jnp.clip(jnp.sum(pick * counts[None, :], axis=1) - inside, 0, TILE), 0)
    pad = cdiv(2 * PAGE, TILE) * TILE
    token = jnp.pad(token, (0, pad))
    gate = jnp.pad(gate, (0, pad))
    bounds = jnp.concatenate([jnp.zeros((1,), jnp.int32), ends, jnp.full((LANES - 1 - n_local,), ends[-1], jnp.int32)])
    return (tile_e, tile_first, tile_row, tile_n, tile_end[-1:], token, gate), bounds


def solution(mesh):
    ep_size = mesh.shape['ep']
    dp_size = mesh.shape['dp']
    tok_spec = P(('dp', 'ep'), None)
    route_spec = P(None, ('dp', 'ep'), None)
    whole_spec = P(None, None, None)
    expert_spec = P(None, 'ep', None, None)
    ep_pairs = [(i, 1 - i) for i in range(ep_size)]
    core_pairs = [(i, i ^ 1) for i in range(dp_size)]

    def device_step(tokens, d_out, expert_ids, gate_vals, w_mix, w_gate, w_up, w_down):
        n_layers = w_mix.shape[0]
        n_local = w_gate.shape[1]
        n_experts = n_local * ep_size
        tok, d_model = tokens.shape
        top_k = expert_ids.shape[2]
        parts = d_model // LANES
        cap = cdiv(CAP_FACTOR * tok * top_k, n_experts)
        ep_id = lax.axis_index('ep').astype(jnp.int32)
        dp_id = lax.axis_index('dp').astype(jnp.int32)
        ep = ep_id.reshape(1)
        core = (dp_id % 2).reshape(1)
        weights = (jnp.swapaxes(w_gate, 2, 3), jnp.swapaxes(w_up, 2, 3), w_down)

        def swap(x):
            return lax.ppermute(x, 'ep', ep_pairs)

        def spread(x):
            return lax.all_gather(x, ('dp', 'ep'), axis=0, tiled=True)

        def slab(x):
            return x.reshape(tok, parts, LANES)

        def mixed(x, layer):
            return (x.astype(jnp.float32) + jnp.dot(x, w_mix[layer], preferred_element_type=jnp.float32)).astype(jnp.bfloat16)

        ids = jnp.swapaxes(expert_ids, 1, 2)
        gates = jnp.swapaxes(gate_vals, 1, 2)
        mine = jnp.stack([ids.astype(jnp.float32), gates])
        theirs = swap(mine)
        both = jnp.where(ep_id == 0, jnp.stack([mine, theirs], 2), jnp.stack([theirs, mine], 2))
        both_ids = both[0].astype(jnp.int32)
        tables, packed = [], []
        for layer in range(n_layers):
            table, bounds = route_tables(both_ids[layer], both[1, layer], ep_id, n_local)
            tables.append(table)
            token, gate = table[5], table[6]
            packed.append(jnp.stack([jnp.concatenate([token + dp_id * (2 * tok), jnp.pad(bounds, (0, PAGE - LANES))])
                                     .astype(jnp.float32), jnp.pad(gate, (0, PAGE))]))
        rows = packed[0].shape[1]
        shared = lax.all_gather(jnp.stack(packed), 'dp', axis=2)
        shared = shared.reshape(n_layers, 2, dp_size, rows)

        d_slab = slab(d_out)
        d_other = swap(d_slab)
        d_spread = spread(d_slab)

        x_in, u_slabs, u_others, xs, u_spreads = tokens, [], [], [], []
        for layer in range(n_layers):
            u = mixed(x_in, layer)
            u_slab = slab(u)
            u_other = swap(u_slab)
            own, other = token_kernel(forward_body, "experts_forward", layer, tables[layer], ep, (u_slab, u_other), weights)
            xs.append(x_in)
            u_slabs.append(u_slab)
            u_others.append(u_other)
            u_spreads.append(spread(u_slab))
            x_in = (u.astype(jnp.float32) + own + swap(other)).astype(jnp.bfloat16)
        layer_out = x_in

        d_y, full = d_out, None
        d_mix = [None] * n_layers
        for layer in reversed(range(n_layers)):
            own, other = token_kernel(backward_body, "experts_backward", layer, tables[layer], ep,
                                      (u_slabs[layer], u_others[layer], d_slab, d_other), weights)
            d_u = (d_y.astype(jnp.float32) + own + swap(other)).astype(jnp.bfloat16)
            ids_all = shared[layer, 0].astype(jnp.int32)
            starts = ids_all[:, rows - PAGE:rows - PAGE + LANES].reshape(-1)
            full, half = weight_grads(layer, starts, core, u_spreads[layer], d_spread, ids_all.reshape(-1),
                                      shared[layer, 1].reshape(-1), weights, full, cap)
            full = merge_half(layer, core, [lax.ppermute(x, 'dp', core_pairs) for x in half], full)
            d_mix[layer] = lax.psum(jnp.einsum('td,te->de', xs[layer], d_u, preferred_element_type=jnp.float32)
                                    .astype(jnp.bfloat16), ('dp', 'ep'))
            d_y = (d_u.astype(jnp.float32)
                   + jnp.einsum('te,de->td', d_u, w_mix[layer], preferred_element_type=jnp.float32)).astype(jnp.bfloat16)
            if layer:
                d_slab = slab(d_y)
                d_other = swap(d_slab)
                d_spread = spread(d_slab)
        return (layer_out, d_y, jnp.stack(d_mix), jnp.swapaxes(full[0], 2, 3), jnp.swapaxes(full[1], 2, 3), full[2])

    return jax.shard_map(device_step, mesh=mesh,
                         in_specs=(tok_spec, tok_spec, route_spec, route_spec, whole_spec,
                                   expert_spec, expert_spec, expert_spec),
                         out_specs=(tok_spec, tok_spec, whole_spec, expert_spec, expert_spec, expert_spec),
                         check_vma=False)
```

```python
import functools

import jax
import jax.numpy as jnp
from jax import lax
from jax.experimental import pallas as pl
from jax.experimental.pallas import tpu as pltpu
from jax.sharding import PartitionSpec as P


CAP_FACTOR = 3
LANES = 128
TILE = 128
WTILE = 256
BATCH = 16
UNROLL = 16
SLOTS = 4
PAGE = 1024
VMEM_LIMIT = 62 * 2**20


def cdiv(a, b):
    return (a + b - 1) // b


def nt_dot(a, b):
    return lax.dot_general(a, b, (((1,), (1,)), ((), ())), preferred_element_type=jnp.float32)


def tn_dot(a, b):
    return lax.dot_general(a, b, (((0,), (0,)), ((), ())), preferred_element_type=jnp.float32)


def nn_dot(a, b):
    return lax.dot_general(a, b, (((1,), (0,)), ((), ())), preferred_element_type=jnp.float32)


def load_rows(ref, start, rows, parts):
    cols = [ref[pl.ds(start * parts + k, rows, stride=parts), :] for k in range(parts)]
    return jnp.concatenate(cols, axis=1).astype(jnp.bfloat16)


def store_rows(ref, start, vals, parts):
    rows = vals.shape[0]
    for k in range(parts):
        ref[pl.ds(start * parts + k, rows, stride=parts), :] = vals[:, k * LANES:(k + 1) * LANES]


def fetch_pair(first, other, dst, sem, ep, tok):
    copies = (pltpu.make_async_copy(first, dst.at[pl.ds(ep * tok, tok)], sem.at[0]),
              pltpu.make_async_copy(other, dst.at[pl.ds((1 - ep) * tok, tok)], sem.at[1]))
    return copies


def add_rows(acc, vals_ref, idx, gat, row, parts):
    for b in range(0, TILE, BATCH):
        toks = [idx[row + b + r] for r in range(BATCH)]
        gates = [gat[row + b + r] for r in range(BATCH)]
        vals = [acc[pl.ds(toks[r] * parts, parts), :] + gates[r] * vals_ref[pl.ds((b + r) * parts, parts), :]
                for r in range(BATCH)]
        for r in reversed(range(BATCH)):
            acc[pl.ds(toks[r] * parts, parts), :] = vals[r]


def write_sums(acc, own_ref, other_ref, ep, tok, parts):
    step = min(32, tok)

    def copy_out(q, carry):
        r0 = pl.multiple_of(q * step, step)
        for k in range(parts):
            cols = slice(k * LANES, (k + 1) * LANES)
            own_ref[pl.ds(r0, step), cols] = acc[pl.ds((ep * tok + r0) * parts + k, step, stride=parts), :]
            other_ref[pl.ds(r0, step), cols] = acc[pl.ds(((1 - ep) * tok + r0) * parts + k, step, stride=parts), :]
        return carry

    lax.fori_loop(0, tok // step, copy_out, 0)


def expert_copies(weights, buf, sem, layer, e):
    slot = lax.rem(e, SLOTS)
    ff = weights[0].shape[2]
    return [pltpu.make_async_copy(w.at[layer, e], buf.at[slot, pl.ds(k * ff, ff)], sem.at[slot])
            for k, w in enumerate(weights)]


def run_tiles(step, weights, wbuf, wsem, tile_e, tile_first, n_steps, layer, copies):
    n_local = weights[0].shape[1]
    ahead = list(copies) + expert_copies(weights, wbuf, wsem, layer, 0)
    for c in ahead:
        c.start()
    for e in range(1, min(SLOTS - 1, n_local)):
        for c in expert_copies(weights, wbuf, wsem, layer, e):
            c.start()
    for c in ahead:
        c.wait()

    def one(i, carry):
        e = tile_e[i + 1]

        @pl.when(tile_first[i + 1] == 1)
        def _():
            for c in expert_copies(weights, wbuf, wsem, layer, e):
                c.wait()

        @pl.when((tile_first[i + 1] == 1) & (e + SLOTS - 2 < n_local))
        def _():
            for c in expert_copies(weights, wbuf, wsem, layer, e + SLOTS - 2):
                c.start()

        step(i, lax.rem(e, SLOTS))
        return carry

    lax.fori_loop(0, n_steps, one, 0)


def forward_body(te, tf, tr, tn, nt, idx, gat, epr, u_own, u_oth, g_ref, up_ref, w_ref, own_ref, other_ref,
                 usc, ut, ot, acc, wbuf, sem, wsem, *, layer, tok, parts):
    ff = g_ref.shape[2]
    ep = epr[0]
    acc[...] = jnp.zeros_like(acc)
    ot[...] = jnp.zeros_like(ot)
    ut[...] = jnp.zeros_like(ut)

    def step(i, slot):
        u = load_rows(ut, 0, TILE, parts)
        ab = nt_dot(wbuf[slot, :2 * ff], u)
        add_rows(acc, ot, idx, gat, tr[i], parts)
        row = tr[i + 2]
        for r in range(TILE):
            ut[pl.ds(parts * r, parts), :] = usc[idx[row + r]].astype(jnp.float32)
        a, b = ab[:ff], ab[ff:]
        h = (a * jax.nn.sigmoid(a) * b).astype(jnp.bfloat16)
        o = tn_dot(h, wbuf[slot, 2 * ff:]).astype(jnp.bfloat16).astype(jnp.float32)
        live = lax.broadcasted_iota(jnp.int32, o.shape, 0) < tn[i + 1]
        store_rows(ot, 0, jnp.where(live, o, 0.0), parts)

    run_tiles(step, (g_ref, up_ref, w_ref), wbuf, wsem, te, tf, nt[0] + 2, layer,
              fetch_pair(u_own, u_oth, usc, sem, ep, tok))
    write_sums(acc, own_ref, other_ref, ep, tok, parts)


def backward_body(te, tf, tr, tn, nt, idx, gat, epr, u_own, u_oth, d_own, d_oth, g_ref, up_ref, w_ref, own_ref, other_ref,
                  usc, dsc, ut, ct, vt, acc, wbuf, sem, wsem, *, layer, tok, parts):
    ff = g_ref.shape[2]
    ep = epr[0]
    acc[...] = jnp.zeros_like(acc)
    vt[...] = jnp.zeros_like(vt)
    ut[...] = jnp.zeros_like(ut)
    ct[...] = jnp.zeros_like(ct)

    def step(i, slot):
        u = load_rows(ut, 0, TILE, parts)
        c = load_rows(ct, 0, TILE, parts)
        gu = wbuf[slot, :2 * ff]
        ab = nt_dot(gu, u)
        dh = nt_dot(wbuf[slot, 2 * ff:], c)
        add_rows(acc, vt, idx, gat, tr[i], parts)
        row = tr[i + 2]
        for r in range(TILE):
            t = idx[row + r]
            ut[pl.ds(parts * r, parts), :] = usc[t].astype(jnp.float32)
            ct[pl.ds(parts * r, parts), :] = gat[row + r] * dsc[t].astype(jnp.float32)
        a, b = ab[:ff], ab[ff:]
        s = jax.nn.sigmoid(a)
        da = (dh * b * (s * (1.0 + a * (1.0 - s)))).astype(jnp.bfloat16)
        db = (dh * (a * s)).astype(jnp.bfloat16)
        v = tn_dot(jnp.concatenate([da, db], axis=0), gu).astype(jnp.bfloat16).astype(jnp.float32)
        live = lax.broadcasted_iota(jnp.int32, v.shape, 0) < tn[i + 1]
        store_rows(vt, 0, jnp.where(live, v, 0.0), parts)

    run_tiles(step, (g_ref, up_ref, w_ref), wbuf, wsem, te, tf, nt[0] + 2, layer,
              fetch_pair(u_own, u_oth, usc, sem.at[0], ep, tok) + fetch_pair(d_own, d_oth, dsc, sem.at[1], ep, tok))
    write_sums(acc, own_ref, other_ref, ep, tok, parts)


def token_kernel(body, layer, tables, ep, slabs, weights):
    tok, parts, _ = slabs[0].shape
    _, n_local, ff, d_model = weights[0].shape
    n_pairs = len(slabs) // 2
    rows_spec = pl.BlockSpec((tok, d_model), lambda i, *_: (0, 0))
    any_spec = pl.BlockSpec(memory_space=pl.ANY)
    sem_shape = (2,) if n_pairs == 1 else (2, 2)
    copies = 8 * tok
    return pl.pallas_call(
        functools.partial(body, layer=layer, tok=tok, parts=parts),
        grid_spec=pltpu.PrefetchScalarGridSpec(
            num_scalar_prefetch=len(tables) + 1,
            grid=(1,),
            in_specs=[any_spec] * (len(slabs) + 3),
            out_specs=[rows_spec] * 2,
            scratch_shapes=[pltpu.VMEM((2 * tok, parts, LANES), jnp.bfloat16)] * n_pairs
            + [pltpu.VMEM((TILE * parts, LANES), jnp.float32)] * (n_pairs + 1)
            + [pltpu.VMEM((2 * tok * parts, LANES), jnp.float32), pltpu.VMEM((SLOTS, 3 * ff, d_model), jnp.bfloat16),
               pltpu.SemaphoreType.DMA(sem_shape), pltpu.SemaphoreType.DMA((SLOTS,))],
        ),
        out_shape=[jax.ShapeDtypeStruct((tok, d_model), jnp.float32)] * 2,
        compiler_params=pltpu.CompilerParams(dimension_semantics=("arbitrary",), vmem_limit_bytes=VMEM_LIMIT),
        cost_estimate=pl.CostEstimate(flops=(3 + 3 * (n_pairs - 1)) * 2 * copies * d_model * ff * 4,
                                      bytes_accessed=3 * n_local * ff * d_model * 2, transcendentals=0),
    )(*tables, ep, *slabs, *weights)


def weight_grad_body(st, exps, u_all, d_all, idx_all, gat_all, *refs, rows, src, page_rows, parts, n_exp, n_alias):
    g_ref, up_ref, w_ref = refs[:3]
    dg_ref, du_ref, dw_ref, og_ref, ou_ref, ow_ref, usc, dsc, ut, ct, gacc, wacc, idx_s, gat_s, sem, tsem = refs[3 + n_alias:]
    e = pl.program_id(0)
    ff = g_ref.shape[2]
    per_slot = src * page_rows

    def table_copies(exp, slot):
        out = []
        for d in range(src):
            first = st[d * LANES + exps[exp]]
            at = pl.multiple_of(lax.div(first, PAGE) * PAGE + d * rows, PAGE)
            to = pl.multiple_of(slot * per_slot + d * page_rows, PAGE)
            out.append(pltpu.make_async_copy(idx_all.at[pl.ds(at, page_rows)], idx_s.at[pl.ds(to, page_rows)], tsem.at[0]))
            out.append(pltpu.make_async_copy(gat_all.at[pl.ds(at, page_rows)], gat_s.at[pl.ds(to, page_rows)], tsem.at[1]))
        return out

    slot = lax.rem(e, 2)

    @pl.when(e == 0)
    def _():
        cu = pltpu.make_async_copy(u_all, usc, sem.at[0])
        cd = pltpu.make_async_copy(d_all, dsc, sem.at[1])
        cu.start()
        cd.start()
        for c in table_copies(0, 0):
            c.start()

        def clear(q, carry):
            ut[pl.ds(pl.multiple_of(q * 256, 256), 256), :] = jnp.zeros((256, LANES), jnp.float32)
            return carry

        lax.fori_loop(0, ut.shape[0] // 256, clear, 0)
        cu.wait()
        cd.wait()

    for c in table_copies(e, slot):
        c.wait()

    @pl.when(e + 1 < n_exp)
    def _():
        for c in table_copies(e + 1, 1 - slot):
            c.start()

    off = 0
    for d in range(src):
        first = st[d * LANES + exps[e]]
        count = st[d * LANES + exps[e] + 1] - first
        p0 = slot * per_slot + d * page_rows + lax.rem(first, PAGE)

        def gather(q, carry, p0=p0, off=off):
            p = p0 + q * UNROLL
            o = (off + q * UNROLL) * parts
            for r in range(UNROLL):
                t = idx_s[p + r]
                ut[pl.ds(o + r * parts, parts), :] = usc[t].astype(jnp.float32)
                ct[pl.ds(o + r * parts, parts), :] = gat_s[p + r] * dsc[t].astype(jnp.float32)
            return carry

        lax.fori_loop(0, lax.div(count + UNROLL - 1, UNROLL), gather, 0)
        off = off + count
    tiles = lax.div(off + WTILE - 1, WTILE)

    def clear_tail(q, carry):
        ct[pl.ds((off + q * 8) * parts, 8 * parts), :] = jnp.zeros((8 * parts, LANES), jnp.float32)
        return carry

    lax.fori_loop(0, lax.div(tiles * WTILE - off + 7, 8), clear_tail, 0)
    gacc[...] = jnp.zeros_like(gacc)
    wacc[...] = jnp.zeros_like(wacc)

    def tile(j, carry):
        u = load_rows(ut, j * WTILE, WTILE, parts)
        c = load_rows(ct, j * WTILE, WTILE, parts)
        ab = nt_dot(jnp.concatenate([g_ref[0, 0], up_ref[0, 0]], axis=0), u)
        dh = nt_dot(w_ref[0, 0], c)
        a, b = ab[:ff], ab[ff:]
        s = jax.nn.sigmoid(a)
        act = a * s
        h = (act * b).astype(jnp.bfloat16)
        da = (dh * b * (s * (1.0 + a * (1.0 - s)))).astype(jnp.bfloat16)
        db = (dh * act).astype(jnp.bfloat16)
        gacc[...] += nn_dot(jnp.concatenate([da, db], axis=0), u)
        wacc[...] += nn_dot(h, c)
        return carry

    lax.fori_loop(0, tiles, tile, 0)
    dg = gacc[:ff].astype(jnp.bfloat16)
    du = gacc[ff:].astype(jnp.bfloat16)
    dw = wacc[...].astype(jnp.bfloat16)
    dg_ref[0, 0], du_ref[0, 0], dw_ref[0, 0] = dg, du, dw
    og_ref[0], ou_ref[0], ow_ref[0] = dg, du, dw


def weight_grads(layer, starts, exps, u_all, d_all, idx_all, gat_all, weights, full, cap):
    n_tok, parts, _ = u_all.shape
    n_layers, n_local, ff, d_model = weights[0].shape
    n_exp = n_local // 2
    src = starts.shape[0] // LANES
    rows = idx_all.shape[0] // src
    page_rows = cdiv(PAGE - 1 + 2 * cap + UNROLL, PAGE) * PAGE
    max_rows = cdiv(src * 2 * cap, WTILE) * WTILE + max(UNROLL, 8)
    max_rows = cdiv(max_rows, 64) * 64
    any_spec = pl.BlockSpec(memory_space=pl.ANY)
    mine = pl.BlockSpec((1, 1, ff, d_model), lambda e, st, exps: (layer, exps[e], 0, 0))
    half = pl.BlockSpec((1, ff, d_model), lambda e, st, exps: (e, 0, 0))
    aliased = list(full) if full is not None else []
    outs = pl.pallas_call(
        functools.partial(weight_grad_body, rows=rows, src=src, page_rows=page_rows, parts=parts, n_exp=n_exp,
                          n_alias=len(aliased)),
        grid_spec=pltpu.PrefetchScalarGridSpec(
            num_scalar_prefetch=2,
            grid=(n_exp,),
            in_specs=[any_spec] * 4 + [mine] * 3 + [any_spec] * len(aliased),
            out_specs=[mine] * 3 + [half] * 3,
            scratch_shapes=[pltpu.VMEM((n_tok, parts, LANES), jnp.bfloat16)] * 2
            + [pltpu.VMEM((max_rows * parts, LANES), jnp.float32)] * 2
            + [pltpu.VMEM((2 * ff, d_model), jnp.float32), pltpu.VMEM((ff, d_model), jnp.float32),
               pltpu.SMEM((2 * src * page_rows,), jnp.int32), pltpu.SMEM((2 * src * page_rows,), jnp.float32),
               pltpu.SemaphoreType.DMA((2,)), pltpu.SemaphoreType.DMA((2,))],
        ),
        out_shape=[jax.ShapeDtypeStruct((n_layers, n_local, ff, d_model), jnp.bfloat16)] * 3
        + [jax.ShapeDtypeStruct((n_exp, ff, d_model), jnp.bfloat16)] * 3,
        input_output_aliases={9 + k: k for k in range(len(aliased))},
        compiler_params=pltpu.CompilerParams(dimension_semantics=("arbitrary",), vmem_limit_bytes=VMEM_LIMIT),
        cost_estimate=pl.CostEstimate(flops=6 * 2 * n_tok * 2 * d_model * ff * 4,
                                      bytes_accessed=n_tok * d_model * 4 + 9 * n_exp * ff * d_model * 2, transcendentals=0),
        name="weight_grads",
    )(starts, exps, u_all, d_all, idx_all, gat_all, *weights, *aliased)
    return outs[:3], outs[3:]


def merge_body(exps, a, b, c, f0, f1, f2, o0, o1, o2):
    o0[0, 0], o1[0, 0], o2[0, 0] = a[0], b[0], c[0]


def merge_half(layer, exps, half, full):
    _, n_local, ff, d_model = full[0].shape
    n_exp = n_local // 2
    any_spec = pl.BlockSpec(memory_space=pl.ANY)
    part = pl.BlockSpec((1, ff, d_model), lambda e, exps: (e, 0, 0))
    place = pl.BlockSpec((1, 1, ff, d_model), lambda e, exps: (layer, exps[e], 0, 0))
    return pl.pallas_call(
        merge_body,
        grid_spec=pltpu.PrefetchScalarGridSpec(
            num_scalar_prefetch=1, grid=(n_exp,), in_specs=[part] * 3 + [any_spec] * 3, out_specs=[place] * 3),
        out_shape=[jax.ShapeDtypeStruct(x.shape, x.dtype) for x in full],
        input_output_aliases={4: 0, 5: 1, 6: 2},
        compiler_params=pltpu.CompilerParams(dimension_semantics=("arbitrary",)),
        cost_estimate=pl.CostEstimate(flops=0, bytes_accessed=6 * n_exp * ff * d_model * 2, transcendentals=0),
        name="merge_half",
    )(exps, *half, *full)


def route_tables(ids, gates, ep, n_local):
    n_src, top_k, tok = ids.shape
    n = n_src * top_k * tok
    local = ids - ep * n_local
    here = (local >= 0) & (local < n_local)
    group = jnp.where(here, local, n_local).reshape(-1)
    key, gate = lax.sort((group * n + jnp.arange(n, dtype=jnp.int32), gates.reshape(-1)), num_keys=1, is_stable=False)
    copy = key % n
    token = copy // (top_k * tok) * tok + copy % tok
    counts = jnp.sum((group[:, None] == jnp.arange(n_local)[None, :]).astype(jnp.int32), axis=0)
    ends = jnp.cumsum(counts)
    starts = ends - counts
    n_tiles = jnp.maximum((counts + TILE - 1) // TILE, 1)
    tile_end = jnp.cumsum(n_tiles)
    tile_id = jnp.arange(n // TILE + n_local + 4, dtype=jnp.int32) - 2
    tile_e = jnp.minimum(jnp.sum((tile_end[None, :] <= tile_id[:, None]).astype(jnp.int32), axis=1), n_local - 1)
    pick = (tile_e[:, None] == jnp.arange(n_local)[None, :]).astype(jnp.int32)
    inside = (tile_id - jnp.sum(pick * (tile_end - n_tiles)[None, :], axis=1)) * TILE
    real = (tile_id >= 0) & (tile_id < tile_end[-1])
    tile_row = jnp.where(real, jnp.sum(pick * starts[None, :], axis=1) + inside, 0)
    tile_first = (real & (inside == 0) & (tile_e > 0)).astype(jnp.int32)
    tile_n = jnp.where(real, jnp.clip(jnp.sum(pick * counts[None, :], axis=1) - inside, 0, TILE), 0)
    pad = cdiv(2 * PAGE, TILE) * TILE
    token = jnp.pad(token, (0, pad))
    gate = jnp.pad(gate, (0, pad))
    bounds = jnp.concatenate([jnp.zeros((1,), jnp.int32), ends, jnp.full((LANES - 1 - n_local,), ends[-1], jnp.int32)])
    return (tile_e, tile_first, tile_row, tile_n, tile_end[-1:], token, gate), bounds


def split_experts(bounds, core):
    n_local = bounds.shape[1] - 1
    load = jnp.sum(bounds[:, 1:] - bounds[:, :-1], axis=0)
    ids = jnp.arange(n_local, dtype=jnp.int32)
    ahead = (load[None, :] > load[:, None]) | ((load[None, :] == load[:, None]) & (ids[None, :] < ids[:, None]))
    rank = jnp.sum(ahead.astype(jnp.int32), axis=1)
    turn = jnp.arange(n_local // 2, dtype=jnp.int32)

    def dealt(which):
        want = 2 * turn + (which + turn) % 2
        return jnp.sum((rank[None, :] == want[:, None]).astype(jnp.int32) * ids[None, :], axis=1)

    return dealt(core), dealt(1 - core)


def after(x, *earlier):
    return lax.optimization_barrier((x, *earlier))[0]


def solution(mesh):
    ep_size = mesh.shape['ep']
    dp_size = mesh.shape['dp']
    tok_spec = P(('dp', 'ep'), None)
    route_spec = P(None, ('dp', 'ep'), None)
    whole_spec = P(None, None, None)
    expert_spec = P(None, 'ep', None, None)
    ep_pairs = [(i, 1 - i) for i in range(ep_size)]
    core_pairs = [(i, i ^ 1) for i in range(dp_size)]

    def device_body(tokens, d_out, expert_ids, gate_vals, w_mix, w_gate, w_up, w_down):
        n_layers = w_mix.shape[0]
        n_local = w_gate.shape[1]
        n_experts = n_local * ep_size
        tok, d_model = tokens.shape
        top_k = expert_ids.shape[2]
        parts = d_model // LANES
        cap = cdiv(CAP_FACTOR * tok * top_k, n_experts)
        ep_id = lax.axis_index('ep').astype(jnp.int32)
        dp_id = lax.axis_index('dp').astype(jnp.int32)
        ep = ep_id.reshape(1)
        weights = (jnp.swapaxes(w_gate, 2, 3), jnp.swapaxes(w_up, 2, 3), w_down)

        def swap(x):
            return lax.ppermute(x, 'ep', ep_pairs)

        def spread(x):
            return lax.all_gather(x, ('dp', 'ep'), axis=0, tiled=True)

        def slab(x):
            return x.reshape(tok, parts, LANES)

        def mixed(x, layer):
            return (x.astype(jnp.float32) + jnp.dot(x, w_mix[layer], preferred_element_type=jnp.float32)).astype(jnp.bfloat16)

        ids = jnp.swapaxes(expert_ids, 1, 2)
        gates = jnp.swapaxes(gate_vals, 1, 2)
        mine = jnp.stack([ids.astype(jnp.float32), gates])
        theirs = swap(mine)
        both = jnp.where(ep_id == 0, jnp.stack([mine, theirs], 2), jnp.stack([theirs, mine], 2))
        both_ids = both[0].astype(jnp.int32)
        tables, packed = [], []
        for layer in range(n_layers):
            table, bounds = route_tables(both_ids[layer], both[1, layer], ep_id, n_local)
            tables.append(table)
            token, gate = table[5], table[6]
            packed.append(jnp.stack([jnp.concatenate([token + dp_id * (2 * tok), jnp.pad(bounds, (0, PAGE - LANES))])
                                     .astype(jnp.float32), jnp.pad(gate, (0, PAGE))]))
        rows = packed[0].shape[1]
        shared = lax.all_gather(jnp.stack(packed), 'dp', axis=2)
        shared = shared.reshape(n_layers, 2, dp_size, rows)

        d_slab = slab(d_out)
        d_other = swap(d_slab)
        d_spread = spread(d_slab)

        top = n_layers - 1
        x_in, u_slabs, u_others, xs, u_spreads = tokens, [], [], [], []
        for layer in range(n_layers):
            u = mixed(x_in, layer)
            u_slabs.append(slab(u))
            u_others.append(swap(u_slabs[layer]))
            xs.append(x_in)
            u_spreads.append(spread(u_slabs[layer]))
            if layer < top:
                own, other = token_kernel(forward_body, layer, tables[layer], ep,
                                          (u_slabs[layer], u_others[layer]), weights)
                x_in = (u.astype(jnp.float32) + own + swap(other)).astype(jnp.bfloat16)

        d_y, full = d_out, None
        d_mix = [None] * n_layers
        for layer in reversed(range(n_layers)):
            own, other = token_kernel(backward_body, layer, tables[layer], ep,
                                      (u_slabs[layer], u_others[layer], d_slab, d_other), weights)
            d_u = (d_y.astype(jnp.float32) + own + swap(other)).astype(jnp.bfloat16)
            last = other
            if layer == top:
                y_own, y_other = token_kernel(forward_body, top, tables[top], ep,
                                              (after(u_slabs[top], other), u_others[top]), weights)
                layer_out = (u.astype(jnp.float32) + y_own + swap(y_other)).astype(jnp.bfloat16)
                last = y_other
            shared_l, _ = lax.optimization_barrier((shared[layer], last))
            ids_all = shared_l[0].astype(jnp.int32)
            starts = ids_all[:, rows - PAGE:rows - PAGE + LANES]
            mine_e, theirs_e = split_experts(starts[:, :n_local + 1], dp_id % 2)
            full, half = weight_grads(layer, starts.reshape(-1), mine_e, u_spreads[layer], d_spread, ids_all.reshape(-1),
                                      shared_l[1].reshape(-1), weights, full, cap)
            full = merge_half(layer, theirs_e, [lax.ppermute(x, 'dp', core_pairs) for x in half], full)
            d_mix[layer] = jnp.einsum('td,te->de', xs[layer], d_u, preferred_element_type=jnp.float32).astype(jnp.bfloat16)
            d_y = (d_u.astype(jnp.float32)
                   + jnp.einsum('te,de->td', d_u, w_mix[layer], preferred_element_type=jnp.float32)).astype(jnp.bfloat16)
            if layer:
                d_slab = slab(d_y)
                d_other = swap(d_slab)
                d_spread = spread(d_slab)
        d_mix = lax.psum(jnp.stack(d_mix), ('dp', 'ep'))
        return (layer_out, d_y, d_mix, jnp.swapaxes(full[0], 2, 3), jnp.swapaxes(full[1], 2, 3), full[2])

    return jax.shard_map(device_body, mesh=mesh,
                         in_specs=(tok_spec, tok_spec, route_spec, route_spec, whole_spec,
                                   expert_spec, expert_spec, expert_spec),
                         out_specs=(tok_spec, tok_spec, whole_spec, expert_spec, expert_spec, expert_spec),
                         check_vma=False)
```

```python
import functools

import jax
import jax.numpy as jnp
from jax import lax
from jax.experimental import pallas as pl
from jax.experimental.pallas import tpu as pltpu
from jax.sharding import PartitionSpec as P


CAP_FACTOR = 3
LANES = 128
TILE = 128
WTILE = 256
BATCH = 16
SLOTS = 4
PAGE = 1024
VMEM_LIMIT = 62 * 2**20


def cdiv(a, b):
    return (a + b - 1) // b


def nt_dot(a, b):
    return lax.dot_general(a, b, (((1,), (1,)), ((), ())), preferred_element_type=jnp.float32)


def tn_dot(a, b):
    return lax.dot_general(a, b, (((0,), (0,)), ((), ())), preferred_element_type=jnp.float32)


def nn_dot(a, b):
    return lax.dot_general(a, b, (((1,), (0,)), ((), ())), preferred_element_type=jnp.float32)


def load_rows(ref, start, rows, parts):
    cols = [ref[pl.ds(start * parts + k, rows, stride=parts), :] for k in range(parts)]
    return jnp.concatenate(cols, axis=1).astype(jnp.bfloat16)


def store_rows(ref, start, vals, parts):
    rows = vals.shape[0]
    for k in range(parts):
        ref[pl.ds(start * parts + k, rows, stride=parts), :] = vals[:, k * LANES:(k + 1) * LANES]


def fetch_pair(own, other, dst, sem):
    n = own.shape[0]
    return (pltpu.make_async_copy(own, dst.at[pl.ds(0, n)], sem.at[0]),
            pltpu.make_async_copy(other, dst.at[pl.ds(n, n)], sem.at[1]))


def add_rows(acc, vals_ref, idx, gat, row, parts):
    for b in range(0, TILE, BATCH):
        toks = [idx[row + b + r] for r in range(BATCH)]
        gates = [gat[row + b + r] for r in range(BATCH)]
        vals = [acc[pl.ds(toks[r] * parts, parts), :] + gates[r] * vals_ref[pl.ds((b + r) * parts, parts), :]
                for r in range(BATCH)]
        for r in reversed(range(BATCH)):
            acc[pl.ds(toks[r] * parts, parts), :] = vals[r]


def write_sums(acc, own_ref, other_ref, tok, parts):
    step = min(32, tok)

    def copy_out(q, carry):
        r0 = pl.multiple_of(q * step, step)
        for k in range(parts):
            cols = slice(k * LANES, (k + 1) * LANES)
            own_ref[pl.ds(r0, step), cols] = acc[pl.ds(r0 * parts + k, step, stride=parts), :]
            other_ref[pl.ds(r0, step), cols] = acc[pl.ds((tok + r0) * parts + k, step, stride=parts), :]
        return carry

    lax.fori_loop(0, tok // step, copy_out, 0)


def expert_copies(weights, buf, sem, layer, e):
    slot = lax.rem(e, SLOTS)
    ff = weights[0].shape[2]
    return [pltpu.make_async_copy(w.at[layer, e], buf.at[slot, pl.ds(k * ff, ff)], sem.at[slot])
            for k, w in enumerate(weights)]


def run_tiles(step, weights, wbuf, wsem, tile_e, tile_first, n_steps, layer, copies):
    n_local = weights[0].shape[1]
    ahead = list(copies) + expert_copies(weights, wbuf, wsem, layer, 0)
    for c in ahead:
        c.start()
    for e in range(1, min(SLOTS - 1, n_local)):
        for c in expert_copies(weights, wbuf, wsem, layer, e):
            c.start()
    for c in ahead:
        c.wait()

    def one(i, carry):
        e = tile_e[i + 1]

        @pl.when(tile_first[i + 1] == 1)
        def _():
            for c in expert_copies(weights, wbuf, wsem, layer, e):
                c.wait()

        @pl.when((tile_first[i + 1] == 1) & (e + SLOTS - 2 < n_local))
        def _():
            for c in expert_copies(weights, wbuf, wsem, layer, e + SLOTS - 2):
                c.start()

        step(i, lax.rem(e, SLOTS))
        return carry

    lax.fori_loop(0, n_steps, one, 0)


def forward_body(te, tf, tr, tn, nt, idx, gat, u_own, u_oth, g_ref, up_ref, w_ref, own_ref, other_ref,
                 usc, ut, ot, acc, wbuf, sem, wsem, *, layer, tok, parts):
    ff = g_ref.shape[2]
    acc[...] = jnp.zeros_like(acc)
    ot[...] = jnp.zeros_like(ot)
    ut[...] = jnp.zeros_like(ut)

    def step(i, slot):
        u = load_rows(ut, 0, TILE, parts)
        ab = nt_dot(wbuf[slot, :2 * ff], u)
        add_rows(acc, ot, idx, gat, tr[i], parts)
        row = tr[i + 2]
        for r in range(TILE):
            ut[pl.ds(parts * r, parts), :] = usc[idx[row + r]].astype(jnp.float32)
        a, b = ab[:ff], ab[ff:]
        h = (a * jax.nn.sigmoid(a) * b).astype(jnp.bfloat16)
        o = tn_dot(h, wbuf[slot, 2 * ff:]).astype(jnp.bfloat16).astype(jnp.float32)
        live = lax.broadcasted_iota(jnp.int32, o.shape, 0) < tn[i + 1]
        store_rows(ot, 0, jnp.where(live, o, 0.0), parts)

    run_tiles(step, (g_ref, up_ref, w_ref), wbuf, wsem, te, tf, nt[0] + 2, layer,
              fetch_pair(u_own, u_oth, usc, sem))
    write_sums(acc, own_ref, other_ref, tok, parts)


def backward_body(te, tf, tr, tn, nt, idx, gat, u_own, u_oth, d_own, d_oth, g_ref, up_ref, w_ref, own_ref, other_ref,
                  usc, dsc, ut, ct, vt, acc, wbuf, sem, wsem, *, layer, tok, parts):
    ff = g_ref.shape[2]
    acc[...] = jnp.zeros_like(acc)
    vt[...] = jnp.zeros_like(vt)
    ut[...] = jnp.zeros_like(ut)
    ct[...] = jnp.zeros_like(ct)

    def step(i, slot):
        u = load_rows(ut, 0, TILE, parts)
        c = load_rows(ct, 0, TILE, parts)
        gu = wbuf[slot, :2 * ff]
        ab = nt_dot(gu, u)
        dh = nt_dot(wbuf[slot, 2 * ff:], c)
        add_rows(acc, vt, idx, gat, tr[i], parts)
        row = tr[i + 2]
        for r in range(TILE):
            t = idx[row + r]
            ut[pl.ds(parts * r, parts), :] = usc[t].astype(jnp.float32)
            ct[pl.ds(parts * r, parts), :] = gat[row + r] * dsc[t].astype(jnp.float32)
        a, b = ab[:ff], ab[ff:]
        s = jax.nn.sigmoid(a)
        da = (dh * b * (s * (1.0 + a * (1.0 - s)))).astype(jnp.bfloat16)
        db = (dh * (a * s)).astype(jnp.bfloat16)
        v = tn_dot(jnp.concatenate([da, db], axis=0), gu).astype(jnp.bfloat16).astype(jnp.float32)
        live = lax.broadcasted_iota(jnp.int32, v.shape, 0) < tn[i + 1]
        store_rows(vt, 0, jnp.where(live, v, 0.0), parts)

    run_tiles(step, (g_ref, up_ref, w_ref), wbuf, wsem, te, tf, nt[0] + 2, layer,
              fetch_pair(u_own, u_oth, usc, sem.at[0]) + fetch_pair(d_own, d_oth, dsc, sem.at[1]))
    write_sums(acc, own_ref, other_ref, tok, parts)


def token_kernel(body, layer, tables, slabs, weights):
    tok, parts, _ = slabs[0].shape
    _, n_local, ff, d_model = weights[0].shape
    n_pairs = len(slabs) // 2
    rows_spec = pl.BlockSpec((tok, d_model), lambda i, *_: (0, 0))
    any_spec = pl.BlockSpec(memory_space=pl.ANY)
    sem_shape = (2,) if n_pairs == 1 else (2, 2)
    copies = 8 * tok
    return pl.pallas_call(
        functools.partial(body, layer=layer, tok=tok, parts=parts),
        grid_spec=pltpu.PrefetchScalarGridSpec(
            num_scalar_prefetch=len(tables),
            grid=(1,),
            in_specs=[any_spec] * (len(slabs) + 3),
            out_specs=[rows_spec] * 2,
            scratch_shapes=[pltpu.VMEM((2 * tok, parts, LANES), jnp.bfloat16)] * n_pairs
            + [pltpu.VMEM((TILE * parts, LANES), jnp.float32)] * (n_pairs + 1)
            + [pltpu.VMEM((2 * tok * parts, LANES), jnp.float32), pltpu.VMEM((SLOTS, 3 * ff, d_model), jnp.bfloat16),
               pltpu.SemaphoreType.DMA(sem_shape), pltpu.SemaphoreType.DMA((SLOTS,))],
        ),
        out_shape=[jax.ShapeDtypeStruct((tok, d_model), jnp.float32)] * 2,
        compiler_params=pltpu.CompilerParams(dimension_semantics=("arbitrary",), vmem_limit_bytes=VMEM_LIMIT),
        cost_estimate=pl.CostEstimate(flops=(3 + 3 * (n_pairs - 1)) * 2 * copies * d_model * ff * 4,
                                      bytes_accessed=3 * n_local * ff * d_model * 2, transcendentals=0),
    )(*tables, *slabs, *weights)


def merge_tables_body(st, exps, table, idx_ref, gate_ref, buf, *, src, n_exp, src_rows, out_rows):
    layer, e = pl.program_id(0), pl.program_id(1)
    exp = exps[layer * n_exp + e]
    buf[...] = jnp.zeros_like(buf)
    row = lax.broadcasted_iota(jnp.int32, (8, LANES), 0)
    lane = lax.broadcasted_iota(jnp.int32, (8, LANES), 1)
    off = 0
    for d in range(src):
        at = (layer * src + d) * LANES + exp
        first = st[at]
        count = st[at + 1] - first
        to = lax.rem(off, LANES) + LANES
        shift = to - lax.rem(first, LANES)
        over = lax.rem(shift, LANES)
        start = lax.div(off, LANES)
        place = row * LANES + lane
        take = (place >= to) & (place < to + count)
        for kind in range(2):
            x = table[0, kind, pl.ds(d * src_rows + lax.div(first, LANES), 8), :]
            x = pltpu.roll(pltpu.roll(x, over, 1), lax.div(shift, LANES), 0)
            x = jnp.where(lane >= over, x, pltpu.roll(x, 1, 0))
            old = buf[kind, pl.ds(start, 8), :]
            buf[kind, pl.ds(start, 8), :] = jnp.where(take, x, old)
        off = off + count
    idx_ref[0, 0] = buf[0, pl.ds(1, out_rows), :].astype(jnp.int32)
    gate_ref[0, 0] = buf[1, pl.ds(1, out_rows), :]


def merge_tables(shared, starts, exps, out_rows):
    n_layers, _, src, rows = shared.shape
    n_exp = exps.shape[1]
    exps = exps.reshape(-1)
    src_rows = rows // LANES
    out = pl.BlockSpec((1, 1, out_rows, LANES), lambda l, e, *_: (l, e, 0, 0))
    return pl.pallas_call(
        functools.partial(merge_tables_body, src=src, n_exp=n_exp, src_rows=src_rows, out_rows=out_rows),
        grid_spec=pltpu.PrefetchScalarGridSpec(
            num_scalar_prefetch=2,
            grid=(n_layers, n_exp),
            in_specs=[pl.BlockSpec((1, 2, src * src_rows, LANES), lambda l, e, *_: (l, 0, 0, 0))],
            out_specs=[out] * 2,
            scratch_shapes=[pltpu.VMEM((2, out_rows + 16, LANES), jnp.float32)],
        ),
        out_shape=[jax.ShapeDtypeStruct((n_layers, n_exp, out_rows, LANES), jnp.int32),
                   jax.ShapeDtypeStruct((n_layers, n_exp, out_rows, LANES), jnp.float32)],
        compiler_params=pltpu.CompilerParams(dimension_semantics=("arbitrary", "arbitrary")),
        cost_estimate=pl.CostEstimate(flops=10**9, bytes_accessed=4 * shared.size, transcendentals=0),
        name="merge_tables",
    )(starts, exps, shared.reshape(n_layers, 2, src * src_rows, LANES))


def weight_grad_body(exps, tiles, u_own, u_oth, d_own, d_oth, idx_all, gate_ref, *refs, parts, n_exp, n_alias, layer, page):
    g_ref, up_ref, w_ref = refs[:3]
    (dg_ref, du_ref, dw_ref, og_ref, ou_ref, ow_ref,
     usc, dsc, ut, dt, ub, cb, gacc, wacc, idx_s, sem, tsem) = refs[3 + n_alias:]
    e = pl.program_id(0)
    ff = g_ref.shape[2]
    slots = 3

    def table_copy(exp):
        slot = lax.rem(exp, slots)
        at = pl.multiple_of((layer * n_exp + exp) * page, PAGE)
        to = pl.multiple_of(slot * page, PAGE)
        return pltpu.make_async_copy(idx_all.at[pl.ds(at, page)], idx_s.at[pl.ds(to, page)], tsem.at[slot])

    def gather_row(at, r):
        t = idx_s[at]
        ut[pl.ds(r * parts, parts), :] = usc[t].astype(jnp.float32)
        dt[pl.ds(r * parts, parts), :] = dsc[t].astype(jnp.float32)

    @pl.when(e == 0)
    def _():
        copies = fetch_pair(u_own, u_oth, usc, sem.at[0]) + fetch_pair(d_own, d_oth, dsc, sem.at[1])
        for c in copies:
            c.start()
        table_copy(0).start()
        table_copy(1).start()
        table_copy(0).wait()
        for c in copies:
            c.wait()

        def first_rows(q, carry):
            for r in range(16):
                gather_row(q * 16 + r, q * 16 + r)
            return carry

        lax.fori_loop(0, WTILE // 16, first_rows, 0)

    @pl.when(e + 1 < n_exp)
    def _():
        table_copy(e + 1).wait()

    @pl.when(e + 2 < n_exp)
    def _():
        table_copy(e + 2).start()

    gacc[...] = jnp.zeros_like(gacc)
    wacc[...] = jnp.zeros_like(wacc)
    here = lax.rem(e, slots) * page
    there = lax.rem(jnp.minimum(e + 1, n_exp - 1), slots) * page
    n_tiles = tiles[layer * n_exp + e]
    gate_rows = WTILE // LANES

    def tile(j, carry):
        ub[...] = load_rows(ut, 0, WTILE, parts)
        gates = [jnp.broadcast_to(gate_ref[0, 0, pl.ds(j * gate_rows + q, 1), :], (LANES, LANES)).T for q in range(gate_rows)]
        for k in range(parts):
            for q in range(gate_rows):
                d = dt[pl.ds(q * LANES * parts + k, LANES, stride=parts), :]
                cb[q * LANES:(q + 1) * LANES, k * LANES:(k + 1) * LANES] = (d * gates[q]).astype(jnp.bfloat16)
        ab = nt_dot(jnp.concatenate([g_ref[0, 0], up_ref[0, 0]], axis=0), ub[...])
        dh = nt_dot(w_ref[0, 0], cb[...])
        nxt = jnp.where(j + 1 < n_tiles, here + (j + 1) * WTILE, there)
        for r in range(WTILE):
            gather_row(nxt + r, r)
        a, b = ab[:ff], ab[ff:]
        s = jax.nn.sigmoid(a)
        act = a * s
        h = (act * b).astype(jnp.bfloat16)
        da = (dh * b * (s * (1.0 + a * (1.0 - s)))).astype(jnp.bfloat16)
        db = (dh * act).astype(jnp.bfloat16)
        gacc[...] += nn_dot(jnp.concatenate([da, db], axis=0), ub[...])
        wacc[...] += nn_dot(h, cb[...])
        return carry

    lax.fori_loop(0, n_tiles, tile, 0)
    dg = gacc[:ff].astype(jnp.bfloat16)
    du = gacc[ff:].astype(jnp.bfloat16)
    dw = wacc[...].astype(jnp.bfloat16)
    dg_ref[0, 0], du_ref[0, 0], dw_ref[0, 0] = dg, du, dw
    og_ref[0], ou_ref[0], ow_ref[0] = dg, du, dw


def weight_grads(layer, exps, tiles, u_alls, d_alls, idx_all, gates, weights, full):
    n_src, parts, _ = u_alls[0].shape
    n_tok = 2 * n_src
    n_layers, n_local, ff, d_model = weights[0].shape
    n_exp = n_local // 2
    out_rows = gates.shape[2]
    page = out_rows * LANES
    any_spec = pl.BlockSpec(memory_space=pl.ANY)
    mine = pl.BlockSpec((1, 1, ff, d_model), lambda e, exps, tiles: (layer, exps[e], 0, 0))
    half = pl.BlockSpec((1, ff, d_model), lambda e, *_: (e, 0, 0))
    gate_spec = pl.BlockSpec((1, 1, out_rows, LANES), lambda e, *_: (layer, e, 0, 0))
    aliased = list(full) if full is not None else []
    outs = pl.pallas_call(
        functools.partial(weight_grad_body, parts=parts, n_exp=n_exp, n_alias=len(aliased), layer=layer, page=page),
        grid_spec=pltpu.PrefetchScalarGridSpec(
            num_scalar_prefetch=2,
            grid=(n_exp,),
            in_specs=[any_spec] * 5 + [gate_spec] + [mine] * 3 + [any_spec] * len(aliased),
            out_specs=[mine] * 3 + [half] * 3,
            scratch_shapes=[pltpu.VMEM((n_tok, parts, LANES), jnp.bfloat16)] * 2
            + [pltpu.VMEM((WTILE * parts, LANES), jnp.float32)] * 2
            + [pltpu.VMEM((WTILE, d_model), jnp.bfloat16)] * 2
            + [pltpu.VMEM((2 * ff, d_model), jnp.float32), pltpu.VMEM((ff, d_model), jnp.float32),
               pltpu.SMEM((3 * page,), jnp.int32), pltpu.SemaphoreType.DMA((2, 2)), pltpu.SemaphoreType.DMA((3,))],
        ),
        out_shape=[jax.ShapeDtypeStruct((n_layers, n_local, ff, d_model), jnp.bfloat16)] * 3
        + [jax.ShapeDtypeStruct((n_exp, ff, d_model), jnp.bfloat16)] * 3,
        input_output_aliases={11 + k: k for k in range(len(aliased))},
        compiler_params=pltpu.CompilerParams(dimension_semantics=("arbitrary",), vmem_limit_bytes=VMEM_LIMIT),
        cost_estimate=pl.CostEstimate(flops=6 * 2 * n_tok * 2 * d_model * ff * 4,
                                      bytes_accessed=n_tok * d_model * 4 + 9 * n_exp * ff * d_model * 2, transcendentals=0),
        name="weight_grads",
    )(exps, tiles, *u_alls, *d_alls, idx_all, gates, *weights, *aliased)
    return outs[:3], outs[3:]


def merge_body(exps, a, b, c, f0, f1, f2, o0, o1, o2):
    o0[0, 0], o1[0, 0], o2[0, 0] = a[0], b[0], c[0]


def merge_half(layer, exps, half, full):
    _, n_local, ff, d_model = full[0].shape
    n_exp = n_local // 2
    any_spec = pl.BlockSpec(memory_space=pl.ANY)
    part = pl.BlockSpec((1, ff, d_model), lambda e, exps: (e, 0, 0))
    place = pl.BlockSpec((1, 1, ff, d_model), lambda e, exps: (layer, exps[e], 0, 0))
    return pl.pallas_call(
        merge_body,
        grid_spec=pltpu.PrefetchScalarGridSpec(
            num_scalar_prefetch=1, grid=(n_exp,), in_specs=[part] * 3 + [any_spec] * 3, out_specs=[place] * 3),
        out_shape=[jax.ShapeDtypeStruct(x.shape, x.dtype) for x in full],
        input_output_aliases={4: 0, 5: 1, 6: 2},
        compiler_params=pltpu.CompilerParams(dimension_semantics=("arbitrary",)),
        cost_estimate=pl.CostEstimate(flops=0, bytes_accessed=6 * n_exp * ff * d_model * 2, transcendentals=0),
        name="merge_half",
    )(exps, *half, *full)


def route_tables(ids, gates, ep, n_local):
    n_src, top_k, tok = ids.shape
    n = n_src * top_k * tok
    local = ids - ep * n_local
    here = (local >= 0) & (local < n_local)
    group = jnp.where(here, local, n_local).reshape(-1)
    key, gate = lax.sort((group * n + jnp.arange(n, dtype=jnp.int32), gates.reshape(-1)), num_keys=1, is_stable=False)
    copy = key % n
    token = copy // (top_k * tok) * tok + copy % tok
    counts = jnp.sum((group[:, None] == jnp.arange(n_local)[None, :]).astype(jnp.int32), axis=0)
    ends = jnp.cumsum(counts)
    starts = ends - counts
    n_tiles = jnp.maximum((counts + TILE - 1) // TILE, 1)
    tile_end = jnp.cumsum(n_tiles)
    tile_id = jnp.arange(n // TILE + n_local + 4, dtype=jnp.int32) - 2
    tile_e = jnp.minimum(jnp.sum((tile_end[None, :] <= tile_id[:, None]).astype(jnp.int32), axis=1), n_local - 1)
    pick = (tile_e[:, None] == jnp.arange(n_local)[None, :]).astype(jnp.int32)
    inside = (tile_id - jnp.sum(pick * (tile_end - n_tiles)[None, :], axis=1)) * TILE
    real = (tile_id >= 0) & (tile_id < tile_end[-1])
    tile_row = jnp.where(real, jnp.sum(pick * starts[None, :], axis=1) + inside, 0)
    tile_first = (real & (inside == 0) & (tile_e > 0)).astype(jnp.int32)
    tile_n = jnp.where(real, jnp.clip(jnp.sum(pick * counts[None, :], axis=1) - inside, 0, TILE), 0)
    pad = cdiv(2 * PAGE, TILE) * TILE
    token = jnp.pad(token, (0, pad))
    gate = jnp.pad(gate, (0, pad))
    bounds = jnp.concatenate([jnp.zeros((1,), jnp.int32), ends, jnp.full((LANES - 1 - n_local,), ends[-1], jnp.int32)])
    return (tile_e, tile_first, tile_row, tile_n, tile_end[-1:], token, gate), bounds


def split_experts(bounds, core):
    n_local = bounds.shape[1] - 1
    load = jnp.sum(bounds[:, 1:] - bounds[:, :-1], axis=0)
    ids = jnp.arange(n_local, dtype=jnp.int32)
    ahead = (load[None, :] > load[:, None]) | ((load[None, :] == load[:, None]) & (ids[None, :] < ids[:, None]))
    rank = jnp.sum(ahead.astype(jnp.int32), axis=1)
    turn = jnp.arange(n_local // 2, dtype=jnp.int32)

    def dealt(which):
        want = 2 * turn + (which + turn) % 2
        return (rank[None, :] == want[:, None]).astype(jnp.int32)

    mine, theirs = dealt(core), dealt(1 - core)
    tiles = jnp.maximum((jnp.sum(mine * load[None, :], axis=1) + WTILE - 1) // WTILE, 1)
    return jnp.sum(mine * ids[None, :], axis=1), jnp.sum(theirs * ids[None, :], axis=1), tiles


def after(x, *earlier):
    return lax.optimization_barrier((x, *earlier))[0]


def solution(mesh):
    ep_size = mesh.shape['ep']
    dp_size = mesh.shape['dp']
    tok_spec = P(('dp', 'ep'), None)
    route_spec = P(None, ('dp', 'ep'), None)
    whole_spec = P(None, None, None)
    expert_spec = P(None, 'ep', None, None)
    ep_pairs = [(i, 1 - i) for i in range(ep_size)]
    core_pairs = [(i, i ^ 1) for i in range(dp_size)]

    def device_body(tokens, d_out, expert_ids, gate_vals, w_mix, w_gate, w_up, w_down):
        n_layers = w_mix.shape[0]
        n_local = w_gate.shape[1]
        n_experts = n_local * ep_size
        tok, d_model = tokens.shape
        top_k = expert_ids.shape[2]
        parts = d_model // LANES
        cap = cdiv(CAP_FACTOR * tok * top_k, n_experts)
        ep_id = lax.axis_index('ep').astype(jnp.int32)
        dp_id = lax.axis_index('dp').astype(jnp.int32)
        weights = (jnp.swapaxes(w_gate, 2, 3), jnp.swapaxes(w_up, 2, 3), w_down)

        def swap(x):
            return lax.ppermute(x, 'ep', ep_pairs)

        def spread(x):
            return lax.all_gather(x, 'dp', axis=0, tiled=True)

        def slab(x):
            return x.reshape(tok, parts, LANES)

        def mixed(x, layer):
            return (x.astype(jnp.float32) + jnp.dot(x, w_mix[layer], preferred_element_type=jnp.float32)).astype(jnp.bfloat16)

        ids = jnp.swapaxes(expert_ids, 1, 2)
        gates = jnp.swapaxes(gate_vals, 1, 2)
        mine = jnp.stack([ids.astype(jnp.float32), gates])
        theirs = swap(mine)
        both = jnp.stack([mine, theirs], 2)
        both_ids = both[0].astype(jnp.int32)
        tables, packed = [], []
        for layer in range(n_layers):
            table, bounds = route_tables(both_ids[layer], both[1, layer], ep_id, n_local)
            tables.append(table)
            token, gate = table[5], table[6]
            spot = lax.div(token, tok) * (dp_size * tok) + dp_id * tok + lax.rem(token, tok)
            packed.append(jnp.stack([jnp.concatenate([spot, jnp.pad(bounds, (0, PAGE - LANES))])
                                     .astype(jnp.float32), jnp.pad(gate, (0, PAGE))]))
        rows = packed[0].shape[1]
        shared = lax.all_gather(jnp.stack(packed), 'dp', axis=2)
        shared = shared.reshape(n_layers, 2, dp_size, rows)
        starts = shared[:, 0, :, rows - PAGE:rows - PAGE + LANES].astype(jnp.int32)
        split = [split_experts(starts[layer, :, :n_local + 1], dp_id % 2) for layer in range(n_layers)]
        mine_e, theirs_e, tiles = (jnp.stack(x) for x in zip(*split))
        list_rows = cdiv(cdiv(dp_size * 2 * cap, LANES), 8) * 8 + 8
        idx_all, gate_all = merge_tables(shared, starts.reshape(-1), mine_e, list_rows)
        idx_all = idx_all.reshape(-1)

        d_slab = slab(d_out)
        d_other = swap(d_slab)
        d_spread = (spread(d_slab), spread(d_other))

        top = n_layers - 1
        x_in, u_slabs, u_others, xs, u_spreads = tokens, [], [], [], []
        for layer in range(n_layers):
            u = mixed(x_in, layer)
            u_slabs.append(slab(u))
            u_others.append(swap(u_slabs[layer]))
            xs.append(x_in)
            u_spreads.append((spread(u_slabs[layer]), spread(u_others[layer])))
            if layer < top:
                own, other = token_kernel(forward_body, layer, tables[layer],
                                          (u_slabs[layer], u_others[layer]), weights)
                x_in = (u.astype(jnp.float32) + own + swap(other)).astype(jnp.bfloat16)

        d_y, full = d_out, None
        d_mix = [None] * n_layers
        for layer in reversed(range(n_layers)):
            own, other = token_kernel(backward_body, layer, tables[layer],
                                      (u_slabs[layer], u_others[layer], d_slab, d_other), weights)
            d_u = (d_y.astype(jnp.float32) + own + swap(other)).astype(jnp.bfloat16)
            last = other
            if layer == top:
                y_own, y_other = token_kernel(forward_body, top, tables[top],
                                              (after(u_slabs[top], other), u_others[top]), weights)
                layer_out = (u.astype(jnp.float32) + y_own + swap(y_other)).astype(jnp.bfloat16)
                last = y_other
            full, half = weight_grads(layer, mine_e[layer], after(tiles, last).reshape(-1), u_spreads[layer], d_spread,
                                      idx_all, gate_all, weights, full)
            full = merge_half(layer, theirs_e[layer], [lax.ppermute(x, 'dp', core_pairs) for x in half], full)
            d_mix[layer] = jnp.einsum('td,te->de', xs[layer], d_u, preferred_element_type=jnp.float32).astype(jnp.bfloat16)
            d_y = (d_u.astype(jnp.float32)
                   + jnp.einsum('te,de->td', d_u, w_mix[layer], preferred_element_type=jnp.float32)).astype(jnp.bfloat16)
            if layer:
                d_slab = slab(d_y)
                d_other = swap(d_slab)
                d_spread = (spread(d_slab), spread(d_other))
        d_mix = lax.psum(jnp.stack(d_mix), ('dp', 'ep'))
        return (layer_out, d_y, d_mix, jnp.swapaxes(full[0], 2, 3), jnp.swapaxes(full[1], 2, 3), full[2])

    return jax.shard_map(device_body, mesh=mesh,
                         in_specs=(tok_spec, tok_spec, route_spec, route_spec, whole_spec,
                                   expert_spec, expert_spec, expert_spec),
                         out_specs=(tok_spec, tok_spec, whole_spec, expert_spec, expert_spec, expert_spec),
                         check_vma=False)
```

```python
import functools

import jax
import jax.numpy as jnp
from jax import lax
from jax.experimental import pallas as pl
from jax.experimental.pallas import tpu as pltpu
from jax.sharding import PartitionSpec as P


CAP_FACTOR = 3
LANES = 128
TILE = 128
WTILE = 256
BATCH = 16
SLOTS = 6
PAGE = 1024
VMEM_LIMIT = 62 * 2**20


def cdiv(a, b):
    return (a + b - 1) // b


def nt_dot(a, b):
    return lax.dot_general(a, b, (((1,), (1,)), ((), ())), preferred_element_type=jnp.float32)


def tn_dot(a, b):
    return lax.dot_general(a, b, (((0,), (0,)), ((), ())), preferred_element_type=jnp.float32)


def nn_dot(a, b):
    return lax.dot_general(a, b, (((1,), (0,)), ((), ())), preferred_element_type=jnp.float32)


def clear(ref):
    step = min(64, ref.shape[0])

    def one(q, carry):
        ref[pl.ds(pl.multiple_of(q * step, step), step), :] = jnp.zeros((step, ref.shape[1]), ref.dtype)
        return carry

    lax.fori_loop(0, ref.shape[0] // step, one, 0)


def load_rows(ref, start, rows, parts):
    cols = [ref[pl.ds(start * parts + k, rows, stride=parts), :] for k in range(parts)]
    return jnp.concatenate(cols, axis=1).astype(jnp.bfloat16)


def fetch_pair(own, other, dst, sem):
    n = own.shape[0]
    return (pltpu.make_async_copy(own, dst.at[pl.ds(0, n)], sem.at[0]),
            pltpu.make_async_copy(other, dst.at[pl.ds(n, n)], sem.at[1]))


def add_rows(acc, vals_ref, idx, row, parts):
    for b in range(0, TILE, BATCH):
        at = [pl.multiple_of(idx[row + b + r], parts) for r in range(BATCH)]
        vals = [acc[pl.ds(at[r], parts), :] + vals_ref[pl.ds((b + r) * parts, parts), :] for r in range(BATCH)]
        for r in reversed(range(BATCH)):
            acc[pl.ds(at[r], parts), :] = vals[r]


def spread_column(row):
    return jnp.broadcast_to(row, (LANES, LANES)).T


def tile_gates(gates, row):
    pair = gates[pl.ds(lax.div(row, LANES), 2), :]
    skip = lax.rem(row, LANES)
    pair = pltpu.roll(pair, lax.rem(LANES - skip, LANES), 1)
    lane = lax.broadcasted_iota(jnp.int32, (1, LANES), 1)
    return spread_column(jnp.where(lane < LANES - skip, pair[:1], pair[1:]))


def widen(src, dst, parts):
    step = 8

    def one(q, carry):
        for r in range(step):
            dst[pl.ds((q * step + r) * parts, parts), :] = src[q * step + r].astype(jnp.float32)
        return carry

    lax.fori_loop(0, src.shape[0] // step, one, 0)


def write_sums(acc, own_ref, other_ref, tok, parts):
    step = min(32, tok)

    def copy_out(q, carry):
        r0 = pl.multiple_of(q * step, step)
        for k in range(parts):
            cols = slice(k * LANES, (k + 1) * LANES)
            own_ref[pl.ds(r0, step), cols] = acc[pl.ds(r0 * parts + k, step, stride=parts), :]
            other_ref[pl.ds(r0, step), cols] = acc[pl.ds((tok + r0) * parts + k, step, stride=parts), :]
        return carry

    lax.fori_loop(0, tok // step, copy_out, 0)


def expert_copies(weights, buf, sem, layer, e):
    slot = lax.rem(e, SLOTS)
    ff = weights[0].shape[2]
    return [pltpu.make_async_copy(w.at[layer, e], buf.at[slot, pl.ds(k * ff, ff)], sem.at[slot])
            for k, w in enumerate(weights)]


def run_tiles(step, weights, wbuf, wsem, tile_e, tile_first, n_steps, layer, prepare):
    n_local = weights[0].shape[1]
    for e in range(min(SLOTS - 1, n_local)):
        for c in expert_copies(weights, wbuf, wsem, layer, e):
            c.start()
    prepare()
    for c in expert_copies(weights, wbuf, wsem, layer, 0):
        c.wait()

    def one(i, carry):
        e = tile_e[i + 2]

        @pl.when(tile_first[i + 2] == 1)
        def _():
            for c in expert_copies(weights, wbuf, wsem, layer, e):
                c.wait()

        @pl.when((tile_first[i + 2] == 1) & (e + SLOTS - 2 < n_local))
        def _():
            for c in expert_copies(weights, wbuf, wsem, layer, e + SLOTS - 2):
                c.start()

        step(i, lax.rem(e, SLOTS), lax.rem(tile_e[i + 1], SLOTS))
        return carry

    lax.fori_loop(0, n_steps, one, 0)


def forward_body(te, tf, tr, tn, nt, idx, gates, u_own, u_oth, g_ref, up_ref, w_ref, own_ref, other_ref,
                 usc, uf, ut, ot, acc, ht, wbuf, sem, wsem, *, layer, tok, parts):
    ff = g_ref.shape[2]

    def prepare():
        copies = fetch_pair(u_own, u_oth, usc, sem)
        for c in copies:
            c.start()
        for ref in (acc, ot, ut, ht):
            clear(ref)
        for c in copies:
            c.wait()
        widen(usc, uf, parts)

    def step(i, slot, slot_before):
        o = tn_dot(ht[...], wbuf[slot_before, 2 * ff:]).astype(jnp.bfloat16).astype(jnp.float32)
        u = load_rows(ut, 0, TILE, parts)
        ab = nt_dot(wbuf[slot, :2 * ff], u)
        add_rows(acc, ot, idx, tr[i], parts)
        row = tr[i + 3]
        for r in range(TILE):
            ut[pl.ds(parts * r, parts), :] = uf[pl.ds(pl.multiple_of(idx[row + r], parts), parts), :]
        live = lax.broadcasted_iota(jnp.int32, (TILE, LANES), 0) < tn[i + 1]
        gate = tile_gates(gates, tr[i + 1])
        for k in range(parts):
            o_k = jnp.where(live, o[:, k * LANES:(k + 1) * LANES] * gate, 0.0)
            ot[pl.ds(k, TILE, stride=parts), :] = o_k
        a, b = ab[:ff], ab[ff:]
        ht[...] = (a * jax.nn.sigmoid(a) * b).astype(jnp.bfloat16)

    run_tiles(step, (g_ref, up_ref, w_ref), wbuf, wsem, te, tf, nt[0] + 3, layer, prepare)
    write_sums(acc, own_ref, other_ref, tok, parts)


def backward_body(te, tf, tr, tn, nt, idx, gates, u_own, u_oth, d_own, d_oth, g_ref, up_ref, w_ref, own_ref, other_ref,
                  usc, dsc, uf, df, ut, dt, vt, acc, da_t, wbuf, sem, wsem, *, layer, tok, parts):
    ff = g_ref.shape[2]

    def prepare():
        copies = fetch_pair(u_own, u_oth, usc, sem.at[0]) + fetch_pair(d_own, d_oth, dsc, sem.at[1])
        for c in copies:
            c.start()
        for ref in (acc, vt, ut, dt, da_t):
            clear(ref)
        for c in copies:
            c.wait()
        widen(usc, uf, parts)
        widen(dsc, df, parts)

    def step(i, slot, slot_before):
        v = tn_dot(da_t[...], wbuf[slot_before, :2 * ff]).astype(jnp.bfloat16).astype(jnp.float32)
        u = load_rows(ut, 0, TILE, parts)
        gate = tile_gates(gates, tr[i + 2])
        c = jnp.concatenate([(dt[pl.ds(k, TILE, stride=parts), :] * gate).astype(jnp.bfloat16) for k in range(parts)], axis=1)
        ab = nt_dot(wbuf[slot, :2 * ff], u)
        dh = nt_dot(wbuf[slot, 2 * ff:], c)
        add_rows(acc, vt, idx, tr[i], parts)
        row = tr[i + 3]
        for r in range(TILE):
            at = pl.multiple_of(idx[row + r], parts)
            ut[pl.ds(parts * r, parts), :] = uf[pl.ds(at, parts), :]
            dt[pl.ds(parts * r, parts), :] = df[pl.ds(at, parts), :]
        live = lax.broadcasted_iota(jnp.int32, (TILE, LANES), 0) < tn[i + 1]
        gate = tile_gates(gates, tr[i + 1])
        for k in range(parts):
            v_k = jnp.where(live, v[:, k * LANES:(k + 1) * LANES] * gate, 0.0)
            vt[pl.ds(k, TILE, stride=parts), :] = v_k
        a, b = ab[:ff], ab[ff:]
        s = jax.nn.sigmoid(a)
        da_t[:ff] = (dh * b * (s * (1.0 + a * (1.0 - s)))).astype(jnp.bfloat16)
        da_t[ff:] = (dh * (a * s)).astype(jnp.bfloat16)

    run_tiles(step, (g_ref, up_ref, w_ref), wbuf, wsem, te, tf, nt[0] + 3, layer, prepare)
    write_sums(acc, own_ref, other_ref, tok, parts)


def token_kernel(body, layer, tables, slabs, weights):
    tok, parts, _ = slabs[0].shape
    _, n_local, ff, d_model = weights[0].shape
    n_pairs = len(slabs) // 2
    rows_spec = pl.BlockSpec((tok, d_model), lambda i, *_: (0, 0))
    any_spec = pl.BlockSpec(memory_space=pl.ANY)
    sem_shape = (2,) if n_pairs == 1 else (2, 2)
    copies = 8 * tok
    return pl.pallas_call(
        functools.partial(body, layer=layer, tok=tok, parts=parts),
        grid_spec=pltpu.PrefetchScalarGridSpec(
            num_scalar_prefetch=len(tables) - 1,
            grid=(1,),
            in_specs=[pl.BlockSpec(tables[-1].shape, lambda i, *_: (0, 0))] + [any_spec] * (len(slabs) + 3),
            out_specs=[rows_spec] * 2,
            scratch_shapes=[pltpu.VMEM((2 * tok, parts, LANES), jnp.bfloat16)] * n_pairs
            + [pltpu.VMEM((2 * tok * parts, LANES), jnp.float32)] * n_pairs
            + [pltpu.VMEM((TILE * parts, LANES), jnp.float32)] * (n_pairs + 1)
            + [pltpu.VMEM((2 * tok * parts, LANES), jnp.float32), pltpu.VMEM((n_pairs * ff, TILE), jnp.bfloat16),
               pltpu.VMEM((SLOTS, 3 * ff, d_model), jnp.bfloat16),
               pltpu.SemaphoreType.DMA(sem_shape), pltpu.SemaphoreType.DMA((SLOTS,))],
        ),
        out_shape=[jax.ShapeDtypeStruct((tok, d_model), jnp.float32)] * 2,
        compiler_params=pltpu.CompilerParams(dimension_semantics=("arbitrary",), vmem_limit_bytes=VMEM_LIMIT),
        cost_estimate=pl.CostEstimate(flops=(3 + 3 * (n_pairs - 1)) * 2 * copies * d_model * ff * 4,
                                      bytes_accessed=3 * n_local * ff * d_model * 2, transcendentals=0),
    )(*tables, *slabs, *weights)


def merge_tables_body(st, exps, table, idx_ref, gate_ref, buf, *, src, n_exp, src_rows, out_rows, pad_row):
    layer, e = pl.program_id(0), pl.program_id(1)
    exp = exps[layer * n_exp + e]
    buf[0] = jnp.full(buf.shape[1:], float(pad_row), jnp.float32)
    buf[1] = jnp.zeros(buf.shape[1:], jnp.float32)
    row = lax.broadcasted_iota(jnp.int32, (8, LANES), 0)
    lane = lax.broadcasted_iota(jnp.int32, (8, LANES), 1)
    off = 0
    for d in range(src):
        at = (layer * src + d) * LANES + exp
        first = st[at]
        count = st[at + 1] - first
        to = lax.rem(off, LANES) + LANES
        shift = to - lax.rem(first, LANES)
        over = lax.rem(shift, LANES)
        start = lax.div(off, LANES)
        place = row * LANES + lane
        take = (place >= to) & (place < to + count)
        for kind in range(2):
            x = table[0, kind, pl.ds(d * src_rows + lax.div(first, LANES), 8), :]
            x = pltpu.roll(pltpu.roll(x, over, 1), lax.div(shift, LANES), 0)
            x = jnp.where(lane >= over, x, pltpu.roll(x, 1, 0))
            old = buf[kind, pl.ds(start, 8), :]
            buf[kind, pl.ds(start, 8), :] = jnp.where(take, x, old)
        off = off + count
    idx_ref[0, 0] = buf[0, pl.ds(1, out_rows), :].astype(jnp.int32)
    gate_ref[0, 0] = buf[1, pl.ds(1, out_rows), :]


def merge_tables(shared, starts, exps, out_rows, pad_row):
    n_layers, _, src, rows = shared.shape
    n_exp = exps.shape[1]
    exps = exps.reshape(-1)
    src_rows = rows // LANES
    out = pl.BlockSpec((1, 1, out_rows, LANES), lambda l, e, *_: (l, e, 0, 0))
    return pl.pallas_call(
        functools.partial(merge_tables_body, src=src, n_exp=n_exp, src_rows=src_rows, out_rows=out_rows,
                          pad_row=pad_row),
        grid_spec=pltpu.PrefetchScalarGridSpec(
            num_scalar_prefetch=2,
            grid=(n_layers, n_exp),
            in_specs=[pl.BlockSpec((1, 2, src * src_rows, LANES), lambda l, e, *_: (l, 0, 0, 0))],
            out_specs=[out] * 2,
            scratch_shapes=[pltpu.VMEM((2, out_rows + 16, LANES), jnp.float32)],
        ),
        out_shape=[jax.ShapeDtypeStruct((n_layers, n_exp, out_rows, LANES), jnp.int32),
                   jax.ShapeDtypeStruct((n_layers, n_exp, out_rows, LANES), jnp.float32)],
        compiler_params=pltpu.CompilerParams(dimension_semantics=("arbitrary", "arbitrary")),
        cost_estimate=pl.CostEstimate(flops=10**9, bytes_accessed=4 * shared.size, transcendentals=0),
        name="merge_tables",
    )(starts, exps, shared.reshape(n_layers, 2, src * src_rows, LANES))


def weight_grad_body(exps, tiles, begins, ud_own, ud_oth, idx_all, gate_ref, *refs, parts, n_exp, n_alias, layer, page):
    g_ref, up_ref, w_ref = refs[:3]
    (dg_ref, du_ref, dw_ref, og_ref, ou_ref, ow_ref,
     uds, ut, dt, u0, c0, d0, h0, u1, c1, d1, h1, gacc, wacc, idx_s, sem, tsem) = refs[3 + n_alias:]
    e = pl.program_id(0)
    ff = g_ref.shape[2]
    slots = 3
    both = ((u0, c0, d0, h0), (u1, c1, d1, h1))

    def table_copy(exp):
        slot = lax.rem(exp, slots)
        at = pl.multiple_of((layer * n_exp + exp) * page, PAGE)
        to = pl.multiple_of(slot * page, PAGE)
        return pltpu.make_async_copy(idx_all.at[pl.ds(at, page)], idx_s.at[pl.ds(to, page)], tsem.at[slot])

    def gather_row(at, r):
        x = uds[idx_s[at]].astype(jnp.float32)
        ut[pl.ds(r * parts, parts), :] = x[:parts]
        dt[pl.ds(r * parts, parts), :] = x[parts:]

    @pl.when(e == 0)
    def _():
        copies = fetch_pair(ud_own, ud_oth, uds, sem)
        for c in copies:
            c.start()
        table_copy(0).start()
        table_copy(1).start()
        n_rows = ud_own.shape[0] * 2
        uds[pl.ds(n_rows, 8)] = jnp.zeros((8, 2 * parts, LANES), jnp.bfloat16)
        for ref in (*both[0], *both[1], gacc, wacc):
            clear(ref)
        table_copy(0).wait()
        for c in copies:
            c.wait()

        def first_rows(q, carry):
            for r in range(16):
                gather_row(q * 16 + r, q * 16 + r)
            return carry

        lax.fori_loop(0, WTILE // 16, first_rows, 0)

    @pl.when(e + 1 < n_exp)
    def _():
        table_copy(e + 1).wait()

    @pl.when(e + 2 < n_exp)
    def _():
        table_copy(e + 2).start()

    here = lax.rem(e, slots) * page
    there = lax.rem(jnp.minimum(e + 1, n_exp - 1), slots) * page
    n_tiles = tiles[layer * (n_exp + 1) + e]
    begin = begins[layer * (n_exp + 1) + e]
    gate_rows = WTILE // LANES

    def compute(j, new, old):
        un, cn, dn, hn = new
        uo, co, do, ho = old
        gacc[...] += nn_dot(do[...], uo[...])
        wacc[...] += nn_dot(ho[...], co[...])
        un[...] = load_rows(ut, 0, WTILE, parts)
        gates = [spread_column(gate_ref[0, 0, pl.ds(j * gate_rows + q, 1), :]) for q in range(gate_rows)]
        for k in range(parts):
            for q in range(gate_rows):
                d = dt[pl.ds(q * LANES * parts + k, LANES, stride=parts), :]
                cn[q * LANES:(q + 1) * LANES, k * LANES:(k + 1) * LANES] = (d * gates[q]).astype(jnp.bfloat16)
        ab = nt_dot(jnp.concatenate([g_ref[0, 0], up_ref[0, 0]], axis=0), un[...])
        dh = nt_dot(w_ref[0, 0], cn[...])
        nxt = jnp.where(j + 1 < n_tiles, here + (j + 1) * WTILE, there)
        for r in range(WTILE):
            gather_row(nxt + r, r)
        a, b = ab[:ff], ab[ff:]
        s = jax.nn.sigmoid(a)
        act = a * s
        hn[...] = (act * b).astype(jnp.bfloat16)
        dn[:ff] = (dh * b * (s * (1.0 + a * (1.0 - s)))).astype(jnp.bfloat16)
        dn[ff:] = (dh * act).astype(jnp.bfloat16)

    def tile(j, carry):
        odd = lax.rem(begin + j, 2)

        @pl.when(odd == 0)
        def _():
            compute(j, both[0], both[1])

        @pl.when(odd == 1)
        def _():
            compute(j, both[1], both[0])

        @pl.when(j == 0)
        def _():
            dg = gacc[:ff].astype(jnp.bfloat16)
            du = gacc[ff:].astype(jnp.bfloat16)
            dw = wacc[...].astype(jnp.bfloat16)
            dg_ref[0, 0], du_ref[0, 0], dw_ref[0, 0] = dg, du, dw
            og_ref[0], ou_ref[0], ow_ref[0] = dg, du, dw
            gacc[...] = jnp.zeros_like(gacc)
            wacc[...] = jnp.zeros_like(wacc)

        return carry

    lax.fori_loop(0, n_tiles, tile, 0)


def weight_grads(layer, exps, tiles, ud_alls, idx_all, gates, weights, full):
    n_src, parts2, _ = ud_alls[0].shape
    parts = parts2 // 2
    n_tok = 2 * n_src
    n_layers, n_local, ff, d_model = weights[0].shape
    n_exp = n_local // 2
    out_rows = gates.shape[2]
    page = out_rows * LANES
    tiles = jnp.concatenate([tiles, jnp.ones((n_layers, 1), jnp.int32)], axis=1)
    begins = jnp.cumsum(tiles, axis=1) - tiles
    any_spec = pl.BlockSpec(memory_space=pl.ANY)
    mine = pl.BlockSpec((1, 1, ff, d_model), lambda e, exps, *_: (layer, exps[jnp.minimum(e, n_exp - 1)], 0, 0))
    done = pl.BlockSpec((1, 1, ff, d_model), lambda e, exps, *_: (layer, exps[jnp.maximum(e - 1, 0)], 0, 0))
    half = pl.BlockSpec((1, ff, d_model), lambda e, *_: (jnp.maximum(e - 1, 0), 0, 0))
    gate_spec = pl.BlockSpec((1, 1, out_rows, LANES), lambda e, *_: (layer, jnp.minimum(e, n_exp - 1), 0, 0))
    aliased = list(full) if full is not None else []
    tile_set = [pltpu.VMEM((WTILE, d_model), jnp.bfloat16)] * 2 + [pltpu.VMEM((2 * ff, WTILE), jnp.bfloat16),
                                                                 pltpu.VMEM((ff, WTILE), jnp.bfloat16)]
    outs = pl.pallas_call(
        functools.partial(weight_grad_body, parts=parts, n_exp=n_exp, n_alias=len(aliased), layer=layer, page=page),
        grid_spec=pltpu.PrefetchScalarGridSpec(
            num_scalar_prefetch=3,
            grid=(n_exp + 1,),
            in_specs=[any_spec] * 3 + [gate_spec] + [mine] * 3 + [any_spec] * len(aliased),
            out_specs=[done] * 3 + [half] * 3,
            scratch_shapes=[pltpu.VMEM((n_tok + 8, parts2, LANES), jnp.bfloat16)]
            + [pltpu.VMEM((WTILE * parts, LANES), jnp.float32)] * 2 + tile_set * 2
            + [pltpu.VMEM((2 * ff, d_model), jnp.float32), pltpu.VMEM((ff, d_model), jnp.float32),
               pltpu.SMEM((3 * page,), jnp.int32), pltpu.SemaphoreType.DMA((2,)), pltpu.SemaphoreType.DMA((3,))],
        ),
        out_shape=[jax.ShapeDtypeStruct((n_layers, n_local, ff, d_model), jnp.bfloat16)] * 3
        + [jax.ShapeDtypeStruct((n_exp, ff, d_model), jnp.bfloat16)] * 3,
        input_output_aliases={10 + k: k for k in range(len(aliased))},
        compiler_params=pltpu.CompilerParams(dimension_semantics=("arbitrary",), vmem_limit_bytes=VMEM_LIMIT),
        cost_estimate=pl.CostEstimate(flops=6 * 2 * n_tok * 2 * d_model * ff * 4,
                                      bytes_accessed=n_tok * d_model * 4 + 9 * n_exp * ff * d_model * 2, transcendentals=0),
        name="weight_grads",
    )(exps, tiles.reshape(-1), begins.reshape(-1), *ud_alls, idx_all, gates, *weights, *aliased)
    return outs[:3], outs[3:]


def merge_body(exps, a, b, c, f0, f1, f2, o0, o1, o2):
    o0[0, 0], o1[0, 0], o2[0, 0] = a[0], b[0], c[0]


def merge_half(layer, exps, half, full):
    _, n_local, ff, d_model = full[0].shape
    n_exp = n_local // 2
    any_spec = pl.BlockSpec(memory_space=pl.ANY)
    part = pl.BlockSpec((1, ff, d_model), lambda e, exps: (e, 0, 0))
    place = pl.BlockSpec((1, 1, ff, d_model), lambda e, exps: (layer, exps[e], 0, 0))
    return pl.pallas_call(
        merge_body,
        grid_spec=pltpu.PrefetchScalarGridSpec(
            num_scalar_prefetch=1, grid=(n_exp,), in_specs=[part] * 3 + [any_spec] * 3, out_specs=[place] * 3),
        out_shape=[jax.ShapeDtypeStruct(x.shape, x.dtype) for x in full],
        input_output_aliases={4: 0, 5: 1, 6: 2},
        compiler_params=pltpu.CompilerParams(dimension_semantics=("arbitrary",)),
        cost_estimate=pl.CostEstimate(flops=0, bytes_accessed=6 * n_exp * ff * d_model * 2, transcendentals=0),
        name="merge_half",
    )(exps, *half, *full)


def route_tables(ids, gates, ep, n_local):
    n_src, top_k, tok = ids.shape
    n = n_src * top_k * tok
    local = ids - ep * n_local
    here = (local >= 0) & (local < n_local)
    group = jnp.where(here, local, n_local).reshape(-1)
    key, gate = lax.sort((group * n + jnp.arange(n, dtype=jnp.int32), gates.reshape(-1)), num_keys=1, is_stable=False)
    copy = key % n
    token = copy // (top_k * tok) * tok + copy % tok
    counts = jnp.sum((group[:, None] == jnp.arange(n_local)[None, :]).astype(jnp.int32), axis=0)
    ends = jnp.cumsum(counts)
    starts = ends - counts
    n_tiles = jnp.maximum((counts + TILE - 1) // TILE, 1)
    tile_end = jnp.cumsum(n_tiles)
    tile_id = jnp.arange(n // TILE + n_local + 8, dtype=jnp.int32) - 3
    tile_e = jnp.minimum(jnp.sum((tile_end[None, :] <= tile_id[:, None]).astype(jnp.int32), axis=1), n_local - 1)
    pick = (tile_e[:, None] == jnp.arange(n_local)[None, :]).astype(jnp.int32)
    inside = (tile_id - jnp.sum(pick * (tile_end - n_tiles)[None, :], axis=1)) * TILE
    real = (tile_id >= 0) & (tile_id < tile_end[-1])
    tile_row = jnp.where(real, jnp.sum(pick * starts[None, :], axis=1) + inside, 0)
    tile_first = (real & (inside == 0) & (tile_e > 0)).astype(jnp.int32)
    tile_n = jnp.where(real, jnp.clip(jnp.sum(pick * counts[None, :], axis=1) - inside, 0, TILE), 0)
    pad = cdiv(2 * PAGE, TILE) * TILE
    token = jnp.pad(token, (0, pad))
    gate = jnp.pad(gate, (0, pad))
    bounds = jnp.concatenate([jnp.zeros((1,), jnp.int32), ends, jnp.full((LANES - 1 - n_local,), ends[-1], jnp.int32)])
    return (tile_e, tile_first, tile_row, tile_n, tile_end[-1:], token, gate), bounds


def split_experts(bounds, core):
    n_local = bounds.shape[1] - 1
    load = jnp.sum(bounds[:, 1:] - bounds[:, :-1], axis=0)
    ids = jnp.arange(n_local, dtype=jnp.int32)
    ahead = (load[None, :] > load[:, None]) | ((load[None, :] == load[:, None]) & (ids[None, :] < ids[:, None]))
    rank = jnp.sum(ahead.astype(jnp.int32), axis=1)
    turn = jnp.arange(n_local // 2, dtype=jnp.int32)

    def dealt(which):
        want = 2 * turn + (which + turn) % 2
        return (rank[None, :] == want[:, None]).astype(jnp.int32)

    mine, theirs = dealt(core), dealt(1 - core)
    tiles = jnp.maximum((jnp.sum(mine * load[None, :], axis=1) + WTILE - 1) // WTILE, 1)
    return jnp.sum(mine * ids[None, :], axis=1), jnp.sum(theirs * ids[None, :], axis=1), tiles


def after(x, *earlier):
    return lax.optimization_barrier((x, *earlier))[0]


def solution(mesh):
    ep_size = mesh.shape['ep']
    dp_size = mesh.shape['dp']
    tok_spec = P(('dp', 'ep'), None)
    route_spec = P(None, ('dp', 'ep'), None)
    whole_spec = P(None, None, None)
    expert_spec = P(None, 'ep', None, None)
    ep_pairs = [(i, 1 - i) for i in range(ep_size)]
    core_pairs = [(i, i ^ 1) for i in range(dp_size)]

    def device_body(tokens, d_out, expert_ids, gate_vals, w_mix, w_gate, w_up, w_down):
        n_layers = w_mix.shape[0]
        n_local = w_gate.shape[1]
        n_experts = n_local * ep_size
        tok, d_model = tokens.shape
        top_k = expert_ids.shape[2]
        parts = d_model // LANES
        cap = cdiv(CAP_FACTOR * tok * top_k, n_experts)
        ep_id = lax.axis_index('ep').astype(jnp.int32)
        dp_id = lax.axis_index('dp').astype(jnp.int32)
        weights = (jnp.swapaxes(w_gate, 2, 3), jnp.swapaxes(w_up, 2, 3), w_down)

        def swap(x):
            return lax.ppermute(x, 'ep', ep_pairs)

        def spread(x):
            return lax.all_gather(x, 'dp', axis=0, tiled=True)

        def slab(x):
            return x.reshape(tok, parts, LANES)

        def mixed(x, layer):
            return (x.astype(jnp.float32) + jnp.dot(x, w_mix[layer], preferred_element_type=jnp.float32)).astype(jnp.bfloat16)

        ids = jnp.swapaxes(expert_ids, 1, 2)
        gates = jnp.swapaxes(gate_vals, 1, 2)
        mine = jnp.stack([ids.astype(jnp.float32), gates])
        theirs = swap(mine)
        both = jnp.stack([mine, theirs], 2)
        tables, packed = [], []

        def add_tables(pair):
            table, bounds = route_tables(pair[0].astype(jnp.int32), pair[1], ep_id, n_local)
            token, gate = table[5], table[6]
            tables.append((*table[:5], token * parts, gate.reshape(-1, LANES)))
            spot = lax.div(token, tok) * (dp_size * tok) + dp_id * tok + lax.rem(token, tok)
            packed.append(jnp.stack([jnp.concatenate([spot, jnp.pad(bounds, (0, PAGE - LANES))])
                                     .astype(jnp.float32), jnp.pad(gate, (0, PAGE))]))

        add_tables(both[:, 0])

        d_slab = slab(d_out)
        d_other = swap(d_slab)

        top = n_layers - 1
        x_in, u_slabs, u_others, xs = tokens, [], [], []
        for layer in range(n_layers):
            u = mixed(x_in, layer)
            u_slabs.append(slab(u))
            u_others.append(swap(u_slabs[layer]))
            xs.append(x_in)
            if layer < top:
                own, other = token_kernel(forward_body, layer, tables[layer],
                                          (u_slabs[layer], u_others[layer]), weights)
                sent = swap(other)
                add_tables(after(both[:, layer + 1], other))
                x_in = (u.astype(jnp.float32) + own + sent).astype(jnp.bfloat16)

        rows = packed[0].shape[1]
        shared = lax.all_gather(jnp.stack(packed), 'dp', axis=2)
        shared = shared.reshape(n_layers, 2, dp_size, rows)
        starts = shared[:, 0, :, rows - PAGE:rows - PAGE + LANES].astype(jnp.int32)
        split = [split_experts(starts[layer, :, :n_local + 1], dp_id % 2) for layer in range(n_layers)]
        mine_e, theirs_e, tiles = (jnp.stack(x) for x in zip(*split))
        list_rows = cdiv(cdiv(dp_size * 2 * cap, LANES), 8) * 8 + 8
        idx_all, gate_all = merge_tables(shared, starts.reshape(-1), mine_e, list_rows, dp_size * 2 * tok)
        idx_all = idx_all.reshape(-1)

        d_y, full = d_out, None
        d_mix = [None] * n_layers
        for layer in reversed(range(n_layers)):
            spreads = [spread(jnp.concatenate(x, axis=1)) for x in ((u_slabs[layer], d_slab), (u_others[layer], d_other))]
            own, other = token_kernel(backward_body, layer, tables[layer],
                                      (u_slabs[layer], u_others[layer], d_slab, d_other), weights)
            d_u = (d_y.astype(jnp.float32) + own + swap(other)).astype(jnp.bfloat16)
            last = other
            if layer == top:
                y_own, y_other = token_kernel(forward_body, top, tables[top],
                                              (after(u_slabs[top], other), u_others[top]), weights)
                layer_out = (u.astype(jnp.float32) + y_own + swap(y_other)).astype(jnp.bfloat16)
                last = y_other
            full, half = weight_grads(layer, mine_e[layer], after(tiles, last), spreads, idx_all, gate_all, weights, full)
            full = merge_half(layer, theirs_e[layer], [lax.ppermute(x, 'dp', core_pairs) for x in half], full)
            d_mix[layer] = jnp.einsum('td,te->de', xs[layer], d_u, preferred_element_type=jnp.float32).astype(jnp.bfloat16)
            d_y = (d_u.astype(jnp.float32)
                   + jnp.einsum('te,de->td', d_u, w_mix[layer], preferred_element_type=jnp.float32)).astype(jnp.bfloat16)
            if layer:
                d_slab = slab(d_y)
                d_other = swap(d_slab)
        d_mix = lax.psum(jnp.stack(d_mix), ('dp', 'ep'))
        return (layer_out, d_y, d_mix, jnp.swapaxes(full[0], 2, 3), jnp.swapaxes(full[1], 2, 3), full[2])

    return jax.shard_map(device_body, mesh=mesh,
                         in_specs=(tok_spec, tok_spec, route_spec, route_spec, whole_spec,
                                   expert_spec, expert_spec, expert_spec),
                         out_specs=(tok_spec, tok_spec, whole_spec, expert_spec, expert_spec, expert_spec),
                         check_vma=False)
```

```python
import functools

import jax
import jax.numpy as jnp
from jax import lax
from jax.experimental import pallas as pl
from jax.experimental.pallas import tpu as pltpu
from jax.sharding import PartitionSpec as P


CAP_FACTOR = 3
LANES = 128
TILE = 128
WTILE = 256
PITCH = 9
BATCH = 16
SLOTS = 6
PAGE = 1024
VMEM_LIMIT = 62 * 2**20


def cdiv(a, b):
    return (a + b - 1) // b


def nt_dot(a, b):
    return lax.dot_general(a, b, (((1,), (1,)), ((), ())), preferred_element_type=jnp.float32)


def tn_dot(a, b):
    return lax.dot_general(a, b, (((0,), (0,)), ((), ())), preferred_element_type=jnp.float32)


def nn_dot(a, b):
    return lax.dot_general(a, b, (((1,), (0,)), ((), ())), preferred_element_type=jnp.float32)


def clear(ref):
    step = min(64, ref.shape[0])

    def one(q, carry):
        ref[pl.ds(pl.multiple_of(q * step, step), step), :] = jnp.zeros((step, ref.shape[1]), ref.dtype)
        return carry

    lax.fori_loop(0, ref.shape[0] // step, one, 0)


def load_rows(ref, start, rows, parts):
    cols = [ref[pl.ds(start * parts + k, rows, stride=parts), :] for k in range(parts)]
    return jnp.concatenate(cols, axis=1).astype(jnp.bfloat16)


def fetch_rows(sources, halves, dst, sem):
    n = sources[0].shape[0]
    return [pltpu.make_async_copy(sources[k], dst.at[pl.ds(k * n, n)], sem.at[k]) for k in halves]


def fetch_pair(own, other, dst, sem):
    n = own.shape[0]
    return (pltpu.make_async_copy(own, dst.at[pl.ds(0, n)], sem.at[0]),
            pltpu.make_async_copy(other, dst.at[pl.ds(n, n)], sem.at[1]))


def add_rows(acc, vals_ref, idx, row, parts):
    for b in range(0, TILE, BATCH):
        at = [pl.multiple_of(idx[row + b + r], parts) for r in range(BATCH)]
        vals = [acc[pl.ds(at[r], parts), :] + vals_ref[pl.ds((b + r) * parts, parts), :] for r in range(BATCH)]
        for r in reversed(range(BATCH)):
            acc[pl.ds(at[r], parts), :] = vals[r]


def spread_column(row):
    return jnp.broadcast_to(row, (LANES, LANES)).T


def tile_gates(gates, row):
    pair = gates[pl.ds(lax.div(row, LANES), 2), :]
    skip = lax.rem(row, LANES)
    pair = pltpu.roll(pair, lax.rem(LANES - skip, LANES), 1)
    lane = lax.broadcasted_iota(jnp.int32, (1, LANES), 1)
    return spread_column(jnp.where(lane < LANES - skip, pair[:1], pair[1:]))


def widen(src, dst, parts, halves, tok):
    step = 8

    def one(q, carry):
        for r in range(step):
            dst[pl.ds((q * step + r) * parts, parts), :] = src[q * step + r].astype(jnp.float32)
        return carry

    lax.fori_loop(halves[0] * tok // step, (halves[-1] + 1) * tok // step, one, 0)


def write_sums(acc, outs, tok, parts, halves):
    step = min(32, tok)

    def copy_out(q, carry):
        r0 = pl.multiple_of(q * step, step)
        for k in range(parts):
            cols = slice(k * LANES, (k + 1) * LANES)
            for out, half in zip(outs, halves):
                out[pl.ds(r0, step), cols] = acc[pl.ds((half * tok + r0) * parts + k, step, stride=parts), :]
        return carry

    lax.fori_loop(0, tok // step, copy_out, 0)


def expert_copies(weights, buf, sem, layer, e):
    slot = lax.rem(e, SLOTS)
    ff = weights[0].shape[2]
    return [pltpu.make_async_copy(w.at[layer, e], buf.at[slot, pl.ds(k * ff, ff)], sem.at[slot])
            for k, w in enumerate(weights)]


def run_tiles(step, weights, wbuf, wsem, tile_e, tile_first, n_steps, layer, prepare):
    n_local = weights[0].shape[1]
    for e in range(min(SLOTS - 1, n_local)):
        for c in expert_copies(weights, wbuf, wsem, layer, e):
            c.start()
    prepare()
    for c in expert_copies(weights, wbuf, wsem, layer, 0):
        c.wait()

    def one(i, carry):
        e = tile_e[i + 2]

        @pl.when(tile_first[i + 2] == 1)
        def _():
            for c in expert_copies(weights, wbuf, wsem, layer, e):
                c.wait()

        @pl.when((tile_first[i + 2] == 1) & (e + SLOTS - 2 < n_local))
        def _():
            for c in expert_copies(weights, wbuf, wsem, layer, e + SLOTS - 2):
                c.start()

        step(i, lax.rem(e, SLOTS), lax.rem(tile_e[i + 1], SLOTS))
        return carry

    lax.fori_loop(0, n_steps, one, 0)


def forward_body(te, tf, tr, tn, nt, idx, gates, u_own, u_oth, g_ref, up_ref, w_ref, *refs, layer, tok, parts, halves):
    ff = g_ref.shape[2]
    outs, (usc, uf, ut, ot, acc, ht, wbuf, sem, wsem) = refs[:len(halves)], refs[len(halves):]

    def prepare():
        copies = fetch_rows((u_own, u_oth), halves, usc, sem)
        for c in copies:
            c.start()
        for ref in (acc, ot, ut, ht):
            clear(ref)
        for c in copies:
            c.wait()
        widen(usc, uf, parts, halves, tok)

    def step(i, slot, slot_before):
        o = tn_dot(ht[...], wbuf[slot_before, 2 * ff:]).astype(jnp.bfloat16).astype(jnp.float32)
        u = load_rows(ut, 0, TILE, parts)
        ab = nt_dot(wbuf[slot, :2 * ff], u)
        add_rows(acc, ot, idx, tr[i], parts)
        row = tr[i + 3]
        for r in range(TILE):
            ut[pl.ds(parts * r, parts), :] = uf[pl.ds(pl.multiple_of(idx[row + r], parts), parts), :]
        live = lax.broadcasted_iota(jnp.int32, (TILE, LANES), 0) < tn[i + 1]
        gate = tile_gates(gates, tr[i + 1])
        for k in range(parts):
            o_k = jnp.where(live, o[:, k * LANES:(k + 1) * LANES] * gate, 0.0)
            ot[pl.ds(k, TILE, stride=parts), :] = o_k
        a, b = ab[:ff], ab[ff:]
        ht[...] = (a * jax.nn.sigmoid(a) * b).astype(jnp.bfloat16)

    run_tiles(step, (g_ref, up_ref, w_ref), wbuf, wsem, te, tf, nt[0] + 3, layer, prepare)
    write_sums(acc, outs, tok, parts, halves)


def backward_body(te, tf, tr, tn, nt, idx, gates, u_own, u_oth, d_own, d_oth, g_ref, up_ref, w_ref, *refs, layer, tok, parts,
                  halves):
    ff = g_ref.shape[2]
    outs, (usc, dsc, uf, df, ut, dt, vt, acc, da_t, wbuf, sem, wsem) = refs[:len(halves)], refs[len(halves):]

    def prepare():
        copies = fetch_rows((u_own, u_oth), halves, usc, sem.at[0]) + fetch_rows((d_own, d_oth), halves, dsc, sem.at[1])
        for c in copies:
            c.start()
        for ref in (acc, vt, ut, dt, da_t):
            clear(ref)
        for c in copies:
            c.wait()
        widen(usc, uf, parts, halves, tok)
        widen(dsc, df, parts, halves, tok)

    def step(i, slot, slot_before):
        v = tn_dot(da_t[...], wbuf[slot_before, :2 * ff]).astype(jnp.bfloat16).astype(jnp.float32)
        u = load_rows(ut, 0, TILE, parts)
        gate = tile_gates(gates, tr[i + 2])
        c = jnp.concatenate([(dt[pl.ds(k, TILE, stride=parts), :] * gate).astype(jnp.bfloat16) for k in range(parts)], axis=1)
        ab = nt_dot(wbuf[slot, :2 * ff], u)
        dh = nt_dot(wbuf[slot, 2 * ff:], c)
        add_rows(acc, vt, idx, tr[i], parts)
        row = tr[i + 3]
        for r in range(TILE):
            at = pl.multiple_of(idx[row + r], parts)
            ut[pl.ds(parts * r, parts), :] = uf[pl.ds(at, parts), :]
            dt[pl.ds(parts * r, parts), :] = df[pl.ds(at, parts), :]
        live = lax.broadcasted_iota(jnp.int32, (TILE, LANES), 0) < tn[i + 1]
        gate = tile_gates(gates, tr[i + 1])
        for k in range(parts):
            v_k = jnp.where(live, v[:, k * LANES:(k + 1) * LANES] * gate, 0.0)
            vt[pl.ds(k, TILE, stride=parts), :] = v_k
        a, b = ab[:ff], ab[ff:]
        s = jax.nn.sigmoid(a)
        da_t[:ff] = (dh * b * (s * (1.0 + a * (1.0 - s)))).astype(jnp.bfloat16)
        da_t[ff:] = (dh * (a * s)).astype(jnp.bfloat16)

    run_tiles(step, (g_ref, up_ref, w_ref), wbuf, wsem, te, tf, nt[0] + 3, layer, prepare)
    write_sums(acc, outs, tok, parts, halves)


def token_kernel(body, layer, tables, slabs, weights, halves=(0, 1)):
    tok, parts, _ = slabs[0].shape
    _, n_local, ff, d_model = weights[0].shape
    n_pairs = len(slabs) // 2
    rows_spec = pl.BlockSpec((tok, d_model), lambda i, *_: (0, 0))
    any_spec = pl.BlockSpec(memory_space=pl.ANY)
    sem_shape = (2,) if n_pairs == 1 else (2, 2)
    copies = 8 * tok
    return pl.pallas_call(
        functools.partial(body, layer=layer, tok=tok, parts=parts, halves=halves),
        grid_spec=pltpu.PrefetchScalarGridSpec(
            num_scalar_prefetch=len(tables) - 1,
            grid=(1,),
            in_specs=[pl.BlockSpec(tables[-1].shape, lambda i, *_: (0, 0))] + [any_spec] * (len(slabs) + 3),
            out_specs=[rows_spec] * len(halves),
            scratch_shapes=[pltpu.VMEM((2 * tok, parts, LANES), jnp.bfloat16)] * n_pairs
            + [pltpu.VMEM((2 * tok * parts, LANES), jnp.float32)] * n_pairs
            + [pltpu.VMEM((TILE * parts, LANES), jnp.float32)] * (n_pairs + 1)
            + [pltpu.VMEM((2 * tok * parts, LANES), jnp.float32), pltpu.VMEM((n_pairs * ff, TILE), jnp.bfloat16),
               pltpu.VMEM((SLOTS, 3 * ff, d_model), jnp.bfloat16),
               pltpu.SemaphoreType.DMA(sem_shape), pltpu.SemaphoreType.DMA((SLOTS,))],
        ),
        out_shape=[jax.ShapeDtypeStruct((tok, d_model), jnp.float32)] * len(halves),
        compiler_params=pltpu.CompilerParams(dimension_semantics=("arbitrary",), vmem_limit_bytes=VMEM_LIMIT),
        cost_estimate=pl.CostEstimate(flops=(3 + 3 * (n_pairs - 1)) * 2 * copies * d_model * ff * 4,
                                      bytes_accessed=3 * n_local * ff * d_model * 2, transcendentals=0),
    )(*tables, *slabs, *weights)


def merge_tables_body(st, exps, table, idx_ref, gate_ref, buf, *, src, n_exp, n_layers, out_rows, pad_row):
    group = idx_ref.shape[1]
    layer = pl.program_id(0)

    def one(q, carry):
        merge_expert(exps[layer * n_exp + pl.program_id(1) * group + q], layer, st, table, idx_ref.at[0, q], gate_ref.at[0, q],
                     buf, src, n_layers, out_rows, pad_row)
        return carry

    lax.fori_loop(0, group, one, 0)


def merge_expert(exp, layer, st, table, idx_out, gate_out, buf, src, n_layers, out_rows, pad_row):
    buf[0] = jnp.full(buf.shape[1:], float(pad_row), jnp.float32)
    buf[1] = jnp.zeros(buf.shape[1:], jnp.float32)
    row = lax.broadcasted_iota(jnp.int32, (8, LANES), 0)
    lane = lax.broadcasted_iota(jnp.int32, (8, LANES), 1)
    off = 0
    for d in range(src):
        at = (d * n_layers + layer) * LANES + exp
        first = st[at]
        count = st[at + 1] - first
        to = lax.rem(off, LANES) + LANES
        shift = to - lax.rem(first, LANES)
        over = lax.rem(shift, LANES)
        start = lax.div(off, LANES)
        place = row * LANES + lane
        take = (place >= to) & (place < to + count)
        for kind in range(2):
            x = table[d, 0, kind, pl.ds(lax.div(first, LANES), 8), :]
            x = pltpu.roll(pltpu.roll(x, over, 1), lax.div(shift, LANES), 0)
            x = jnp.where(lane >= over, x, pltpu.roll(x, 1, 0))
            old = buf[kind, pl.ds(start, 8), :]
            buf[kind, pl.ds(start, 8), :] = jnp.where(take, x, old)
        off = off + count
    idx_out[...] = buf[0, pl.ds(1, out_rows), :].astype(jnp.int32)
    gate_out[...] = buf[1, pl.ds(1, out_rows), :]


def merge_tables(shared, starts, exps, out_rows, pad_row):
    src, n_layers, _, rows, _ = shared.shape
    n_exp = exps.shape[1]
    group = 8 if n_exp % 8 == 0 else 1
    out = pl.BlockSpec((1, group, out_rows, LANES), lambda l, e, *_: (l, e, 0, 0))
    return pl.pallas_call(
        functools.partial(merge_tables_body, src=src, n_exp=n_exp, n_layers=n_layers, out_rows=out_rows,
                          pad_row=pad_row),
        grid_spec=pltpu.PrefetchScalarGridSpec(
            num_scalar_prefetch=2,
            grid=(n_layers, n_exp // group),
            in_specs=[pl.BlockSpec((src, 1, 2, rows, LANES), lambda l, e, *_: (0, l, 0, 0, 0))],
            out_specs=[out] * 2,
            scratch_shapes=[pltpu.VMEM((2, out_rows + 16, LANES), jnp.float32)],
        ),
        out_shape=[jax.ShapeDtypeStruct((n_layers, n_exp, out_rows, LANES), jnp.int32),
                   jax.ShapeDtypeStruct((n_layers, n_exp, out_rows, LANES), jnp.float32)],
        compiler_params=pltpu.CompilerParams(dimension_semantics=("arbitrary", "arbitrary")),
        cost_estimate=pl.CostEstimate(flops=10**9, bytes_accessed=4 * shared.size, transcendentals=0),
        name="merge_tables",
    )(starts.reshape(-1), exps.reshape(-1), shared)


def weight_grad_body(exps, tiles, begins, ud_own, ud_oth, idx_all, gate_ref, *refs, parts, n_exp, n_alias, layer, page):
    g_ref, up_ref, w_ref = refs[:3]
    (dg_ref, du_ref, dw_ref, og_ref, ou_ref, ow_ref,
     uds, rows, u0, c0, d0, h0, u1, c1, d1, h1, gacc, wacc, idx_s, sem, tsem) = refs[3 + n_alias:]
    e = pl.program_id(0)
    ff = g_ref.shape[2]
    slots = 3
    both = ((u0, c0, d0, h0), (u1, c1, d1, h1))

    def table_copy(exp):
        slot = lax.rem(exp, slots)
        at = pl.multiple_of((layer * n_exp + exp) * page, PAGE)
        to = pl.multiple_of(slot * page, PAGE)
        return pltpu.make_async_copy(idx_all.at[pl.ds(at, page)], idx_s.at[pl.ds(to, page)], tsem.at[slot])

    def gather_row(at, r):
        rows[pl.ds(r * PITCH, 2 * parts), :] = uds[idx_s[at]].astype(jnp.float32)

    def column(first, count, k):
        return rows[pl.ds(first * PITCH + k, count, stride=PITCH), :]

    @pl.when(e == 0)
    def _():
        copies = fetch_pair(ud_own, ud_oth, uds, sem)
        for c in copies:
            c.start()
        table_copy(0).start()
        table_copy(1).start()
        n_rows = ud_own.shape[0] * 2
        uds[pl.ds(n_rows, 8)] = jnp.zeros((8, 2 * parts, LANES), jnp.bfloat16)
        for ref in (*both[0], *both[1], gacc, wacc):
            clear(ref)
        table_copy(0).wait()
        for c in copies:
            c.wait()

        def first_rows(q, carry):
            for r in range(16):
                gather_row(q * 16 + r, q * 16 + r)
            return carry

        lax.fori_loop(0, WTILE // 16, first_rows, 0)

    @pl.when(e + 1 < n_exp)
    def _():
        table_copy(e + 1).wait()

    @pl.when(e + 2 < n_exp)
    def _():
        table_copy(e + 2).start()

    here = lax.rem(e, slots) * page
    there = lax.rem(jnp.minimum(e + 1, n_exp - 1), slots) * page
    n_tiles = tiles[layer * (n_exp + 1) + e]
    begin = begins[layer * (n_exp + 1) + e]
    gate_rows = WTILE // LANES

    def compute(j, new, old):
        un, cn, dn, hn = new
        uo, co, do, ho = old
        gacc[...] += nn_dot(do[...], uo[...])
        wacc[...] += nn_dot(ho[...], co[...])
        un[...] = jnp.concatenate([column(0, WTILE, k) for k in range(parts)], axis=1).astype(jnp.bfloat16)
        gates = [spread_column(gate_ref[0, 0, pl.ds(j * gate_rows + q, 1), :]) for q in range(gate_rows)]
        for k in range(parts):
            for q in range(gate_rows):
                d = column(q * LANES, LANES, parts + k)
                cn[q * LANES:(q + 1) * LANES, k * LANES:(k + 1) * LANES] = (d * gates[q]).astype(jnp.bfloat16)
        ab = nt_dot(jnp.concatenate([g_ref[0, 0], up_ref[0, 0]], axis=0), un[...])
        dh = nt_dot(w_ref[0, 0], cn[...])
        nxt = jnp.where(j + 1 < n_tiles, here + (j + 1) * WTILE, there)
        for r in range(WTILE):
            gather_row(nxt + r, r)
        a, b = ab[:ff], ab[ff:]
        s = jax.nn.sigmoid(a)
        act = a * s
        hn[...] = (act * b).astype(jnp.bfloat16)
        dn[:ff] = (dh * b * (s * (1.0 + a * (1.0 - s)))).astype(jnp.bfloat16)
        dn[ff:] = (dh * act).astype(jnp.bfloat16)

    def tile(j, carry):
        odd = lax.rem(begin + j, 2)

        @pl.when(odd == 0)
        def _():
            compute(j, both[0], both[1])

        @pl.when(odd == 1)
        def _():
            compute(j, both[1], both[0])

        @pl.when(j == 0)
        def _():
            dg = gacc[:ff].astype(jnp.bfloat16)
            du = gacc[ff:].astype(jnp.bfloat16)
            dw = wacc[...].astype(jnp.bfloat16)
            dg_ref[0, 0], du_ref[0, 0], dw_ref[0, 0] = dg, du, dw
            og_ref[0], ou_ref[0], ow_ref[0] = dg, du, dw
            gacc[...] = jnp.zeros_like(gacc)
            wacc[...] = jnp.zeros_like(wacc)

        return carry

    lax.fori_loop(0, n_tiles, tile, 0)


def weight_grads(layer, exps, tiles, ud_alls, idx_all, gates, weights, full):
    n_src, parts2, _ = ud_alls[0].shape
    parts = parts2 // 2
    n_tok = 2 * n_src
    n_layers, n_local, ff, d_model = weights[0].shape
    n_exp = n_local // 2
    out_rows = gates.shape[2]
    page = out_rows * LANES
    tiles = jnp.concatenate([tiles, jnp.ones((n_layers, 1), jnp.int32)], axis=1)
    begins = jnp.cumsum(tiles, axis=1) - tiles
    any_spec = pl.BlockSpec(memory_space=pl.ANY)
    mine = pl.BlockSpec((1, 1, ff, d_model), lambda e, exps, *_: (layer, exps[jnp.minimum(e, n_exp - 1)], 0, 0))
    done = pl.BlockSpec((1, 1, ff, d_model), lambda e, exps, *_: (layer, exps[jnp.maximum(e - 1, 0)], 0, 0))
    half = pl.BlockSpec((1, ff, d_model), lambda e, *_: (jnp.maximum(e - 1, 0), 0, 0))
    gate_spec = pl.BlockSpec((1, 1, out_rows, LANES), lambda e, *_: (layer, jnp.minimum(e, n_exp - 1), 0, 0))
    aliased = list(full) if full is not None else []
    tile_set = [pltpu.VMEM((WTILE, d_model), jnp.bfloat16)] * 2 + [pltpu.VMEM((2 * ff, WTILE), jnp.bfloat16),
                                                                 pltpu.VMEM((ff, WTILE), jnp.bfloat16)]
    outs = pl.pallas_call(
        functools.partial(weight_grad_body, parts=parts, n_exp=n_exp, n_alias=len(aliased), layer=layer, page=page),
        grid_spec=pltpu.PrefetchScalarGridSpec(
            num_scalar_prefetch=3,
            grid=(n_exp + 1,),
            in_specs=[any_spec] * 3 + [gate_spec] + [mine] * 3 + [any_spec] * len(aliased),
            out_specs=[done] * 3 + [half] * 3,
            scratch_shapes=[pltpu.VMEM((n_tok + 8, parts2, LANES), jnp.bfloat16)]
            + [pltpu.VMEM((WTILE * PITCH + 16, LANES), jnp.float32)] + tile_set * 2
            + [pltpu.VMEM((2 * ff, d_model), jnp.float32), pltpu.VMEM((ff, d_model), jnp.float32),
               pltpu.SMEM((3 * page,), jnp.int32), pltpu.SemaphoreType.DMA((2,)), pltpu.SemaphoreType.DMA((3,))],
        ),
        out_shape=[jax.ShapeDtypeStruct((n_layers, n_local, ff, d_model), jnp.bfloat16)] * 3
        + [jax.ShapeDtypeStruct((n_exp, ff, d_model), jnp.bfloat16)] * 3,
        input_output_aliases={10 + k: k for k in range(len(aliased))},
        compiler_params=pltpu.CompilerParams(dimension_semantics=("arbitrary",), vmem_limit_bytes=VMEM_LIMIT),
        cost_estimate=pl.CostEstimate(flops=6 * 2 * n_tok * 2 * d_model * ff * 4,
                                      bytes_accessed=n_tok * d_model * 4 + 9 * n_exp * ff * d_model * 2, transcendentals=0),
        name="weight_grads",
    )(exps, tiles.reshape(-1), begins.reshape(-1), *ud_alls, idx_all, gates, *weights, *aliased)
    return outs[:3], outs[3:]


def merge_body(exps, a, b, c, f0, f1, f2, o0, o1, o2, buf, in_sem, out_sem, *, layer, n_exp):
    halves, wholes = (a, b, c), (o0, o1, o2)

    def arrive(k, q):
        return pltpu.make_async_copy(halves[k].at[q], buf.at[k, q], in_sem.at[k, q])

    def leave(k, q):
        return pltpu.make_async_copy(buf.at[k, q], wholes[k].at[layer, exps[q]], out_sem)

    def each(act):
        def one(q, carry):
            for k in range(3):
                act(k, q)
            return carry

        lax.fori_loop(0, n_exp, one, 0)

    def pass_on(k, q):
        arrive(k, q).wait()
        leave(k, q).start()

    each(lambda k, q: arrive(k, q).start())
    each(pass_on)
    each(lambda k, q: leave(k, q).wait())


def merge_half(layer, exps, half, full):
    n_exp, ff, d_model = half[0].shape
    any_spec = pl.BlockSpec(memory_space=pl.ANY)
    return pl.pallas_call(
        functools.partial(merge_body, layer=layer, n_exp=n_exp),
        grid_spec=pltpu.PrefetchScalarGridSpec(
            num_scalar_prefetch=1, grid=(1,), in_specs=[any_spec] * 6, out_specs=[any_spec] * 3,
            scratch_shapes=[pltpu.VMEM((3, n_exp, ff, d_model), jnp.bfloat16), pltpu.SemaphoreType.DMA((3, n_exp)),
                            pltpu.SemaphoreType.DMA]),
        out_shape=[jax.ShapeDtypeStruct(x.shape, x.dtype) for x in full],
        input_output_aliases={4: 0, 5: 1, 6: 2},
        compiler_params=pltpu.CompilerParams(dimension_semantics=("arbitrary",), vmem_limit_bytes=VMEM_LIMIT),
        cost_estimate=pl.CostEstimate(flops=10**9, bytes_accessed=6 * n_exp * ff * d_model * 2, transcendentals=0),
        name="merge_half",
    )(exps, *half, *full)


def route_tables(ids, gates, ep, n_local, split):
    n_src, top_k, tok = ids.shape
    n = n_src * top_k * tok
    local = ids - ep * n_local
    here = (local >= 0) & (local < n_local)
    group = jnp.where(here, local, n_local).reshape(-1)
    key, gate = lax.sort((group * n + jnp.arange(n, dtype=jnp.int32), gates.reshape(-1)), num_keys=1, is_stable=False)
    copy = key % n
    token = copy // (top_k * tok) * tok + copy % tok
    hits = (group.reshape(n_src, -1)[:, :, None] == jnp.arange(n_local)[None, None, :]).astype(jnp.int32)
    half_counts = jnp.sum(hits, axis=1)
    counts = jnp.sum(half_counts, axis=0)
    ends = jnp.cumsum(counts)
    starts = ends - counts
    pad = cdiv(2 * PAGE, TILE) * TILE
    token = jnp.pad(token, (0, pad))
    gate = jnp.pad(gate, (0, pad))
    bounds = jnp.concatenate([jnp.zeros((1,), jnp.int32), ends, jnp.full((LANES - 1 - n_local,), ends[-1], jnp.int32)])
    whole = tile_list(starts, counts, n)
    lists = (whole,)
    if split:
        lists = (tile_list(starts, half_counts[0], n // 2), tile_list(starts + half_counts[0], half_counts[1], n // 2))
    return lists, whole, token, gate, bounds


def tile_list(starts, counts, most):
    n_local = starts.shape[0]
    n_tiles = jnp.maximum((counts + TILE - 1) // TILE, 1)
    tile_end = jnp.cumsum(n_tiles)
    tile_id = jnp.arange(most // TILE + n_local + 8, dtype=jnp.int32) - 3
    tile_e = jnp.minimum(jnp.sum((tile_end[None, :] <= tile_id[:, None]).astype(jnp.int32), axis=1), n_local - 1)
    pick = (tile_e[:, None] == jnp.arange(n_local)[None, :]).astype(jnp.int32)
    inside = (tile_id - jnp.sum(pick * (tile_end - n_tiles)[None, :], axis=1)) * TILE
    real = (tile_id >= 0) & (tile_id < tile_end[-1])
    tile_row = jnp.where(real, jnp.sum(pick * starts[None, :], axis=1) + inside, 0)
    tile_first = (real & (inside == 0) & (tile_e > 0)).astype(jnp.int32)
    tile_n = jnp.where(real, jnp.clip(jnp.sum(pick * counts[None, :], axis=1) - inside, 0, TILE), 0)
    return tile_e, tile_first, tile_row, tile_n, tile_end[-1:]


def split_experts(bounds, core):
    n_local = bounds.shape[1] - 1
    load = jnp.sum(bounds[:, 1:] - bounds[:, :-1], axis=0)
    ids = jnp.arange(n_local, dtype=jnp.int32)
    ahead = (load[None, :] > load[:, None]) | ((load[None, :] == load[:, None]) & (ids[None, :] < ids[:, None]))
    rank = jnp.sum(ahead.astype(jnp.int32), axis=1)
    turn = jnp.arange(n_local // 2, dtype=jnp.int32)

    def dealt(which):
        want = 2 * turn + (which + turn) % 2
        return (rank[None, :] == want[:, None]).astype(jnp.int32)

    mine, theirs = dealt(core), dealt(1 - core)
    tiles = jnp.maximum((jnp.sum(mine * load[None, :], axis=1) + WTILE - 1) // WTILE, 1)
    return jnp.sum(mine * ids[None, :], axis=1), jnp.sum(theirs * ids[None, :], axis=1), tiles


def after(x, *earlier):
    return lax.optimization_barrier((x, *earlier))[0]


def solution(mesh):
    ep_size = mesh.shape['ep']
    dp_size = mesh.shape['dp']
    tok_spec = P(('dp', 'ep'), None)
    route_spec = P(None, ('dp', 'ep'), None)
    whole_spec = P(None, None, None)
    expert_spec = P(None, 'ep', None, None)
    ep_pairs = [(i, 1 - i) for i in range(ep_size)]
    core_pairs = [(i, i ^ 1) for i in range(dp_size)]

    def device_body(tokens, d_out, expert_ids, gate_vals, w_mix, w_gate, w_up, w_down):
        n_layers = w_mix.shape[0]
        n_local = w_gate.shape[1]
        n_experts = n_local * ep_size
        tok, d_model = tokens.shape
        top_k = expert_ids.shape[2]
        parts = d_model // LANES
        cap = cdiv(CAP_FACTOR * tok * top_k, n_experts)
        ep_id = lax.axis_index('ep').astype(jnp.int32)
        dp_id = lax.axis_index('dp').astype(jnp.int32)
        weights = (jnp.swapaxes(w_gate, 2, 3), jnp.swapaxes(w_up, 2, 3), w_down)

        def swap(x):
            return lax.ppermute(x, 'ep', ep_pairs)

        def spread(x):
            return lax.all_gather(x, 'dp', axis=0, tiled=True)

        def slab(x):
            return x.reshape(tok, parts, LANES)

        def mixed(x, layer):
            return (x.astype(jnp.float32) + jnp.dot(x, w_mix[layer], preferred_element_type=jnp.float32)).astype(jnp.bfloat16)

        ids = jnp.swapaxes(expert_ids, 1, 2)
        gates = jnp.swapaxes(gate_vals, 1, 2)
        mine = jnp.stack([ids.astype(jnp.float32), gates])
        theirs = swap(mine)
        both = jnp.stack([mine, theirs], 2)
        top = n_layers - 1
        tables, combined, packed = [], [], []

        def add_tables(layer, pair):
            lists, whole, token, gate, bounds = route_tables(pair[0].astype(jnp.int32), pair[1], ep_id, n_local, layer < top)
            gate_rows = gate.reshape(-1, LANES)
            at = token * parts
            tables.append([(*tiles, at, gate_rows) for tiles in lists])
            combined.append(tables[layer][-1] if layer == top else (*whole, at, gate_rows))
            spot = lax.div(token, tok) * (dp_size * tok) + dp_id * tok + lax.rem(token, tok)
            first = jnp.concatenate([spot.reshape(-1, LANES), jnp.pad(bounds.reshape(1, LANES), ((0, 7), (0, 0)))])
            packed.append(jnp.stack([first.astype(jnp.float32), jnp.pad(gate_rows, ((0, 8), (0, 0)))]))

        add_tables(0, both[:, 0])

        d_slab = slab(d_out)
        d_other = swap(d_slab)

        x_in, u_slabs, u_others, xs = tokens, [], [], []
        for layer in range(n_layers):
            u = mixed(x_in, layer)
            u_slabs.append(slab(u))
            u_others.append(swap(u_slabs[layer]))
            xs.append(x_in)
            if layer < top:
                slabs = (u_slabs[layer], u_others[layer])
                other, = token_kernel(forward_body, layer, tables[layer][1], slabs, weights, (1,))
                sent = swap(other)
                own, = token_kernel(forward_body, layer, tables[layer][0],
                                    (after(u_slabs[layer], other), u_others[layer]), weights, (0,))
                add_tables(layer + 1, after(both[:, layer + 1], other))
                x_in = (u.astype(jnp.float32) + own + sent).astype(jnp.bfloat16)

        shared = lax.all_gather(jnp.stack(packed), 'dp', axis=0)
        starts = shared[:, :, 0, -8].astype(jnp.int32)
        split = [split_experts(starts[:, layer, :n_local + 1], dp_id % 2) for layer in range(n_layers)]
        mine_e, theirs_e, tiles = (jnp.stack(x) for x in zip(*split))
        list_rows = cdiv(cdiv(dp_size * 2 * cap, LANES), 8) * 8 + 8
        idx_all, gate_all = merge_tables(shared, starts, mine_e, list_rows, dp_size * 2 * tok)
        idx_all = idx_all.reshape(-1)

        d_y, full, halves = d_out, None, []
        d_mix = [None] * n_layers
        for layer in reversed(range(n_layers)):
            spreads = [spread(jnp.concatenate(x, axis=1)) for x in ((u_slabs[layer], d_slab), (u_others[layer], d_other))]
            slabs = (u_slabs[layer], u_others[layer], d_slab, d_other)
            own, other = token_kernel(backward_body, layer, combined[layer], slabs, weights)
            d_u = (d_y.astype(jnp.float32) + own + swap(other)).astype(jnp.bfloat16)
            last = other
            if layer == top:
                y_own, y_other = token_kernel(forward_body, top, combined[top],
                                              (after(u_slabs[top], other), u_others[top]), weights)
                layer_out = (u.astype(jnp.float32) + y_own + swap(y_other)).astype(jnp.bfloat16)
                last = y_other
            full, half = weight_grads(layer, mine_e[layer], after(tiles, last), spreads, idx_all, gate_all, weights, full)
            halves.append((layer, [lax.ppermute(x, 'dp', core_pairs) for x in half]))
            d_mix[layer] = jnp.einsum('td,te->de', xs[layer], d_u, preferred_element_type=jnp.float32).astype(jnp.bfloat16)
            d_y = (d_u.astype(jnp.float32)
                   + jnp.einsum('te,de->td', d_u, w_mix[layer], preferred_element_type=jnp.float32)).astype(jnp.bfloat16)
            if layer:
                d_slab = slab(d_y)
                d_other = swap(d_slab)
        for layer, half in halves:
            full = merge_half(layer, theirs_e[layer], half, full)
        d_mix = lax.psum(jnp.stack(d_mix), ('dp', 'ep'))
        return (layer_out, d_y, d_mix, jnp.swapaxes(full[0], 2, 3), jnp.swapaxes(full[1], 2, 3), full[2])

    return jax.shard_map(device_body, mesh=mesh,
                         in_specs=(tok_spec, tok_spec, route_spec, route_spec, whole_spec,
                                   expert_spec, expert_spec, expert_spec),
                         out_specs=(tok_spec, tok_spec, whole_spec, expert_spec, expert_spec, expert_spec),
                         check_vma=False)
```

```python
import functools

import jax
import jax.numpy as jnp
from jax import lax
from jax.experimental import pallas as pl
from jax.experimental.pallas import tpu as pltpu
from jax.sharding import PartitionSpec as P


CAP_FACTOR = 3
LANES = 128
TILE = 96
HALF_TILE = 64
WTILE = 256
PARTS = 2
PITCH = 9
BATCH = 16
SLOTS = 6
PAGE = 1024
VMEM_LIMIT = 62 * 2**20


def cdiv(a, b):
    return (a + b - 1) // b


def nt_dot(a, b):
    return lax.dot_general(a, b, (((1,), (1,)), ((), ())), preferred_element_type=jnp.float32)


def tn_dot(a, b):
    return lax.dot_general(a, b, (((0,), (0,)), ((), ())), preferred_element_type=jnp.float32)


def nn_dot(a, b):
    return lax.dot_general(a, b, (((1,), (0,)), ((), ())), preferred_element_type=jnp.float32)


def clear(ref):
    step = next(n for n in (64, 48, 32, 16, 8) if ref.shape[0] % n == 0)

    def one(q, carry):
        ref[pl.ds(pl.multiple_of(q * step, step), step), :] = jnp.zeros((step, ref.shape[1]), ref.dtype)
        return carry

    lax.fori_loop(0, ref.shape[0] // step, one, 0)


def load_rows(ref, start, rows, parts):
    cols = [ref[pl.ds(start * parts + k, rows, stride=parts), :] for k in range(parts)]
    return jnp.concatenate(cols, axis=1).astype(jnp.bfloat16)


def fetch_rows(sources, halves, dst, sem):
    n = sources[0].shape[0]
    return [pltpu.make_async_copy(sources[k], dst.at[pl.ds(k * n, n)], sem.at[k]) for k in halves]


def add_rows(acc, vals_ref, idx, row, tile, pitch, width):
    for b in range(0, tile, BATCH):
        at = [pl.multiple_of(idx[row + b + r], 4) for r in range(BATCH)]
        vals = [acc[pl.ds(at[r], width), :] + vals_ref[pl.ds((b + r) * pitch, width), :] for r in range(BATCH)]
        for r in reversed(range(BATCH)):
            acc[pl.ds(at[r], width), :] = vals[r]


def spread_column(row):
    return jnp.broadcast_to(row, (LANES, LANES)).T


def tile_gates(gates, row):
    pair = gates[pl.ds(lax.div(row, LANES), 2), :]
    skip = lax.rem(row, LANES)
    pair = pltpu.roll(pair, lax.rem(LANES - skip, LANES), 1)
    lane = lax.broadcasted_iota(jnp.int32, (1, LANES), 1)
    return spread_column(jnp.where(lane < LANES - skip, pair[:1], pair[1:]))


def widen(src, dst, pitch, halves, tok):
    step = 8

    def one(q, carry):
        for r in range(step):
            dst[pl.ds((q * step + r) * pitch, pitch), :] = src[q * step + r].astype(jnp.float32)
        return carry

    lax.fori_loop(halves[0] * tok // step, (halves[-1] + 1) * tok // step, one, 0)


def write_sums(acc, outs, tok, parts, pitch, places):
    step = min(32, tok)

    def copy_out(q, carry):
        r0 = pl.multiple_of(q * step, step)
        for k in range(parts):
            cols = slice(k * LANES, (k + 1) * LANES)
            for out, (half, part) in zip(outs, places):
                first = (half * tok + r0) * pitch + part * parts + k
                out[pl.ds(r0, step), cols] = acc[pl.ds(first, step, stride=pitch), :]
        return carry

    lax.fori_loop(0, tok // step, copy_out, 0)


def expert_copies(weights, buf, sem, layer, e):
    slot = lax.rem(e, SLOTS)
    ff = weights[0].shape[2]
    return [pltpu.make_async_copy(w.at[layer, e], buf.at[slot, pl.ds(k * ff, ff)], sem.at[slot])
            for k, w in enumerate(weights)]


def run_tiles(step, weights, wbuf, wsem, tile_e, tile_first, n_steps, layer, prepare):
    n_local = weights[0].shape[1]
    for e in range(min(SLOTS - 1, n_local)):
        for c in expert_copies(weights, wbuf, wsem, layer, e):
            c.start()
    prepare()
    for c in expert_copies(weights, wbuf, wsem, layer, 0):
        c.wait()

    def one(i, carry):
        e = tile_e[i + 2]

        @pl.when(tile_first[i + 2] == 1)
        def _():
            for c in expert_copies(weights, wbuf, wsem, layer, e):
                c.wait()

        @pl.when((tile_first[i + 2] == 1) & (e + SLOTS - 2 < n_local))
        def _():
            for c in expert_copies(weights, wbuf, wsem, layer, e + SLOTS - 2):
                c.start()

        step(i, lax.rem(e, SLOTS), lax.rem(tile_e[i + 1], SLOTS))
        return carry

    lax.fori_loop(0, n_steps, one, 0)


def forward_body(te, tf, tr, tn, nt, idx, gates, u_own, u_oth, g_ref, up_ref, w_ref, *refs, layer, tok, parts, tile, halves):
    ff = g_ref.shape[2]
    outs, (usc, uf, ut, ot, acc, ht, wbuf, sem, wsem) = refs[:len(halves)], refs[len(halves):]

    def prepare():
        copies = fetch_rows((u_own, u_oth), halves, usc, sem)
        for c in copies:
            c.start()
        for ref in (acc, ot, ut, ht):
            clear(ref)
        for c in copies:
            c.wait()
        widen(usc, uf, parts, halves, tok)

    def step(i, slot, slot_before):
        o = tn_dot(ht[...], wbuf[slot_before, 2 * ff:]).astype(jnp.bfloat16).astype(jnp.float32)
        u = load_rows(ut, 0, tile, parts)
        ab = nt_dot(wbuf[slot, :2 * ff], u)
        add_rows(acc, ot, idx, tr[i], tile, parts, parts)
        row = tr[i + 3]
        for r in range(tile):
            ut[pl.ds(parts * r, parts), :] = uf[pl.ds(pl.multiple_of(idx[row + r], parts), parts), :]
        live = lax.broadcasted_iota(jnp.int32, (tile, LANES), 0) < tn[i + 1]
        gate = tile_gates(gates, tr[i + 1])[:tile]
        for k in range(parts):
            o_k = jnp.where(live, o[:, k * LANES:(k + 1) * LANES] * gate, 0.0)
            ot[pl.ds(k, tile, stride=parts), :] = o_k
        a, b = ab[:ff], ab[ff:]
        ht[...] = (a * jax.nn.sigmoid(a) * b).astype(jnp.bfloat16)

    run_tiles(step, (g_ref, up_ref, w_ref), wbuf, wsem, te, tf, nt[0] + 3, layer, prepare)
    write_sums(acc, outs, tok, parts, parts, [(half, 0) for half in halves])


def backward_body(te, tf, tr, tn, nt, idx, gates, u_own, u_oth, d_own, d_oth, g_ref, up_ref, w_ref, *refs, layer, tok, parts, tile,
                  forward):
    ff = g_ref.shape[2]
    n_out = 4 if forward else 2
    outs, (uds, udf, rows, vt, acc, da_t, ht, wbuf, sem, wsem) = refs[:n_out], refs[n_out:]
    pitch = 2 * parts
    width = pitch if forward else parts

    def prepare():
        copies = [pltpu.make_async_copy(src, uds.at[pl.ds((k % 2) * tok, tok), pl.ds((k // 2) * parts, parts)], sem.at[k])
                  for k, src in enumerate((u_own, u_oth, d_own, d_oth))]
        for c in copies:
            c.start()
        for ref in (acc, vt, rows, da_t, ht):
            clear(ref)
        for c in copies:
            c.wait()
        widen(uds, udf, pitch, (0, 1), tok)

    def column(k):
        return rows[pl.ds(k, tile, stride=PITCH), :]

    def step(i, slot, slot_before):
        results = [tn_dot(da_t[...], wbuf[slot_before, :2 * ff])]
        if forward:
            results.insert(0, tn_dot(ht[...], wbuf[slot_before, 2 * ff:]))
        u = jnp.concatenate([column(k) for k in range(parts)], axis=1).astype(jnp.bfloat16)
        gate = tile_gates(gates, tr[i + 2])[:tile]
        c = jnp.concatenate([(column(parts + k) * gate).astype(jnp.bfloat16) for k in range(parts)], axis=1)
        ab = nt_dot(wbuf[slot, :2 * ff], u)
        dh = nt_dot(wbuf[slot, 2 * ff:], c)
        add_rows(acc, vt, idx, tr[i], tile, PITCH, width)
        row = tr[i + 3]
        for r in range(tile):
            rows[pl.ds(PITCH * r, pitch), :] = udf[pl.ds(pl.multiple_of(idx[row + r], pitch), pitch), :]
        live = lax.broadcasted_iota(jnp.int32, (tile, LANES), 0) < tn[i + 1]
        gate = tile_gates(gates, tr[i + 1])[:tile]
        for q, result in enumerate(results):
            v = result.astype(jnp.bfloat16).astype(jnp.float32)
            for k in range(parts):
                v_k = jnp.where(live, v[:, k * LANES:(k + 1) * LANES] * gate, 0.0)
                vt[pl.ds(q * parts + k, tile, stride=PITCH), :] = v_k
        a, b = ab[:ff], ab[ff:]
        s = jax.nn.sigmoid(a)
        act = a * s
        if forward:
            ht[...] = (act * b).astype(jnp.bfloat16)
        da_t[:ff] = (dh * b * (s * (1.0 + a * (1.0 - s)))).astype(jnp.bfloat16)
        da_t[ff:] = (dh * act).astype(jnp.bfloat16)

    run_tiles(step, (g_ref, up_ref, w_ref), wbuf, wsem, te, tf, nt[0] + 3, layer, prepare)
    places = [(0, 0), (1, 0), (0, 1), (1, 1)] if forward else [(0, 0), (1, 0)]
    write_sums(acc, outs, tok, parts, pitch, places)


def token_kernel(layer, tables, slabs, weights, halves=(0, 1), forward=True):
    tok, parts, _ = slabs[0].shape
    _, n_local, ff, d_model = weights[0].shape
    backward = len(slabs) == 4
    tile = TILE if len(halves) == 2 else HALF_TILE
    rows_spec = pl.BlockSpec((tok, d_model), lambda i, *_: (0, 0))
    any_spec = pl.BlockSpec(memory_space=pl.ANY)
    common = [pltpu.VMEM((SLOTS, 3 * ff, d_model), jnp.bfloat16)]
    if backward:
        body = functools.partial(backward_body, forward=forward)
        n_out = 4 if forward else 2
        scratch = [pltpu.VMEM((2 * tok, 2 * parts, LANES), jnp.bfloat16), pltpu.VMEM((2 * tok * 2 * parts, LANES), jnp.float32),
                   pltpu.VMEM((tile * PITCH + 16, LANES), jnp.float32), pltpu.VMEM((tile * PITCH + 16, LANES), jnp.float32),
                   pltpu.VMEM((2 * tok * 2 * parts, LANES), jnp.float32), pltpu.VMEM((2 * ff, tile), jnp.bfloat16),
                   pltpu.VMEM((ff, tile), jnp.bfloat16)] + common
        scratch += [pltpu.SemaphoreType.DMA((4,)), pltpu.SemaphoreType.DMA((SLOTS,))]
    else:
        body = functools.partial(forward_body, halves=halves)
        n_out = len(halves)
        scratch = [pltpu.VMEM((2 * tok, parts, LANES), jnp.bfloat16), pltpu.VMEM((2 * tok * parts, LANES), jnp.float32),
                   pltpu.VMEM((tile * parts, LANES), jnp.float32), pltpu.VMEM((tile * parts, LANES), jnp.float32),
                   pltpu.VMEM((2 * tok * parts, LANES), jnp.float32), pltpu.VMEM((ff, tile), jnp.bfloat16)] + common
        scratch += [pltpu.SemaphoreType.DMA((2,)), pltpu.SemaphoreType.DMA((SLOTS,))]
    work = (4 * backward + 3 * (not backward or forward)) * len(halves)
    return pl.pallas_call(
        functools.partial(body, layer=layer, tok=tok, parts=parts, tile=tile),
        grid_spec=pltpu.PrefetchScalarGridSpec(
            num_scalar_prefetch=len(tables) - 1,
            grid=(1,),
            in_specs=[pl.BlockSpec(tables[-1].shape, lambda i, *_: (0, 0))] + [any_spec] * (len(slabs) + 3),
            out_specs=[rows_spec] * n_out,
            scratch_shapes=scratch,
        ),
        out_shape=[jax.ShapeDtypeStruct((tok, d_model), jnp.float32)] * n_out,
        compiler_params=pltpu.CompilerParams(dimension_semantics=("arbitrary",), vmem_limit_bytes=VMEM_LIMIT),
        cost_estimate=pl.CostEstimate(flops=work * 2 * 8 * tok * d_model * ff * 4,
                                      bytes_accessed=3 * n_local * ff * d_model * 2, transcendentals=0),
        name="experts_backward" if backward else "experts_forward",
    )(*tables, *slabs, *weights)


def merge_tables_body(st, exps, table, idx_ref, gate_ref, buf, *, src, n_exp, n_layers, out_rows, pad_row):
    group = idx_ref.shape[1]
    layer = pl.program_id(0)

    def one(q, carry):
        merge_expert(exps[layer * n_exp + pl.program_id(1) * group + q], layer, st, table, idx_ref.at[0, q], gate_ref.at[0, q],
                     buf, src, n_layers, out_rows, pad_row)
        return carry

    lax.fori_loop(0, group, one, 0)


def merge_expert(exp, layer, st, table, idx_out, gate_out, buf, src, n_layers, out_rows, pad_row):
    buf[0] = jnp.full(buf.shape[1:], float(pad_row), jnp.float32)
    buf[1] = jnp.zeros(buf.shape[1:], jnp.float32)
    row = lax.broadcasted_iota(jnp.int32, (8, LANES), 0)
    lane = lax.broadcasted_iota(jnp.int32, (8, LANES), 1)
    off = 0
    for d in range(src):
        at = (d * n_layers + layer) * LANES + exp
        first = st[at]
        count = st[at + 1] - first
        to = lax.rem(off, LANES) + LANES
        shift = to - lax.rem(first, LANES)
        over = lax.rem(shift, LANES)
        start = lax.div(off, LANES)
        place = row * LANES + lane
        take = (place >= to) & (place < to + count)
        for kind in range(2):
            x = table[d, 0, kind, pl.ds(lax.div(first, LANES), 8), :]
            x = pltpu.roll(pltpu.roll(x, over, 1), lax.div(shift, LANES), 0)
            x = jnp.where(lane >= over, x, pltpu.roll(x, 1, 0))
            old = buf[kind, pl.ds(start, 8), :]
            buf[kind, pl.ds(start, 8), :] = jnp.where(take, x, old)
        off = off + count
    idx_out[...] = buf[0, pl.ds(1, out_rows), :].astype(jnp.int32)
    gate_out[...] = buf[1, pl.ds(1, out_rows), :]


def merge_tables(shared, starts, exps, out_rows, pad_row):
    src, n_layers, _, rows, _ = shared.shape
    n_exp = exps.shape[1]
    group = 8 if n_exp % 8 == 0 else 1
    out = pl.BlockSpec((1, group, out_rows, LANES), lambda l, e, *_: (l, e, 0, 0))
    return pl.pallas_call(
        functools.partial(merge_tables_body, src=src, n_exp=n_exp, n_layers=n_layers, out_rows=out_rows,
                          pad_row=pad_row),
        grid_spec=pltpu.PrefetchScalarGridSpec(
            num_scalar_prefetch=2,
            grid=(n_layers, n_exp // group),
            in_specs=[pl.BlockSpec((src, 1, 2, rows, LANES), lambda l, e, *_: (0, l, 0, 0, 0))],
            out_specs=[out] * 2,
            scratch_shapes=[pltpu.VMEM((2, out_rows + 16, LANES), jnp.float32)],
        ),
        out_shape=[jax.ShapeDtypeStruct((n_layers, n_exp, out_rows, LANES), jnp.int32),
                   jax.ShapeDtypeStruct((n_layers, n_exp, out_rows, LANES), jnp.float32)],
        compiler_params=pltpu.CompilerParams(dimension_semantics=("arbitrary", "arbitrary")),
        cost_estimate=pl.CostEstimate(flops=10**9, bytes_accessed=4 * shared.size, transcendentals=0),
        name="merge_tables",
    )(starts.reshape(-1), exps.reshape(-1), shared)


def weight_grad_body(exps, tiles, begins, u_own, u_oth, d_own, d_oth, idx_all, gate_ref, *refs, parts, n_exp, n_alias, first_list,
                     page):
    g_ref, up_ref, w_ref = refs[:3]
    (dg_ref, du_ref, dw_ref, og_ref, ou_ref, ow_ref,
     uds, rows, u0, c0, d0, h0, u1, c1, d1, h1, gacc, wacc, idx_s, sem, tsem) = refs[3 + n_alias:]
    e = pl.program_id(0)
    ff = g_ref.shape[2]
    slots = 3
    both = ((u0, c0, d0, h0), (u1, c1, d1, h1))

    def table_copy(exp):
        slot = lax.rem(exp, slots)
        at = pl.multiple_of((first_list + exp) * page, PAGE)
        to = pl.multiple_of(slot * page, PAGE)
        return pltpu.make_async_copy(idx_all.at[pl.ds(at, page)], idx_s.at[pl.ds(to, page)], tsem.at[slot])

    def gather_row(at, r):
        rows[pl.ds(r * PITCH, 2 * parts), :] = uds[idx_s[at]].astype(jnp.float32)

    def column(first, count, k):
        return rows[pl.ds(first * PITCH + k, count, stride=PITCH), :]

    @pl.when(e == 0)
    def _():
        n_half = u_own.shape[0]
        copies = [pltpu.make_async_copy(src, uds.at[pl.ds((k % 2) * n_half, n_half), pl.ds((k // 2) * parts, parts)], sem.at[k])
                  for k, src in enumerate((u_own, u_oth, d_own, d_oth))]
        for c in copies:
            c.start()
        table_copy(0).start()
        table_copy(1).start()
        n_rows = n_half * 2
        uds[pl.ds(n_rows, 8)] = jnp.zeros((8, 2 * parts, LANES), jnp.bfloat16)
        for ref in (*both[0], *both[1], gacc, wacc):
            clear(ref)
        table_copy(0).wait()
        for c in copies:
            c.wait()

        def first_rows(q, carry):
            for r in range(16):
                gather_row(q * 16 + r, q * 16 + r)
            return carry

        lax.fori_loop(0, WTILE // 16, first_rows, 0)

    @pl.when(e + 1 < n_exp)
    def _():
        table_copy(e + 1).wait()

    @pl.when(e + 2 < n_exp)
    def _():
        table_copy(e + 2).start()

    here = lax.rem(e, slots) * page
    there = lax.rem(jnp.minimum(e + 1, n_exp - 1), slots) * page
    n_tiles = tiles[e]
    begin = begins[e]
    gate_rows = WTILE // LANES

    def compute(j, new, old):
        un, cn, dn, hn = new
        uo, co, do, ho = old
        gacc[...] += nn_dot(do[...], uo[...])
        wacc[...] += nn_dot(ho[...], co[...])
        un[...] = jnp.concatenate([column(0, WTILE, k) for k in range(parts)], axis=1).astype(jnp.bfloat16)
        gates = [spread_column(gate_ref[0, 0, pl.ds(j * gate_rows + q, 1), :]) for q in range(gate_rows)]
        for k in range(parts):
            for q in range(gate_rows):
                d = column(q * LANES, LANES, parts + k)
                cn[q * LANES:(q + 1) * LANES, k * LANES:(k + 1) * LANES] = (d * gates[q]).astype(jnp.bfloat16)
        ab = nt_dot(jnp.concatenate([g_ref[0, 0], up_ref[0, 0]], axis=0), un[...])
        dh = nt_dot(w_ref[0, 0], cn[...])
        nxt = jnp.where(j + 1 < n_tiles, here + (j + 1) * WTILE, there)
        for r in range(WTILE):
            gather_row(nxt + r, r)
        a, b = ab[:ff], ab[ff:]
        s = jax.nn.sigmoid(a)
        act = a * s
        hn[...] = (act * b).astype(jnp.bfloat16)
        dn[:ff] = (dh * b * (s * (1.0 + a * (1.0 - s)))).astype(jnp.bfloat16)
        dn[ff:] = (dh * act).astype(jnp.bfloat16)

    def tile(j, carry):
        odd = lax.rem(begin + j, 2)

        @pl.when(odd == 0)
        def _():
            compute(j, both[0], both[1])

        @pl.when(odd == 1)
        def _():
            compute(j, both[1], both[0])

        @pl.when(j == 0)
        def _():
            dg = gacc[:ff].astype(jnp.bfloat16)
            du = gacc[ff:].astype(jnp.bfloat16)
            dw = wacc[...].astype(jnp.bfloat16)
            dg_ref[0, 0], du_ref[0, 0], dw_ref[0, 0] = dg, du, dw
            og_ref[0], ou_ref[0], ow_ref[0] = dg, du, dw
            gacc[...] = jnp.zeros_like(gacc)
            wacc[...] = jnp.zeros_like(wacc)

        return carry

    lax.fori_loop(0, n_tiles, tile, 0)


def weight_grads(layer, part, exps, tiles, rows, idx_all, gates, weights, full):
    n_half, parts, _ = rows[0].shape
    n_tok = 2 * n_half
    n_layers, n_local, ff, d_model = weights[0].shape
    n_own = exps.shape[1]
    n_exp = n_own // PARTS
    first = part * n_exp
    out_rows = gates.shape[2]
    page = out_rows * LANES
    exps = lax.slice_in_dim(exps[layer], first, first + n_exp)
    tiles = jnp.concatenate([lax.slice_in_dim(tiles[layer], first, first + n_exp), jnp.ones((1,), jnp.int32)])
    begins = jnp.cumsum(tiles) - tiles
    any_spec = pl.BlockSpec(memory_space=pl.ANY)
    mine = pl.BlockSpec((1, 1, ff, d_model), lambda e, exps, *_: (layer, exps[jnp.minimum(e, n_exp - 1)], 0, 0))
    done = pl.BlockSpec((1, 1, ff, d_model), lambda e, exps, *_: (layer, exps[jnp.maximum(e - 1, 0)], 0, 0))
    half = pl.BlockSpec((1, ff, d_model), lambda e, *_: (jnp.maximum(e - 1, 0), 0, 0))
    gate_spec = pl.BlockSpec((1, 1, out_rows, LANES), lambda e, *_: (layer, first + jnp.minimum(e, n_exp - 1), 0, 0))
    aliased = list(full) if full is not None else []
    tile_set = [pltpu.VMEM((WTILE, d_model), jnp.bfloat16)] * 2 + [pltpu.VMEM((2 * ff, WTILE), jnp.bfloat16),
                                                                 pltpu.VMEM((ff, WTILE), jnp.bfloat16)]
    outs = pl.pallas_call(
        functools.partial(weight_grad_body, parts=parts, n_exp=n_exp, n_alias=len(aliased), first_list=layer * n_own + first,
                          page=page),
        grid_spec=pltpu.PrefetchScalarGridSpec(
            num_scalar_prefetch=3,
            grid=(n_exp + 1,),
            in_specs=[any_spec] * 5 + [gate_spec] + [mine] * 3 + [any_spec] * len(aliased),
            out_specs=[done] * 3 + [half] * 3,
            scratch_shapes=[pltpu.VMEM((n_tok + 8, 2 * parts, LANES), jnp.bfloat16)]
            + [pltpu.VMEM((WTILE * PITCH + 16, LANES), jnp.float32)] + tile_set * 2
            + [pltpu.VMEM((2 * ff, d_model), jnp.float32), pltpu.VMEM((ff, d_model), jnp.float32),
               pltpu.SMEM((3 * page,), jnp.int32), pltpu.SemaphoreType.DMA((4,)), pltpu.SemaphoreType.DMA((3,))],
        ),
        out_shape=[jax.ShapeDtypeStruct((n_layers, n_local, ff, d_model), jnp.bfloat16)] * 3
        + [jax.ShapeDtypeStruct((n_exp, ff, d_model), jnp.bfloat16)] * 3,
        input_output_aliases={12 + k: k for k in range(len(aliased))},
        compiler_params=pltpu.CompilerParams(dimension_semantics=("arbitrary",), vmem_limit_bytes=VMEM_LIMIT),
        cost_estimate=pl.CostEstimate(flops=6 * 2 * n_tok * 2 * d_model * ff * 4 // PARTS,
                                      bytes_accessed=n_tok * d_model * 4 + 9 * n_exp * ff * d_model * 2, transcendentals=0),
        name="weight_grads",
    )(exps, tiles, begins, *rows, idx_all, gates, *weights, *aliased)
    return outs[:3], outs[3:]


def merge_body(exps, a, b, c, f0, f1, f2, o0, o1, o2, buf, in_sem, out_sem, *, layer, n_exp):
    halves, wholes = (a, b, c), (o0, o1, o2)

    def arrive(k, q):
        return pltpu.make_async_copy(halves[k].at[q], buf.at[k, q], in_sem.at[k, q])

    def leave(k, q):
        return pltpu.make_async_copy(buf.at[k, q], wholes[k].at[layer, exps[q]], out_sem)

    def each(act):
        def one(q, carry):
            for k in range(3):
                act(k, q)
            return carry

        lax.fori_loop(0, n_exp, one, 0)

    def pass_on(k, q):
        arrive(k, q).wait()
        leave(k, q).start()

    each(lambda k, q: arrive(k, q).start())
    each(pass_on)
    each(lambda k, q: leave(k, q).wait())


def merge_half(layer, exps, half, full):
    n_exp, ff, d_model = half[0].shape
    any_spec = pl.BlockSpec(memory_space=pl.ANY)
    return pl.pallas_call(
        functools.partial(merge_body, layer=layer, n_exp=n_exp),
        grid_spec=pltpu.PrefetchScalarGridSpec(
            num_scalar_prefetch=1, grid=(1,), in_specs=[any_spec] * 6, out_specs=[any_spec] * 3,
            scratch_shapes=[pltpu.VMEM((3, n_exp, ff, d_model), jnp.bfloat16), pltpu.SemaphoreType.DMA((3, n_exp)),
                            pltpu.SemaphoreType.DMA]),
        out_shape=[jax.ShapeDtypeStruct(x.shape, x.dtype) for x in full],
        input_output_aliases={4: 0, 5: 1, 6: 2},
        compiler_params=pltpu.CompilerParams(dimension_semantics=("arbitrary",), vmem_limit_bytes=VMEM_LIMIT),
        cost_estimate=pl.CostEstimate(flops=10**9, bytes_accessed=6 * n_exp * ff * d_model * 2, transcendentals=0),
        name="merge_half",
    )(exps, *half, *full)


def route_tables(ids, gates, ep, n_local, split):
    n_src, top_k, tok = ids.shape
    n = n_src * top_k * tok
    local = ids - ep * n_local
    here = (local >= 0) & (local < n_local)
    group = jnp.where(here, local, n_local).reshape(-1)
    key, gate = lax.sort((group * n + jnp.arange(n, dtype=jnp.int32), gates.reshape(-1)), num_keys=1, is_stable=False)
    copy = key % n
    token = copy // (top_k * tok) * tok + copy % tok
    hits = (group.reshape(n_src, -1)[:, :, None] == jnp.arange(n_local)[None, None, :]).astype(jnp.int32)
    half_counts = jnp.sum(hits, axis=1)
    counts = jnp.sum(half_counts, axis=0)
    ends = jnp.cumsum(counts)
    starts = ends - counts
    pad = 2 * PAGE
    token = jnp.pad(token, (0, pad))
    gate = jnp.pad(gate, (0, pad))
    bounds = jnp.concatenate([jnp.zeros((1,), jnp.int32), ends, jnp.full((LANES - 1 - n_local,), ends[-1], jnp.int32)])
    whole = tile_list(starts, counts, n, TILE)
    lists = (whole,)
    if split:
        lists = (tile_list(starts, half_counts[0], n // 2, HALF_TILE),
                 tile_list(starts + half_counts[0], half_counts[1], n // 2, HALF_TILE))
    return lists, whole, token, gate, bounds


def tile_list(starts, counts, most, tile):
    n_local = starts.shape[0]
    n_tiles = jnp.maximum((counts + tile - 1) // tile, 1)
    tile_end = jnp.cumsum(n_tiles)
    tile_id = jnp.arange(most // tile + n_local + 8, dtype=jnp.int32) - 3
    tile_e = jnp.minimum(jnp.sum((tile_end[None, :] <= tile_id[:, None]).astype(jnp.int32), axis=1), n_local - 1)
    pick = (tile_e[:, None] == jnp.arange(n_local)[None, :]).astype(jnp.int32)
    inside = (tile_id - jnp.sum(pick * (tile_end - n_tiles)[None, :], axis=1)) * tile
    real = (tile_id >= 0) & (tile_id < tile_end[-1])
    tile_row = jnp.where(real, jnp.sum(pick * starts[None, :], axis=1) + inside, 0)
    tile_first = (real & (inside == 0) & (tile_e > 0)).astype(jnp.int32)
    tile_n = jnp.where(real, jnp.clip(jnp.sum(pick * counts[None, :], axis=1) - inside, 0, tile), 0)
    return tile_e, tile_first, tile_row, tile_n, tile_end[-1:]


def split_experts(bounds, core):
    n_local = bounds.shape[1] - 1
    load = jnp.sum(bounds[:, 1:] - bounds[:, :-1], axis=0)
    ids = jnp.arange(n_local, dtype=jnp.int32)
    ahead = (load[None, :] > load[:, None]) | ((load[None, :] == load[:, None]) & (ids[None, :] < ids[:, None]))
    rank = jnp.sum(ahead.astype(jnp.int32), axis=1)
    turn = jnp.concatenate([jnp.arange(k, n_local // 2, PARTS, dtype=jnp.int32) for k in range(PARTS)])

    def dealt(which):
        want = 2 * turn + (which + turn) % 2
        return (rank[None, :] == want[:, None]).astype(jnp.int32)

    mine, theirs = dealt(core), dealt(1 - core)
    tiles = jnp.maximum((jnp.sum(mine * load[None, :], axis=1) + WTILE - 1) // WTILE, 1)
    return jnp.sum(mine * ids[None, :], axis=1), jnp.sum(theirs * ids[None, :], axis=1), tiles


def after(x, *earlier):
    return lax.optimization_barrier((x, *earlier))[0]


def solution(mesh):
    ep_size = mesh.shape['ep']
    dp_size = mesh.shape['dp']
    tok_spec = P(('dp', 'ep'), None)
    route_spec = P(None, ('dp', 'ep'), None)
    whole_spec = P(None, None, None)
    expert_spec = P(None, 'ep', None, None)
    ep_pairs = [(i, 1 - i) for i in range(ep_size)]
    core_pairs = [(i, i ^ 1) for i in range(dp_size)]

    def device_body(tokens, d_out, expert_ids, gate_vals, w_mix, w_gate, w_up, w_down):
        n_layers = w_mix.shape[0]
        n_local = w_gate.shape[1]
        n_experts = n_local * ep_size
        tok, d_model = tokens.shape
        top_k = expert_ids.shape[2]
        parts = d_model // LANES
        cap = cdiv(CAP_FACTOR * tok * top_k, n_experts)
        ep_id = lax.axis_index('ep').astype(jnp.int32)
        dp_id = lax.axis_index('dp').astype(jnp.int32)
        weights = (jnp.swapaxes(w_gate, 2, 3), jnp.swapaxes(w_up, 2, 3), w_down)

        def swap(x):
            return lax.ppermute(x, 'ep', ep_pairs)

        def spread(x):
            return lax.all_gather(x, 'dp', axis=0, tiled=True)

        def slab(x):
            return x.reshape(tok, parts, LANES)

        def mixed(x, layer):
            return (x.astype(jnp.float32) + jnp.dot(x, w_mix[layer], preferred_element_type=jnp.float32)).astype(jnp.bfloat16)

        ids = jnp.swapaxes(expert_ids, 1, 2)
        gates = jnp.swapaxes(gate_vals, 1, 2)
        mine = jnp.stack([ids.astype(jnp.float32), gates])
        u = mixed(tokens, 0)
        u_slab = slab(u)
        theirs = swap(after(mine, u_slab))
        both = jnp.stack([mine, theirs], 2)
        top = n_layers - 1
        tables, combined, packed = [], [], []

        def add_tables(layer, pair):
            lists, whole, token, gate, bounds = route_tables(pair[0].astype(jnp.int32), pair[1], ep_id, n_local, layer < top)
            gate_rows = gate.reshape(-1, LANES)
            tables.append([(*tiles, token * parts, gate_rows) for tiles in lists])
            combined.append((*whole, token * (2 * parts), gate_rows))
            spot = lax.div(token, tok) * (dp_size * tok) + dp_id * tok + lax.rem(token, tok)
            first = jnp.concatenate([spot.reshape(-1, LANES), jnp.pad(bounds.reshape(1, LANES), ((0, 7), (0, 0)))])
            packed.append(jnp.stack([first.astype(jnp.float32), jnp.pad(gate_rows, ((0, 8), (0, 0)))]))

        add_tables(0, both[:, 0])

        d_slab = slab(d_out)
        d_other = swap(d_slab)
        d_rows = (spread(d_slab), spread(d_other))

        x_in, u_slabs, u_others, xs = tokens, [u_slab], [swap(u_slab)], []
        for layer in range(n_layers):
            if layer:
                u = mixed(x_in, layer)
                u_slabs.append(slab(u))
                u_others.append(swap(u_slabs[layer]))
            xs.append(x_in)
            if layer < top:
                slabs = (u_slabs[layer], u_others[layer])
                other, = token_kernel(layer, tables[layer][1], slabs, weights, (1,))
                sent = swap(other)
                own, = token_kernel(layer, tables[layer][0], (after(u_slabs[layer], other, d_other), u_others[layer]), weights,
                                    (0,))
                add_tables(layer + 1, after(both[:, layer + 1], own))
                x_in = (u.astype(jnp.float32) + own + sent).astype(jnp.bfloat16)

        shared = lax.all_gather(jnp.stack(packed), 'dp', axis=0)
        starts = shared[:, :, 0, -8].astype(jnp.int32)
        split = [split_experts(starts[:, layer, :n_local + 1], dp_id % 2) for layer in range(n_layers)]
        mine_e, theirs_e, tiles = (jnp.stack(x) for x in zip(*split))
        list_rows = cdiv(cdiv(dp_size * 2 * cap, LANES), 8) * 8 + 8
        idx_all, gate_all = merge_tables(shared, starts, mine_e, list_rows, dp_size * 2 * tok)
        idx_all = idx_all.reshape(-1)

        d_y, full, halves = d_out, None, []
        d_mix = [None] * n_layers
        for layer in reversed(range(n_layers)):
            u_rows = tuple(spread(x) for x in (u_slabs[layer], u_others[layer]))
            slabs = (u_slabs[layer], u_others[layer], d_slab, d_other)
            *sums, own, other = token_kernel(layer, combined[layer], slabs, weights, forward=layer == top)
            if layer == top:
                y_own, y_other = sums
            d_u = (d_y.astype(jnp.float32) + own + swap(other)).astype(jnp.bfloat16)

            def grads(part, full, *earlier):
                full, half = weight_grads(layer, part, mine_e, after(tiles, *earlier), u_rows + d_rows, idx_all, gate_all, weights,
                                          full)
                halves.append((layer, part, [lax.ppermute(x, 'dp', core_pairs) for x in half]))
                return full

            full = grads(0, full, other)
            d_mix[layer] = jnp.einsum('td,te->de', xs[layer], d_u, preferred_element_type=jnp.float32).astype(jnp.bfloat16)
            d_y = (d_u.astype(jnp.float32)
                   + jnp.einsum('te,de->td', d_u, w_mix[layer], preferred_element_type=jnp.float32)).astype(jnp.bfloat16)
            if layer:
                next_slab = slab(d_y)
                next_other = swap(next_slab)
                next_rows = (spread(next_slab), spread(next_other))
                if layer == top:
                    layer_out = (u.astype(jnp.float32) + y_own + swap(after(y_other, next_other))).astype(jnp.bfloat16)
            for part in range(1, PARTS):
                full = grads(part, full, d_y)
            if layer:
                d_slab, d_other, d_rows = next_slab, next_other, next_rows
        for layer, part, half in halves:
            n_exp = half[0].shape[0]
            full = merge_half(layer, lax.slice_in_dim(theirs_e[layer], part * n_exp, (part + 1) * n_exp), half, full)
        d_mix = lax.psum(jnp.stack(d_mix), ('dp', 'ep'))
        return (layer_out, d_y, d_mix, jnp.swapaxes(full[0], 2, 3), jnp.swapaxes(full[1], 2, 3), full[2])

    return jax.shard_map(device_body, mesh=mesh,
                         in_specs=(tok_spec, tok_spec, route_spec, route_spec, whole_spec,
                                   expert_spec, expert_spec, expert_spec),
                         out_specs=(tok_spec, tok_spec, whole_spec, expert_spec, expert_spec, expert_spec),
                         check_vma=False)
```

```python
import functools
import math

import jax
import jax.numpy as jnp
from jax import lax
from jax.experimental import pallas as pl
from jax.experimental.pallas import tpu as pltpu
from jax.sharding import PartitionSpec as P


CAP_FACTOR = 3
LANES = 128
TILE = 96
HALF_TILE = 64
WTILE = 256
PITCH = 9
BATCH = 16
SLOTS = 8
PAGE = 1024
VMEM_LIMIT = 62 * 2**20


def cdiv(a, b):
    return (a + b - 1) // b


def nt_dot(a, b):
    return lax.dot_general(a, b, (((1,), (1,)), ((), ())), preferred_element_type=jnp.float32)


def tn_dot(a, b):
    return lax.dot_general(a, b, (((0,), (0,)), ((), ())), preferred_element_type=jnp.float32)


def nn_dot(a, b):
    return lax.dot_general(a, b, (((1,), (0,)), ((), ())), preferred_element_type=jnp.float32)


def clear(ref):
    step = next(n for n in (64, 48, 32, 16, 8) if ref.shape[0] % n == 0)

    def one(q, carry):
        ref[pl.ds(pl.multiple_of(q * step, step), step), :] = jnp.zeros((step, ref.shape[1]), ref.dtype)
        return carry

    lax.fori_loop(0, ref.shape[0] // step, one, 0)


def add_rows(acc, vals_ref, idx, row, tile, pitch, width):
    for b in range(0, tile, BATCH):
        at = [pl.multiple_of(idx[row + b + r], 4) for r in range(BATCH)]
        vals = [acc[pl.ds(at[r], width), :] + vals_ref[pl.ds((b + r) * pitch, width), :] for r in range(BATCH)]
        for r in reversed(range(BATCH)):
            acc[pl.ds(at[r], width), :] = vals[r]


def spread_column(row):
    return jnp.broadcast_to(row, (LANES, LANES)).T


def tile_gates(gates, row):
    pair = gates[pl.ds(lax.div(row, LANES), 2), :]
    skip = lax.rem(row, LANES)
    pair = pltpu.roll(pair, lax.rem(LANES - skip, LANES), 1)
    lane = lax.broadcasted_iota(jnp.int32, (1, LANES), 1)
    return spread_column(jnp.where(lane < LANES - skip, pair[:1], pair[1:]))


def widen(src, dst, pitch, halves, tok):
    step = 8

    def one(q, carry):
        for r in range(step):
            dst[pl.ds((q * step + r) * pitch, pitch), :] = src[q * step + r].astype(jnp.float32)
        return carry

    lax.fori_loop(halves[0] * tok // step, (halves[-1] + 1) * tok // step, one, 0)


def write_sums(acc, outs, tok, parts, pitch, halves):
    step = min(32, tok)

    def copy_out(q, carry):
        r0 = pl.multiple_of(q * step, step)
        for k in range(parts):
            for out, half in zip(outs, halves):
                first = (half * tok + r0) * pitch + k
                out[pl.ds(r0, step), k * LANES:(k + 1) * LANES] = acc[pl.ds(first, step, stride=pitch), :]
        return carry

    lax.fori_loop(0, tok // step, copy_out, 0)


def expert_copies(weights, buf, sem, layer, e):
    slot = lax.rem(e, SLOTS)
    ff = weights[0].shape[2]
    return [pltpu.make_async_copy(w.at[layer, e], buf.at[slot, pl.ds(k * ff, ff)], sem.at[slot])
            for k, w in enumerate(weights)]


def run_tiles(step, weights, wbuf, wsem, runs, tile, layer, prepare):
    n_local = weights[0].shape[1]
    for e in range(SLOTS - 1):
        for c in expert_copies(weights, wbuf, wsem, layer, e):
            c.start()
    prepare()
    for c in expert_copies(weights, wbuf, wsem, layer, 0):
        c.wait()

    def length(e):
        return runs[n_local + e] - runs[e]

    def add_tiles(e, total):
        return total + jnp.maximum(lax.div(length(e) + tile - 1, tile), 1)

    def one(i, carry):
        (e, row, left), (e1, row1, n1), (e2, row2, n2), row3 = carry

        @pl.when(e1 != e2)
        def _():
            for c in expert_copies(weights, wbuf, wsem, layer, e1):
                c.wait()

        @pl.when((e1 != e2) & (e1 + SLOTS - 2 < n_local))
        def _():
            for c in expert_copies(weights, wbuf, wsem, layer, e1 + SLOTS - 2):
                c.start()

        step(row, (lax.rem(e1, SLOTS), row1), (lax.rem(e2, SLOTS), row2, n2), row3)
        more = left > tile
        e_next = jnp.minimum(e + 1, n_local - 1)
        fresh = jnp.where(e + 1 < n_local, length(e_next), 0)
        ahead = (jnp.where(more, e, e_next), jnp.where(more, row + tile, runs[e_next]), jnp.where(more, left - tile, fresh))
        return ahead, (e, row, jnp.minimum(left, tile)), (e1, row1, n1), row2

    none = (0, 0, 0)
    lax.fori_loop(0, lax.fori_loop(0, n_local, add_tiles, 0) + 3, one, ((0, runs[0], length(0)), none, none, 0))


def token_body(runs, idx, gates, *refs, layer, tok, parts, tile, halves, backward):
    n_in = 4 if backward else 2
    sources, weights, outs, refs = refs[:n_in], refs[n_in:n_in + 3], refs[n_in + 3:n_in + 3 + len(halves)], refs[n_in + 3 + len(halves):]
    narrow, wide, rows, vt, acc, mid, wbuf, sem, wsem = refs
    ff = weights[0].shape[2]
    width = parts * n_in // 2
    pitch = width + 1

    def prepare():
        copies = [pltpu.make_async_copy(src, narrow.at[pl.ds(k % 2 * tok, tok), pl.ds(k // 2 * parts, parts)], sem.at[k])
                  for k, src in enumerate(sources) if k % 2 in halves]
        for c in copies:
            c.start()
        for ref in (acc, vt, rows, mid):
            clear(ref)
        for c in copies:
            c.wait()
        widen(narrow, wide, width, halves, tok)

    def column(k):
        return rows[pl.ds(k, tile, stride=pitch), :]

    def step(row, here, before, done):
        slot, row1 = here
        slot2, row2, n2 = before
        old = wbuf[slot2, :2 * ff] if backward else wbuf[slot2, 2 * ff:]
        v = tn_dot(mid[...], old).astype(jnp.bfloat16).astype(jnp.float32)
        u = jnp.concatenate([column(k) for k in range(parts)], axis=1).astype(jnp.bfloat16)
        ab = nt_dot(wbuf[slot, :2 * ff], u)
        if backward:
            gate = tile_gates(gates, row1)[:tile]
            c = jnp.concatenate([(column(parts + k) * gate).astype(jnp.bfloat16) for k in range(parts)], axis=1)
            dh = nt_dot(wbuf[slot, 2 * ff:], c)
        add_rows(acc, vt, idx, done, tile, parts + 1, parts)
        for r in range(tile):
            rows[pl.ds(pitch * r, width), :] = wide[pl.ds(pl.multiple_of(idx[row + r], width), width), :]
        live = lax.broadcasted_iota(jnp.int32, (tile, LANES), 0) < n2
        gate = tile_gates(gates, row2)[:tile]
        for k in range(parts):
            v_k = jnp.where(live, v[:, k * LANES:(k + 1) * LANES] * gate, 0.0)
            vt[pl.ds(k, tile, stride=parts + 1), :] = v_k
        a, b = ab[:ff], ab[ff:]
        s = jax.nn.sigmoid(a)
        act = a * s
        if backward:
            mid[:ff] = (dh * b * (s * (1.0 + a * (1.0 - s)))).astype(jnp.bfloat16)
            mid[ff:] = (dh * act).astype(jnp.bfloat16)
        else:
            mid[...] = (act * b).astype(jnp.bfloat16)

    run_tiles(step, weights, wbuf, wsem, runs, tile, layer, prepare)
    write_sums(acc, outs, tok, parts, width, halves)


def token_kernel(layer, runs, table, slabs, weights, halves=(0, 1)):
    idx, gates = table
    tok, parts, _ = slabs[0].shape
    _, n_local, ff, d_model = weights[0].shape
    backward = len(slabs) > 2
    tile = TILE if len(halves) == 2 else HALF_TILE
    width = parts * len(slabs) // 2
    rows_spec = pl.BlockSpec((tok, d_model), lambda i, *_: (0, 0))
    any_spec = pl.BlockSpec(memory_space=pl.ANY)
    tile_rows = cdiv(tile * (width + 1), 16) * 16
    work = (4 if backward else 3) * len(halves)
    return pl.pallas_call(
        functools.partial(token_body, layer=layer, tok=tok, parts=parts, tile=tile, halves=halves, backward=backward),
        grid_spec=pltpu.PrefetchScalarGridSpec(
            num_scalar_prefetch=2,
            grid=(1,),
            in_specs=[pl.BlockSpec(gates.shape, lambda i, *_: (0, 0))] + [any_spec] * (len(slabs) + 3),
            out_specs=[rows_spec] * len(halves),
            scratch_shapes=[pltpu.VMEM((2 * tok, width, LANES), jnp.bfloat16), pltpu.VMEM((2 * tok * width, LANES), jnp.float32),
                            pltpu.VMEM((tile_rows, LANES), jnp.float32), pltpu.VMEM((tile_rows, LANES), jnp.float32),
                            pltpu.VMEM((2 * tok * width, LANES), jnp.float32),
                            pltpu.VMEM((2 * ff if backward else ff, tile), jnp.bfloat16),
                            pltpu.VMEM((SLOTS, 3 * ff, d_model), jnp.bfloat16),
                            pltpu.SemaphoreType.DMA((len(slabs),)), pltpu.SemaphoreType.DMA((SLOTS,))],
        ),
        out_shape=[jax.ShapeDtypeStruct((tok, d_model), jnp.float32)] * len(halves),
        compiler_params=pltpu.CompilerParams(dimension_semantics=("arbitrary",), vmem_limit_bytes=VMEM_LIMIT),
        cost_estimate=pl.CostEstimate(flops=work * 2 * 8 * tok * d_model * ff * 4,
                                      bytes_accessed=3 * n_local * ff * d_model * 2, transcendentals=0),
        name="experts_backward" if backward else "experts_forward",
    )(runs, idx, gates, *slabs, *weights)


def merge_tables_body(st, exps, layers, table, idx_ref, gate_ref, buf, *, out_rows, pad_row):
    group = idx_ref.shape[0]

    def one(q, carry):
        item = pl.program_id(0) * group + q
        merge_expert(exps[item], layers[item], st, table, idx_ref.at[q], gate_ref.at[q], buf, out_rows, pad_row)
        return carry

    lax.fori_loop(0, group, one, 0)


def merge_expert(exp, layer, st, table, idx_out, gate_out, buf, out_rows, pad_row):
    src, n_layers = table.shape[:2]
    buf[0] = jnp.full(buf.shape[1:], float(pad_row), jnp.float32)
    buf[1] = jnp.zeros(buf.shape[1:], jnp.float32)
    row = lax.broadcasted_iota(jnp.int32, (8, LANES), 0)
    lane = lax.broadcasted_iota(jnp.int32, (8, LANES), 1)
    off = 0
    for d in range(src):
        at = (d * n_layers + layer) * LANES + exp
        first = st[at]
        count = st[at + 1] - first
        to = lax.rem(off, LANES) + LANES
        shift = to - lax.rem(first, LANES)
        over = lax.rem(shift, LANES)
        start = lax.div(off, LANES)
        place = row * LANES + lane
        take = (place >= to) & (place < to + count)
        for kind in range(2):
            x = table[d, layer, kind, pl.ds(lax.div(first, LANES), 8), :]
            x = pltpu.roll(pltpu.roll(x, over, 1), lax.div(shift, LANES), 0)
            x = jnp.where(lane >= over, x, pltpu.roll(x, 1, 0))
            old = buf[kind, pl.ds(start, 8), :]
            buf[kind, pl.ds(start, 8), :] = jnp.where(take, x, old)
        off = off + count
    idx_out[...] = buf[0, pl.ds(1, out_rows), :].astype(jnp.int32)
    gate_out[...] = buf[1, pl.ds(1, out_rows), :]


def merge_tables(shared, starts, exps, layers, out_rows, pad_row):
    n_items = exps.shape[0]
    group = math.gcd(n_items, 8)
    out = pl.BlockSpec((group, out_rows, LANES), lambda g, *_: (g, 0, 0))
    return pl.pallas_call(
        functools.partial(merge_tables_body, out_rows=out_rows, pad_row=pad_row),
        grid_spec=pltpu.PrefetchScalarGridSpec(
            num_scalar_prefetch=3,
            grid=(n_items // group,),
            in_specs=[pl.BlockSpec(shared.shape, lambda g, *_: (0,) * shared.ndim)],
            out_specs=[out] * 2,
            scratch_shapes=[pltpu.VMEM((2, out_rows + 16, LANES), jnp.float32)],
        ),
        out_shape=[jax.ShapeDtypeStruct((n_items, out_rows, LANES), jnp.int32),
                   jax.ShapeDtypeStruct((n_items, out_rows, LANES), jnp.float32)],
        compiler_params=pltpu.CompilerParams(dimension_semantics=("arbitrary",)),
        cost_estimate=pl.CostEstimate(flops=10**9, bytes_accessed=4 * shared.size, transcendentals=0),
        name="merge_tables",
    )(starts.reshape(-1), exps, layers, shared)


def weight_grad_body(exps, tiles, begins, u_own, u_oth, d_own, d_oth, idx_all, gate_ref, *refs, parts, n_exp, n_alias, first_list,
                     page):
    g_ref, up_ref, w_ref = refs[:3]
    (dg_ref, du_ref, dw_ref, og_ref, ou_ref, ow_ref,
     uds, rows, u0, c0, d0, h0, u1, c1, d1, h1, gacc, wacc, idx_s, sem, tsem) = refs[3 + n_alias:]
    e = pl.program_id(0)
    ff = g_ref.shape[2]
    slots = 3
    both = ((u0, c0, d0, h0), (u1, c1, d1, h1))

    def table_copy(exp):
        slot = lax.rem(exp, slots)
        at = pl.multiple_of((first_list + exp) * page, PAGE)
        to = pl.multiple_of(slot * page, PAGE)
        return pltpu.make_async_copy(idx_all.at[pl.ds(at, page)], idx_s.at[pl.ds(to, page)], tsem.at[slot])

    def gather_row(at, r):
        rows[pl.ds(r * PITCH, 2 * parts), :] = uds[idx_s[at]].astype(jnp.float32)

    def column(first, count, k):
        return rows[pl.ds(first * PITCH + k, count, stride=PITCH), :]

    @pl.when(e == 0)
    def _():
        n_half = u_own.shape[0]
        copies = [pltpu.make_async_copy(src, uds.at[pl.ds((k % 2) * n_half, n_half), pl.ds((k // 2) * parts, parts)], sem.at[k])
                  for k, src in enumerate((u_own, u_oth, d_own, d_oth))]
        for c in copies:
            c.start()
        table_copy(0).start()
        table_copy(1).start()
        n_rows = n_half * 2
        uds[pl.ds(n_rows, 8)] = jnp.zeros((8, 2 * parts, LANES), jnp.bfloat16)
        for ref in (*both[0], *both[1], gacc, wacc):
            clear(ref)
        table_copy(0).wait()
        for c in copies:
            c.wait()

        def first_rows(q, carry):
            for r in range(16):
                gather_row(q * 16 + r, q * 16 + r)
            return carry

        lax.fori_loop(0, WTILE // 16, first_rows, 0)

    @pl.when(e + 1 < n_exp)
    def _():
        table_copy(e + 1).wait()

    @pl.when(e + 2 < n_exp)
    def _():
        table_copy(e + 2).start()

    here = lax.rem(e, slots) * page
    there = lax.rem(jnp.minimum(e + 1, n_exp - 1), slots) * page
    n_tiles = tiles[e]
    begin = begins[e]
    gate_rows = WTILE // LANES

    def compute(j, new, old):
        un, cn, dn, hn = new
        uo, co, do, ho = old
        gacc[...] += nn_dot(do[...], uo[...])
        wacc[...] += nn_dot(ho[...], co[...])
        un[...] = jnp.concatenate([column(0, WTILE, k) for k in range(parts)], axis=1).astype(jnp.bfloat16)
        gates = [spread_column(gate_ref[0, pl.ds(j * gate_rows + q, 1), :]) for q in range(gate_rows)]
        for k in range(parts):
            for q in range(gate_rows):
                d = column(q * LANES, LANES, parts + k)
                cn[q * LANES:(q + 1) * LANES, k * LANES:(k + 1) * LANES] = (d * gates[q]).astype(jnp.bfloat16)
        ab = nt_dot(jnp.concatenate([g_ref[0, 0], up_ref[0, 0]], axis=0), un[...])
        dh = nt_dot(w_ref[0, 0], cn[...])
        nxt = jnp.where(j + 1 < n_tiles, here + (j + 1) * WTILE, there)
        for r in range(WTILE):
            gather_row(nxt + r, r)
        a, b = ab[:ff], ab[ff:]
        s = jax.nn.sigmoid(a)
        act = a * s
        hn[...] = (act * b).astype(jnp.bfloat16)
        dn[:ff] = (dh * b * (s * (1.0 + a * (1.0 - s)))).astype(jnp.bfloat16)
        dn[ff:] = (dh * act).astype(jnp.bfloat16)

    def tile(j, carry):
        odd = lax.rem(begin + j, 2)

        @pl.when(odd == 0)
        def _():
            compute(j, both[0], both[1])

        @pl.when(odd == 1)
        def _():
            compute(j, both[1], both[0])

        @pl.when(j == 0)
        def _():
            dg = gacc[:ff].astype(jnp.bfloat16)
            du = gacc[ff:].astype(jnp.bfloat16)
            dw = wacc[...].astype(jnp.bfloat16)
            dg_ref[0, 0], du_ref[0, 0], dw_ref[0, 0] = dg, du, dw
            og_ref[0], ou_ref[0], ow_ref[0] = dg, du, dw
            gacc[...] = jnp.zeros_like(gacc)
            wacc[...] = jnp.zeros_like(wacc)

        return carry

    lax.fori_loop(0, n_tiles, tile, 0)


def weight_grads(layer, first, exps, tiles, rows, idx_all, gates, weights, full):
    n_half, parts, _ = rows[0].shape
    n_tok = 2 * n_half
    n_layers, n_local, ff, d_model = weights[0].shape
    n_exp = exps.shape[0]
    out_rows = gates.shape[1]
    page = out_rows * LANES
    tiles = jnp.concatenate([tiles, jnp.ones((1,), jnp.int32)])
    begins = jnp.cumsum(tiles) - tiles
    any_spec = pl.BlockSpec(memory_space=pl.ANY)
    mine = pl.BlockSpec((1, 1, ff, d_model), lambda e, exps, *_: (layer, exps[jnp.minimum(e, n_exp - 1)], 0, 0))
    done = pl.BlockSpec((1, 1, ff, d_model), lambda e, exps, *_: (layer, exps[jnp.maximum(e - 1, 0)], 0, 0))
    half = pl.BlockSpec((1, ff, d_model), lambda e, *_: (jnp.maximum(e - 1, 0), 0, 0))
    gate_spec = pl.BlockSpec((1, out_rows, LANES), lambda e, *_: (first + jnp.minimum(e, n_exp - 1), 0, 0))
    aliased = list(full) if full is not None else []
    tile_set = [pltpu.VMEM((WTILE, d_model), jnp.bfloat16)] * 2 + [pltpu.VMEM((2 * ff, WTILE), jnp.bfloat16),
                                                                 pltpu.VMEM((ff, WTILE), jnp.bfloat16)]
    outs = pl.pallas_call(
        functools.partial(weight_grad_body, parts=parts, n_exp=n_exp, n_alias=len(aliased), first_list=first, page=page),
        grid_spec=pltpu.PrefetchScalarGridSpec(
            num_scalar_prefetch=3,
            grid=(n_exp + 1,),
            in_specs=[any_spec] * 5 + [gate_spec] + [mine] * 3 + [any_spec] * len(aliased),
            out_specs=[done] * 3 + [half] * 3,
            scratch_shapes=[pltpu.VMEM((n_tok + 8, 2 * parts, LANES), jnp.bfloat16)]
            + [pltpu.VMEM((WTILE * PITCH + 16, LANES), jnp.float32)] + tile_set * 2
            + [pltpu.VMEM((2 * ff, d_model), jnp.float32), pltpu.VMEM((ff, d_model), jnp.float32),
               pltpu.SMEM((3 * page,), jnp.int32), pltpu.SemaphoreType.DMA((4,)), pltpu.SemaphoreType.DMA((3,))],
        ),
        out_shape=[jax.ShapeDtypeStruct((n_layers, n_local, ff, d_model), jnp.bfloat16)] * 3
        + [jax.ShapeDtypeStruct((n_exp, ff, d_model), jnp.bfloat16)] * 3,
        input_output_aliases={12 + k: k for k in range(len(aliased))},
        compiler_params=pltpu.CompilerParams(dimension_semantics=("arbitrary",), vmem_limit_bytes=VMEM_LIMIT),
        cost_estimate=pl.CostEstimate(flops=6 * n_tok * n_exp * d_model * ff,
                                      bytes_accessed=n_tok * d_model * 4 + 9 * n_exp * ff * d_model * 2, transcendentals=0),
        name="weight_grads",
    )(exps, tiles, begins, *rows, idx_all, gates, *weights, *aliased)
    return outs[:3], outs[3:]


def merge_body(exps, a, b, c, f0, f1, f2, o0, o1, o2, buf, in_sem, out_sem, *, layer, n_exp):
    halves, wholes = (a, b, c), (o0, o1, o2)

    def arrive(k, q):
        return pltpu.make_async_copy(halves[k].at[q], buf.at[k, q], in_sem.at[k, q])

    def leave(k, q):
        return pltpu.make_async_copy(buf.at[k, q], wholes[k].at[layer, exps[q]], out_sem)

    def each(act):
        def one(q, carry):
            for k in range(3):
                act(k, q)
            return carry

        lax.fori_loop(0, n_exp, one, 0)

    def pass_on(k, q):
        arrive(k, q).wait()
        leave(k, q).start()

    each(lambda k, q: arrive(k, q).start())
    each(pass_on)
    each(lambda k, q: leave(k, q).wait())


def merge_half(layer, exps, half, full):
    n_exp, ff, d_model = half[0].shape
    any_spec = pl.BlockSpec(memory_space=pl.ANY)
    return pl.pallas_call(
        functools.partial(merge_body, layer=layer, n_exp=n_exp),
        grid_spec=pltpu.PrefetchScalarGridSpec(
            num_scalar_prefetch=1, grid=(1,), in_specs=[any_spec] * 6, out_specs=[any_spec] * 3,
            scratch_shapes=[pltpu.VMEM((3, n_exp, ff, d_model), jnp.bfloat16), pltpu.SemaphoreType.DMA((3, n_exp)),
                            pltpu.SemaphoreType.DMA]),
        out_shape=[jax.ShapeDtypeStruct(x.shape, x.dtype) for x in full],
        input_output_aliases={4: 0, 5: 1, 6: 2},
        compiler_params=pltpu.CompilerParams(dimension_semantics=("arbitrary",), vmem_limit_bytes=VMEM_LIMIT),
        cost_estimate=pl.CostEstimate(flops=10**9, bytes_accessed=6 * n_exp * ff * d_model * 2, transcendentals=0),
        name="merge_half",
    )(exps, *half, *full)


def route_tables(ids, gates, ep, n_local):
    n_src, top_k, tok = ids.shape
    n = n_src * top_k * tok
    local = ids - ep * n_local
    here = (local >= 0) & (local < n_local)
    group = jnp.where(here, local, n_local).reshape(-1)
    key, gate = lax.sort((group * n + jnp.arange(n, dtype=jnp.int32), gates.reshape(-1)), num_keys=1, is_stable=False)
    copy = key % n
    token = copy // (top_k * tok) * tok + copy % tok
    token = jnp.pad(token, (0, 2 * PAGE))
    gate = jnp.pad(gate, (0, 2 * PAGE)).reshape(-1, LANES)
    lane = jnp.arange(LANES, dtype=jnp.int32)
    bounds = jnp.sum((group[:, None] < lane[None, :]).astype(jnp.int32), axis=0)
    own = jnp.sum((group[:n // n_src, None] == lane[None, :]).astype(jnp.int32), axis=0)
    starts, ends = bounds[:n_local], bounds[1:n_local + 1]
    middle = starts + own[:n_local]
    runs = [jnp.concatenate(x) for x in ((starts, middle), (middle, ends), (starts, ends))]
    return runs, token, gate, bounds


def deal_experts(bounds, n_local, n_lists):
    load = jnp.sum(bounds[:, 1:n_local + 1] - bounds[:, :n_local], axis=0)
    ids = jnp.arange(n_local, dtype=jnp.int32)
    ahead = (load[None, :] > load[:, None]) | ((load[None, :] == load[:, None]) & (ids[None, :] < ids[:, None]))
    rank = jnp.sum(ahead.astype(jnp.int32), axis=1)
    turn, which = jnp.arange(n_local // n_lists)[None, :], jnp.arange(n_lists)[:, None]
    want = n_lists * turn + jnp.where(turn % 2 == 0, which, n_lists - 1 - which)
    pick = (rank[None, None, :] == want[:, :, None]).astype(jnp.int32)
    tiles = jnp.maximum((jnp.sum(pick * load, axis=2) + WTILE - 1) // WTILE, 1)
    return jnp.sum(pick * ids, axis=2), tiles


def after(x, *earlier):
    return lax.optimization_barrier((x, *earlier))[0]


def solution(mesh):
    ep_size = mesh.shape['ep']
    dp_size = mesh.shape['dp']
    tok_spec = P(('dp', 'ep'), None)
    route_spec = P(None, ('dp', 'ep'), None)
    whole_spec = P(None, None, None)
    expert_spec = P(None, 'ep', None, None)
    ep_pairs = [(i, 1 - i) for i in range(ep_size)]
    core_pairs = [(i, i ^ 1) for i in range(dp_size)]
    chip_pairs = [(i, i ^ (2 << i % 2)) for i in range(dp_size)]

    def device_body(tokens, d_out, expert_ids, gate_vals, w_mix, w_gate, w_up, w_down):
        n_layers = w_mix.shape[0]
        n_local = w_gate.shape[1]
        n_experts = n_local * ep_size
        tok, d_model = tokens.shape
        top_k = expert_ids.shape[2]
        parts = d_model // LANES
        cap = cdiv(CAP_FACTOR * tok * top_k, n_experts)
        ep_id = lax.axis_index('ep').astype(jnp.int32)
        dp_id = lax.axis_index('dp').astype(jnp.int32)
        weights = (jnp.swapaxes(w_gate, 2, 3), jnp.swapaxes(w_up, 2, 3), w_down)

        def swap(x):
            return lax.ppermute(x, 'ep', ep_pairs)

        def spread(x):
            return lax.all_gather(x, 'dp', axis=0, tiled=True)

        def trade(x, pairs):
            return [lax.ppermute(y, 'dp', pairs) for y in x]

        def slab(x):
            return x.reshape(tok, parts, LANES)

        def mixed(x, layer):
            return (x.astype(jnp.float32) + jnp.dot(x, w_mix[layer], preferred_element_type=jnp.float32)).astype(jnp.bfloat16)

        ids = jnp.swapaxes(expert_ids, 1, 2)
        gates = jnp.swapaxes(gate_vals, 1, 2)
        mine = jnp.stack([ids.astype(jnp.float32), gates])
        u = mixed(tokens, 0)
        u_slab = slab(u)
        theirs = swap(after(mine, u_slab))
        both = jnp.stack([mine, theirs], 2)
        top = n_layers - 1
        runs, tables, packed = [], [], []

        def add_tables(pair):
            run, token, gate, bounds = route_tables(pair[0].astype(jnp.int32), pair[1], ep_id, n_local)
            runs.append(run)
            tables.append([(token * parts, gate), (token * (2 * parts), gate)])
            spot = lax.div(token, tok) * (dp_size * tok) + dp_id * tok + lax.rem(token, tok)
            first = jnp.concatenate([spot.reshape(-1, LANES), jnp.pad(bounds.reshape(1, LANES), ((0, 7), (0, 0)))])
            packed.append(jnp.stack([first.astype(jnp.float32), jnp.pad(gate, ((0, 8), (0, 0)))]))

        add_tables(both[:, 0])

        x_in, u_slabs, u_others, xs = tokens, [u_slab], [swap(u_slab)], []
        d_slab = slab(d_out)
        d_other = swap(after(d_slab, u_others[0]))
        d_rows = (spread(d_slab), spread(d_other))
        for layer in range(n_layers):
            if layer:
                u = mixed(x_in, layer)
                u_slabs.append(slab(u))
                u_others.append(swap(u_slabs[layer]))
            xs.append(x_in)
            if layer < top:
                other, = token_kernel(layer, runs[layer][1], tables[layer][0], (u_slabs[layer], u_others[layer]), weights, (1,))
                sent = swap(other)
                own, = token_kernel(layer, runs[layer][0], tables[layer][0], (after(u_slabs[layer], other), u_others[layer]),
                                    weights, (0,))
                add_tables(after(both[:, layer + 1], own))
                x_in = (u.astype(jnp.float32) + own + sent).astype(jnp.bfloat16)

        shared = lax.all_gather(jnp.stack(packed), 'dp', axis=0)
        starts = shared[:, :, 0, -8].astype(jnp.int32)
        core = dp_id % 2
        kind = (dp_id // 2 + dp_id // 4) % 2
        dealt = [deal_experts(starts[:, layer], n_local, 4 if layer == top else 2) for layer in range(n_layers)]
        places = [2 * kind + core if layer == top else core for layer in range(n_layers)]
        mine = [lists[place] for (lists, _), place in zip(dealt, places)]
        firsts = [sum(x.shape[0] for x in mine[:layer]) for layer in range(n_layers)]
        list_rows = cdiv(cdiv(dp_size * 2 * cap, LANES), 8) * 8 + 8
        idx_all, gate_all = merge_tables(shared, starts, jnp.concatenate(mine),
                                         jnp.concatenate([jnp.full_like(x, layer) for layer, x in enumerate(mine)]),
                                         list_rows, dp_size * 2 * tok)
        idx_all = idx_all.reshape(-1)

        d_y, full, arrived = d_out, None, []
        d_mix = [None] * n_layers
        for layer in reversed(range(n_layers)):
            u_rows = tuple(spread(x) for x in (u_slabs[layer], u_others[layer]))
            slabs = (u_slabs[layer], u_others[layer], d_slab, d_other)
            own, other = token_kernel(layer, runs[layer][2], tables[layer][1], slabs, weights)
            d_u = (d_y.astype(jnp.float32) + own + swap(other)).astype(jnp.bfloat16)
            last = other
            if layer == top:
                y_own, last = token_kernel(top, runs[top][2], tables[top][0], (after(u_slabs[top], other), u_others[top]), weights)
            d_mix[layer] = jnp.einsum('td,te->de', xs[layer], d_u, preferred_element_type=jnp.float32).astype(jnp.bfloat16)
            d_y = (d_u.astype(jnp.float32)
                   + jnp.einsum('te,de->td', d_u, w_mix[layer], preferred_element_type=jnp.float32)).astype(jnp.bfloat16)
            tiles = dealt[layer][1][places[layer]]
            full, part = weight_grads(layer, firsts[layer], mine[layer], after(tiles, last), u_rows + d_rows, idx_all, gate_all,
                                      weights, full)
            lists = dealt[layer][0]
            if layer == top:
                far = trade(part, chip_pairs)
                near = trade(part, core_pairs)
                arrived.append((layer, lists[2 * kind + 1 - core], near))
                arrived.append((layer, lists[2 - 2 * kind + core], far))
                arrived.append((layer, lists[3 - 2 * kind - core], trade(far, core_pairs)))
            else:
                arrived.append((layer, lists[1 - core], trade(part, core_pairs)))
            if layer:
                d_slab = slab(d_y)
                d_other = swap(d_slab)
                d_rows = (spread(d_slab), spread(d_other))
                if layer == top:
                    layer_out = (u.astype(jnp.float32) + y_own + swap(after(last, d_other))).astype(jnp.bfloat16)
        for layer, names, part in arrived:
            full = merge_half(layer, names, part, full)
        d_mix = lax.psum(jnp.stack(d_mix), ('dp', 'ep'))
        return (layer_out, d_y, d_mix, jnp.swapaxes(full[0], 2, 3), jnp.swapaxes(full[1], 2, 3), full[2])

    return jax.shard_map(device_body, mesh=mesh,
                         in_specs=(tok_spec, tok_spec, route_spec, route_spec, whole_spec,
                                   expert_spec, expert_spec, expert_spec),
                         out_specs=(tok_spec, tok_spec, whole_spec, expert_spec, expert_spec, expert_spec),
                         check_vma=False)
```

```python
import functools
import math

import jax
import jax.numpy as jnp
from jax import lax
from jax.experimental import pallas as pl
from jax.experimental.pallas import tpu as pltpu
from jax.sharding import PartitionSpec as P


CAP_FACTOR = 3
LANES = 128
TILE = 96
HALF_TILE = 64
WTILE = 768
SOURCES = 8
CHUNK = 256
PITCH = 9
BATCH = 16
SLOTS = 8
PAGE = 1024
VMEM_LIMIT = 62 * 2**20


def cdiv(a, b):
    return (a + b - 1) // b


def nt_dot(a, b):
    return lax.dot_general(a, b, (((1,), (1,)), ((), ())), preferred_element_type=jnp.float32)


def tn_dot(a, b):
    return lax.dot_general(a, b, (((0,), (0,)), ((), ())), preferred_element_type=jnp.float32)


def nn_dot(a, b):
    return lax.dot_general(a, b, (((1,), (0,)), ((), ())), preferred_element_type=jnp.float32)


def clear(ref):
    step = next(n for n in (64, 48, 32, 16, 8) if ref.shape[0] % n == 0)

    def one(q, carry):
        ref[pl.ds(pl.multiple_of(q * step, step), step), :] = jnp.zeros((step, ref.shape[1]), ref.dtype)
        return carry

    lax.fori_loop(0, ref.shape[0] // step, one, 0)


def add_rows(acc, vals_ref, idx, row, tile, pitch, width):
    for b in range(0, tile, BATCH):
        at = [pl.multiple_of(idx[row + b + r], 4) for r in range(BATCH)]
        vals = [acc[pl.ds(at[r], width), :] + vals_ref[pl.ds((b + r) * pitch, width), :] for r in range(BATCH)]
        for r in reversed(range(BATCH)):
            acc[pl.ds(at[r], width), :] = vals[r]


def spread_column(row):
    return jnp.broadcast_to(row, (LANES, LANES)).T


def tile_gates(gates, row):
    pair = gates[pl.ds(lax.div(row, LANES), 2), :]
    skip = lax.rem(row, LANES)
    pair = pltpu.roll(pair, lax.rem(LANES - skip, LANES), 1)
    lane = lax.broadcasted_iota(jnp.int32, (1, LANES), 1)
    return spread_column(jnp.where(lane < LANES - skip, pair[:1], pair[1:]))


def widen(src, dst, pitch, halves, tok):
    step = 8

    def one(q, carry):
        for r in range(step):
            dst[pl.ds((q * step + r) * pitch, pitch), :] = src[q * step + r].astype(jnp.float32)
        return carry

    lax.fori_loop(halves[0] * tok // step, (halves[-1] + 1) * tok // step, one, 0)


def write_sums(acc, outs, tok, parts, pitch, halves):
    step = min(32, tok)

    def copy_out(q, carry):
        r0 = pl.multiple_of(q * step, step)
        for k in range(parts):
            for out, half in zip(outs, halves):
                first = (half * tok + r0) * pitch + k
                out[pl.ds(r0, step), k * LANES:(k + 1) * LANES] = acc[pl.ds(first, step, stride=pitch), :]
        return carry

    lax.fori_loop(0, tok // step, copy_out, 0)


def expert_copies(weights, buf, sem, layer, e):
    slot = lax.rem(e, SLOTS)
    ff = weights[0].shape[2]
    return [pltpu.make_async_copy(w.at[layer, e], buf.at[slot, pl.ds(k * ff, ff)], sem.at[slot])
            for k, w in enumerate(weights)]


def run_tiles(step, weights, wbuf, wsem, runs, tile, layer, prepare):
    n_local = weights[0].shape[1]
    for e in range(SLOTS - 2):
        for c in expert_copies(weights, wbuf, wsem, layer, e):
            c.start()
    prepare()
    for c in expert_copies(weights, wbuf, wsem, layer, 0):
        c.wait()

    def length(e):
        return runs[n_local + e] - runs[e]

    def add_tiles(e, total):
        return total + jnp.maximum(lax.div(length(e) + tile - 1, tile), 1)

    def one(i, carry):
        (e, row, left), (e1, row1, n1), (e2, row2, n2), row3 = carry

        @pl.when(e != e1)
        def _():
            for c in expert_copies(weights, wbuf, wsem, layer, e):
                c.wait()

        @pl.when((e != e1) & (e + SLOTS - 3 < n_local))
        def _():
            for c in expert_copies(weights, wbuf, wsem, layer, e + SLOTS - 3):
                c.start()

        step(row, (lax.rem(e1, SLOTS), row1), (lax.rem(e2, SLOTS), row2, n2), row3)
        more = left > tile
        e_next = jnp.minimum(e + 1, n_local - 1)
        fresh = jnp.where(e + 1 < n_local, length(e_next), 0)
        ahead = (jnp.where(more, e, e_next), jnp.where(more, row + tile, runs[e_next]), jnp.where(more, left - tile, fresh))
        return ahead, (e, row, jnp.minimum(left, tile)), (e1, row1, n1), row2

    none = (0, 0, 0)
    lax.fori_loop(0, lax.fori_loop(0, n_local, add_tiles, 0) + 3, one, ((0, runs[0], length(0)), none, none, 0))


def token_body(runs, idx, gates, *refs, layer, tok, parts, tile, halves, backward):
    n_in = 4 if backward else 2
    sources, weights, outs, refs = refs[:n_in], refs[n_in:n_in + 3], refs[n_in + 3:n_in + 3 + len(halves)], refs[n_in + 3 + len(halves):]
    narrow, wide, rows, vt, acc, mid, wbuf, sem, wsem = refs
    ff = weights[0].shape[2]
    width = parts * n_in // 2
    pitch = width + 1

    def prepare():
        copies = [pltpu.make_async_copy(src, narrow.at[pl.ds(k % 2 * tok, tok), pl.ds(k // 2 * parts, parts)], sem.at[k])
                  for k, src in enumerate(sources) if k % 2 in halves]
        for c in copies:
            c.start()
        for ref in (acc, vt, rows, mid):
            clear(ref)
        for c in copies:
            c.wait()
        widen(narrow, wide, width, halves, tok)

    def column(k):
        return rows[pl.ds(k, tile, stride=pitch), :]

    def step(row, here, before, done):
        slot, row1 = here
        slot2, row2, n2 = before
        old = wbuf[slot2, :2 * ff] if backward else wbuf[slot2, 2 * ff:]
        v = tn_dot(mid[...], old).astype(jnp.bfloat16).astype(jnp.float32)
        u = jnp.concatenate([column(k) for k in range(parts)], axis=1).astype(jnp.bfloat16)
        ab = nt_dot(wbuf[slot, :2 * ff], u)
        if backward:
            gate = tile_gates(gates, row1)[:tile]
            c = jnp.concatenate([(column(parts + k) * gate).astype(jnp.bfloat16) for k in range(parts)], axis=1)
            dh = nt_dot(wbuf[slot, 2 * ff:], c)
        add_rows(acc, vt, idx, done, tile, parts + 1, parts)
        for r in range(tile):
            rows[pl.ds(pitch * r, width), :] = wide[pl.ds(pl.multiple_of(idx[row + r], width), width), :]
        live = lax.broadcasted_iota(jnp.int32, (tile, LANES), 0) < n2
        gate = tile_gates(gates, row2)[:tile]
        for k in range(parts):
            v_k = jnp.where(live, v[:, k * LANES:(k + 1) * LANES] * gate, 0.0)
            vt[pl.ds(k, tile, stride=parts + 1), :] = v_k
        a, b = ab[:ff], ab[ff:]
        s = jax.nn.sigmoid(a)
        act = a * s
        if backward:
            mid[:ff] = (dh * b * (s * (1.0 + a * (1.0 - s)))).astype(jnp.bfloat16)
            mid[ff:] = (dh * act).astype(jnp.bfloat16)
        else:
            mid[...] = (act * b).astype(jnp.bfloat16)

    run_tiles(step, weights, wbuf, wsem, runs, tile, layer, prepare)
    write_sums(acc, outs, tok, parts, width, halves)


def token_kernel(layer, runs, table, slabs, weights, halves=(0, 1)):
    idx, gates = table
    tok, parts, _ = slabs[0].shape
    _, n_local, ff, d_model = weights[0].shape
    backward = len(slabs) > 2
    tile = TILE if len(halves) == 2 else HALF_TILE
    width = parts * len(slabs) // 2
    rows_spec = pl.BlockSpec((tok, d_model), lambda i, *_: (0, 0))
    any_spec = pl.BlockSpec(memory_space=pl.ANY)
    tile_rows = cdiv(tile * (width + 1), 16) * 16
    work = (4 if backward else 3) * len(halves)
    return pl.pallas_call(
        functools.partial(token_body, layer=layer, tok=tok, parts=parts, tile=tile, halves=halves, backward=backward),
        grid_spec=pltpu.PrefetchScalarGridSpec(
            num_scalar_prefetch=2,
            grid=(1,),
            in_specs=[pl.BlockSpec(gates.shape, lambda i, *_: (0, 0))] + [any_spec] * (len(slabs) + 3),
            out_specs=[rows_spec] * len(halves),
            scratch_shapes=[pltpu.VMEM((2 * tok, width, LANES), jnp.bfloat16), pltpu.VMEM((2 * tok * width, LANES), jnp.float32),
                            pltpu.VMEM((tile_rows, LANES), jnp.float32), pltpu.VMEM((tile_rows, LANES), jnp.float32),
                            pltpu.VMEM((2 * tok * width, LANES), jnp.float32),
                            pltpu.VMEM((2 * ff if backward else ff, tile), jnp.bfloat16),
                            pltpu.VMEM((SLOTS, 3 * ff, d_model), jnp.bfloat16),
                            pltpu.SemaphoreType.DMA((len(slabs),)), pltpu.SemaphoreType.DMA((SLOTS,))],
        ),
        out_shape=[jax.ShapeDtypeStruct((tok, d_model), jnp.float32)] * len(halves),
        compiler_params=pltpu.CompilerParams(dimension_semantics=("arbitrary",), vmem_limit_bytes=VMEM_LIMIT),
        cost_estimate=pl.CostEstimate(flops=work * 2 * 8 * tok * d_model * ff * 4,
                                      bytes_accessed=3 * n_local * ff * d_model * 2, transcendentals=0),
        name="experts_backward" if backward else "experts_forward",
    )(runs, idx, gates, *slabs, *weights)


def merge_tables_body(st, exps, layers, table, idx_ref, gate_ref, buf, *, out_rows, pad_row):
    group = idx_ref.shape[0]

    def one(q, carry):
        item = pl.program_id(0) * group + q
        merge_expert(exps[item], layers[item], st, table, idx_ref.at[q], gate_ref.at[q], buf, out_rows, pad_row)
        return carry

    lax.fori_loop(0, group, one, 0)


def merge_expert(exp, layer, st, table, idx_out, gate_out, buf, out_rows, pad_row):
    src, n_layers = table.shape[:2]
    buf[0] = jnp.full(buf.shape[1:], float(pad_row), jnp.float32)
    buf[1] = jnp.zeros(buf.shape[1:], jnp.float32)
    row = lax.broadcasted_iota(jnp.int32, (8, LANES), 0)
    lane = lax.broadcasted_iota(jnp.int32, (8, LANES), 1)
    off = 0
    for d in range(src):
        at = (d * n_layers + layer) * LANES + exp
        first = st[at]
        count = st[at + 1] - first
        to = lax.rem(off, LANES) + LANES
        shift = to - lax.rem(first, LANES)
        over = lax.rem(shift, LANES)
        start = lax.div(off, LANES)
        place = row * LANES + lane
        take = (place >= to) & (place < to + count)
        for kind in range(2):
            x = table[d, layer, kind, pl.ds(lax.div(first, LANES), 8), :]
            x = pltpu.roll(pltpu.roll(x, over, 1), lax.div(shift, LANES), 0)
            x = jnp.where(lane >= over, x, pltpu.roll(x, 1, 0))
            old = buf[kind, pl.ds(start, 8), :]
            buf[kind, pl.ds(start, 8), :] = jnp.where(take, x, old)
        off = off + count
    idx_out[...] = buf[0, pl.ds(1, out_rows), :].astype(jnp.int32)
    gate_out[...] = buf[1, pl.ds(1, out_rows), :]


def merge_tables(shared, starts, exps, layers, out_rows, pad_row):
    n_items = exps.shape[0]
    group = math.gcd(n_items, 8)
    out = pl.BlockSpec((group, out_rows, LANES), lambda g, *_: (g, 0, 0))
    return pl.pallas_call(
        functools.partial(merge_tables_body, out_rows=out_rows, pad_row=pad_row),
        grid_spec=pltpu.PrefetchScalarGridSpec(
            num_scalar_prefetch=3,
            grid=(n_items // group,),
            in_specs=[pl.BlockSpec(shared.shape, lambda g, *_: (0,) * shared.ndim)],
            out_specs=[out] * 2,
            scratch_shapes=[pltpu.VMEM((2, out_rows + 16, LANES), jnp.float32)],
        ),
        out_shape=[jax.ShapeDtypeStruct((n_items, out_rows, LANES), jnp.int32),
                   jax.ShapeDtypeStruct((n_items, out_rows, LANES), jnp.float32)],
        compiler_params=pltpu.CompilerParams(dimension_semantics=("arbitrary",)),
        cost_estimate=pl.CostEstimate(flops=10**9, bytes_accessed=4 * shared.size, transcendentals=0),
        name="merge_tables",
    )(starts.reshape(-1), exps, layers, shared)


def weight_grad_body(exps, tiles, begins, *refs, parts, n_exp, n_alias, n_rows, first_list, page):
    rows_in, refs = refs[:sum(n_rows)], refs[sum(n_rows):]
    idx_all, gate_ref, g_ref, up_ref, w_ref = refs[:5]
    (dg_ref, du_ref, dw_ref, og_ref, ou_ref, ow_ref,
     uds, rows, u0, c0, d0, h0, u1, c1, d1, h1, gacc, wacc, idx_s, sem, tsem) = refs[5 + n_alias:]
    e = pl.program_id(0)
    ff = g_ref.shape[2]
    slots = 3
    both = ((u0, c0, d0, h0), (u1, c1, d1, h1))

    def table_copy(exp):
        slot = lax.rem(exp, slots)
        at = pl.multiple_of((first_list + exp) * page, PAGE)
        to = pl.multiple_of(slot * page, PAGE)
        return pltpu.make_async_copy(idx_all.at[pl.ds(at, page)], idx_s.at[pl.ds(to, page)], tsem.at[slot])

    def gather_row(at, r):
        rows[pl.ds(r * PITCH, 2 * parts), :] = uds[idx_s[at]].astype(jnp.float32)

    def column(first, count, k):
        return rows[pl.ds(first * PITCH + k, count, stride=PITCH), :]

    @pl.when(e == 0)
    def _():
        n_tok = uds.shape[0] - 8
        copies = []
        for kind, arrays in enumerate((rows_in[:n_rows[0]], rows_in[n_rows[0]:])):
            part = pl.ds(kind * parts, parts)
            if len(arrays) == 1:
                copies.append(pltpu.make_async_copy(arrays[0], uds.at[pl.ds(0, n_tok), part], sem.at[kind]))
                continue
            run = n_tok // (2 * SOURCES)
            for q in range(2 * SOURCES):
                copies.append(pltpu.make_async_copy(arrays[q % 2].at[pl.ds(q // 2 * run, run)],
                                                    uds.at[pl.ds(q * run, run), part], sem.at[kind]))
        for c in copies:
            c.start()
        table_copy(0).start()
        table_copy(1).start()
        uds[pl.ds(n_tok, 8)] = jnp.zeros((8, 2 * parts, LANES), jnp.bfloat16)
        for ref in (*both[0], *both[1], gacc, wacc):
            clear(ref)
        table_copy(0).wait()
        for c in copies:
            c.wait()

        def first_rows(q, carry):
            for r in range(16):
                gather_row(q * 16 + r, q * 16 + r)
            return carry

        lax.fori_loop(0, WTILE // 16, first_rows, 0)

    @pl.when(e + 1 < n_exp)
    def _():
        table_copy(e + 1).wait()

    @pl.when(e + 2 < n_exp)
    def _():
        table_copy(e + 2).start()

    here = lax.rem(e, slots) * page
    there = lax.rem(jnp.minimum(e + 1, n_exp - 1), slots) * page
    n_tiles = tiles[e]
    begin = begins[e]
    gate_rows = WTILE // LANES

    def compute(j, new, old):
        un, cn, dn, hn = new
        uo, co, do, ho = old
        gacc[...] += nn_dot(do[...], uo[...])
        wacc[...] += nn_dot(ho[...], co[...])
        nxt = jnp.where(j + 1 < n_tiles, here + (j + 1) * WTILE, there)
        gu = jnp.concatenate([g_ref[0, 0], up_ref[0, 0]], axis=0)
        for q in range(0, WTILE, CHUNK):
            part = slice(q, q + CHUNK)
            un[part] = jnp.concatenate([column(q, CHUNK, k) for k in range(parts)], axis=1).astype(jnp.bfloat16)
            for p in range(q, q + CHUNK, LANES):
                gate = spread_column(gate_ref[0, pl.ds(j * gate_rows + p // LANES, 1), :])
                for k in range(parts):
                    d = column(p, LANES, parts + k)
                    cn[p:p + LANES, k * LANES:(k + 1) * LANES] = (d * gate).astype(jnp.bfloat16)
            ab = nt_dot(gu, un[part])
            dh = nt_dot(w_ref[0, 0], cn[part])
            for r in range(q, q + CHUNK):
                gather_row(nxt + r, r)
            a, b = ab[:ff], ab[ff:]
            s = jax.nn.sigmoid(a)
            act = a * s
            hn[:, part] = (act * b).astype(jnp.bfloat16)
            dn[:ff, part] = (dh * b * (s * (1.0 + a * (1.0 - s)))).astype(jnp.bfloat16)
            dn[ff:, part] = (dh * act).astype(jnp.bfloat16)

    def tile(j, carry):
        odd = lax.rem(begin + j, 2)

        @pl.when(odd == 0)
        def _():
            compute(j, both[0], both[1])

        @pl.when(odd == 1)
        def _():
            compute(j, both[1], both[0])

        @pl.when(j == 0)
        def _():
            dg = gacc[:ff].astype(jnp.bfloat16)
            du = gacc[ff:].astype(jnp.bfloat16)
            dw = wacc[...].astype(jnp.bfloat16)
            dg_ref[0, 0], du_ref[0, 0], dw_ref[0, 0] = dg, du, dw
            og_ref[0], ou_ref[0], ow_ref[0] = dg, du, dw
            gacc[...] = jnp.zeros_like(gacc)
            wacc[...] = jnp.zeros_like(wacc)

        return carry

    lax.fori_loop(0, n_tiles, tile, 0)


def weight_grads(layer, first, exps, tiles, rows, idx_all, gates, weights, full):
    parts = rows[0][0].shape[1]
    n_tok = sum(x.shape[0] for x in rows[0])
    n_layers, n_local, ff, d_model = weights[0].shape
    n_exp = exps.shape[0]
    out_rows = gates.shape[1]
    page = out_rows * LANES
    tiles = jnp.concatenate([tiles, jnp.ones((1,), jnp.int32)])
    begins = jnp.cumsum(tiles) - tiles
    any_spec = pl.BlockSpec(memory_space=pl.ANY)
    mine = pl.BlockSpec((1, 1, ff, d_model), lambda e, exps, *_: (layer, exps[jnp.minimum(e, n_exp - 1)], 0, 0))
    done = pl.BlockSpec((1, 1, ff, d_model), lambda e, exps, *_: (layer, exps[jnp.maximum(e - 1, 0)], 0, 0))
    half = pl.BlockSpec((1, ff, d_model), lambda e, *_: (jnp.maximum(e - 1, 0), 0, 0))
    gate_spec = pl.BlockSpec((1, out_rows, LANES), lambda e, *_: (first + jnp.minimum(e, n_exp - 1), 0, 0))
    aliased = list(full) if full is not None else []
    tile_set = [pltpu.VMEM((WTILE, d_model), jnp.bfloat16)] * 2 + [pltpu.VMEM((2 * ff, WTILE), jnp.bfloat16),
                                                                 pltpu.VMEM((ff, WTILE), jnp.bfloat16)]
    outs = pl.pallas_call(
        functools.partial(weight_grad_body, parts=parts, n_exp=n_exp, n_alias=len(aliased),
                          n_rows=[len(x) for x in rows], first_list=first, page=page),
        grid_spec=pltpu.PrefetchScalarGridSpec(
            num_scalar_prefetch=3,
            grid=(n_exp + 1,),
            in_specs=[any_spec] * (sum(len(x) for x in rows) + 1) + [gate_spec] + [mine] * 3 + [any_spec] * len(aliased),
            out_specs=[done] * 3 + [half] * 3,
            scratch_shapes=[pltpu.VMEM((n_tok + 8, 2 * parts, LANES), jnp.bfloat16)]
            + [pltpu.VMEM((WTILE * PITCH + 16, LANES), jnp.float32)] + tile_set * 2
            + [pltpu.VMEM((2 * ff, d_model), jnp.float32), pltpu.VMEM((ff, d_model), jnp.float32),
               pltpu.SMEM((3 * page,), jnp.int32), pltpu.SemaphoreType.DMA((2,)), pltpu.SemaphoreType.DMA((3,))],
        ),
        out_shape=[jax.ShapeDtypeStruct((n_layers, n_local, ff, d_model), jnp.bfloat16)] * 3
        + [jax.ShapeDtypeStruct((n_exp, ff, d_model), jnp.bfloat16)] * 3,
        input_output_aliases={sum(len(x) for x in rows) + 8 + k: k for k in range(len(aliased))},
        compiler_params=pltpu.CompilerParams(dimension_semantics=("arbitrary",), vmem_limit_bytes=VMEM_LIMIT),
        cost_estimate=pl.CostEstimate(flops=6 * n_tok * n_exp * d_model * ff,
                                      bytes_accessed=n_tok * d_model * 4 + 9 * n_exp * ff * d_model * 2, transcendentals=0),
        name="weight_grads",
    )(exps, tiles, begins, *rows[0], *rows[1], idx_all, gates, *weights, *aliased)
    return outs[:3], outs[3:]


def merge_body(exps, a, b, c, f0, f1, f2, o0, o1, o2, buf, in_sem, out_sem, *, layer, n_exp):
    halves, wholes = (a, b, c), (o0, o1, o2)

    def arrive(k, q):
        return pltpu.make_async_copy(halves[k].at[q], buf.at[k, q], in_sem.at[k, q])

    def leave(k, q):
        return pltpu.make_async_copy(buf.at[k, q], wholes[k].at[layer, exps[q]], out_sem)

    def each(act):
        def one(q, carry):
            for k in range(3):
                act(k, q)
            return carry

        lax.fori_loop(0, n_exp, one, 0)

    def pass_on(k, q):
        arrive(k, q).wait()
        leave(k, q).start()

    each(lambda k, q: arrive(k, q).start())
    each(pass_on)
    each(lambda k, q: leave(k, q).wait())


def merge_half(layer, exps, half, full):
    n_exp, ff, d_model = half[0].shape
    any_spec = pl.BlockSpec(memory_space=pl.ANY)
    return pl.pallas_call(
        functools.partial(merge_body, layer=layer, n_exp=n_exp),
        grid_spec=pltpu.PrefetchScalarGridSpec(
            num_scalar_prefetch=1, grid=(1,), in_specs=[any_spec] * 6, out_specs=[any_spec] * 3,
            scratch_shapes=[pltpu.VMEM((3, n_exp, ff, d_model), jnp.bfloat16), pltpu.SemaphoreType.DMA((3, n_exp)),
                            pltpu.SemaphoreType.DMA]),
        out_shape=[jax.ShapeDtypeStruct(x.shape, x.dtype) for x in full],
        input_output_aliases={4: 0, 5: 1, 6: 2},
        compiler_params=pltpu.CompilerParams(dimension_semantics=("arbitrary",), vmem_limit_bytes=VMEM_LIMIT),
        cost_estimate=pl.CostEstimate(flops=10**9, bytes_accessed=6 * n_exp * ff * d_model * 2, transcendentals=0),
        name="merge_half",
    )(exps, *half, *full)


def join_body(a, b, out, sem):
    n = a.shape[0]
    copies = [pltpu.make_async_copy(x, out.at[pl.ds(k * n, n)], sem.at[k]) for k, x in enumerate((a, b))]
    for c in copies:
        c.start()
    for c in copies:
        c.wait()


def join_rows(a, b):
    n, parts, _ = a.shape
    any_spec = pl.BlockSpec(memory_space=pl.ANY)
    return pl.pallas_call(
        join_body, in_specs=[any_spec] * 2, out_shape=jax.ShapeDtypeStruct((2 * n, parts, LANES), a.dtype),
        out_specs=pl.BlockSpec(memory_space=pltpu.VMEM), scratch_shapes=[pltpu.SemaphoreType.DMA((2,))],
        cost_estimate=pl.CostEstimate(flops=10**8, bytes_accessed=4 * a.size * a.dtype.itemsize, transcendentals=0),
        name="join_rows",
    )(a, b)


def route_tables(ids, gates, ep, n_local):
    n_src, top_k, tok = ids.shape
    n = n_src * top_k * tok
    local = ids - ep * n_local
    here = (local >= 0) & (local < n_local)
    group = jnp.where(here, local, n_local).reshape(-1)
    key, gate = lax.sort((group * n + jnp.arange(n, dtype=jnp.int32), gates.reshape(-1)), num_keys=1, is_stable=False)
    copy = key % n
    token = copy // (top_k * tok) * tok + copy % tok
    token = jnp.pad(token, (0, 2 * PAGE))
    gate = jnp.pad(gate, (0, 2 * PAGE)).reshape(-1, LANES)
    ids = jnp.arange(n_local, dtype=jnp.int32)
    hits = jnp.sum((group.reshape(n_src, -1)[:, :, None] == ids).astype(jnp.int32), axis=1)
    starts = jnp.sum((ids[None, :] < ids[:, None]).astype(jnp.int32) * jnp.sum(hits, axis=0), axis=1)
    ends = starts + jnp.sum(hits, axis=0)
    middle = starts + hits[0]
    bounds = jnp.pad(starts, (0, LANES - n_local), constant_values=0) + jnp.where(jnp.arange(LANES) < n_local, 0, ends[-1])
    runs = [jnp.concatenate(x) for x in ((starts, middle), (middle, ends), (starts, ends))]
    return runs, token, gate, bounds


def deal_experts(bounds, n_local, n_lists):
    load = jnp.sum(bounds[:, 1:n_local + 1] - bounds[:, :n_local], axis=0)
    ids = jnp.arange(n_local, dtype=jnp.int32)
    ahead = (load[None, :] > load[:, None]) | ((load[None, :] == load[:, None]) & (ids[None, :] < ids[:, None]))
    rank = jnp.sum(ahead.astype(jnp.int32), axis=1)
    turn, which = jnp.arange(n_local // n_lists)[None, :], jnp.arange(n_lists)[:, None]
    want = n_lists * turn + jnp.where(turn % 2 == 0, which, n_lists - 1 - which)
    pick = (rank[None, None, :] == want[:, :, None]).astype(jnp.int32)
    tiles = jnp.maximum((jnp.sum(pick * load, axis=2) + WTILE - 1) // WTILE, 1)
    return jnp.sum(pick * ids, axis=2), tiles


def after(x, *earlier):
    return lax.optimization_barrier((x, *earlier))[0]


def solution(mesh):
    ep_size = mesh.shape['ep']
    dp_size = mesh.shape['dp']
    tok_spec = P(('dp', 'ep'), None)
    route_spec = P(None, ('dp', 'ep'), None)
    whole_spec = P(None, None, None)
    expert_spec = P(None, 'ep', None, None)
    ep_pairs = [(i, 1 - i) for i in range(ep_size)]
    core_pairs = [(i, i ^ 1) for i in range(dp_size)]

    def device_body(tokens, d_out, expert_ids, gate_vals, w_mix, w_gate, w_up, w_down):
        n_layers = w_mix.shape[0]
        n_local = w_gate.shape[1]
        n_experts = n_local * ep_size
        tok, d_model = tokens.shape
        top_k = expert_ids.shape[2]
        parts = d_model // LANES
        cap = cdiv(CAP_FACTOR * tok * top_k, n_experts)
        ep_id = lax.axis_index('ep').astype(jnp.int32)
        dp_id = lax.axis_index('dp').astype(jnp.int32)
        weights = (jnp.swapaxes(w_gate, 2, 3), jnp.swapaxes(w_up, 2, 3), w_down)

        def swap(x):
            return lax.ppermute(x, 'ep', ep_pairs)

        def spread(x):
            return lax.all_gather(x, 'dp', axis=0, tiled=True)

        def trade(x, pairs):
            return [lax.ppermute(y, 'dp', pairs) for y in x]

        def slab(x):
            return x.reshape(tok, parts, LANES)

        def mixed(x, layer):
            return (x.astype(jnp.float32) + jnp.dot(x, w_mix[layer], preferred_element_type=jnp.float32)).astype(jnp.bfloat16)

        ids = jnp.swapaxes(expert_ids, 1, 2)
        gates = jnp.swapaxes(gate_vals, 1, 2)
        mine = jnp.stack([ids.astype(jnp.float32), gates])
        u = mixed(tokens, 0)
        u_slab = slab(u)
        theirs = swap(after(mine, u_slab))
        both = jnp.stack([mine, theirs], 2)
        top = n_layers - 1
        runs, tables, packed = [], [], []

        def add_tables(pair):
            run, token, gate, bounds = route_tables(pair[0].astype(jnp.int32), pair[1], ep_id, n_local)
            runs.append(run)
            tables.append([(token * parts, gate), (token * (2 * parts), gate)])
            spot = dp_id * (2 * tok) + token
            first = jnp.concatenate([spot.reshape(-1, LANES), jnp.pad(bounds.reshape(1, LANES), ((0, 7), (0, 0)))])
            packed.append(jnp.stack([first.astype(jnp.float32), jnp.pad(gate, ((0, 8), (0, 0)))]))

        add_tables(both[:, 0])

        x_in, u_slabs, u_others, xs = tokens, [u_slab], [swap(u_slab)], []
        d_slab = slab(d_out)
        d_other = swap(after(d_slab, u_others[0]))
        d_rows = (spread(join_rows(d_slab, d_other)),)
        for layer in range(n_layers):
            if layer:
                u = mixed(x_in, layer)
                u_slabs.append(slab(u))
                u_others.append(swap(u_slabs[layer]))
            xs.append(x_in)
            if layer < top:
                other, = token_kernel(layer, runs[layer][1], tables[layer][0], (u_slabs[layer], u_others[layer]), weights, (1,))
                sent = swap(other)
                own, = token_kernel(layer, runs[layer][0], tables[layer][0], (after(u_slabs[layer], other), u_others[layer]),
                                    weights, (0,))
                add_tables(after(both[:, layer + 1], own))
                x_in = (u.astype(jnp.float32) + own + sent).astype(jnp.bfloat16)

        shared = lax.all_gather(jnp.stack(packed), 'dp', axis=0)
        starts = shared[:, :, 0, -8].astype(jnp.int32)
        core = dp_id % 2
        dealt = [deal_experts(starts[:, layer], n_local, 2) for layer in range(n_layers)]
        mine = [lists[core] for lists, _ in dealt]
        firsts = [sum(x.shape[0] for x in mine[:layer]) for layer in range(n_layers)]
        list_rows = cdiv(cdiv(dp_size * 2 * cap, LANES), 8) * 8 + 8
        idx_all, gate_all = merge_tables(shared, starts, jnp.concatenate(mine),
                                         jnp.concatenate([jnp.full_like(x, layer) for layer, x in enumerate(mine)]),
                                         list_rows, dp_size * 2 * tok)
        idx_all = idx_all.reshape(-1)

        d_y, full, arrived = d_out, None, []
        d_mix = [None] * n_layers
        for layer in reversed(range(n_layers)):
            both_u = (u_slabs[layer], u_others[layer])
            u_rows = tuple(spread(x) for x in (both_u if layer < top else (join_rows(*both_u),)))
            slabs = (u_slabs[layer], u_others[layer], d_slab, d_other)
            own, other = token_kernel(layer, runs[layer][2], tables[layer][1], slabs, weights)
            d_u = (d_y.astype(jnp.float32) + own + swap(other)).astype(jnp.bfloat16)
            last = other
            if layer == top:
                y_own, last = token_kernel(top, runs[top][2], tables[top][0], (after(u_slabs[top], other), u_others[top]), weights)
            d_mix[layer] = jnp.einsum('td,te->de', xs[layer], d_u, preferred_element_type=jnp.float32).astype(jnp.bfloat16)
            d_y = (d_u.astype(jnp.float32)
                   + jnp.einsum('te,de->td', d_u, w_mix[layer], preferred_element_type=jnp.float32)).astype(jnp.bfloat16)
            lists, tiles = dealt[layer]
            full, part = weight_grads(layer, firsts[layer], mine[layer], after(tiles[core], last), (u_rows, d_rows), idx_all,
                                      gate_all, weights, full)
            arrived.append((layer, lists[1 - core], trade(part, core_pairs)))
            if layer:
                d_slab = slab(d_y)
                d_other = swap(d_slab)
                d_rows = (spread(join_rows(d_slab, d_other)),)
                if layer == top:
                    layer_out = (u.astype(jnp.float32) + y_own + swap(after(last, d_other))).astype(jnp.bfloat16)
        for layer, names, part in arrived:
            full = merge_half(layer, names, part, full)
        d_mix = lax.psum(jnp.stack(d_mix), ('dp', 'ep'))
        return (layer_out, d_y, d_mix, jnp.swapaxes(full[0], 2, 3), jnp.swapaxes(full[1], 2, 3), full[2])

    return jax.shard_map(device_body, mesh=mesh,
                         in_specs=(tok_spec, tok_spec, route_spec, route_spec, whole_spec,
                                   expert_spec, expert_spec, expert_spec),
                         out_specs=(tok_spec, tok_spec, whole_spec, expert_spec, expert_spec, expert_spec),
                         check_vma=False)
```

```python
import functools
import math

import jax
import jax.numpy as jnp
from jax import lax
from jax.experimental import pallas as pl
from jax.experimental.pallas import tpu as pltpu
from jax.sharding import PartitionSpec as P


CAP_FACTOR = 3
LANES = 128
TILE = 96
HALF_TILE = 64
WTILE = 768
SOURCES = 8
CHUNK = 256
PITCH = 9
BATCH = 16
SLOTS = 8
PAGE = 1024
VMEM_LIMIT = 62 * 2**20


def cdiv(a, b):
    return (a + b - 1) // b


def nt_dot(a, b):
    return lax.dot_general(a, b, (((1,), (1,)), ((), ())), preferred_element_type=jnp.float32)


def tn_dot(a, b):
    return lax.dot_general(a, b, (((0,), (0,)), ((), ())), preferred_element_type=jnp.float32)


def nn_dot(a, b):
    return lax.dot_general(a, b, (((1,), (0,)), ((), ())), preferred_element_type=jnp.float32)


def clear(ref):
    step = next(n for n in (64, 48, 32, 16, 8) if ref.shape[0] % n == 0)

    def one(q, carry):
        ref[pl.ds(pl.multiple_of(q * step, step), step), :] = jnp.zeros((step, ref.shape[1]), ref.dtype)
        return carry

    lax.fori_loop(0, ref.shape[0] // step, one, 0)


def add_rows(acc, vals_ref, idx, row, tile, pitch, width):
    for b in range(0, tile, BATCH):
        at = [pl.multiple_of(idx[row + b + r], 4) for r in range(BATCH)]
        vals = [acc[pl.ds(at[r], width), :] + vals_ref[pl.ds((b + r) * pitch, width), :] for r in range(BATCH)]
        for r in reversed(range(BATCH)):
            acc[pl.ds(at[r], width), :] = vals[r]


def spread_column(row):
    return jnp.broadcast_to(row, (LANES, LANES)).T


def tile_gates(gates, row):
    pair = gates[pl.ds(lax.div(row, LANES), 2), :]
    skip = lax.rem(row, LANES)
    pair = pltpu.roll(pair, lax.rem(LANES - skip, LANES), 1)
    lane = lax.broadcasted_iota(jnp.int32, (1, LANES), 1)
    return spread_column(jnp.where(lane < LANES - skip, pair[:1], pair[1:]))


def widen(src, dst, pitch, halves, tok):
    step = 8

    def one(q, carry):
        for r in range(step):
            dst[pl.ds((q * step + r) * pitch, pitch), :] = src[q * step + r].astype(jnp.float32)
        return carry

    lax.fori_loop(halves[0] * tok // step, (halves[-1] + 1) * tok // step, one, 0)


def write_sums(acc, outs, tok, parts, pitch, halves):
    step = min(32, tok)

    def copy_out(q, carry):
        r0 = pl.multiple_of(q * step, step)
        for k in range(parts):
            for out, half in zip(outs, halves):
                first = (half * tok + r0) * pitch + k
                out[pl.ds(r0, step), k * LANES:(k + 1) * LANES] = acc[pl.ds(first, step, stride=pitch), :]
        return carry

    lax.fori_loop(0, tok // step, copy_out, 0)


def expert_copies(weights, buf, sem, layer, e):
    slot = lax.rem(e, SLOTS)
    ff = weights[0].shape[2]
    return [pltpu.make_async_copy(w.at[layer, e], buf.at[slot, pl.ds(k * ff, ff)], sem.at[slot])
            for k, w in enumerate(weights)]


def run_tiles(step, weights, wbuf, wsem, runs, tile, layer, prepare):
    n_local = weights[0].shape[1]
    for e in range(SLOTS - 2):
        for c in expert_copies(weights, wbuf, wsem, layer, e):
            c.start()
    prepare()
    for c in expert_copies(weights, wbuf, wsem, layer, 0):
        c.wait()

    def length(e):
        return runs[n_local + e] - runs[e]

    def add_tiles(e, total):
        return total + jnp.maximum(lax.div(length(e) + tile - 1, tile), 1)

    def one(i, carry):
        (e, row, left), (e1, row1, n1), (e2, row2, n2), row3 = carry

        @pl.when(e != e1)
        def _():
            for c in expert_copies(weights, wbuf, wsem, layer, e):
                c.wait()

        @pl.when((e != e1) & (e + SLOTS - 3 < n_local))
        def _():
            for c in expert_copies(weights, wbuf, wsem, layer, e + SLOTS - 3):
                c.start()

        step(row, (lax.rem(e1, SLOTS), row1), (lax.rem(e2, SLOTS), row2, n2), row3)
        more = left > tile
        e_next = jnp.minimum(e + 1, n_local - 1)
        fresh = jnp.where(e + 1 < n_local, length(e_next), 0)
        ahead = (jnp.where(more, e, e_next), jnp.where(more, row + tile, runs[e_next]), jnp.where(more, left - tile, fresh))
        return ahead, (e, row, jnp.minimum(left, tile)), (e1, row1, n1), row2

    none = (0, 0, 0)
    lax.fori_loop(0, lax.fori_loop(0, n_local, add_tiles, 0) + 3, one, ((0, runs[0], length(0)), none, none, 0))


def token_body(runs, idx, gates, *refs, layer, tok, parts, tile, halves, backward):
    n_in = 4 if backward else 2
    sources, weights, outs, refs = refs[:n_in], refs[n_in:n_in + 3], refs[n_in + 3:n_in + 3 + len(halves)], refs[n_in + 3 + len(halves):]
    narrow, wide, rows, vt, acc, mid, wbuf, sem, wsem = refs
    ff = weights[0].shape[2]
    width = parts * n_in // 2
    pitch = width + 1

    def prepare():
        copies = [pltpu.make_async_copy(src, narrow.at[pl.ds(k % 2 * tok, tok), pl.ds(k // 2 * parts, parts)], sem.at[k])
                  for k, src in enumerate(sources) if k % 2 in halves]
        for c in copies:
            c.start()
        for ref in (acc, vt, rows, mid):
            clear(ref)
        for c in copies:
            c.wait()
        widen(narrow, wide, width, halves, tok)

    def column(k):
        return rows[pl.ds(k, tile, stride=pitch), :]

    def step(row, here, before, done):
        slot, row1 = here
        slot2, row2, n2 = before
        old = wbuf[slot2, :2 * ff] if backward else wbuf[slot2, 2 * ff:]
        v = tn_dot(mid[...], old).astype(jnp.bfloat16).astype(jnp.float32)
        u = jnp.concatenate([column(k) for k in range(parts)], axis=1).astype(jnp.bfloat16)
        ab = nt_dot(wbuf[slot, :2 * ff], u)
        if backward:
            gate = tile_gates(gates, row1)[:tile]
            c = jnp.concatenate([(column(parts + k) * gate).astype(jnp.bfloat16) for k in range(parts)], axis=1)
            dh = nt_dot(wbuf[slot, 2 * ff:], c)
        add_rows(acc, vt, idx, done, tile, parts + 1, parts)
        for r in range(tile):
            rows[pl.ds(pitch * r, width), :] = wide[pl.ds(pl.multiple_of(idx[row + r], width), width), :]
        live = lax.broadcasted_iota(jnp.int32, (tile, LANES), 0) < n2
        gate = tile_gates(gates, row2)[:tile]
        for k in range(parts):
            v_k = jnp.where(live, v[:, k * LANES:(k + 1) * LANES] * gate, 0.0)
            vt[pl.ds(k, tile, stride=parts + 1), :] = v_k
        a, b = ab[:ff], ab[ff:]
        s = jax.nn.sigmoid(a)
        act = a * s
        if backward:
            mid[:ff] = (dh * b * (s * (1.0 + a * (1.0 - s)))).astype(jnp.bfloat16)
            mid[ff:] = (dh * act).astype(jnp.bfloat16)
        else:
            mid[...] = (act * b).astype(jnp.bfloat16)

    run_tiles(step, weights, wbuf, wsem, runs, tile, layer, prepare)
    write_sums(acc, outs, tok, parts, width, halves)


def token_kernel(layer, runs, table, slabs, weights, halves=(0, 1)):
    idx, gates = table
    tok, parts, _ = slabs[0].shape
    _, n_local, ff, d_model = weights[0].shape
    backward = len(slabs) > 2
    tile = TILE if len(halves) == 2 else HALF_TILE
    width = parts * len(slabs) // 2
    rows_spec = pl.BlockSpec((tok, d_model), lambda i, *_: (0, 0))
    any_spec = pl.BlockSpec(memory_space=pl.ANY)
    tile_rows = cdiv(tile * (width + 1), 16) * 16
    work = (4 if backward else 3) * len(halves)
    return pl.pallas_call(
        functools.partial(token_body, layer=layer, tok=tok, parts=parts, tile=tile, halves=halves, backward=backward),
        grid_spec=pltpu.PrefetchScalarGridSpec(
            num_scalar_prefetch=2,
            grid=(1,),
            in_specs=[pl.BlockSpec(gates.shape, lambda i, *_: (0, 0))] + [any_spec] * (len(slabs) + 3),
            out_specs=[rows_spec] * len(halves),
            scratch_shapes=[pltpu.VMEM((2 * tok, width, LANES), jnp.bfloat16), pltpu.VMEM((2 * tok * width, LANES), jnp.float32),
                            pltpu.VMEM((tile_rows, LANES), jnp.float32), pltpu.VMEM((tile_rows, LANES), jnp.float32),
                            pltpu.VMEM((2 * tok * width, LANES), jnp.float32),
                            pltpu.VMEM((2 * ff if backward else ff, tile), jnp.bfloat16),
                            pltpu.VMEM((SLOTS, 3 * ff, d_model), jnp.bfloat16),
                            pltpu.SemaphoreType.DMA((len(slabs),)), pltpu.SemaphoreType.DMA((SLOTS,))],
        ),
        out_shape=[jax.ShapeDtypeStruct((tok, d_model), jnp.float32)] * len(halves),
        compiler_params=pltpu.CompilerParams(dimension_semantics=("arbitrary",), vmem_limit_bytes=VMEM_LIMIT),
        cost_estimate=pl.CostEstimate(flops=work * 2 * 8 * tok * d_model * ff * 4,
                                      bytes_accessed=3 * n_local * ff * d_model * 2, transcendentals=0),
        name="experts_backward" if backward else "experts_forward",
    )(runs, idx, gates, *slabs, *weights)


def merge_tables_body(st, exps, layers, table, idx_ref, gate_ref, buf, *, out_rows, pad_row):
    group = idx_ref.shape[0]

    def one(q, carry):
        item = pl.program_id(0) * group + q
        merge_expert(exps[item], layers[item], st, table, idx_ref.at[q], gate_ref.at[q], buf, out_rows, pad_row)
        return carry

    lax.fori_loop(0, group, one, 0)


def merge_expert(exp, layer, st, table, idx_out, gate_out, buf, out_rows, pad_row):
    src, n_layers = table.shape[:2]
    buf[0] = jnp.full(buf.shape[1:], float(pad_row), jnp.float32)
    buf[1] = jnp.zeros(buf.shape[1:], jnp.float32)
    row = lax.broadcasted_iota(jnp.int32, (8, LANES), 0)
    lane = lax.broadcasted_iota(jnp.int32, (8, LANES), 1)
    off = 0
    for d in range(src):
        at = (d * n_layers + layer) * LANES + exp
        first = st[at]
        count = st[at + 1] - first
        to = lax.rem(off, LANES) + LANES
        shift = to - lax.rem(first, LANES)
        over = lax.rem(shift, LANES)
        start = lax.div(off, LANES)
        place = row * LANES + lane
        take = (place >= to) & (place < to + count)
        for kind in range(2):
            x = table[d, layer, kind, pl.ds(lax.div(first, LANES), 8), :]
            x = pltpu.roll(pltpu.roll(x, over, 1), lax.div(shift, LANES), 0)
            x = jnp.where(lane >= over, x, pltpu.roll(x, 1, 0))
            old = buf[kind, pl.ds(start, 8), :]
            buf[kind, pl.ds(start, 8), :] = jnp.where(take, x, old)
        off = off + count
    idx_out[...] = buf[0, pl.ds(1, out_rows), :].astype(jnp.int32)
    gate_out[...] = buf[1, pl.ds(1, out_rows), :]


def merge_tables(shared, starts, exps, layers, out_rows, pad_row):
    n_items = exps.shape[0]
    group = math.gcd(n_items, 8)
    out = pl.BlockSpec((group, out_rows, LANES), lambda g, *_: (g, 0, 0))
    return pl.pallas_call(
        functools.partial(merge_tables_body, out_rows=out_rows, pad_row=pad_row),
        grid_spec=pltpu.PrefetchScalarGridSpec(
            num_scalar_prefetch=3,
            grid=(n_items // group,),
            in_specs=[pl.BlockSpec(shared.shape, lambda g, *_: (0,) * shared.ndim)],
            out_specs=[out] * 2,
            scratch_shapes=[pltpu.VMEM((2, out_rows + 16, LANES), jnp.float32)],
        ),
        out_shape=[jax.ShapeDtypeStruct((n_items, out_rows, LANES), jnp.int32),
                   jax.ShapeDtypeStruct((n_items, out_rows, LANES), jnp.float32)],
        compiler_params=pltpu.CompilerParams(dimension_semantics=("arbitrary",)),
        cost_estimate=pl.CostEstimate(flops=10**9, bytes_accessed=4 * shared.size, transcendentals=0),
        name="merge_tables",
    )(starts.reshape(-1), exps, layers, shared)


def weight_grad_body(exps, tiles, begins, *refs, parts, n_exp, n_alias, first_list, page):
    rows_in, refs = refs[:4], refs[4:]
    idx_all, gate_ref, g_ref, up_ref, w_ref = refs[:5]
    (dg_ref, du_ref, dw_ref, og_ref, ou_ref, ow_ref,
     uds, rows, u0, c0, d0, h0, u1, c1, d1, h1, gacc, wacc, idx_s, sem, tsem) = refs[5 + n_alias:]
    e = pl.program_id(0)
    ff = g_ref.shape[2]
    slots = 3
    both = ((u0, c0, d0, h0), (u1, c1, d1, h1))

    def table_copy(exp):
        slot = lax.rem(exp, slots)
        at = pl.multiple_of((first_list + exp) * page, PAGE)
        to = pl.multiple_of(slot * page, PAGE)
        return pltpu.make_async_copy(idx_all.at[pl.ds(at, page)], idx_s.at[pl.ds(to, page)], tsem.at[slot])

    def gather_row(at, r):
        rows[pl.ds(r * PITCH, 2 * parts), :] = uds[idx_s[at]].astype(jnp.float32)

    def column(first, count, k):
        return rows[pl.ds(first * PITCH + k, count, stride=PITCH), :]

    @pl.when(e == 0)
    def _():
        n_tok = uds.shape[0] - 8
        run = n_tok // (2 * SOURCES)
        copies = [pltpu.make_async_copy(src.at[pl.ds(q * run, run)],
                                        uds.at[pl.ds((2 * q + k % 2) * run, run), pl.ds(k // 2 * parts, parts)], sem.at[k])
                  for q in range(SOURCES) for k, src in enumerate(rows_in)]
        for c in copies:
            c.start()
        table_copy(0).start()
        table_copy(1).start()
        uds[pl.ds(n_tok, 8)] = jnp.zeros((8, 2 * parts, LANES), jnp.bfloat16)
        for ref in (*both[0], *both[1], gacc, wacc):
            clear(ref)
        table_copy(0).wait()
        for c in copies:
            c.wait()

        def first_rows(q, carry):
            for r in range(16):
                gather_row(q * 16 + r, q * 16 + r)
            return carry

        lax.fori_loop(0, WTILE // 16, first_rows, 0)

    @pl.when(e + 1 < n_exp)
    def _():
        table_copy(e + 1).wait()

    @pl.when(e + 2 < n_exp)
    def _():
        table_copy(e + 2).start()

    here = lax.rem(e, slots) * page
    there = lax.rem(jnp.minimum(e + 1, n_exp - 1), slots) * page
    n_tiles = tiles[e]
    begin = begins[e]
    gate_rows = WTILE // LANES

    def compute(j, new, old):
        un, cn, dn, hn = new
        uo, co, do, ho = old
        gacc[...] += nn_dot(do[...], uo[...])
        wacc[...] += nn_dot(ho[...], co[...])
        nxt = jnp.where(j + 1 < n_tiles, here + (j + 1) * WTILE, there)
        gu = jnp.concatenate([g_ref[0, 0], up_ref[0, 0]], axis=0)
        for q in range(0, WTILE, CHUNK):
            part = slice(q, q + CHUNK)
            un[part] = jnp.concatenate([column(q, CHUNK, k) for k in range(parts)], axis=1).astype(jnp.bfloat16)
            for p in range(q, q + CHUNK, LANES):
                gate = spread_column(gate_ref[0, pl.ds(j * gate_rows + p // LANES, 1), :])
                for k in range(parts):
                    d = column(p, LANES, parts + k)
                    cn[p:p + LANES, k * LANES:(k + 1) * LANES] = (d * gate).astype(jnp.bfloat16)
            ab = nt_dot(gu, un[part])
            dh = nt_dot(w_ref[0, 0], cn[part])
            for r in range(q, q + CHUNK):
                gather_row(nxt + r, r)
            a, b = ab[:ff], ab[ff:]
            s = jax.nn.sigmoid(a)
            act = a * s
            hn[:, part] = (act * b).astype(jnp.bfloat16)
            dn[:ff, part] = (dh * b * (s * (1.0 + a * (1.0 - s)))).astype(jnp.bfloat16)
            dn[ff:, part] = (dh * act).astype(jnp.bfloat16)

    def tile(j, carry):
        odd = lax.rem(begin + j, 2)

        @pl.when(odd == 0)
        def _():
            compute(j, both[0], both[1])

        @pl.when(odd == 1)
        def _():
            compute(j, both[1], both[0])

        @pl.when(j == 0)
        def _():
            dg = gacc[:ff].astype(jnp.bfloat16)
            du = gacc[ff:].astype(jnp.bfloat16)
            dw = wacc[...].astype(jnp.bfloat16)
            dg_ref[0, 0], du_ref[0, 0], dw_ref[0, 0] = dg, du, dw
            og_ref[0], ou_ref[0], ow_ref[0] = dg, du, dw
            gacc[...] = jnp.zeros_like(gacc)
            wacc[...] = jnp.zeros_like(wacc)

        return carry

    lax.fori_loop(0, n_tiles, tile, 0)


def weight_grads(layer, first, exps, tiles, rows, idx_all, gates, weights, full):
    n_half, parts, _ = rows[0].shape
    n_tok = 2 * n_half
    n_layers, n_local, ff, d_model = weights[0].shape
    n_exp = exps.shape[0]
    out_rows = gates.shape[1]
    page = out_rows * LANES
    tiles = jnp.concatenate([tiles, jnp.ones((1,), jnp.int32)])
    begins = jnp.cumsum(tiles) - tiles
    any_spec = pl.BlockSpec(memory_space=pl.ANY)
    mine = pl.BlockSpec((1, 1, ff, d_model), lambda e, exps, *_: (layer, exps[jnp.minimum(e, n_exp - 1)], 0, 0))
    done = pl.BlockSpec((1, 1, ff, d_model), lambda e, exps, *_: (layer, exps[jnp.maximum(e - 1, 0)], 0, 0))
    half = pl.BlockSpec((1, ff, d_model), lambda e, *_: (jnp.maximum(e - 1, 0), 0, 0))
    gate_spec = pl.BlockSpec((1, out_rows, LANES), lambda e, *_: (first + jnp.minimum(e, n_exp - 1), 0, 0))
    aliased = list(full) if full is not None else []
    tile_set = [pltpu.VMEM((WTILE, d_model), jnp.bfloat16)] * 2 + [pltpu.VMEM((2 * ff, WTILE), jnp.bfloat16),
                                                                 pltpu.VMEM((ff, WTILE), jnp.bfloat16)]
    outs = pl.pallas_call(
        functools.partial(weight_grad_body, parts=parts, n_exp=n_exp, n_alias=len(aliased), first_list=first, page=page),
        grid_spec=pltpu.PrefetchScalarGridSpec(
            num_scalar_prefetch=3,
            grid=(n_exp + 1,),
            in_specs=[any_spec] * 5 + [gate_spec] + [mine] * 3 + [any_spec] * len(aliased),
            out_specs=[done] * 3 + [half] * 3,
            scratch_shapes=[pltpu.VMEM((n_tok + 8, 2 * parts, LANES), jnp.bfloat16)]
            + [pltpu.VMEM((WTILE * PITCH + 16, LANES), jnp.float32)] + tile_set * 2
            + [pltpu.VMEM((2 * ff, d_model), jnp.float32), pltpu.VMEM((ff, d_model), jnp.float32),
               pltpu.SMEM((3 * page,), jnp.int32), pltpu.SemaphoreType.DMA((4,)), pltpu.SemaphoreType.DMA((3,))],
        ),
        out_shape=[jax.ShapeDtypeStruct((n_layers, n_local, ff, d_model), jnp.bfloat16)] * 3
        + [jax.ShapeDtypeStruct((n_exp, ff, d_model), jnp.bfloat16)] * 3,
        input_output_aliases={12 + k: k for k in range(len(aliased))},
        compiler_params=pltpu.CompilerParams(dimension_semantics=("arbitrary",), vmem_limit_bytes=VMEM_LIMIT),
        cost_estimate=pl.CostEstimate(flops=6 * n_tok * n_exp * d_model * ff,
                                      bytes_accessed=n_tok * d_model * 4 + 9 * n_exp * ff * d_model * 2, transcendentals=0),
        name="weight_grads",
    )(exps, tiles, begins, *rows, idx_all, gates, *weights, *aliased)
    return outs[:3], outs[3:]


def merge_body(exps, a, b, c, f0, f1, f2, o0, o1, o2, buf, in_sem, out_sem, *, layer, n_exp):
    halves, wholes = (a, b, c), (o0, o1, o2)

    def arrive(k, q):
        return pltpu.make_async_copy(halves[k].at[q], buf.at[k, q], in_sem.at[k, q])

    def leave(k, q):
        return pltpu.make_async_copy(buf.at[k, q], wholes[k].at[layer, exps[q]], out_sem)

    def each(act):
        def one(q, carry):
            for k in range(3):
                act(k, q)
            return carry

        lax.fori_loop(0, n_exp, one, 0)

    def pass_on(k, q):
        arrive(k, q).wait()
        leave(k, q).start()

    each(lambda k, q: arrive(k, q).start())
    each(pass_on)
    each(lambda k, q: leave(k, q).wait())


def merge_half(layer, exps, half, full):
    n_exp, ff, d_model = half[0].shape
    any_spec = pl.BlockSpec(memory_space=pl.ANY)
    return pl.pallas_call(
        functools.partial(merge_body, layer=layer, n_exp=n_exp),
        grid_spec=pltpu.PrefetchScalarGridSpec(
            num_scalar_prefetch=1, grid=(1,), in_specs=[any_spec] * 6, out_specs=[any_spec] * 3,
            scratch_shapes=[pltpu.VMEM((3, n_exp, ff, d_model), jnp.bfloat16), pltpu.SemaphoreType.DMA((3, n_exp)),
                            pltpu.SemaphoreType.DMA]),
        out_shape=[jax.ShapeDtypeStruct(x.shape, x.dtype) for x in full],
        input_output_aliases={4: 0, 5: 1, 6: 2},
        compiler_params=pltpu.CompilerParams(dimension_semantics=("arbitrary",), vmem_limit_bytes=VMEM_LIMIT),
        cost_estimate=pl.CostEstimate(flops=10**9, bytes_accessed=6 * n_exp * ff * d_model * 2, transcendentals=0),
        name="merge_half",
    )(exps, *half, *full)


def route_tables(ids, gates, ep, n_local):
    n_src, top_k, tok = ids.shape
    n = n_src * top_k * tok
    local = ids - ep * n_local
    here = (local >= 0) & (local < n_local)
    group = jnp.where(here, local, n_local).reshape(-1)
    key, gate = lax.sort((group * n + jnp.arange(n, dtype=jnp.int32), gates.reshape(-1)), num_keys=1, is_stable=False)
    copy = key % n
    token = copy // (top_k * tok) * tok + copy % tok
    token = jnp.pad(token, (0, 2 * PAGE))
    gate = jnp.pad(gate, (0, 2 * PAGE)).reshape(-1, LANES)
    ids = jnp.arange(n_local, dtype=jnp.int32)
    hits = jnp.sum((group.reshape(n_src, -1)[:, :, None] == ids).astype(jnp.int32), axis=1)
    starts = jnp.sum((ids[None, :] < ids[:, None]).astype(jnp.int32) * jnp.sum(hits, axis=0), axis=1)
    ends = starts + jnp.sum(hits, axis=0)
    middle = starts + hits[0]
    bounds = jnp.pad(starts, (0, LANES - n_local), constant_values=0) + jnp.where(jnp.arange(LANES) < n_local, 0, ends[-1])
    runs = [jnp.concatenate(x) for x in ((starts, middle), (middle, ends), (starts, ends))]
    return runs, token, gate, bounds


def deal_experts(bounds, n_local, n_lists):
    load = jnp.sum(bounds[:, 1:n_local + 1] - bounds[:, :n_local], axis=0)
    ids = jnp.arange(n_local, dtype=jnp.int32)
    ahead = (load[None, :] > load[:, None]) | ((load[None, :] == load[:, None]) & (ids[None, :] < ids[:, None]))
    rank = jnp.sum(ahead.astype(jnp.int32), axis=1)
    turn, which = jnp.arange(n_local // n_lists)[None, :], jnp.arange(n_lists)[:, None]
    want = n_lists * turn + jnp.where(turn % 2 == 0, which, n_lists - 1 - which)
    pick = (rank[None, None, :] == want[:, :, None]).astype(jnp.int32)
    tiles = jnp.maximum((jnp.sum(pick * load, axis=2) + WTILE - 1) // WTILE, 1)
    return jnp.sum(pick * ids, axis=2), tiles


def after(x, *earlier):
    return lax.optimization_barrier((x, *earlier))[0]


def solution(mesh):
    ep_size = mesh.shape['ep']
    dp_size = mesh.shape['dp']
    tok_spec = P(('dp', 'ep'), None)
    route_spec = P(None, ('dp', 'ep'), None)
    whole_spec = P(None, None, None)
    expert_spec = P(None, 'ep', None, None)
    ep_pairs = [(i, 1 - i) for i in range(ep_size)]
    core_pairs = [(i, i ^ 1) for i in range(dp_size)]

    def device_body(tokens, d_out, expert_ids, gate_vals, w_mix, w_gate, w_up, w_down):
        n_layers = w_mix.shape[0]
        n_local = w_gate.shape[1]
        n_experts = n_local * ep_size
        tok, d_model = tokens.shape
        top_k = expert_ids.shape[2]
        parts = d_model // LANES
        cap = cdiv(CAP_FACTOR * tok * top_k, n_experts)
        ep_id = lax.axis_index('ep').astype(jnp.int32)
        dp_id = lax.axis_index('dp').astype(jnp.int32)
        weights = (jnp.swapaxes(w_gate, 2, 3), jnp.swapaxes(w_up, 2, 3), w_down)

        def swap(x):
            return lax.ppermute(x, 'ep', ep_pairs)

        def spread(x):
            return [lax.all_gather(y, 'dp', axis=0, tiled=True) for y in x]

        def trade(x, pairs):
            return [lax.ppermute(y, 'dp', pairs) for y in x]

        def slab(x):
            return x.reshape(tok, parts, LANES)

        def mixed(x, layer):
            return (x.astype(jnp.float32) + jnp.dot(x, w_mix[layer], preferred_element_type=jnp.float32)).astype(jnp.bfloat16)

        ids = jnp.swapaxes(expert_ids, 1, 2)
        gates = jnp.swapaxes(gate_vals, 1, 2)
        mine = jnp.stack([ids.astype(jnp.float32), gates])
        u = mixed(tokens, 0)
        u_slab = slab(u)
        theirs = swap(after(mine, u_slab))
        both = jnp.stack([mine, theirs], 2)
        top = n_layers - 1
        runs, tables, packed = [], [], []

        def add_tables(pair):
            run, token, gate, bounds = route_tables(pair[0].astype(jnp.int32), pair[1], ep_id, n_local)
            runs.append(run)
            tables.append([(token * parts, gate), (token * (2 * parts), gate)])
            spot = dp_id * (2 * tok) + token
            first = jnp.concatenate([spot.reshape(-1, LANES), jnp.pad(bounds.reshape(1, LANES), ((0, 7), (0, 0)))])
            packed.append(jnp.stack([first.astype(jnp.float32), jnp.pad(gate, ((0, 8), (0, 0)))]))

        add_tables(both[:, 0])

        x_in, u_slabs, u_others, xs = tokens, [u_slab], [swap(u_slab)], []
        d_slab = slab(d_out)
        d_other = swap(after(d_slab, u_others[0]))
        d_rows = spread((d_slab, d_other))
        for layer in range(n_layers):
            if layer:
                u = mixed(x_in, layer)
                u_slabs.append(slab(u))
                u_others.append(swap(u_slabs[layer]))
                add_tables(after(both[:, layer], u_slabs[layer]))
            xs.append(x_in)
            if layer < top:
                other, = token_kernel(layer, runs[layer][1], tables[layer][0], (u_slabs[layer], u_others[layer]), weights, (1,))
                sent = swap(other)
                own, = token_kernel(layer, runs[layer][0], tables[layer][0], (after(u_slabs[layer], other), u_others[layer]),
                                    weights, (0,))
                x_in = (u.astype(jnp.float32) + own + sent).astype(jnp.bfloat16)

        shared = lax.all_gather(jnp.stack(packed), 'dp', axis=0)
        starts = shared[:, :, 0, -8].astype(jnp.int32)
        core = dp_id % 2
        dealt = [deal_experts(starts[:, layer], n_local, 2) for layer in range(n_layers)]
        mine = [lists[core] for lists, _ in dealt]
        firsts = [sum(x.shape[0] for x in mine[:layer]) for layer in range(n_layers)]
        list_rows = cdiv(cdiv(dp_size * 2 * cap, LANES), 8) * 8 + 8
        idx_all, gate_all = merge_tables(shared, starts, jnp.concatenate(mine),
                                         jnp.concatenate([jnp.full_like(x, layer) for layer, x in enumerate(mine)]),
                                         list_rows, dp_size * 2 * tok)
        idx_all = idx_all.reshape(-1)

        d_y, full, arrived = d_out, None, []
        d_mix = [None] * n_layers
        for layer in reversed(range(n_layers)):
            u_rows = spread((u_slabs[layer], u_others[layer]))
            slabs = (u_slabs[layer], u_others[layer], d_slab, d_other)
            own, other = token_kernel(layer, runs[layer][2], tables[layer][1], slabs, weights)
            d_u = (d_y.astype(jnp.float32) + own + swap(other)).astype(jnp.bfloat16)
            last = other
            if layer == top:
                y_own, last = token_kernel(top, runs[top][2], tables[top][0], (after(u_slabs[top], other), u_others[top]), weights)
            d_mix[layer] = jnp.einsum('td,te->de', xs[layer], d_u, preferred_element_type=jnp.float32).astype(jnp.bfloat16)
            d_y = (d_u.astype(jnp.float32)
                   + jnp.einsum('te,de->td', d_u, w_mix[layer], preferred_element_type=jnp.float32)).astype(jnp.bfloat16)
            lists, tiles = dealt[layer]
            full, part = weight_grads(layer, firsts[layer], mine[layer], after(tiles[core], last), u_rows + d_rows, idx_all,
                                      gate_all, weights, full)
            arrived.append((layer, lists[1 - core], trade(part, core_pairs)))
            if layer:
                d_slab = slab(d_y)
                d_other = swap(d_slab)
                d_rows = spread((d_slab, d_other))
                if layer == top:
                    layer_out = (u.astype(jnp.float32) + y_own + swap(after(last, d_other))).astype(jnp.bfloat16)
        for layer, names, part in arrived:
            full = merge_half(layer, names, part, full)
        d_mix = lax.psum(jnp.stack(d_mix), ('dp', 'ep'))
        return (layer_out, d_y, d_mix, jnp.swapaxes(full[0], 2, 3), jnp.swapaxes(full[1], 2, 3), full[2])

    return jax.shard_map(device_body, mesh=mesh,
                         in_specs=(tok_spec, tok_spec, route_spec, route_spec, whole_spec,
                                   expert_spec, expert_spec, expert_spec),
                         out_specs=(tok_spec, tok_spec, whole_spec, expert_spec, expert_spec, expert_spec),
                         check_vma=False)
```

```python
import functools
import math

import jax
import jax.numpy as jnp
from jax import lax
from jax.experimental import pallas as pl
from jax.experimental.pallas import tpu as pltpu
from jax.sharding import PartitionSpec as P


CAP_FACTOR = 3
LANES = 128
TILE = 96
HALF_TILE = 64
WTILE = 768
PARTS = 2
SOURCES = 8
CHUNK = 256
PITCH = 9
BATCH = 16
SLOTS = 8
PAGE = 1024
VMEM_LIMIT = 62 * 2**20


def cdiv(a, b):
    return (a + b - 1) // b


def nt_dot(a, b):
    return lax.dot_general(a, b, (((1,), (1,)), ((), ())), preferred_element_type=jnp.float32)


def tn_dot(a, b):
    return lax.dot_general(a, b, (((0,), (0,)), ((), ())), preferred_element_type=jnp.float32)


def nn_dot(a, b):
    return lax.dot_general(a, b, (((1,), (0,)), ((), ())), preferred_element_type=jnp.float32)


def clear(ref):
    step = next(n for n in (64, 48, 32, 16, 8) if ref.shape[0] % n == 0)

    def one(q, carry):
        ref[pl.ds(pl.multiple_of(q * step, step), step), :] = jnp.zeros((step, ref.shape[1]), ref.dtype)
        return carry

    lax.fori_loop(0, ref.shape[0] // step, one, 0)


def add_rows(acc, vals_ref, idx, row, tile, pitch, width):
    for b in range(0, tile, BATCH):
        at = [pl.multiple_of(idx[row + b + r], 4) for r in range(BATCH)]
        vals = [acc[pl.ds(at[r], width), :] + vals_ref[pl.ds((b + r) * pitch, width), :] for r in range(BATCH)]
        for r in reversed(range(BATCH)):
            acc[pl.ds(at[r], width), :] = vals[r]


def spread_column(row):
    return jnp.broadcast_to(row, (LANES, LANES)).T


def tile_gates(gates, row):
    pair = gates[pl.ds(lax.div(row, LANES), 2), :]
    skip = lax.rem(row, LANES)
    pair = pltpu.roll(pair, lax.rem(LANES - skip, LANES), 1)
    lane = lax.broadcasted_iota(jnp.int32, (1, LANES), 1)
    return spread_column(jnp.where(lane < LANES - skip, pair[:1], pair[1:]))


def widen(src, dst, pitch, halves, tok):
    step = 32

    def one(q, carry):
        for r in range(step):
            dst[pl.ds((q * step + r) * pitch, pitch), :] = src[q * step + r].astype(jnp.float32)
        return carry

    lax.fori_loop(halves[0] * tok // step, (halves[-1] + 1) * tok // step, one, 0)


def write_sums(acc, outs, tok, parts, pitch, halves):
    step = min(32, tok)

    def copy_out(q, carry):
        r0 = pl.multiple_of(q * step, step)
        for k in range(parts):
            for out, half in zip(outs, halves):
                first = (half * tok + r0) * pitch + k
                out[pl.ds(r0, step), k * LANES:(k + 1) * LANES] = acc[pl.ds(first, step, stride=pitch), :]
        return carry

    lax.fori_loop(0, tok // step, copy_out, 0)


def expert_copies(weights, buf, sem, layer, e):
    slot = lax.rem(e, SLOTS)
    ff = weights[0].shape[2]
    return [pltpu.make_async_copy(w.at[layer, e], buf.at[slot, pl.ds(k * ff, ff)], sem.at[slot])
            for k, w in enumerate(weights)]


def run_tiles(step, weights, wbuf, wsem, runs, tile, layer, prepare):
    n_local = weights[0].shape[1]
    for e in range(SLOTS - 2):
        for c in expert_copies(weights, wbuf, wsem, layer, e):
            c.start()
    prepare()
    for c in expert_copies(weights, wbuf, wsem, layer, 0):
        c.wait()

    def length(e):
        return runs[n_local + e] - runs[e]

    def add_tiles(e, total):
        return total + jnp.maximum(lax.div(length(e) + tile - 1, tile), 1)

    def one(i, carry):
        (e, row, left), (e1, row1, n1), (e2, row2, n2), row3 = carry

        @pl.when(e != e1)
        def _():
            for c in expert_copies(weights, wbuf, wsem, layer, e):
                c.wait()

        @pl.when((e != e1) & (e + SLOTS - 3 < n_local))
        def _():
            for c in expert_copies(weights, wbuf, wsem, layer, e + SLOTS - 3):
                c.start()

        step(row, (lax.rem(e1, SLOTS), row1), (lax.rem(e2, SLOTS), row2, n2), row3)
        more = left > tile
        e_next = jnp.minimum(e + 1, n_local - 1)
        fresh = jnp.where(e + 1 < n_local, length(e_next), 0)
        ahead = (jnp.where(more, e, e_next), jnp.where(more, row + tile, runs[e_next]), jnp.where(more, left - tile, fresh))
        return ahead, (e, row, jnp.minimum(left, tile)), (e1, row1, n1), row2

    none = (0, 0, 0)
    lax.fori_loop(0, lax.fori_loop(0, n_local, add_tiles, 0) + 3, one, ((0, runs[0], length(0)), none, none, 0))


def token_body(runs, idx, gates, *refs, layer, tok, parts, tile, halves, backward):
    n_in = 4 if backward else 2
    sources, weights, outs, refs = refs[:n_in], refs[n_in:n_in + 3], refs[n_in + 3:n_in + 3 + len(halves)], refs[n_in + 3 + len(halves):]
    narrow, wide, rows, vt, acc, mid, wbuf, sem, wsem = refs
    ff = weights[0].shape[2]
    width = parts * n_in // 2
    pitch = width + 1

    def prepare():
        copies = [pltpu.make_async_copy(src, narrow.at[pl.ds(k % 2 * tok, tok), pl.ds(k // 2 * parts, parts)], sem.at[k])
                  for k, src in enumerate(sources) if k % 2 in halves]
        for c in copies:
            c.start()
        for ref in (acc, vt, rows, mid):
            clear(ref)
        for c in copies:
            c.wait()
        widen(narrow, wide, width, halves, tok)

    def column(k):
        return rows[pl.ds(k, tile, stride=pitch), :]

    def step(row, here, before, done):
        slot, row1 = here
        slot2, row2, n2 = before
        old = wbuf[slot2, :2 * ff] if backward else wbuf[slot2, 2 * ff:]
        v = tn_dot(mid[...], old).astype(jnp.bfloat16).astype(jnp.float32)
        u = jnp.concatenate([column(k) for k in range(parts)], axis=1).astype(jnp.bfloat16)
        ab = nt_dot(wbuf[slot, :2 * ff], u)
        if backward:
            gate = tile_gates(gates, row1)[:tile]
            c = jnp.concatenate([(column(parts + k) * gate).astype(jnp.bfloat16) for k in range(parts)], axis=1)
            dh = nt_dot(wbuf[slot, 2 * ff:], c)
        add_rows(acc, vt, idx, done, tile, parts + 1, parts)
        for r in range(tile):
            rows[pl.ds(pitch * r, width), :] = wide[pl.ds(pl.multiple_of(idx[row + r], width), width), :]
        live = lax.broadcasted_iota(jnp.int32, (tile, LANES), 0) < n2
        gate = tile_gates(gates, row2)[:tile]
        for k in range(parts):
            v_k = jnp.where(live, v[:, k * LANES:(k + 1) * LANES] * gate, 0.0)
            vt[pl.ds(k, tile, stride=parts + 1), :] = v_k
        a, b = ab[:ff], ab[ff:]
        s = jax.nn.sigmoid(a)
        act = a * s
        if backward:
            mid[:ff] = (dh * b * (s * (1.0 + a * (1.0 - s)))).astype(jnp.bfloat16)
            mid[ff:] = (dh * act).astype(jnp.bfloat16)
        else:
            mid[...] = (act * b).astype(jnp.bfloat16)

    run_tiles(step, weights, wbuf, wsem, runs, tile, layer, prepare)
    write_sums(acc, outs, tok, parts, width, halves)


def token_kernel(layer, runs, table, slabs, weights, halves=(0, 1)):
    idx, gates = table
    tok, parts, _ = slabs[0].shape
    _, n_local, ff, d_model = weights[0].shape
    backward = len(slabs) > 2
    tile = TILE if len(halves) == 2 else HALF_TILE
    width = parts * len(slabs) // 2
    rows_spec = pl.BlockSpec((tok, d_model), lambda i, *_: (0, 0))
    any_spec = pl.BlockSpec(memory_space=pl.ANY)
    tile_rows = cdiv(tile * (width + 1), 16) * 16
    work = (4 if backward else 3) * len(halves)
    return pl.pallas_call(
        functools.partial(token_body, layer=layer, tok=tok, parts=parts, tile=tile, halves=halves, backward=backward),
        grid_spec=pltpu.PrefetchScalarGridSpec(
            num_scalar_prefetch=2,
            grid=(1,),
            in_specs=[pl.BlockSpec(gates.shape, lambda i, *_: (0, 0))] + [any_spec] * (len(slabs) + 3),
            out_specs=[rows_spec] * len(halves),
            scratch_shapes=[pltpu.VMEM((2 * tok, width, LANES), jnp.bfloat16), pltpu.VMEM((2 * tok * width, LANES), jnp.float32),
                            pltpu.VMEM((tile_rows, LANES), jnp.float32), pltpu.VMEM((tile_rows, LANES), jnp.float32),
                            pltpu.VMEM((2 * tok * width, LANES), jnp.float32),
                            pltpu.VMEM((2 * ff if backward else ff, tile), jnp.bfloat16),
                            pltpu.VMEM((SLOTS, 3 * ff, d_model), jnp.bfloat16),
                            pltpu.SemaphoreType.DMA((len(slabs),)), pltpu.SemaphoreType.DMA((SLOTS,))],
        ),
        out_shape=[jax.ShapeDtypeStruct((tok, d_model), jnp.float32)] * len(halves),
        compiler_params=pltpu.CompilerParams(dimension_semantics=("arbitrary",), vmem_limit_bytes=VMEM_LIMIT),
        cost_estimate=pl.CostEstimate(flops=work * 2 * 8 * tok * d_model * ff * 4,
                                      bytes_accessed=3 * n_local * ff * d_model * 2, transcendentals=0),
        name="experts_backward" if backward else "experts_forward",
    )(runs, idx, gates, *slabs, *weights)


def merge_tables_body(st, exps, layers, table, idx_ref, gate_ref, buf, *, out_rows, pad_row):
    group = idx_ref.shape[0]

    def one(q, carry):
        item = pl.program_id(0) * group + q
        merge_expert(exps[item], layers[item], st, table, idx_ref.at[q], gate_ref.at[q], buf, out_rows, pad_row)
        return carry

    lax.fori_loop(0, group, one, 0)


def merge_expert(exp, layer, st, table, idx_out, gate_out, buf, out_rows, pad_row):
    src, n_layers = table.shape[:2]
    buf[0] = jnp.full(buf.shape[1:], float(pad_row), jnp.float32)
    buf[1] = jnp.zeros(buf.shape[1:], jnp.float32)
    row = lax.broadcasted_iota(jnp.int32, (8, LANES), 0)
    lane = lax.broadcasted_iota(jnp.int32, (8, LANES), 1)
    off = 0
    for d in range(src):
        at = (d * n_layers + layer) * LANES + exp
        first = st[at]
        count = st[at + 1] - first
        to = lax.rem(off, LANES) + LANES
        shift = to - lax.rem(first, LANES)
        over = lax.rem(shift, LANES)
        start = lax.div(off, LANES)
        place = row * LANES + lane
        take = (place >= to) & (place < to + count)
        for kind in range(2):
            x = table[d, layer, kind, pl.ds(lax.div(first, LANES), 8), :]
            x = pltpu.roll(pltpu.roll(x, over, 1), lax.div(shift, LANES), 0)
            x = jnp.where(lane >= over, x, pltpu.roll(x, 1, 0))
            old = buf[kind, pl.ds(start, 8), :]
            buf[kind, pl.ds(start, 8), :] = jnp.where(take, x, old)
        off = off + count
    idx_out[...] = buf[0, pl.ds(1, out_rows), :].astype(jnp.int32)
    gate_out[...] = buf[1, pl.ds(1, out_rows), :]


def merge_tables(shared, starts, exps, layers, out_rows, pad_row):
    n_items = exps.shape[0]
    group = math.gcd(n_items, 8)
    out = pl.BlockSpec((group, out_rows, LANES), lambda g, *_: (g, 0, 0))
    return pl.pallas_call(
        functools.partial(merge_tables_body, out_rows=out_rows, pad_row=pad_row),
        grid_spec=pltpu.PrefetchScalarGridSpec(
            num_scalar_prefetch=3,
            grid=(n_items // group,),
            in_specs=[pl.BlockSpec(shared.shape, lambda g, *_: (0,) * shared.ndim)],
            out_specs=[out] * 2,
            scratch_shapes=[pltpu.VMEM((2, out_rows + 16, LANES), jnp.float32)],
        ),
        out_shape=[jax.ShapeDtypeStruct((n_items, out_rows, LANES), jnp.int32),
                   jax.ShapeDtypeStruct((n_items, out_rows, LANES), jnp.float32)],
        compiler_params=pltpu.CompilerParams(dimension_semantics=("arbitrary",)),
        cost_estimate=pl.CostEstimate(flops=10**9, bytes_accessed=4 * shared.size, transcendentals=0),
        name="merge_tables",
    )(starts.reshape(-1), exps, layers, shared)


def weight_grad_body(exps, tiles, begins, offsets, names, *refs, parts, n_exp, n_alias, n_moved, first_list, page, layer):
    rows_in, refs = refs[:4], refs[4:]
    idx_all, gate_ref, g_ref, up_ref, w_ref = refs[:5]
    moved, whole, refs = refs[5:5 + n_moved], refs[5 + n_moved:5 + n_moved + n_alias], refs[5 + n_moved + n_alias:]
    (dg_ref, du_ref, dw_ref, og_ref, ou_ref, ow_ref,
     uds, rows, u0, c0, d0, h0, u1, c1, d1, h1, gacc, wacc, idx_s, seen, sem, tsem, *move_refs) = refs
    e = pl.program_id(0)
    ff = g_ref.shape[2]
    slots = 3
    both = ((u0, c0, d0, h0), (u1, c1, d1, h1))

    def table_copy(exp):
        slot = lax.rem(exp, slots)
        at = pl.multiple_of((first_list + exp) * page, PAGE)
        to = pl.multiple_of(slot * page, PAGE)
        return pltpu.make_async_copy(idx_all.at[pl.ds(at, page)], idx_s.at[pl.ds(to, page)], tsem.at[slot])

    def gather_row(at, r):
        rows[pl.ds(r * PITCH, 2 * parts), :] = uds[idx_s[at]].astype(jnp.float32)

    def column(first, count, k):
        return rows[pl.ds(first * PITCH + k, count, stride=PITCH), :]

    n_tok = uds.shape[0] - 8
    run = n_tok // (2 * SOURCES)

    def row_copies(q):
        return [pltpu.make_async_copy(src.at[pl.ds(q * run, run)],
                                      uds.at[pl.ds((2 * q + k % 2) * run, run), pl.ds(k // 2 * parts, parts)], sem.at[q])
                for k, src in enumerate(rows_in)]

    def wait_rows(limit):
        def one(q, carry):
            @pl.when((q >= seen[0]) & (offsets[q] < limit))
            def _():
                for c in row_copies(q):
                    c.wait()
                seen[0] = q + 1

            return carry

        @pl.when(seen[0] < SOURCES)
        def _():
            lax.fori_loop(0, SOURCES, one, 0)

    @pl.when(e == 0)
    def _():
        for q in range(SOURCES):
            for c in row_copies(q):
                c.start()
        seen[0] = 0
        table_copy(0).start()
        table_copy(1).start()
        uds[pl.ds(n_tok, 8)] = jnp.zeros((8, 2 * parts, LANES), jnp.bfloat16)
        for ref in (*both[0], *both[1], gacc, wacc):
            clear(ref)
        table_copy(0).wait()
        wait_rows(WTILE)

        def first_rows(q, carry):
            for r in range(16):
                gather_row(q * 16 + r, q * 16 + r)
            return carry

        lax.fori_loop(0, WTILE // 16, first_rows, 0)

    if moved:
        move_step(e, n_exp, layer + 1, names, moved, whole, *move_refs)

    @pl.when(e + 1 < n_exp)
    def _():
        table_copy(e + 1).wait()

    @pl.when(e + 2 < n_exp)
    def _():
        table_copy(e + 2).start()

    here = lax.rem(e, slots) * page
    there = lax.rem(jnp.minimum(e + 1, n_exp - 1), slots) * page
    n_tiles = tiles[e]
    begin = begins[e]
    gate_rows = WTILE // LANES

    def compute(j, new, old):
        un, cn, dn, hn = new
        uo, co, do, ho = old
        gacc[...] += nn_dot(do[...], uo[...])
        wacc[...] += nn_dot(ho[...], co[...])
        nxt = jnp.where(j + 1 < n_tiles, here + (j + 1) * WTILE, there)
        gu = jnp.concatenate([g_ref[0, 0], up_ref[0, 0]], axis=0)
        for q in range(0, WTILE, CHUNK):
            part = slice(q, q + CHUNK)
            un[part] = jnp.concatenate([column(q, CHUNK, k) for k in range(parts)], axis=1).astype(jnp.bfloat16)
            for p in range(q, q + CHUNK, LANES):
                gate = spread_column(gate_ref[0, pl.ds(j * gate_rows + p // LANES, 1), :])
                for k in range(parts):
                    d = column(p, LANES, parts + k)
                    cn[p:p + LANES, k * LANES:(k + 1) * LANES] = (d * gate).astype(jnp.bfloat16)
            ab = nt_dot(gu, un[part])
            dh = nt_dot(w_ref[0, 0], cn[part])
            for r in range(q, q + CHUNK):
                gather_row(nxt + r, r)
            a, b = ab[:ff], ab[ff:]
            s = jax.nn.sigmoid(a)
            act = a * s
            hn[:, part] = (act * b).astype(jnp.bfloat16)
            dn[:ff, part] = (dh * b * (s * (1.0 + a * (1.0 - s)))).astype(jnp.bfloat16)
            dn[ff:, part] = (dh * act).astype(jnp.bfloat16)

    def tile(j, carry):
        odd = lax.rem(begin + j, 2)
        wait_rows(jnp.where((e == 0) & (j + 1 < n_tiles), (j + 2) * WTILE, page * SOURCES))

        @pl.when(odd == 0)
        def _():
            compute(j, both[0], both[1])

        @pl.when(odd == 1)
        def _():
            compute(j, both[1], both[0])

        @pl.when(j == 0)
        def _():
            dg = gacc[:ff].astype(jnp.bfloat16)
            du = gacc[ff:].astype(jnp.bfloat16)
            dw = wacc[...].astype(jnp.bfloat16)
            dg_ref[0, 0], du_ref[0, 0], dw_ref[0, 0] = dg, du, dw
            og_ref[0], ou_ref[0], ow_ref[0] = dg, du, dw
            gacc[...] = jnp.zeros_like(gacc)
            wacc[...] = jnp.zeros_like(wacc)

        return carry

    lax.fori_loop(0, n_tiles, tile, 0)


def move_step(e, n_steps, layer, names, arrived, whole, buf, in_sem, out_sem):
    per = buf.shape[2]

    def arrive(chunk):
        slot = lax.rem(chunk, 2)
        return [pltpu.make_async_copy(x.at[pl.ds(chunk * per, per)], buf.at[slot, k], in_sem.at[slot])
                for k, x in enumerate(arrived)]

    def leave(chunk):
        slot = lax.rem(chunk, 2)
        return [pltpu.make_async_copy(buf.at[slot, k, i], x.at[layer, names[chunk * per + i]], out_sem.at[slot])
                for k, x in enumerate(whole) for i in range(per)]

    def each(when, copies, act):
        @pl.when(when)
        def _():
            for c in copies:
                act(c)

    each(e >= 2, leave(jnp.maximum(e - 2, 0)), lambda c: c.wait())
    each(e < n_steps, arrive(jnp.minimum(e, n_steps - 1)), lambda c: c.start())
    each(e >= 1, arrive(jnp.maximum(e - 1, 0)), lambda c: c.wait())
    each(e >= 1, leave(jnp.maximum(e - 1, 0)), lambda c: c.start())
    each(e == n_steps, leave(n_steps - 1), lambda c: c.wait())


def weight_grads(layer, first, exps, tiles, offsets, rows, idx_all, gates, weights, full, moved=None):
    n_half, parts, _ = rows[0].shape
    n_tok = 2 * n_half
    n_layers, n_local, ff, d_model = weights[0].shape
    n_exp = exps.shape[0]
    out_rows = gates.shape[1]
    page = out_rows * LANES
    tiles = jnp.concatenate([tiles, jnp.ones((1,), jnp.int32)])
    begins = jnp.cumsum(tiles) - tiles
    any_spec = pl.BlockSpec(memory_space=pl.ANY)
    mine = pl.BlockSpec((1, 1, ff, d_model), lambda e, exps, *_: (layer, exps[jnp.minimum(e, n_exp - 1)], 0, 0))
    done = pl.BlockSpec((1, 1, ff, d_model), lambda e, exps, *_: (layer, exps[jnp.maximum(e - 1, 0)], 0, 0))
    half = pl.BlockSpec((1, ff, d_model), lambda e, *_: (jnp.maximum(e - 1, 0), 0, 0))
    gate_spec = pl.BlockSpec((1, out_rows, LANES), lambda e, *_: (first + jnp.minimum(e, n_exp - 1), 0, 0))
    aliased = list(full) if full is not None else []
    tile_set = [pltpu.VMEM((WTILE, d_model), jnp.bfloat16)] * 2 + [pltpu.VMEM((2 * ff, WTILE), jnp.bfloat16),
                                                                 pltpu.VMEM((ff, WTILE), jnp.bfloat16)]
    arrived, names = moved if moved else ([], exps)
    scratch = []
    if moved:
        scratch = [pltpu.VMEM((2, 3, arrived[0].shape[0] // n_exp, ff, d_model), jnp.bfloat16), pltpu.SemaphoreType.DMA((2,)),
                   pltpu.SemaphoreType.DMA((2,))]
    outs = pl.pallas_call(
        functools.partial(weight_grad_body, parts=parts, n_exp=n_exp, n_alias=len(aliased), n_moved=len(arrived), first_list=first,
                          page=page, layer=layer),
        grid_spec=pltpu.PrefetchScalarGridSpec(
            num_scalar_prefetch=5,
            grid=(n_exp + 1,),
            in_specs=[any_spec] * 5 + [gate_spec] + [mine] * 3 + [any_spec] * (len(arrived) + len(aliased)),
            out_specs=[done] * 3 + [half] * 3,
            scratch_shapes=[pltpu.VMEM((n_tok + 8, 2 * parts, LANES), jnp.bfloat16)]
            + [pltpu.VMEM((WTILE * PITCH + 16, LANES), jnp.float32)] + tile_set * 2
            + [pltpu.VMEM((2 * ff, d_model), jnp.float32), pltpu.VMEM((ff, d_model), jnp.float32),
               pltpu.SMEM((3 * page,), jnp.int32), pltpu.SMEM((1,), jnp.int32), pltpu.SemaphoreType.DMA((SOURCES,)),
               pltpu.SemaphoreType.DMA((3,))] + scratch,
        ),
        out_shape=[jax.ShapeDtypeStruct((n_layers, n_local, ff, d_model), jnp.bfloat16)] * 3
        + [jax.ShapeDtypeStruct((n_exp, ff, d_model), jnp.bfloat16)] * 3,
        input_output_aliases={14 + len(arrived) + k: k for k in range(len(aliased))},
        compiler_params=pltpu.CompilerParams(dimension_semantics=("arbitrary",), vmem_limit_bytes=VMEM_LIMIT),
        cost_estimate=pl.CostEstimate(flops=6 * n_tok * n_exp * d_model * ff,
                                      bytes_accessed=n_tok * d_model * 4 + 9 * n_exp * ff * d_model * 2, transcendentals=0),
        name="weight_grads",
    )(exps, tiles, begins, offsets, names, *rows, idx_all, gates, *weights, *arrived, *aliased)
    return outs[:3], outs[3:]


def merge_body(exps, a, b, c, f0, f1, f2, o0, o1, o2, buf, in_sem, out_sem, *, layer, n_exp):
    halves, wholes = (a, b, c), (o0, o1, o2)

    def arrive(k, q):
        return pltpu.make_async_copy(halves[k].at[q], buf.at[k, q], in_sem.at[k, q])

    def leave(k, q):
        return pltpu.make_async_copy(buf.at[k, q], wholes[k].at[layer, exps[q]], out_sem)

    def each(act):
        def one(q, carry):
            for k in range(3):
                act(k, q)
            return carry

        lax.fori_loop(0, n_exp, one, 0)

    def pass_on(k, q):
        arrive(k, q).wait()
        leave(k, q).start()

    each(lambda k, q: arrive(k, q).start())
    each(pass_on)
    each(lambda k, q: leave(k, q).wait())


def merge_half(layer, exps, half, full):
    n_exp, ff, d_model = half[0].shape
    any_spec = pl.BlockSpec(memory_space=pl.ANY)
    return pl.pallas_call(
        functools.partial(merge_body, layer=layer, n_exp=n_exp),
        grid_spec=pltpu.PrefetchScalarGridSpec(
            num_scalar_prefetch=1, grid=(1,), in_specs=[any_spec] * 6, out_specs=[any_spec] * 3,
            scratch_shapes=[pltpu.VMEM((3, n_exp, ff, d_model), jnp.bfloat16), pltpu.SemaphoreType.DMA((3, n_exp)),
                            pltpu.SemaphoreType.DMA]),
        out_shape=[jax.ShapeDtypeStruct(x.shape, x.dtype) for x in full],
        input_output_aliases={4: 0, 5: 1, 6: 2},
        compiler_params=pltpu.CompilerParams(dimension_semantics=("arbitrary",), vmem_limit_bytes=VMEM_LIMIT),
        cost_estimate=pl.CostEstimate(flops=10**9, bytes_accessed=6 * n_exp * ff * d_model * 2, transcendentals=0),
        name="merge_half",
    )(exps, *half, *full)


def route_tables(ids, gates, ep, n_local):
    n_src, top_k, tok = ids.shape
    n = n_src * top_k * tok
    local = ids - ep * n_local
    here = (local >= 0) & (local < n_local)
    group = jnp.where(here, local, n_local).reshape(-1)
    key, gate = lax.sort((group * n + jnp.arange(n, dtype=jnp.int32), gates.reshape(-1)), num_keys=1, is_stable=False)
    copy = key % n
    token = copy // (top_k * tok) * tok + copy % tok
    token = jnp.pad(token, (0, 2 * PAGE))
    gate = jnp.pad(gate, (0, 2 * PAGE)).reshape(-1, LANES)
    ids = jnp.arange(n_local, dtype=jnp.int32)
    hits = jnp.sum((group.reshape(n_src, -1)[:, :, None] == ids).astype(jnp.int32), axis=1)
    starts = jnp.sum((ids[None, :] < ids[:, None]).astype(jnp.int32) * jnp.sum(hits, axis=0), axis=1)
    ends = starts + jnp.sum(hits, axis=0)
    middle = starts + hits[0]
    bounds = jnp.pad(starts, (0, LANES - n_local), constant_values=0) + jnp.where(jnp.arange(LANES) < n_local, 0, ends[-1])
    runs = [jnp.concatenate(x) for x in ((starts, middle), (middle, ends), (starts, ends))]
    return runs, token, gate, bounds


def deal_experts(bounds, n_local, n_lists):
    load = jnp.sum(bounds[:, 1:n_local + 1] - bounds[:, :n_local], axis=0)
    ids = jnp.arange(n_local, dtype=jnp.int32)
    ahead = (load[None, :] > load[:, None]) | ((load[None, :] == load[:, None]) & (ids[None, :] < ids[:, None]))
    rank = jnp.sum(ahead.astype(jnp.int32), axis=1)
    turn, which = jnp.arange(n_local // n_lists)[None, :], jnp.arange(n_lists)[:, None]
    want = n_lists * turn + jnp.where(turn % 2 == 0, which, n_lists - 1 - which)
    pick = (rank[None, None, :] == want[:, :, None]).astype(jnp.int32)
    tiles = jnp.maximum((jnp.sum(pick * load, axis=2) + WTILE - 1) // WTILE, 1)
    return jnp.sum(pick * ids, axis=2), tiles


def source_offsets(bounds, expert):
    lane = jnp.arange(bounds.shape[1], dtype=jnp.int32)
    counts = jnp.sum(bounds * ((lane == expert + 1).astype(jnp.int32) - (lane == expert).astype(jnp.int32)), axis=1)
    place = jnp.arange(bounds.shape[0], dtype=jnp.int32)
    return jnp.sum((place[None, :] < place[:, None]).astype(jnp.int32) * counts, axis=1)


def after(x, *earlier):
    return lax.optimization_barrier((x, *earlier))[0]


def solution(mesh):
    ep_size = mesh.shape['ep']
    dp_size = mesh.shape['dp']
    tok_spec = P(('dp', 'ep'), None)
    route_spec = P(None, ('dp', 'ep'), None)
    whole_spec = P(None, None, None)
    expert_spec = P(None, 'ep', None, None)
    ep_pairs = [(i, 1 - i) for i in range(ep_size)]
    core_pairs = [(i, i ^ 1) for i in range(dp_size)]

    def device_body(tokens, d_out, expert_ids, gate_vals, w_mix, w_gate, w_up, w_down):
        n_layers = w_mix.shape[0]
        n_local = w_gate.shape[1]
        n_experts = n_local * ep_size
        tok, d_model = tokens.shape
        top_k = expert_ids.shape[2]
        parts = d_model // LANES
        cap = cdiv(CAP_FACTOR * tok * top_k, n_experts)
        ep_id = lax.axis_index('ep').astype(jnp.int32)
        dp_id = lax.axis_index('dp').astype(jnp.int32)
        weights = (jnp.swapaxes(w_gate, 2, 3), jnp.swapaxes(w_up, 2, 3), w_down)

        def swap(x):
            return lax.ppermute(x, 'ep', ep_pairs)

        def spread(x):
            return [lax.all_gather(y, 'dp', axis=0, tiled=True) for y in x]

        def slab(x):
            return x.reshape(tok, parts, LANES)

        def mixed(x, layer):
            return (x.astype(jnp.float32) + jnp.dot(x, w_mix[layer], preferred_element_type=jnp.float32)).astype(jnp.bfloat16)

        ids = jnp.swapaxes(expert_ids, 1, 2)
        gates = jnp.swapaxes(gate_vals, 1, 2)
        mine = jnp.stack([ids.astype(jnp.float32), gates])
        u = mixed(tokens, 0)
        u_slab = slab(u)
        theirs = swap(after(mine, u_slab))
        both = jnp.stack([mine, theirs], 2)
        top = n_layers - 1
        runs, tables, packed = [], [], []

        def add_tables(pair):
            run, token, gate, bounds = route_tables(pair[0].astype(jnp.int32), pair[1], ep_id, n_local)
            runs.append(run)
            tables.append([(token * parts, gate), (token * (2 * parts), gate)])
            spot = dp_id * (2 * tok) + token
            first = jnp.concatenate([spot.reshape(-1, LANES), jnp.pad(bounds.reshape(1, LANES), ((0, 7), (0, 0)))])
            packed.append(jnp.stack([first.astype(jnp.float32), jnp.pad(gate, ((0, 8), (0, 0)))]))

        add_tables(both[:, 0])

        x_in, u_slabs, u_others, xs = tokens, [u_slab], [swap(u_slab)], []
        d_slab = slab(d_out)
        d_other = swap(after(d_slab, u_others[0]))
        d_rows = spread((d_slab, d_other))
        for layer in range(n_layers):
            if layer:
                u = mixed(x_in, layer)
                u_slabs.append(slab(u))
                u_others.append(swap(u_slabs[layer]))
                add_tables(after(both[:, layer], u_slabs[layer]))
            xs.append(x_in)
            if layer < top:
                other, = token_kernel(layer, runs[layer][1], tables[layer][0], (u_slabs[layer], u_others[layer]), weights, (1,))
                sent = swap(other)
                own, = token_kernel(layer, runs[layer][0], tables[layer][0], (after(u_slabs[layer], other), u_others[layer]),
                                    weights, (0,))
                x_in = (u.astype(jnp.float32) + own + sent).astype(jnp.bfloat16)

        shared = lax.all_gather(jnp.stack(packed), 'dp', axis=0)
        starts = shared[:, :, 0, -8].astype(jnp.int32)
        core = dp_id % 2
        n_parts = [PARTS] * top + [1]
        dealt = [deal_experts(starts[:, layer], n_local, 2 * n_parts[layer]) for layer in range(n_layers)]
        mine = [dealt[layer][0][core * n_parts[layer] + part] for layer in range(n_layers) for part in range(n_parts[layer])]
        of_layer = [layer for layer in range(n_layers) for _ in range(n_parts[layer])]
        list_rows = cdiv(cdiv(dp_size * 2 * cap, LANES), 8) * 8 + 8
        idx_all, gate_all = merge_tables(shared, starts, jnp.concatenate(mine),
                                         jnp.concatenate([jnp.full_like(x, layer) for x, layer in zip(mine, of_layer)]),
                                         list_rows, dp_size * 2 * tok)
        idx_all = idx_all.reshape(-1)

        d_y, full, arrived = d_out, None, []
        d_mix = [None] * n_layers
        for layer in reversed(range(n_layers)):
            u_rows = spread((u_slabs[layer], u_others[layer]))
            slabs = (u_slabs[layer], u_others[layer], d_slab, d_other)
            own, other = token_kernel(layer, runs[layer][2], tables[layer][1], slabs, weights)
            d_u = (d_y.astype(jnp.float32) + own + swap(other)).astype(jnp.bfloat16)
            last = other
            if layer == top:
                y_own, last = token_kernel(top, runs[top][2], tables[top][0], (after(u_slabs[top], other), u_others[top]), weights)
            d_mix[layer] = jnp.einsum('td,te->de', xs[layer], d_u, preferred_element_type=jnp.float32).astype(jnp.bfloat16)
            d_y = (d_u.astype(jnp.float32)
                   + jnp.einsum('te,de->td', d_u, w_mix[layer], preferred_element_type=jnp.float32)).astype(jnp.bfloat16)
            lists, tiles = dealt[layer]
            for part in range(n_parts[layer]):
                place = of_layer.index(layer) + part
                own_list, its_list = core * n_parts[layer] + part, (1 - core) * n_parts[layer] + part
                first = sum(x.shape[0] for x in mine[:place])
                full, done = weight_grads(layer, first, mine[place], after(tiles[own_list], last),
                                          source_offsets(starts[:, layer], mine[place][0]), u_rows + d_rows, idx_all, gate_all,
                                          weights, full, arrived.pop(0)[2:] if part and arrived else None)
                arrived.append((layer, part, [lax.ppermute(x, 'dp', core_pairs) for x in done], lists[its_list]))
            if layer:
                d_slab = slab(d_y)
                d_other = swap(d_slab)
                d_rows = spread((d_slab, d_other))
                if layer == top:
                    layer_out = (u.astype(jnp.float32) + y_own + swap(after(last, d_other))).astype(jnp.bfloat16)
        for layer, _, part, names in arrived:
            full = merge_half(layer, names, part, full)
        d_mix = lax.psum(jnp.stack(d_mix), ('dp', 'ep'))
        return (layer_out, d_y, d_mix, jnp.swapaxes(full[0], 2, 3), jnp.swapaxes(full[1], 2, 3), full[2])

    return jax.shard_map(device_body, mesh=mesh,
                         in_specs=(tok_spec, tok_spec, route_spec, route_spec, whole_spec,
                                   expert_spec, expert_spec, expert_spec),
                         out_specs=(tok_spec, tok_spec, whole_spec, expert_spec, expert_spec, expert_spec),
                         check_vma=False)
```

```python
import functools
import math

import jax
import jax.numpy as jnp
from jax import lax
from jax.experimental import pallas as pl
from jax.experimental.pallas import tpu as pltpu
from jax.sharding import PartitionSpec as P


CAP_FACTOR = 3
LANES = 128
TILE = 96
HALF_TILE = 64
WTILE = 768
PARTS = 2
AHEAD = 3
SOURCES = 8
CHUNK = 256
PITCH = 9
BATCH = 16
SLOTS = 8
PAGE = 1024
VMEM_LIMIT = 62 * 2**20


def cdiv(a, b):
    return (a + b - 1) // b


def below(n):
    return jnp.tri(n, k=-1, dtype=jnp.int32)


def nt_dot(a, b):
    return lax.dot_general(a, b, (((1,), (1,)), ((), ())), preferred_element_type=jnp.float32)


def tn_dot(a, b):
    return lax.dot_general(a, b, (((0,), (0,)), ((), ())), preferred_element_type=jnp.float32)


def nn_dot(a, b):
    return lax.dot_general(a, b, (((1,), (0,)), ((), ())), preferred_element_type=jnp.float32)


def clear(ref):
    step = next(n for n in (64, 48, 32, 16, 8) if ref.shape[0] % n == 0)

    def one(q, carry):
        ref[pl.ds(pl.multiple_of(q * step, step), step), :] = jnp.zeros((step, ref.shape[1]), ref.dtype)
        return carry

    lax.fori_loop(0, ref.shape[0] // step, one, 0)


def add_rows(acc, vals_ref, idx, row, tile, pitch, width):
    for b in range(0, tile, BATCH):
        at = [pl.multiple_of(idx[row + b + r], 4) for r in range(BATCH)]
        vals = [acc[pl.ds(at[r], width), :] + vals_ref[pl.ds((b + r) * pitch, width), :] for r in range(BATCH)]
        for r in reversed(range(BATCH)):
            acc[pl.ds(at[r], width), :] = vals[r]


def spread_column(row):
    return jnp.broadcast_to(row, (LANES, LANES)).T


def tile_gates(gates, row):
    pair = gates[pl.ds(lax.div(row, LANES), 2), :]
    skip = lax.rem(row, LANES)
    pair = pltpu.roll(pair, lax.rem(LANES - skip, LANES), 1)
    lane = lax.broadcasted_iota(jnp.int32, (1, LANES), 1)
    return spread_column(jnp.where(lane < LANES - skip, pair[:1], pair[1:]))


def widen(src, dst, pitch, halves, tok):
    step = 32

    def one(q, carry):
        for r in range(step):
            dst[pl.ds((q * step + r) * pitch, pitch), :] = src[q * step + r].astype(jnp.float32)
        return carry

    lax.fori_loop(halves[0] * tok // step, (halves[-1] + 1) * tok // step, one, 0)


def write_sums(acc, outs, tok, parts, pitch, halves):
    step = min(32, tok)

    def copy_out(q, carry):
        r0 = pl.multiple_of(q * step, step)
        for k in range(parts):
            for out, half in zip(outs, halves):
                first = (half * tok + r0) * pitch + k
                out[pl.ds(r0, step), k * LANES:(k + 1) * LANES] = acc[pl.ds(first, step, stride=pitch), :]
        return carry

    lax.fori_loop(0, tok // step, copy_out, 0)


def expert_copies(weights, buf, sem, layer, e):
    slot = lax.rem(e, SLOTS)
    ff = weights[0].shape[2]
    return [pltpu.make_async_copy(w.at[layer, e], buf.at[slot, pl.ds(k * ff, ff)], sem.at[slot])
            for k, w in enumerate(weights)]


def run_tiles(step, weights, wbuf, wsem, runs, tile, layer, prepare):
    n_local = weights[0].shape[1]
    for e in range(SLOTS - 2):
        for c in expert_copies(weights, wbuf, wsem, layer, e):
            c.start()
    prepare()
    for c in expert_copies(weights, wbuf, wsem, layer, 0):
        c.wait()

    def length(e):
        return runs[n_local + e] - runs[e]

    def add_tiles(e, total):
        return total + jnp.maximum(lax.div(length(e) + tile - 1, tile), 1)

    def one(i, carry):
        (e, row, left), (e1, row1, n1), (e2, row2, n2), row3 = carry

        @pl.when(e != e1)
        def _():
            for c in expert_copies(weights, wbuf, wsem, layer, e):
                c.wait()

        @pl.when((e != e1) & (e + SLOTS - 3 < n_local))
        def _():
            for c in expert_copies(weights, wbuf, wsem, layer, e + SLOTS - 3):
                c.start()

        step(row, (lax.rem(e1, SLOTS), row1), (lax.rem(e2, SLOTS), row2, n2), row3)
        more = left > tile
        e_next = jnp.minimum(e + 1, n_local - 1)
        fresh = jnp.where(e + 1 < n_local, length(e_next), 0)
        ahead = (jnp.where(more, e, e_next), jnp.where(more, row + tile, runs[e_next]), jnp.where(more, left - tile, fresh))
        return ahead, (e, row, jnp.minimum(left, tile)), (e1, row1, n1), row2

    none = (0, 0, 0)
    lax.fori_loop(0, lax.fori_loop(0, n_local, add_tiles, 0) + 3, one, ((0, runs[0], length(0)), none, none, 0))


def token_body(runs, idx, gates, *refs, layer, tok, parts, tile, halves, backward):
    n_in = 4 if backward else 2
    sources, weights, outs, refs = refs[:n_in], refs[n_in:n_in + 3], refs[n_in + 3:n_in + 3 + len(halves)], refs[n_in + 3 + len(halves):]
    narrow, wide, rows, vt, acc, mid, wbuf, sem, wsem = refs
    ff = weights[0].shape[2]
    width = parts * n_in // 2
    pitch = width + 1

    def prepare():
        copies = [pltpu.make_async_copy(src, narrow.at[pl.ds(k % 2 * tok, tok), pl.ds(k // 2 * parts, parts)], sem.at[k])
                  for k, src in enumerate(sources) if k % 2 in halves]
        for c in copies:
            c.start()
        for ref in (acc, vt, rows, mid):
            clear(ref)
        for c in copies:
            c.wait()
        widen(narrow, wide, width, halves, tok)

    def column(k):
        return rows[pl.ds(k, tile, stride=pitch), :]

    def step(row, here, before, done):
        slot, row1 = here
        slot2, row2, n2 = before
        old = wbuf[slot2, :2 * ff] if backward else wbuf[slot2, 2 * ff:]
        v = tn_dot(mid[...], old).astype(jnp.bfloat16).astype(jnp.float32)
        u = jnp.concatenate([column(k) for k in range(parts)], axis=1).astype(jnp.bfloat16)
        ab = nt_dot(wbuf[slot, :2 * ff], u)
        if backward:
            gate = tile_gates(gates, row1)[:tile]
            c = jnp.concatenate([(column(parts + k) * gate).astype(jnp.bfloat16) for k in range(parts)], axis=1)
            dh = nt_dot(wbuf[slot, 2 * ff:], c)
        add_rows(acc, vt, idx, done, tile, parts + 1, parts)
        for r in range(tile):
            rows[pl.ds(pitch * r, width), :] = wide[pl.ds(pl.multiple_of(idx[row + r], width), width), :]
        live = lax.broadcasted_iota(jnp.int32, (tile, LANES), 0) < n2
        gate = tile_gates(gates, row2)[:tile]
        for k in range(parts):
            v_k = jnp.where(live, v[:, k * LANES:(k + 1) * LANES] * gate, 0.0)
            vt[pl.ds(k, tile, stride=parts + 1), :] = v_k
        a, b = ab[:ff], ab[ff:]
        s = jax.nn.sigmoid(a)
        act = a * s
        if backward:
            mid[:ff] = (dh * b * (s * (1.0 + a * (1.0 - s)))).astype(jnp.bfloat16)
            mid[ff:] = (dh * act).astype(jnp.bfloat16)
        else:
            mid[...] = (act * b).astype(jnp.bfloat16)

    run_tiles(step, weights, wbuf, wsem, runs, tile, layer, prepare)
    write_sums(acc, outs, tok, parts, width, halves)


def token_kernel(layer, runs, table, slabs, weights, halves=(0, 1)):
    idx, gates = table
    tok, parts, _ = slabs[0].shape
    _, n_local, ff, d_model = weights[0].shape
    backward = len(slabs) > 2
    tile = TILE if len(halves) == 2 else HALF_TILE
    width = parts * len(slabs) // 2
    rows_spec = pl.BlockSpec((tok, d_model), lambda i, *_: (0, 0))
    any_spec = pl.BlockSpec(memory_space=pl.ANY)
    tile_rows = cdiv(tile * (width + 1), 16) * 16
    work = (4 if backward else 3) * len(halves)
    return pl.pallas_call(
        functools.partial(token_body, layer=layer, tok=tok, parts=parts, tile=tile, halves=halves, backward=backward),
        grid_spec=pltpu.PrefetchScalarGridSpec(
            num_scalar_prefetch=2,
            grid=(1,),
            in_specs=[pl.BlockSpec(gates.shape, lambda i, *_: (0, 0))] + [any_spec] * (len(slabs) + 3),
            out_specs=[rows_spec] * len(halves),
            scratch_shapes=[pltpu.VMEM((2 * tok, width, LANES), jnp.bfloat16), pltpu.VMEM((2 * tok * width, LANES), jnp.float32),
                            pltpu.VMEM((tile_rows, LANES), jnp.float32), pltpu.VMEM((tile_rows, LANES), jnp.float32),
                            pltpu.VMEM((2 * tok * width, LANES), jnp.float32),
                            pltpu.VMEM((2 * ff if backward else ff, tile), jnp.bfloat16),
                            pltpu.VMEM((SLOTS, 3 * ff, d_model), jnp.bfloat16),
                            pltpu.SemaphoreType.DMA((len(slabs),)), pltpu.SemaphoreType.DMA((SLOTS,))],
        ),
        out_shape=[jax.ShapeDtypeStruct((tok, d_model), jnp.float32)] * len(halves),
        compiler_params=pltpu.CompilerParams(dimension_semantics=("arbitrary",), vmem_limit_bytes=VMEM_LIMIT),
        cost_estimate=pl.CostEstimate(flops=work * 2 * 8 * tok * d_model * ff * 4,
                                      bytes_accessed=3 * n_local * ff * d_model * 2, transcendentals=0),
        name="experts_backward" if backward else "experts_forward",
    )(runs, idx, gates, *slabs, *weights)


def merge_tables_body(st, exps, layers, table, idx_ref, gate_ref, buf, *, out_rows, pad_row):
    group = idx_ref.shape[0]

    def one(q, carry):
        item = pl.program_id(0) * group + q
        merge_expert(exps[item], layers[item], st, table, idx_ref.at[q], gate_ref.at[q], buf, out_rows, pad_row)
        return carry

    lax.fori_loop(0, group, one, 0)


def merge_expert(exp, layer, st, table, idx_out, gate_out, buf, out_rows, pad_row):
    src, n_layers = table.shape[:2]
    buf[0] = jnp.full(buf.shape[1:], float(pad_row), jnp.float32)
    buf[1] = jnp.zeros(buf.shape[1:], jnp.float32)
    row = lax.broadcasted_iota(jnp.int32, (8, LANES), 0)
    lane = lax.broadcasted_iota(jnp.int32, (8, LANES), 1)
    off = 0
    for d in range(src):
        at = (d * n_layers + layer) * LANES + exp
        first = st[at]
        count = st[at + 1] - first
        to = lax.rem(off, LANES) + LANES
        shift = to - lax.rem(first, LANES)
        over = lax.rem(shift, LANES)
        start = lax.div(off, LANES)
        place = row * LANES + lane
        take = (place >= to) & (place < to + count)
        for kind in range(2):
            x = table[d, layer, kind, pl.ds(lax.div(first, LANES), 8), :]
            x = pltpu.roll(pltpu.roll(x, over, 1), lax.div(shift, LANES), 0)
            x = jnp.where(lane >= over, x, pltpu.roll(x, 1, 0))
            old = buf[kind, pl.ds(start, 8), :]
            buf[kind, pl.ds(start, 8), :] = jnp.where(take, x, old)
        off = off + count
    idx_out[...] = buf[0, pl.ds(1, out_rows), :].astype(jnp.int32)
    gate_out[...] = buf[1, pl.ds(1, out_rows), :]


def merge_tables(shared, starts, exps, layers, out_rows, pad_row):
    n_items = exps.shape[0]
    group = math.gcd(n_items, 8)
    out = pl.BlockSpec((group, out_rows, LANES), lambda g, *_: (g, 0, 0))
    return pl.pallas_call(
        functools.partial(merge_tables_body, out_rows=out_rows, pad_row=pad_row),
        grid_spec=pltpu.PrefetchScalarGridSpec(
            num_scalar_prefetch=3,
            grid=(n_items // group,),
            in_specs=[pl.BlockSpec(shared.shape, lambda g, *_: (0,) * shared.ndim)],
            out_specs=[out] * 2,
            scratch_shapes=[pltpu.VMEM((2, out_rows + 16, LANES), jnp.float32)],
        ),
        out_shape=[jax.ShapeDtypeStruct((n_items, out_rows, LANES), jnp.int32),
                   jax.ShapeDtypeStruct((n_items, out_rows, LANES), jnp.float32)],
        compiler_params=pltpu.CompilerParams(dimension_semantics=("arbitrary",)),
        cost_estimate=pl.CostEstimate(flops=10**9, bytes_accessed=4 * shared.size, transcendentals=0),
        name="merge_tables",
    )(starts.reshape(-1), exps, layers, shared)


def weight_grad_body(exps, tiles, begins, offsets, names, *refs, parts, n_exp, n_alias, n_moved, first_list, page, layer):
    rows_in, refs = refs[:4], refs[4:]
    idx_all, gate_ref, g_ref, up_ref, w_ref = refs[:5]
    moved, whole, refs = refs[5:5 + n_moved], refs[5 + n_moved:5 + n_moved + n_alias], refs[5 + n_moved + n_alias:]
    (dg_ref, du_ref, dw_ref, og_ref, ou_ref, ow_ref,
     uds, rows, u0, c0, d0, h0, u1, c1, d1, h1, gacc, wacc, idx_s, seen, sem, tsem, *move_refs) = refs
    e = pl.program_id(0)
    ff = g_ref.shape[2]
    slots = 3
    both = ((u0, c0, d0, h0), (u1, c1, d1, h1))

    def table_copy(exp):
        slot = lax.rem(exp, slots)
        at = pl.multiple_of((first_list + exp) * page, PAGE)
        to = pl.multiple_of(slot * page, PAGE)
        return pltpu.make_async_copy(idx_all.at[pl.ds(at, page)], idx_s.at[pl.ds(to, page)], tsem.at[slot])

    def gather_row(at, r):
        rows[pl.ds(r * PITCH, 2 * parts), :] = uds[idx_s[at]].astype(jnp.float32)

    def column(first, count, k):
        return rows[pl.ds(first * PITCH + k, count, stride=PITCH), :]

    n_tok = uds.shape[0] - 8
    run = n_tok // (2 * SOURCES)

    def row_copies(q):
        return [pltpu.make_async_copy(src.at[pl.ds(q * run, run)],
                                      uds.at[pl.ds((2 * q + k % 2) * run, run), pl.ds(k // 2 * parts, parts)], sem.at[q])
                for k, src in enumerate(rows_in)]

    def wait_rows(limit):
        def one(q, carry):
            @pl.when((q >= seen[0]) & (offsets[q] < limit))
            def _():
                for c in row_copies(q):
                    c.wait()
                seen[0] = q + 1

                @pl.when(q + AHEAD < SOURCES)
                def _():
                    for c in row_copies(q + AHEAD):
                        c.start()

            return carry

        @pl.when(seen[0] < SOURCES)
        def _():
            lax.fori_loop(0, SOURCES, one, 0)

    @pl.when(e == 0)
    def _():
        for q in range(AHEAD):
            for c in row_copies(q):
                c.start()
        seen[0] = 0
        seen[1] = 1
        table_copy(0).start()
        table_copy(1).start()
        uds[pl.ds(n_tok, 8)] = jnp.zeros((8, 2 * parts, LANES), jnp.bfloat16)
        for ref in (*both[0], *both[1]):
            clear(ref)
        table_copy(0).wait()
        wait_rows(WTILE)

        def first_rows(q, carry):
            for r in range(16):
                gather_row(q * 16 + r, q * 16 + r)
            return carry

        lax.fori_loop(0, WTILE // 16, first_rows, 0)

    if moved:
        move_step(e, n_exp, layer + 1, names, moved, whole, *move_refs)

    @pl.when(e + 1 < n_exp)
    def _():
        table_copy(e + 1).wait()

    @pl.when(e + 2 < n_exp)
    def _():
        table_copy(e + 2).start()

    here = lax.rem(e, slots) * page
    there = lax.rem(jnp.minimum(e + 1, n_exp - 1), slots) * page
    n_tiles = tiles[e]
    begin = begins[e]
    gate_rows = WTILE // LANES

    def compute(j, new, old):
        un, cn, dn, hn = new
        uo, co, do, ho = old
        fresh = seen[1] == 1
        gacc[...] = jnp.where(fresh, 0.0, gacc[...]) + nn_dot(do[...], uo[...])
        wacc[...] = jnp.where(fresh, 0.0, wacc[...]) + nn_dot(ho[...], co[...])
        nxt = jnp.where(j + 1 < n_tiles, here + (j + 1) * WTILE, there)
        gu = jnp.concatenate([g_ref[0, 0], up_ref[0, 0]], axis=0)
        for q in range(0, WTILE, CHUNK):
            part = slice(q, q + CHUNK)
            un[part] = jnp.concatenate([column(q, CHUNK, k) for k in range(parts)], axis=1).astype(jnp.bfloat16)
            for p in range(q, q + CHUNK, LANES):
                gate = spread_column(gate_ref[0, pl.ds(j * gate_rows + p // LANES, 1), :])
                for k in range(parts):
                    d = column(p, LANES, parts + k)
                    cn[p:p + LANES, k * LANES:(k + 1) * LANES] = (d * gate).astype(jnp.bfloat16)
            ab = nt_dot(gu, un[part])
            dh = nt_dot(w_ref[0, 0], cn[part])
            for r in range(q, q + CHUNK):
                gather_row(nxt + r, r)
            a, b = ab[:ff], ab[ff:]
            s = jax.nn.sigmoid(a)
            act = a * s
            hn[:, part] = (act * b).astype(jnp.bfloat16)
            dn[:ff, part] = (dh * b * (s * (1.0 + a * (1.0 - s)))).astype(jnp.bfloat16)
            dn[ff:, part] = (dh * act).astype(jnp.bfloat16)

    def tile(j, carry):
        odd = lax.rem(begin + j, 2)
        wait_rows(jnp.where((e == 0) & (j + 1 < n_tiles), (j + 2) * WTILE, page * SOURCES))

        @pl.when(odd == 0)
        def _():
            compute(j, both[0], both[1])

        @pl.when(odd == 1)
        def _():
            compute(j, both[1], both[0])

        seen[1] = jnp.where(j == 0, 1, 0)

        @pl.when(j == 0)
        def _():
            dg = gacc[:ff].astype(jnp.bfloat16)
            du = gacc[ff:].astype(jnp.bfloat16)
            dw = wacc[...].astype(jnp.bfloat16)
            dg_ref[0, 0], du_ref[0, 0], dw_ref[0, 0] = dg, du, dw
            og_ref[0], ou_ref[0], ow_ref[0] = dg, du, dw

        return carry

    lax.fori_loop(0, n_tiles, tile, 0)


def move_step(e, n_steps, layer, names, arrived, whole, buf, in_sem, out_sem):
    per = buf.shape[2]

    def arrive(chunk):
        slot = lax.rem(chunk, 2)
        return [pltpu.make_async_copy(x.at[pl.ds(chunk * per, per)], buf.at[slot, k], in_sem.at[slot])
                for k, x in enumerate(arrived)]

    def leave(chunk):
        slot = lax.rem(chunk, 2)
        return [pltpu.make_async_copy(buf.at[slot, k, i], x.at[layer, names[chunk * per + i]], out_sem.at[slot])
                for k, x in enumerate(whole) for i in range(per)]

    def each(when, copies, act):
        @pl.when(when)
        def _():
            for c in copies:
                act(c)

    each(e >= 2, leave(jnp.maximum(e - 2, 0)), lambda c: c.wait())
    each(e < n_steps, arrive(jnp.minimum(e, n_steps - 1)), lambda c: c.start())
    each(e >= 1, arrive(jnp.maximum(e - 1, 0)), lambda c: c.wait())
    each(e >= 1, leave(jnp.maximum(e - 1, 0)), lambda c: c.start())
    each(e == n_steps, leave(n_steps - 1), lambda c: c.wait())


def weight_grads(layer, first, exps, tiles, offsets, rows, idx_all, gates, weights, full, moved=None):
    n_half, parts, _ = rows[0].shape
    n_tok = 2 * n_half
    n_layers, n_local, ff, d_model = weights[0].shape
    n_exp = exps.shape[0]
    out_rows = gates.shape[1]
    page = out_rows * LANES
    tiles = jnp.concatenate([tiles, jnp.ones((1,), jnp.int32)])
    begins = jnp.cumsum(tiles) - tiles
    any_spec = pl.BlockSpec(memory_space=pl.ANY)
    mine = pl.BlockSpec((1, 1, ff, d_model), lambda e, exps, *_: (layer, exps[jnp.minimum(e, n_exp - 1)], 0, 0))
    done = pl.BlockSpec((1, 1, ff, d_model), lambda e, exps, *_: (layer, exps[jnp.maximum(e - 1, 0)], 0, 0))
    half = pl.BlockSpec((1, ff, d_model), lambda e, *_: (jnp.maximum(e - 1, 0), 0, 0))
    gate_spec = pl.BlockSpec((1, out_rows, LANES), lambda e, *_: (first + jnp.minimum(e, n_exp - 1), 0, 0))
    aliased = list(full) if full is not None else []
    tile_set = [pltpu.VMEM((WTILE, d_model), jnp.bfloat16)] * 2 + [pltpu.VMEM((2 * ff, WTILE), jnp.bfloat16),
                                                                 pltpu.VMEM((ff, WTILE), jnp.bfloat16)]
    arrived, names = moved if moved else ([], exps)
    scratch = []
    if moved:
        scratch = [pltpu.VMEM((2, 3, arrived[0].shape[0] // n_exp, ff, d_model), jnp.bfloat16), pltpu.SemaphoreType.DMA((2,)),
                   pltpu.SemaphoreType.DMA((2,))]
    outs = pl.pallas_call(
        functools.partial(weight_grad_body, parts=parts, n_exp=n_exp, n_alias=len(aliased), n_moved=len(arrived), first_list=first,
                          page=page, layer=layer),
        grid_spec=pltpu.PrefetchScalarGridSpec(
            num_scalar_prefetch=5,
            grid=(n_exp + 1,),
            in_specs=[any_spec] * 5 + [gate_spec] + [mine] * 3 + [any_spec] * (len(arrived) + len(aliased)),
            out_specs=[done] * 3 + [half] * 3,
            scratch_shapes=[pltpu.VMEM((n_tok + 8, 2 * parts, LANES), jnp.bfloat16)]
            + [pltpu.VMEM((WTILE * PITCH + 16, LANES), jnp.float32)] + tile_set * 2
            + [pltpu.VMEM((2 * ff, d_model), jnp.float32), pltpu.VMEM((ff, d_model), jnp.float32),
               pltpu.SMEM((3 * page,), jnp.int32), pltpu.SMEM((2,), jnp.int32), pltpu.SemaphoreType.DMA((SOURCES,)),
               pltpu.SemaphoreType.DMA((3,))] + scratch,
        ),
        out_shape=[jax.ShapeDtypeStruct((n_layers, n_local, ff, d_model), jnp.bfloat16)] * 3
        + [jax.ShapeDtypeStruct((n_exp, ff, d_model), jnp.bfloat16)] * 3,
        input_output_aliases={14 + len(arrived) + k: k for k in range(len(aliased))},
        compiler_params=pltpu.CompilerParams(dimension_semantics=("arbitrary",), vmem_limit_bytes=VMEM_LIMIT),
        cost_estimate=pl.CostEstimate(flops=6 * n_tok * n_exp * d_model * ff,
                                      bytes_accessed=n_tok * d_model * 4 + 9 * n_exp * ff * d_model * 2, transcendentals=0),
        name="weight_grads",
    )(exps, tiles, begins, offsets, names, *rows, idx_all, gates, *weights, *arrived, *aliased)
    return outs[:3], outs[3:]


def merge_body(exps, a, b, c, f0, f1, f2, o0, o1, o2, buf, in_sem, out_sem, *, layer, n_exp):
    halves, wholes = (a, b, c), (o0, o1, o2)

    def arrive(k, q):
        return pltpu.make_async_copy(halves[k].at[q], buf.at[k, q], in_sem.at[k, q])

    def leave(k, q):
        return pltpu.make_async_copy(buf.at[k, q], wholes[k].at[layer, exps[q]], out_sem)

    def each(act):
        def one(q, carry):
            for k in range(3):
                act(k, q)
            return carry

        lax.fori_loop(0, n_exp, one, 0)

    def pass_on(k, q):
        arrive(k, q).wait()
        leave(k, q).start()

    each(lambda k, q: arrive(k, q).start())
    each(pass_on)
    each(lambda k, q: leave(k, q).wait())


def merge_half(layer, exps, half, full):
    n_exp, ff, d_model = half[0].shape
    any_spec = pl.BlockSpec(memory_space=pl.ANY)
    return pl.pallas_call(
        functools.partial(merge_body, layer=layer, n_exp=n_exp),
        grid_spec=pltpu.PrefetchScalarGridSpec(
            num_scalar_prefetch=1, grid=(1,), in_specs=[any_spec] * 6, out_specs=[any_spec] * 3,
            scratch_shapes=[pltpu.VMEM((3, n_exp, ff, d_model), jnp.bfloat16), pltpu.SemaphoreType.DMA((3, n_exp)),
                            pltpu.SemaphoreType.DMA]),
        out_shape=[jax.ShapeDtypeStruct(x.shape, x.dtype) for x in full],
        input_output_aliases={4: 0, 5: 1, 6: 2},
        compiler_params=pltpu.CompilerParams(dimension_semantics=("arbitrary",), vmem_limit_bytes=VMEM_LIMIT),
        cost_estimate=pl.CostEstimate(flops=10**9, bytes_accessed=6 * n_exp * ff * d_model * 2, transcendentals=0),
        name="merge_half",
    )(exps, *half, *full)


def route_tables(ids, gates, ep, n_local):
    n_src, top_k, tok = ids.shape
    n = n_src * top_k * tok
    local = ids - ep * n_local
    here = (local >= 0) & (local < n_local)
    group = jnp.where(here, local, n_local).reshape(-1)
    key, gate = lax.sort((group * n + jnp.arange(n, dtype=jnp.int32), gates.reshape(-1)), num_keys=1, is_stable=False)
    copy = key % n
    token = copy // (top_k * tok) * tok + copy % tok
    token = jnp.pad(token, (0, 2 * PAGE))
    gate = jnp.pad(gate, (0, 2 * PAGE)).reshape(-1, LANES)
    ids = jnp.arange(n_local, dtype=jnp.int32)
    hits = jnp.sum((group.reshape(n_src, -1, 1) == ids).astype(jnp.int32), axis=1)
    starts = jnp.sum(below(n_local) * jnp.sum(hits, axis=0), axis=1)
    ends = starts + jnp.sum(hits, axis=0)
    middle = starts + hits[0]
    bounds = jnp.pad(starts, (0, LANES - n_local), mode='edge')
    bounds = jnp.where(jnp.arange(LANES) < n_local, bounds, ends[-1])
    runs = [jnp.concatenate(x) for x in ((starts, middle), (middle, ends), (starts, ends))]
    return runs, token, gate, bounds


def deal_experts(bounds, n_local, n_lists):
    load = jnp.sum(bounds[:, 1:n_local + 1] - bounds[:, :n_local], axis=0)
    ids = jnp.arange(n_local, dtype=jnp.int32)
    mine = load.reshape(-1, 1)
    rank = jnp.sum((load > mine).astype(jnp.int32) + (load == mine).astype(jnp.int32) * below(n_local), axis=1)
    turn, which = jnp.arange(n_local // n_lists), jnp.arange(n_lists).reshape(-1, 1)
    want = n_lists * turn + jnp.where(turn % 2 == 0, which, n_lists - 1 - which)
    pick = (rank == jnp.expand_dims(want, 2)).astype(jnp.int32)
    tiles = jnp.maximum((jnp.sum(pick * load, axis=2) + WTILE - 1) // WTILE, 1)
    return jnp.sum(pick * ids, axis=2), tiles


def source_offsets(bounds, expert):
    lane = jnp.arange(bounds.shape[1], dtype=jnp.int32)
    counts = jnp.sum(bounds * ((lane == expert + 1).astype(jnp.int32) - (lane == expert).astype(jnp.int32)), axis=1)
    return jnp.sum(below(bounds.shape[0]) * counts, axis=1)


def after(x, *earlier):
    return lax.optimization_barrier((x, *earlier))[0]


def solution(mesh):
    ep_size = mesh.shape['ep']
    dp_size = mesh.shape['dp']
    tok_spec = P(('dp', 'ep'), None)
    route_spec = P(None, ('dp', 'ep'), None)
    whole_spec = P(None, None, None)
    expert_spec = P(None, 'ep', None, None)
    ep_pairs = [(i, 1 - i) for i in range(ep_size)]
    core_pairs = [(i, i ^ 1) for i in range(dp_size)]

    def device_body(tokens, d_out, expert_ids, gate_vals, w_mix, w_gate, w_up, w_down):
        n_layers = w_mix.shape[0]
        n_local = w_gate.shape[1]
        n_experts = n_local * ep_size
        tok, d_model = tokens.shape
        top_k = expert_ids.shape[2]
        parts = d_model // LANES
        cap = cdiv(CAP_FACTOR * tok * top_k, n_experts)
        ep_id = lax.axis_index('ep').astype(jnp.int32)
        dp_id = lax.axis_index('dp').astype(jnp.int32)
        weights = (jnp.swapaxes(w_gate, 2, 3), jnp.swapaxes(w_up, 2, 3), w_down)

        def swap(x):
            return lax.ppermute(x, 'ep', ep_pairs)

        def spread(x):
            return [lax.all_gather(y, 'dp', axis=0, tiled=True) for y in x]

        def slab(x):
            return x.reshape(tok, parts, LANES)

        def mixed(x, layer):
            return (x.astype(jnp.float32) + jnp.dot(x, w_mix[layer], preferred_element_type=jnp.float32)).astype(jnp.bfloat16)

        ids = jnp.swapaxes(expert_ids, 1, 2)
        gates = jnp.swapaxes(gate_vals, 1, 2)
        mine = jnp.stack([ids.astype(jnp.float32), gates])
        u = mixed(tokens, 0)
        u_slab = slab(u)
        theirs = swap(after(mine, u_slab))
        both = jnp.stack([mine, theirs], 2)
        top = n_layers - 1
        runs, tables, packed = [], [], []

        def add_tables(pair):
            run, token, gate, bounds = route_tables(pair[0].astype(jnp.int32), pair[1], ep_id, n_local)
            runs.append(run)
            tables.append([(token * parts, gate), (token * (2 * parts), gate)])
            spot = dp_id * (2 * tok) + token
            first = jnp.concatenate([spot.reshape(-1, LANES), jnp.pad(bounds.reshape(1, LANES), ((0, 7), (0, 0)))])
            packed.append(jnp.stack([first.astype(jnp.float32), jnp.pad(gate, ((0, 8), (0, 0)))]))

        add_tables(both[:, 0])

        x_in, u_slabs, u_others, xs = tokens, [u_slab], [swap(u_slab)], []
        d_slab = slab(d_out)
        d_other = swap(after(d_slab, u_others[0]))
        d_rows = spread((d_slab, d_other))
        for layer in range(n_layers):
            if layer:
                u = mixed(x_in, layer)
                u_slabs.append(slab(u))
                u_others.append(swap(u_slabs[layer]))
                add_tables(after(both[:, layer], u_slabs[layer]))
            xs.append(x_in)
            if layer < top:
                other, = token_kernel(layer, runs[layer][1], tables[layer][0], (u_slabs[layer], u_others[layer]), weights, (1,))
                sent = swap(other)
                own, = token_kernel(layer, runs[layer][0], tables[layer][0], (after(u_slabs[layer], other), u_others[layer]),
                                    weights, (0,))
                x_in = (u.astype(jnp.float32) + own + sent).astype(jnp.bfloat16)

        shared = lax.all_gather(jnp.stack(packed), 'dp', axis=0)
        starts = shared[:, :, 0, -8].astype(jnp.int32)
        core = dp_id % 2
        n_parts = [PARTS] * top + [1]
        dealt = [deal_experts(starts[:, layer], n_local, 2 * n_parts[layer]) for layer in range(n_layers)]
        mine = [dealt[layer][0][core * n_parts[layer] + part] for layer in range(n_layers) for part in range(n_parts[layer])]
        of_layer = [layer for layer in range(n_layers) for _ in range(n_parts[layer])]
        list_rows = cdiv(cdiv(dp_size * 2 * cap, LANES), 8) * 8 + 8
        idx_all, gate_all = merge_tables(shared, starts, jnp.concatenate(mine),
                                         jnp.concatenate([jnp.full_like(x, layer) for x, layer in zip(mine, of_layer)]),
                                         list_rows, dp_size * 2 * tok)
        offsets = [source_offsets(starts[:, layer], x[0]) for x, layer in zip(mine, of_layer)]
        idx_all = idx_all.reshape(-1)

        d_y, full, arrived = d_out, None, []
        d_mix = [None] * n_layers
        for layer in reversed(range(n_layers)):
            u_rows = spread((u_slabs[layer], u_others[layer]))
            slabs = (u_slabs[layer], u_others[layer], d_slab, d_other)
            own, other = token_kernel(layer, runs[layer][2], tables[layer][1], slabs, weights)
            d_u = (d_y.astype(jnp.float32) + own + swap(other)).astype(jnp.bfloat16)
            last = other
            if layer == top:
                y_own, last = token_kernel(top, runs[top][2], tables[top][0], (after(u_slabs[top], other), u_others[top]), weights)
            d_mix[layer] = jnp.einsum('td,te->de', xs[layer], d_u, preferred_element_type=jnp.float32).astype(jnp.bfloat16)
            d_y = (d_u.astype(jnp.float32)
                   + jnp.einsum('te,de->td', d_u, w_mix[layer], preferred_element_type=jnp.float32)).astype(jnp.bfloat16)
            lists, tiles = dealt[layer]
            for part in range(n_parts[layer]):
                place = of_layer.index(layer) + part
                own_list, its_list = core * n_parts[layer] + part, (1 - core) * n_parts[layer] + part
                first = sum(x.shape[0] for x in mine[:place])
                full, done = weight_grads(layer, first, mine[place], after(tiles[own_list], last),
                                          offsets[place], u_rows + d_rows, idx_all, gate_all, weights, full,
                                          arrived.pop(0)[2:] if part and arrived else None)
                arrived.append((layer, part, [lax.ppermute(x, 'dp', core_pairs) for x in done], lists[its_list]))
            if layer:
                d_slab = slab(d_y)
                d_other = swap(d_slab)
                d_rows = spread((d_slab, d_other))
                if layer == top:
                    layer_out = (u.astype(jnp.float32) + y_own + swap(after(last, d_other))).astype(jnp.bfloat16)
        for layer, _, part, names in arrived:
            full = merge_half(layer, names, part, full)
        d_mix = lax.psum(jnp.stack(d_mix), ('dp', 'ep'))
        return (layer_out, d_y, d_mix, jnp.swapaxes(full[0], 2, 3), jnp.swapaxes(full[1], 2, 3), full[2])

    return jax.shard_map(device_body, mesh=mesh,
                         in_specs=(tok_spec, tok_spec, route_spec, route_spec, whole_spec,
                                   expert_spec, expert_spec, expert_spec),
                         out_specs=(tok_spec, tok_spec, whole_spec, expert_spec, expert_spec, expert_spec),
                         check_vma=False)
```

```python
import functools
import math

import jax
import jax.numpy as jnp
from jax import lax
from jax.experimental import pallas as pl
from jax.experimental.pallas import tpu as pltpu
from jax.sharding import PartitionSpec as P


CAP_FACTOR = 3
LANES = 128
TILE = 96
HALF_TILE = 64
WTILE = 768
PARTS = 2
SOURCES = 8
CHUNK = 256
PITCH = 9
BATCH = 16
SLOTS = 8
PAGE = 1024
VMEM_LIMIT = 62 * 2**20


def cdiv(a, b):
    return (a + b - 1) // b


def below(n):
    return jnp.tri(n, k=-1, dtype=jnp.int32)


def nt_dot(a, b):
    return lax.dot_general(a, b, (((1,), (1,)), ((), ())), preferred_element_type=jnp.float32)


def tn_dot(a, b):
    return lax.dot_general(a, b, (((0,), (0,)), ((), ())), preferred_element_type=jnp.float32)


def nn_dot(a, b):
    return lax.dot_general(a, b, (((1,), (0,)), ((), ())), preferred_element_type=jnp.float32)


def clear(ref):
    step = next(n for n in (64, 48, 32, 16, 8) if ref.shape[0] % n == 0)

    def one(q, carry):
        ref[pl.ds(pl.multiple_of(q * step, step), step), :] = jnp.zeros((step, ref.shape[1]), ref.dtype)
        return carry

    lax.fori_loop(0, ref.shape[0] // step, one, 0)


def add_rows(acc, vals_ref, idx, row, tile, pitch, width):
    for b in range(0, tile, BATCH):
        at = [pl.multiple_of(idx[row + b + r], 4) for r in range(BATCH)]
        vals = [acc[pl.ds(at[r], width), :] + vals_ref[pl.ds((b + r) * pitch, width), :] for r in range(BATCH)]
        for r in reversed(range(BATCH)):
            acc[pl.ds(at[r], width), :] = vals[r]


def spread_column(row):
    return jnp.broadcast_to(row, (LANES, LANES)).T


def tile_gates(gates, row):
    pair = gates[pl.ds(lax.div(row, LANES), 2), :]
    skip = lax.rem(row, LANES)
    pair = pltpu.roll(pair, lax.rem(LANES - skip, LANES), 1)
    lane = lax.broadcasted_iota(jnp.int32, (1, LANES), 1)
    return spread_column(jnp.where(lane < LANES - skip, pair[:1], pair[1:]))


def widen(src, dst, pitch, halves, tok):
    step = 32

    def one(q, carry):
        for r in range(step):
            dst[pl.ds((q * step + r) * pitch, pitch), :] = src[q * step + r].astype(jnp.float32)
        return carry

    lax.fori_loop(halves[0] * tok // step, (halves[-1] + 1) * tok // step, one, 0)


def write_sums(acc, outs, tok, parts, pitch, halves):
    step = min(32, tok)

    def copy_out(q, carry):
        r0 = pl.multiple_of(q * step, step)
        for k in range(parts):
            for out, half in zip(outs, halves):
                first = (half * tok + r0) * pitch + k
                out[pl.ds(r0, step), k * LANES:(k + 1) * LANES] = acc[pl.ds(first, step, stride=pitch), :]
        return carry

    lax.fori_loop(0, tok // step, copy_out, 0)


def expert_copies(weights, buf, sem, layer, e):
    slot = lax.rem(e, SLOTS)
    ff = weights[0].shape[2]
    return [pltpu.make_async_copy(w.at[layer, e], buf.at[slot, pl.ds(k * ff, ff)], sem.at[slot])
            for k, w in enumerate(weights)]


def run_tiles(step, weights, wbuf, wsem, runs, tile, layer, prepare):
    n_local = weights[0].shape[1]
    for e in range(SLOTS - 2):
        for c in expert_copies(weights, wbuf, wsem, layer, e):
            c.start()
    prepare()
    for c in expert_copies(weights, wbuf, wsem, layer, 0):
        c.wait()

    def length(e):
        return runs[n_local + e] - runs[e]

    def add_tiles(e, total):
        return total + jnp.maximum(lax.div(length(e) + tile - 1, tile), 1)

    def one(i, carry):
        (e, row, left), (e1, row1, n1), (e2, row2, n2), row3 = carry

        @pl.when(e != e1)
        def _():
            for c in expert_copies(weights, wbuf, wsem, layer, e):
                c.wait()

        @pl.when((e != e1) & (e + SLOTS - 3 < n_local))
        def _():
            for c in expert_copies(weights, wbuf, wsem, layer, e + SLOTS - 3):
                c.start()

        step(row, (lax.rem(e1, SLOTS), row1), (lax.rem(e2, SLOTS), row2, n2), row3)
        more = left > tile
        e_next = jnp.minimum(e + 1, n_local - 1)
        fresh = jnp.where(e + 1 < n_local, length(e_next), 0)
        ahead = (jnp.where(more, e, e_next), jnp.where(more, row + tile, runs[e_next]), jnp.where(more, left - tile, fresh))
        return ahead, (e, row, jnp.minimum(left, tile)), (e1, row1, n1), row2

    none = (0, 0, 0)
    lax.fori_loop(0, lax.fori_loop(0, n_local, add_tiles, 0) + 3, one, ((0, runs[0], length(0)), none, none, 0))


def token_body(runs, idx, gates, *refs, layer, tok, parts, tile, halves, backward):
    n_in = 4 if backward else 2
    sources, weights, outs, refs = refs[:n_in], refs[n_in:n_in + 3], refs[n_in + 3:n_in + 3 + len(halves)], refs[n_in + 3 + len(halves):]
    narrow, wide, rows, vt, acc, mid, wbuf, sem, wsem = refs
    ff = weights[0].shape[2]
    width = parts * n_in // 2
    pitch = width + 1

    def prepare():
        copies = [pltpu.make_async_copy(src, narrow.at[pl.ds(k % 2 * tok, tok), pl.ds(k // 2 * parts, parts)], sem.at[k])
                  for k, src in enumerate(sources) if k % 2 in halves]
        for c in copies:
            c.start()
        for ref in (acc, vt, rows, mid):
            clear(ref)
        for c in copies:
            c.wait()
        widen(narrow, wide, width, halves, tok)

    def column(k):
        return rows[pl.ds(k, tile, stride=pitch), :]

    def step(row, here, before, done):
        slot, row1 = here
        slot2, row2, n2 = before
        old = wbuf[slot2, :2 * ff] if backward else wbuf[slot2, 2 * ff:]
        v = tn_dot(mid[...], old).astype(jnp.bfloat16).astype(jnp.float32)
        u = jnp.concatenate([column(k) for k in range(parts)], axis=1).astype(jnp.bfloat16)
        ab = nt_dot(wbuf[slot, :2 * ff], u)
        if backward:
            gate = tile_gates(gates, row1)[:tile]
            c = jnp.concatenate([(column(parts + k) * gate).astype(jnp.bfloat16) for k in range(parts)], axis=1)
            dh = nt_dot(wbuf[slot, 2 * ff:], c)
        add_rows(acc, vt, idx, done, tile, parts + 1, parts)
        for r in range(tile):
            rows[pl.ds(pitch * r, width), :] = wide[pl.ds(pl.multiple_of(idx[row + r], width), width), :]
        live = lax.broadcasted_iota(jnp.int32, (tile, LANES), 0) < n2
        gate = tile_gates(gates, row2)[:tile]
        for k in range(parts):
            v_k = jnp.where(live, v[:, k * LANES:(k + 1) * LANES] * gate, 0.0)
            vt[pl.ds(k, tile, stride=parts + 1), :] = v_k
        a, b = ab[:ff], ab[ff:]
        s = jax.nn.sigmoid(a)
        act = a * s
        if backward:
            mid[:ff] = (dh * b * (s * (1.0 + a * (1.0 - s)))).astype(jnp.bfloat16)
            mid[ff:] = (dh * act).astype(jnp.bfloat16)
        else:
            mid[...] = (act * b).astype(jnp.bfloat16)

    run_tiles(step, weights, wbuf, wsem, runs, tile, layer, prepare)
    write_sums(acc, outs, tok, parts, width, halves)


def token_kernel(layer, runs, table, slabs, weights, halves=(0, 1)):
    idx, gates = table
    tok, parts, _ = slabs[0].shape
    _, n_local, ff, d_model = weights[0].shape
    backward = len(slabs) > 2
    tile = TILE if len(halves) == 2 else HALF_TILE
    width = parts * len(slabs) // 2
    rows_spec = pl.BlockSpec((tok, d_model), lambda i, *_: (0, 0))
    any_spec = pl.BlockSpec(memory_space=pl.ANY)
    tile_rows = cdiv(tile * (width + 1), 16) * 16
    work = (4 if backward else 3) * len(halves)
    return pl.pallas_call(
        functools.partial(token_body, layer=layer, tok=tok, parts=parts, tile=tile, halves=halves, backward=backward),
        grid_spec=pltpu.PrefetchScalarGridSpec(
            num_scalar_prefetch=2,
            grid=(1,),
            in_specs=[pl.BlockSpec(gates.shape, lambda i, *_: (0, 0))] + [any_spec] * (len(slabs) + 3),
            out_specs=[rows_spec] * len(halves),
            scratch_shapes=[pltpu.VMEM((2 * tok, width, LANES), jnp.bfloat16), pltpu.VMEM((2 * tok * width, LANES), jnp.float32),
                            pltpu.VMEM((tile_rows, LANES), jnp.float32), pltpu.VMEM((tile_rows, LANES), jnp.float32),
                            pltpu.VMEM((2 * tok * width, LANES), jnp.float32),
                            pltpu.VMEM((2 * ff if backward else ff, tile), jnp.bfloat16),
                            pltpu.VMEM((SLOTS, 3 * ff, d_model), jnp.bfloat16),
                            pltpu.SemaphoreType.DMA((len(slabs),)), pltpu.SemaphoreType.DMA((SLOTS,))],
        ),
        out_shape=[jax.ShapeDtypeStruct((tok, d_model), jnp.float32)] * len(halves),
        compiler_params=pltpu.CompilerParams(dimension_semantics=("arbitrary",), vmem_limit_bytes=VMEM_LIMIT),
        cost_estimate=pl.CostEstimate(flops=work * 2 * 8 * tok * d_model * ff * 4,
                                      bytes_accessed=3 * n_local * ff * d_model * 2, transcendentals=0),
        name="experts_backward" if backward else "experts_forward",
    )(runs, idx, gates, *slabs, *weights)


def merge_tables_body(st, exps, layers, table, idx_ref, gate_ref, buf, *, out_rows, pad_row):
    group = idx_ref.shape[0]

    def one(q, carry):
        item = pl.program_id(0) * group + q
        merge_expert(exps[item], layers[item], st, table, idx_ref.at[q], gate_ref.at[q], buf, out_rows, pad_row)
        return carry

    lax.fori_loop(0, group, one, 0)


def merge_expert(exp, layer, st, table, idx_out, gate_out, buf, out_rows, pad_row):
    src, n_layers = table.shape[:2]
    buf[0] = jnp.full(buf.shape[1:], float(pad_row), jnp.float32)
    buf[1] = jnp.zeros(buf.shape[1:], jnp.float32)
    row = lax.broadcasted_iota(jnp.int32, (8, LANES), 0)
    lane = lax.broadcasted_iota(jnp.int32, (8, LANES), 1)
    off = 0
    for d in range(src):
        at = (d * n_layers + layer) * LANES + exp
        first = st[at]
        count = st[at + 1] - first
        to = lax.rem(off, LANES) + LANES
        shift = to - lax.rem(first, LANES)
        over = lax.rem(shift, LANES)
        start = lax.div(off, LANES)
        place = row * LANES + lane
        take = (place >= to) & (place < to + count)
        for kind in range(2):
            x = table[d, layer, kind, pl.ds(lax.div(first, LANES), 8), :]
            x = pltpu.roll(pltpu.roll(x, over, 1), lax.div(shift, LANES), 0)
            x = jnp.where(lane >= over, x, pltpu.roll(x, 1, 0))
            old = buf[kind, pl.ds(start, 8), :]
            buf[kind, pl.ds(start, 8), :] = jnp.where(take, x, old)
        off = off + count
    idx_out[...] = buf[0, pl.ds(1, out_rows), :].astype(jnp.int32)
    gate_out[...] = buf[1, pl.ds(1, out_rows), :]


def merge_tables(shared, starts, exps, layers, out_rows, pad_row):
    n_items = exps.shape[0]
    group = math.gcd(n_items, 8)
    out = pl.BlockSpec((group, out_rows, LANES), lambda g, *_: (g, 0, 0))
    return pl.pallas_call(
        functools.partial(merge_tables_body, out_rows=out_rows, pad_row=pad_row),
        grid_spec=pltpu.PrefetchScalarGridSpec(
            num_scalar_prefetch=3,
            grid=(n_items // group,),
            in_specs=[pl.BlockSpec(shared.shape, lambda g, *_: (0,) * shared.ndim)],
            out_specs=[out] * 2,
            scratch_shapes=[pltpu.VMEM((2, out_rows + 16, LANES), jnp.float32)],
        ),
        out_shape=[jax.ShapeDtypeStruct((n_items, out_rows, LANES), jnp.int32),
                   jax.ShapeDtypeStruct((n_items, out_rows, LANES), jnp.float32)],
        compiler_params=pltpu.CompilerParams(dimension_semantics=("arbitrary",)),
        cost_estimate=pl.CostEstimate(flops=10**9, bytes_accessed=4 * shared.size, transcendentals=0),
        name="merge_tables",
    )(starts.reshape(-1), exps, layers, shared)


def weight_grad_body(exps, tiles, begins, offsets, names, *refs, parts, n_exp, n_alias, n_moved, n_rows, first_list, page, layer):
    u_rows, d_rows, refs = refs[:n_rows[0]], refs[n_rows[0]:sum(n_rows)], refs[sum(n_rows):]
    idx_all, gate_ref, g_ref, up_ref, w_ref = refs[:5]
    moved, whole, refs = refs[5:5 + n_moved], refs[5 + n_moved:5 + n_moved + n_alias], refs[5 + n_moved + n_alias:]
    (dg_ref, du_ref, dw_ref, og_ref, ou_ref, ow_ref,
     uds, rows, u0, c0, d0, h0, u1, c1, d1, h1, gacc, wacc, idx_s, seen, sem, tsem, *move_refs) = refs
    e = pl.program_id(0)
    ff = g_ref.shape[2]
    slots = 3
    both = ((u0, c0, d0, h0), (u1, c1, d1, h1))

    def table_copy(exp):
        slot = lax.rem(exp, slots)
        at = pl.multiple_of((first_list + exp) * page, PAGE)
        to = pl.multiple_of(slot * page, PAGE)
        return pltpu.make_async_copy(idx_all.at[pl.ds(at, page)], idx_s.at[pl.ds(to, page)], tsem.at[slot])

    def gather_row(at, r):
        rows[pl.ds(r * PITCH, 2 * parts), :] = uds[idx_s[at]].astype(jnp.float32)

    def column(first, count, k):
        return rows[pl.ds(first * PITCH + k, count, stride=PITCH), :]

    n_tok = uds.shape[0] - 8

    def row_copies(q):
        out = []
        for kind, arrays in enumerate((u_rows, d_rows)):
            run = n_tok // (SOURCES * len(arrays))
            for k, src in enumerate(arrays):
                place = uds.at[pl.ds((q * len(arrays) + k) * run, run), pl.ds(kind * parts, parts)]
                out.append(pltpu.make_async_copy(src.at[pl.ds(q * run, run)], place, sem.at[q]))
        return out

    def wait_rows(limit):
        def one(q, carry):
            @pl.when((q >= seen[0]) & (offsets[q] < limit))
            def _():
                for c in row_copies(q):
                    c.wait()
                seen[0] = q + 1

            return carry

        @pl.when(seen[0] < SOURCES)
        def _():
            lax.fori_loop(0, SOURCES, one, 0)

    @pl.when(e == 0)
    def _():
        for q in range(SOURCES):
            for c in row_copies(q):
                c.start()
        seen[0] = 0
        table_copy(0).start()
        table_copy(1).start()
        uds[pl.ds(n_tok, 8)] = jnp.zeros((8, 2 * parts, LANES), jnp.bfloat16)
        for ref in (*both[0], *both[1], gacc, wacc):
            clear(ref)
        table_copy(0).wait()
        wait_rows(WTILE)

        def first_rows(q, carry):
            for r in range(16):
                gather_row(q * 16 + r, q * 16 + r)
            return carry

        lax.fori_loop(0, WTILE // 16, first_rows, 0)

    if moved:
        move_step(e, n_exp, layer + 1, names, moved, whole, *move_refs)

    @pl.when(e + 1 < n_exp)
    def _():
        table_copy(e + 1).wait()

    @pl.when(e + 2 < n_exp)
    def _():
        table_copy(e + 2).start()

    here = lax.rem(e, slots) * page
    there = lax.rem(jnp.minimum(e + 1, n_exp - 1), slots) * page
    n_tiles = tiles[e]
    begin = begins[e]
    gate_rows = WTILE // LANES

    def compute(j, new, old):
        un, cn, dn, hn = new
        uo, co, do, ho = old
        gacc[...] += nn_dot(do[...], uo[...])
        wacc[...] += nn_dot(ho[...], co[...])
        nxt = jnp.where(j + 1 < n_tiles, here + (j + 1) * WTILE, there)
        gu = jnp.concatenate([g_ref[0, 0], up_ref[0, 0]], axis=0)
        for q in range(0, WTILE, CHUNK):
            part = slice(q, q + CHUNK)
            un[part] = jnp.concatenate([column(q, CHUNK, k) for k in range(parts)], axis=1).astype(jnp.bfloat16)
            for p in range(q, q + CHUNK, LANES):
                gate = spread_column(gate_ref[0, pl.ds(j * gate_rows + p // LANES, 1), :])
                for k in range(parts):
                    d = column(p, LANES, parts + k)
                    cn[p:p + LANES, k * LANES:(k + 1) * LANES] = (d * gate).astype(jnp.bfloat16)
            ab = nt_dot(gu, un[part])
            dh = nt_dot(w_ref[0, 0], cn[part])
            for r in range(q, q + CHUNK):
                gather_row(nxt + r, r)
            a, b = ab[:ff], ab[ff:]
            s = jax.nn.sigmoid(a)
            act = a * s
            hn[:, part] = (act * b).astype(jnp.bfloat16)
            dn[:ff, part] = (dh * b * (s * (1.0 + a * (1.0 - s)))).astype(jnp.bfloat16)
            dn[ff:, part] = (dh * act).astype(jnp.bfloat16)

    def tile(j, carry):
        odd = lax.rem(begin + j, 2)
        wait_rows(jnp.where((e == 0) & (j + 1 < n_tiles), (j + 2) * WTILE, page * SOURCES))

        @pl.when(odd == 0)
        def _():
            compute(j, both[0], both[1])

        @pl.when(odd == 1)
        def _():
            compute(j, both[1], both[0])

        @pl.when(j == 0)
        def _():
            dg = gacc[:ff].astype(jnp.bfloat16)
            du = gacc[ff:].astype(jnp.bfloat16)
            dw = wacc[...].astype(jnp.bfloat16)
            dg_ref[0, 0], du_ref[0, 0], dw_ref[0, 0] = dg, du, dw
            og_ref[0], ou_ref[0], ow_ref[0] = dg, du, dw
            gacc[...] = jnp.zeros_like(gacc)
            wacc[...] = jnp.zeros_like(wacc)

        return carry

    lax.fori_loop(0, n_tiles, tile, 0)


def move_step(e, n_steps, layer, names, arrived, whole, buf, in_sem, out_sem):
    per = buf.shape[2]

    def arrive(chunk):
        slot = lax.rem(chunk, 2)
        return [pltpu.make_async_copy(x.at[pl.ds(chunk * per, per)], buf.at[slot, k], in_sem.at[slot])
                for k, x in enumerate(arrived)]

    def leave(chunk):
        slot = lax.rem(chunk, 2)
        return [pltpu.make_async_copy(buf.at[slot, k, i], x.at[layer, names[chunk * per + i]], out_sem.at[slot])
                for k, x in enumerate(whole) for i in range(per)]

    def each(when, copies, act):
        @pl.when(when)
        def _():
            for c in copies:
                act(c)

    each(e >= 2, leave(jnp.maximum(e - 2, 0)), lambda c: c.wait())
    each(e < n_steps, arrive(jnp.minimum(e, n_steps - 1)), lambda c: c.start())
    each(e >= 1, arrive(jnp.maximum(e - 1, 0)), lambda c: c.wait())
    each(e >= 1, leave(jnp.maximum(e - 1, 0)), lambda c: c.start())
    each(e == n_steps, leave(n_steps - 1), lambda c: c.wait())


def weight_grads(layer, first, exps, tiles, offsets, rows, idx_all, gates, weights, full, moved=None):
    parts = rows[0][0].shape[1]
    n_tok = sum(x.shape[0] for x in rows[0])
    n_layers, n_local, ff, d_model = weights[0].shape
    n_exp = exps.shape[0]
    out_rows = gates.shape[1]
    page = out_rows * LANES
    tiles = jnp.concatenate([tiles, jnp.ones((1,), jnp.int32)])
    begins = jnp.cumsum(tiles) - tiles
    any_spec = pl.BlockSpec(memory_space=pl.ANY)
    mine = pl.BlockSpec((1, 1, ff, d_model), lambda e, exps, *_: (layer, exps[jnp.minimum(e, n_exp - 1)], 0, 0))
    done = pl.BlockSpec((1, 1, ff, d_model), lambda e, exps, *_: (layer, exps[jnp.maximum(e - 1, 0)], 0, 0))
    half = pl.BlockSpec((1, ff, d_model), lambda e, *_: (jnp.maximum(e - 1, 0), 0, 0))
    gate_spec = pl.BlockSpec((1, out_rows, LANES), lambda e, *_: (first + jnp.minimum(e, n_exp - 1), 0, 0))
    aliased = list(full) if full is not None else []
    tile_set = [pltpu.VMEM((WTILE, d_model), jnp.bfloat16)] * 2 + [pltpu.VMEM((2 * ff, WTILE), jnp.bfloat16),
                                                                 pltpu.VMEM((ff, WTILE), jnp.bfloat16)]
    arrived, names = moved if moved else ([], exps)
    scratch = []
    if moved:
        scratch = [pltpu.VMEM((2, 3, arrived[0].shape[0] // n_exp, ff, d_model), jnp.bfloat16), pltpu.SemaphoreType.DMA((2,)),
                   pltpu.SemaphoreType.DMA((2,))]
    outs = pl.pallas_call(
        functools.partial(weight_grad_body, parts=parts, n_exp=n_exp, n_alias=len(aliased), n_moved=len(arrived),
                          n_rows=[len(x) for x in rows], first_list=first, page=page, layer=layer),
        grid_spec=pltpu.PrefetchScalarGridSpec(
            num_scalar_prefetch=5,
            grid=(n_exp + 1,),
            in_specs=[any_spec] * (len(rows[0] + rows[1]) + 1) + [gate_spec] + [mine] * 3 + [any_spec] * (len(arrived) + len(aliased)),
            out_specs=[done] * 3 + [half] * 3,
            scratch_shapes=[pltpu.VMEM((n_tok + 8, 2 * parts, LANES), jnp.bfloat16)]
            + [pltpu.VMEM((WTILE * PITCH + 16, LANES), jnp.float32)] + tile_set * 2
            + [pltpu.VMEM((2 * ff, d_model), jnp.float32), pltpu.VMEM((ff, d_model), jnp.float32),
               pltpu.SMEM((3 * page,), jnp.int32), pltpu.SMEM((1,), jnp.int32), pltpu.SemaphoreType.DMA((SOURCES,)),
               pltpu.SemaphoreType.DMA((3,))] + scratch,
        ),
        out_shape=[jax.ShapeDtypeStruct((n_layers, n_local, ff, d_model), jnp.bfloat16)] * 3
        + [jax.ShapeDtypeStruct((n_exp, ff, d_model), jnp.bfloat16)] * 3,
        input_output_aliases={10 + len(rows[0] + rows[1] + arrived) + k: k for k in range(len(aliased))},
        compiler_params=pltpu.CompilerParams(dimension_semantics=("arbitrary",), vmem_limit_bytes=VMEM_LIMIT),
        cost_estimate=pl.CostEstimate(flops=6 * n_tok * n_exp * d_model * ff,
                                      bytes_accessed=n_tok * d_model * 4 + 9 * n_exp * ff * d_model * 2, transcendentals=0),
        name="weight_grads",
    )(exps, tiles, begins, offsets, names, *rows[0], *rows[1], idx_all, gates, *weights, *arrived, *aliased)
    return outs[:3], outs[3:]


def merge_body(exps, a, b, c, f0, f1, f2, o0, o1, o2, buf, in_sem, out_sem, *, layer, n_exp):
    halves, wholes = (a, b, c), (o0, o1, o2)

    def arrive(k, q):
        return pltpu.make_async_copy(halves[k].at[q], buf.at[k, q], in_sem.at[k, q])

    def leave(k, q):
        return pltpu.make_async_copy(buf.at[k, q], wholes[k].at[layer, exps[q]], out_sem)

    def each(act):
        def one(q, carry):
            for k in range(3):
                act(k, q)
            return carry

        lax.fori_loop(0, n_exp, one, 0)

    def pass_on(k, q):
        arrive(k, q).wait()
        leave(k, q).start()

    each(lambda k, q: arrive(k, q).start())
    each(pass_on)
    each(lambda k, q: leave(k, q).wait())


def merge_half(layer, exps, half, full):
    n_exp, ff, d_model = half[0].shape
    any_spec = pl.BlockSpec(memory_space=pl.ANY)
    return pl.pallas_call(
        functools.partial(merge_body, layer=layer, n_exp=n_exp),
        grid_spec=pltpu.PrefetchScalarGridSpec(
            num_scalar_prefetch=1, grid=(1,), in_specs=[any_spec] * 6, out_specs=[any_spec] * 3,
            scratch_shapes=[pltpu.VMEM((3, n_exp, ff, d_model), jnp.bfloat16), pltpu.SemaphoreType.DMA((3, n_exp)),
                            pltpu.SemaphoreType.DMA]),
        out_shape=[jax.ShapeDtypeStruct(x.shape, x.dtype) for x in full],
        input_output_aliases={4: 0, 5: 1, 6: 2},
        compiler_params=pltpu.CompilerParams(dimension_semantics=("arbitrary",), vmem_limit_bytes=VMEM_LIMIT),
        cost_estimate=pl.CostEstimate(flops=10**9, bytes_accessed=6 * n_exp * ff * d_model * 2, transcendentals=0),
        name="merge_half",
    )(exps, *half, *full)


def join_body(a, b, out, sem):
    n = a.shape[0]
    copies = [pltpu.make_async_copy(x, out.at[pl.ds(k * n, n)], sem.at[k]) for k, x in enumerate((a, b))]
    for c in copies:
        c.start()
    for c in copies:
        c.wait()


def join_rows(a, b):
    n, parts, _ = a.shape
    any_spec = pl.BlockSpec(memory_space=pl.ANY)
    return pl.pallas_call(
        join_body, in_specs=[any_spec] * 2, out_shape=jax.ShapeDtypeStruct((2 * n, parts, LANES), a.dtype),
        out_specs=pl.BlockSpec(memory_space=pltpu.VMEM), scratch_shapes=[pltpu.SemaphoreType.DMA((2,))], name="join_rows",
    )(a, b)


def route_tables(ids, gates, ep, n_local):
    n_src, top_k, tok = ids.shape
    n = n_src * top_k * tok
    local = ids - ep * n_local
    here = (local >= 0) & (local < n_local)
    group = jnp.where(here, local, n_local).reshape(-1)
    key, gate = lax.sort((group * n + jnp.arange(n, dtype=jnp.int32), gates.reshape(-1)), num_keys=1, is_stable=False)
    copy = key % n
    token = copy // (top_k * tok) * tok + copy % tok
    token = jnp.pad(token, (0, 2 * PAGE))
    gate = jnp.pad(gate, (0, 2 * PAGE)).reshape(-1, LANES)
    ids = jnp.arange(n_local, dtype=jnp.int32)
    hits = jnp.sum((group.reshape(n_src, -1, 1) == ids).astype(jnp.int32), axis=1)
    starts = jnp.sum(below(n_local) * jnp.sum(hits, axis=0), axis=1)
    ends = starts + jnp.sum(hits, axis=0)
    middle = starts + hits[0]
    bounds = jnp.pad(starts, (0, LANES - n_local), mode='edge')
    bounds = jnp.where(jnp.arange(LANES) < n_local, bounds, ends[-1])
    runs = [jnp.concatenate(x) for x in ((starts, middle), (middle, ends), (starts, ends))]
    return runs, token, gate, bounds


def deal_experts(bounds, n_local, n_lists):
    load = jnp.sum(bounds[:, 1:n_local + 1] - bounds[:, :n_local], axis=0)
    ids = jnp.arange(n_local, dtype=jnp.int32)
    mine = load.reshape(-1, 1)
    rank = jnp.sum((load > mine).astype(jnp.int32) + (load == mine).astype(jnp.int32) * below(n_local), axis=1)
    turn, which = jnp.arange(n_local // n_lists), jnp.arange(n_lists).reshape(-1, 1)
    want = n_lists * turn + jnp.where(turn % 2 == 0, which, n_lists - 1 - which)
    pick = (rank == jnp.expand_dims(want, 2)).astype(jnp.int32)
    tiles = jnp.maximum((jnp.sum(pick * load, axis=2) + WTILE - 1) // WTILE, 1)
    return jnp.sum(pick * ids, axis=2), tiles


def source_offsets(bounds, expert):
    lane = jnp.arange(bounds.shape[1], dtype=jnp.int32)
    counts = jnp.sum(bounds * ((lane == expert + 1).astype(jnp.int32) - (lane == expert).astype(jnp.int32)), axis=1)
    return jnp.sum(below(bounds.shape[0]) * counts, axis=1)


def after(x, *earlier):
    return lax.optimization_barrier((x, *earlier))[0]


def solution(mesh):
    ep_size = mesh.shape['ep']
    dp_size = mesh.shape['dp']
    tok_spec = P(('dp', 'ep'), None)
    route_spec = P(None, ('dp', 'ep'), None)
    whole_spec = P(None, None, None)
    expert_spec = P(None, 'ep', None, None)
    ep_pairs = [(i, 1 - i) for i in range(ep_size)]
    core_pairs = [(i, i ^ 1) for i in range(dp_size)]
    chip_pairs = [(i, i ^ (2 << i % 2)) for i in range(dp_size)]

    def device_body(tokens, d_out, expert_ids, gate_vals, w_mix, w_gate, w_up, w_down):
        n_layers = w_mix.shape[0]
        n_local = w_gate.shape[1]
        n_experts = n_local * ep_size
        tok, d_model = tokens.shape
        top_k = expert_ids.shape[2]
        parts = d_model // LANES
        cap = cdiv(CAP_FACTOR * tok * top_k, n_experts)
        ep_id = lax.axis_index('ep').astype(jnp.int32)
        dp_id = lax.axis_index('dp').astype(jnp.int32)
        weights = (jnp.swapaxes(w_gate, 2, 3), jnp.swapaxes(w_up, 2, 3), w_down)

        def swap(x):
            return lax.ppermute(x, 'ep', ep_pairs)

        def spread(x):
            return [lax.all_gather(y, 'dp', axis=0, tiled=True) for y in x]

        def trade(x, pairs):
            return [lax.ppermute(y, 'dp', pairs) for y in x]

        def slab(x):
            return x.reshape(tok, parts, LANES)

        def mixed(x, layer):
            return (x.astype(jnp.float32) + jnp.dot(x, w_mix[layer], preferred_element_type=jnp.float32)).astype(jnp.bfloat16)

        ids = jnp.swapaxes(expert_ids, 1, 2)
        gates = jnp.swapaxes(gate_vals, 1, 2)
        mine = jnp.stack([ids.astype(jnp.float32), gates])
        u = mixed(tokens, 0)
        u_slab = slab(u)
        theirs = swap(after(mine, u_slab))
        both = jnp.stack([mine, theirs], 2)
        top = n_layers - 1
        runs, tables, packed = [], [], []

        def add_tables(pair):
            run, token, gate, bounds = route_tables(pair[0].astype(jnp.int32), pair[1], ep_id, n_local)
            runs.append(run)
            tables.append([(token * parts, gate), (token * (2 * parts), gate)])
            spot = dp_id * (2 * tok) + token
            first = jnp.concatenate([spot.reshape(-1, LANES), jnp.pad(bounds.reshape(1, LANES), ((0, 7), (0, 0)))])
            packed.append(jnp.stack([first.astype(jnp.float32), jnp.pad(gate, ((0, 8), (0, 0)))]))

        add_tables(both[:, 0])

        x_in, u_slabs, u_others, xs = tokens, [u_slab], [swap(u_slab)], []
        d_slab = slab(d_out)
        d_other = swap(after(d_slab, u_others[0]))
        d_rows = spread([join_rows(d_slab, d_other)])
        for layer in range(n_layers):
            if layer:
                u = mixed(x_in, layer)
                u_slabs.append(slab(u))
                u_others.append(swap(u_slabs[layer]))
                add_tables(after(both[:, layer], u_slabs[layer]))
            xs.append(x_in)
            if layer < top:
                other, = token_kernel(layer, runs[layer][1], tables[layer][0], (u_slabs[layer], u_others[layer]), weights, (1,))
                sent = swap(other)
                own, = token_kernel(layer, runs[layer][0], tables[layer][0], (after(u_slabs[layer], other), u_others[layer]),
                                    weights, (0,))
                x_in = (u.astype(jnp.float32) + own + sent).astype(jnp.bfloat16)

        shared = lax.all_gather(jnp.stack(packed), 'dp', axis=0)
        starts = shared[:, :, 0, -8].astype(jnp.int32)
        core = dp_id % 2
        kind = (dp_id // 2 + dp_id // 4) % 2
        dealt = [deal_experts(starts[:, layer], n_local, 2 * PARTS) for layer in range(n_layers)]
        of_layer = [layer for layer in range(top) for _ in range(PARTS)] + [top]
        places = [PARTS * core + part for _ in range(top) for part in range(PARTS)] + [PARTS * core + kind]
        mine = [dealt[layer][0][place] for layer, place in zip(of_layer, places)]
        list_rows = cdiv(cdiv(dp_size * 2 * cap, LANES), 8) * 8 + 8
        idx_all, gate_all = merge_tables(shared, starts, jnp.concatenate(mine),
                                         jnp.concatenate([jnp.full_like(x, layer) for x, layer in zip(mine, of_layer)]),
                                         list_rows, dp_size * 2 * tok)
        offsets = [source_offsets(starts[:, layer], x[0]) for x, layer in zip(mine, of_layer)]
        idx_all = idx_all.reshape(-1)

        d_y, full, arrived = d_out, None, []
        d_mix = [None] * n_layers
        for layer in reversed(range(n_layers)):
            both_u = [u_slabs[layer], u_others[layer]]
            u_rows = spread(both_u if layer < top else [join_rows(*both_u)])
            slabs = (u_slabs[layer], u_others[layer], d_slab, d_other)
            own, other = token_kernel(layer, runs[layer][2], tables[layer][1], slabs, weights)
            d_u = (d_y.astype(jnp.float32) + own + swap(other)).astype(jnp.bfloat16)
            last = other
            if layer == top:
                y_own, last = token_kernel(top, runs[top][2], tables[top][0], (after(u_slabs[top], other), u_others[top]), weights)
            d_mix[layer] = jnp.einsum('td,te->de', xs[layer], d_u, preferred_element_type=jnp.float32).astype(jnp.bfloat16)
            d_y = (d_u.astype(jnp.float32)
                   + jnp.einsum('te,de->td', d_u, w_mix[layer], preferred_element_type=jnp.float32)).astype(jnp.bfloat16)
            lists, tiles = dealt[layer]
            theirs = PARTS * (1 - core)
            for part in range(PARTS if layer < top else 1):
                item = of_layer.index(layer) + part
                first = sum(x.shape[0] for x in mine[:item])
                full, done = weight_grads(layer, first, mine[item], after(tiles[places[item]], last), offsets[item],
                                          (u_rows, d_rows), idx_all, gate_all, weights, full, moved if part else None)
                got = trade(done, core_pairs)
                if layer < top:
                    arrived.insert(1 + 2 * part, (layer, got, lists[theirs + part]))
                    continue
                moved = got, lists[theirs + kind]
                far = trade(done, chip_pairs)
                arrived.append((layer, far, lists[PARTS * core + 1 - kind]))
                arrived.append((layer, trade(far, core_pairs), lists[theirs + 1 - kind]))
            if layer:
                d_slab = slab(d_y)
                d_other = swap(d_slab)
                d_rows = spread([join_rows(d_slab, d_other)])
                if layer == top:
                    layer_out = (u.astype(jnp.float32) + y_own + swap(after(last, d_other))).astype(jnp.bfloat16)
        for layer, got, names in arrived:
            full = merge_half(layer, names, got, full)
        d_mix = lax.psum(jnp.stack(d_mix), ('dp', 'ep'))
        return (layer_out, d_y, d_mix, jnp.swapaxes(full[0], 2, 3), jnp.swapaxes(full[1], 2, 3), full[2])

    return jax.shard_map(device_body, mesh=mesh,
                         in_specs=(tok_spec, tok_spec, route_spec, route_spec, whole_spec,
                                   expert_spec, expert_spec, expert_spec),
                         out_specs=(tok_spec, tok_spec, whole_spec, expert_spec, expert_spec, expert_spec),
                         check_vma=False)
```

```python
import functools
import math

import jax
import jax.numpy as jnp
from jax import lax
from jax.experimental import pallas as pl
from jax.experimental.pallas import tpu as pltpu
from jax.sharding import PartitionSpec as P


CAP_FACTOR = 3
LANES = 128
TILE = 96
HALF_TILE = 64
WTILE = 768
PARTS = 2
SOURCES = 8
CHUNK = 256
PITCH = 9
BATCH = 16
SLOTS = 8
PAGE = 1024
VMEM_LIMIT = 62 * 2**20


def cdiv(a, b):
    return (a + b - 1) // b


def below(n):
    return jnp.tri(n, k=-1, dtype=jnp.int32)


def nt_dot(a, b):
    return lax.dot_general(a, b, (((1,), (1,)), ((), ())), preferred_element_type=jnp.float32)


def tn_dot(a, b):
    return lax.dot_general(a, b, (((0,), (0,)), ((), ())), preferred_element_type=jnp.float32)


def nn_dot(a, b):
    return lax.dot_general(a, b, (((1,), (0,)), ((), ())), preferred_element_type=jnp.float32)


def clear(ref):
    step = next(n for n in (64, 48, 32, 16, 8) if ref.shape[0] % n == 0)

    def one(q, carry):
        ref[pl.ds(pl.multiple_of(q * step, step), step), :] = jnp.zeros((step, ref.shape[1]), ref.dtype)
        return carry

    lax.fori_loop(0, ref.shape[0] // step, one, 0)


def add_rows(acc, vals_ref, idx, row, tile, pitch, width):
    for b in range(0, tile, BATCH):
        at = [idx[row + b + r] * width for r in range(BATCH)]
        vals = [acc[pl.ds(at[r], width), :] + vals_ref[pl.ds((b + r) * pitch, width), :] for r in range(BATCH)]
        for r in reversed(range(BATCH)):
            acc[pl.ds(at[r], width), :] = vals[r]


def spread_column(row):
    return jnp.broadcast_to(row, (LANES, LANES)).T


def tile_gates(gates, row):
    pair = gates[pl.ds(lax.div(row, LANES), 2), :]
    skip = lax.rem(row, LANES)
    pair = pltpu.roll(pair, lax.rem(LANES - skip, LANES), 1)
    lane = lax.broadcasted_iota(jnp.int32, (1, LANES), 1)
    return spread_column(jnp.where(lane < LANES - skip, pair[:1], pair[1:]))


def write_sums(acc, outs, tok, parts, pitch, halves):
    step = min(32, tok)

    def copy_out(q, carry):
        r0 = pl.multiple_of(q * step, step)
        for k in range(parts):
            for out, half in zip(outs, halves):
                first = (half * tok + r0) * pitch + k
                out[pl.ds(r0, step), k * LANES:(k + 1) * LANES] = acc[pl.ds(first, step, stride=pitch), :]
        return carry

    lax.fori_loop(0, tok // step, copy_out, 0)


def expert_copies(weights, buf, sem, layer, e):
    slot = lax.rem(e, SLOTS)
    ff = weights[0].shape[2]
    return [pltpu.make_async_copy(w.at[layer, e], buf.at[slot, pl.ds(k * ff, ff)], sem.at[slot])
            for k, w in enumerate(weights)]


def run_tiles(step, weights, wbuf, wsem, runs, tile, layer, prepare):
    n_local = weights[0].shape[1]
    for e in range(SLOTS - 2):
        for c in expert_copies(weights, wbuf, wsem, layer, e):
            c.start()
    prepare()
    for c in expert_copies(weights, wbuf, wsem, layer, 0):
        c.wait()

    def length(e):
        return runs[n_local + e] - runs[e]

    def add_tiles(e, total):
        return total + jnp.maximum(lax.div(length(e) + tile - 1, tile), 1)

    def one(i, carry):
        (e, row, left), (e1, row1, n1), (e2, row2, n2), row3 = carry

        @pl.when(e != e1)
        def _():
            for c in expert_copies(weights, wbuf, wsem, layer, e):
                c.wait()

        @pl.when((e != e1) & (e + SLOTS - 3 < n_local))
        def _():
            for c in expert_copies(weights, wbuf, wsem, layer, e + SLOTS - 3):
                c.start()

        step(row, (lax.rem(e1, SLOTS), row1), (lax.rem(e2, SLOTS), row2, n2), row3)
        more = left > tile
        e_next = jnp.minimum(e + 1, n_local - 1)
        fresh = jnp.where(e + 1 < n_local, length(e_next), 0)
        ahead = (jnp.where(more, e, e_next), jnp.where(more, row + tile, runs[e_next]), jnp.where(more, left - tile, fresh))
        return ahead, (e, row, jnp.minimum(left, tile)), (e1, row1, n1), row2

    none = (0, 0, 0)
    lax.fori_loop(0, lax.fori_loop(0, n_local, add_tiles, 0) + 3, one, ((0, runs[0], length(0)), none, none, 0))


def token_body(runs, idx, gates, *refs, layer, tok, parts, tile, halves, backward):
    n_in = 4 if backward else 2
    sources, weights, outs, refs = refs[:n_in], refs[n_in:n_in + 3], refs[n_in + 3:n_in + 3 + len(halves)], refs[n_in + 3 + len(halves):]
    slabs, rows, vt, acc, mid, wbuf, sem, wsem = refs
    ff = weights[0].shape[2]
    width = parts * n_in // 2
    pitch = width + 1

    def prepare():
        copies = [pltpu.make_async_copy(src, slabs.at[pl.ds(k % 2 * tok, tok), pl.ds(k // 2 * parts, parts)], sem.at[k])
                  for k, src in enumerate(sources) if k % 2 in halves]
        for c in copies:
            c.start()
        for ref in (acc, vt, rows, mid):
            clear(ref)
        for c in copies:
            c.wait()

    def column(k):
        return rows[pl.ds(k, tile, stride=pitch), :]

    def step(row, here, before, done):
        slot, row1 = here
        slot2, row2, n2 = before
        old = wbuf[slot2, :2 * ff] if backward else wbuf[slot2, 2 * ff:]
        v = tn_dot(mid[...], old).astype(jnp.bfloat16).astype(jnp.float32)
        u = jnp.concatenate([column(k) for k in range(parts)], axis=1).astype(jnp.bfloat16)
        ab = nt_dot(wbuf[slot, :2 * ff], u)
        if backward:
            gate = tile_gates(gates, row1)[:tile]
            c = jnp.concatenate([(column(parts + k) * gate).astype(jnp.bfloat16) for k in range(parts)], axis=1)
            dh = nt_dot(wbuf[slot, 2 * ff:], c)
        add_rows(acc, vt, idx, done, tile, parts + 1, parts)
        for r in range(tile):
            rows[pl.ds(pitch * r, width), :] = slabs[idx[row + r]].astype(jnp.float32)
        live = lax.broadcasted_iota(jnp.int32, (tile, LANES), 0) < n2
        gate = tile_gates(gates, row2)[:tile]
        for k in range(parts):
            v_k = jnp.where(live, v[:, k * LANES:(k + 1) * LANES] * gate, 0.0)
            vt[pl.ds(k, tile, stride=parts + 1), :] = v_k
        a, b = ab[:ff], ab[ff:]
        s = jax.nn.sigmoid(a)
        act = a * s
        if backward:
            mid[:ff] = (dh * b * (s * (1.0 + a * (1.0 - s)))).astype(jnp.bfloat16)
            mid[ff:] = (dh * act).astype(jnp.bfloat16)
        else:
            mid[...] = (act * b).astype(jnp.bfloat16)

    run_tiles(step, weights, wbuf, wsem, runs, tile, layer, prepare)
    write_sums(acc, outs, tok, parts, parts, halves)


def token_kernel(layer, runs, table, slabs, weights, halves=(0, 1)):
    idx, gates = table
    tok, parts, _ = slabs[0].shape
    _, n_local, ff, d_model = weights[0].shape
    backward = len(slabs) > 2
    tile = TILE if len(halves) == 2 else HALF_TILE
    width = parts * len(slabs) // 2
    rows_spec = pl.BlockSpec((tok, d_model), lambda i, *_: (0, 0))
    any_spec = pl.BlockSpec(memory_space=pl.ANY)
    tile_rows = cdiv(tile * (width + 1), 16) * 16
    work = (4 if backward else 3) * len(halves)
    return pl.pallas_call(
        functools.partial(token_body, layer=layer, tok=tok, parts=parts, tile=tile, halves=halves, backward=backward),
        grid_spec=pltpu.PrefetchScalarGridSpec(
            num_scalar_prefetch=2,
            grid=(1,),
            in_specs=[pl.BlockSpec(gates.shape, lambda i, *_: (0, 0))] + [any_spec] * (len(slabs) + 3),
            out_specs=[rows_spec] * len(halves),
            scratch_shapes=[pltpu.VMEM((2 * tok, width, LANES), jnp.bfloat16),
                            pltpu.VMEM((tile_rows, LANES), jnp.float32), pltpu.VMEM((tile_rows, LANES), jnp.float32),
                            pltpu.VMEM((2 * tok * parts, LANES), jnp.float32),
                            pltpu.VMEM((2 * ff if backward else ff, tile), jnp.bfloat16),
                            pltpu.VMEM((SLOTS, 3 * ff, d_model), jnp.bfloat16),
                            pltpu.SemaphoreType.DMA((len(slabs),)), pltpu.SemaphoreType.DMA((SLOTS,))],
        ),
        out_shape=[jax.ShapeDtypeStruct((tok, d_model), jnp.float32)] * len(halves),
        compiler_params=pltpu.CompilerParams(dimension_semantics=("arbitrary",), vmem_limit_bytes=VMEM_LIMIT),
        cost_estimate=pl.CostEstimate(flops=work * 2 * 8 * tok * d_model * ff * 4,
                                      bytes_accessed=3 * n_local * ff * d_model * 2, transcendentals=0),
        name="experts_backward" if backward else "experts_forward",
    )(runs, idx, gates, *slabs, *weights)


def merge_tables_body(st, exps, layers, table, idx_ref, gate_ref, buf, *, out_rows, pad_row):
    group = idx_ref.shape[0]

    def one(q, carry):
        item = pl.program_id(0) * group + q
        merge_expert(exps[item], layers[item], st, table, idx_ref.at[q], gate_ref.at[q], buf, out_rows, pad_row)
        return carry

    lax.fori_loop(0, group, one, 0)


def merge_expert(exp, layer, st, table, idx_out, gate_out, buf, out_rows, pad_row):
    src, n_layers = table.shape[:2]
    buf[0] = jnp.full(buf.shape[1:], float(pad_row), jnp.float32)
    buf[1] = jnp.zeros(buf.shape[1:], jnp.float32)
    row = lax.broadcasted_iota(jnp.int32, (8, LANES), 0)
    lane = lax.broadcasted_iota(jnp.int32, (8, LANES), 1)
    off = 0
    for d in range(src):
        at = (d * n_layers + layer) * LANES + exp
        first = st[at]
        count = st[at + 1] - first
        to = lax.rem(off, LANES) + LANES
        shift = to - lax.rem(first, LANES)
        over = lax.rem(shift, LANES)
        start = lax.div(off, LANES)
        place = row * LANES + lane
        take = (place >= to) & (place < to + count)
        for kind in range(2):
            x = table[d, layer, kind, pl.ds(lax.div(first, LANES), 8), :]
            x = pltpu.roll(pltpu.roll(x, over, 1), lax.div(shift, LANES), 0)
            x = jnp.where(lane >= over, x, pltpu.roll(x, 1, 0))
            old = buf[kind, pl.ds(start, 8), :]
            buf[kind, pl.ds(start, 8), :] = jnp.where(take, x, old)
        off = off + count
    idx_out[...] = buf[0, pl.ds(1, out_rows), :].astype(jnp.int32)
    gate_out[...] = buf[1, pl.ds(1, out_rows), :]


def merge_tables(shared, starts, exps, layers, out_rows, pad_row):
    n_items = exps.shape[0]
    group = math.gcd(n_items, 8)
    out = pl.BlockSpec((group, out_rows, LANES), lambda g, *_: (g, 0, 0))
    return pl.pallas_call(
        functools.partial(merge_tables_body, out_rows=out_rows, pad_row=pad_row),
        grid_spec=pltpu.PrefetchScalarGridSpec(
            num_scalar_prefetch=3,
            grid=(n_items // group,),
            in_specs=[pl.BlockSpec(shared.shape, lambda g, *_: (0,) * shared.ndim)],
            out_specs=[out] * 2,
            scratch_shapes=[pltpu.VMEM((2, out_rows + 16, LANES), jnp.float32)],
        ),
        out_shape=[jax.ShapeDtypeStruct((n_items, out_rows, LANES), jnp.int32),
                   jax.ShapeDtypeStruct((n_items, out_rows, LANES), jnp.float32)],
        compiler_params=pltpu.CompilerParams(dimension_semantics=("arbitrary",)),
        cost_estimate=pl.CostEstimate(flops=10**9, bytes_accessed=4 * shared.size, transcendentals=0),
        name="merge_tables",
    )(starts.reshape(-1), exps, layers, shared)


def weight_grad_body(exps, tiles, begins, offsets, names, *refs, parts, n_exp, n_alias, n_moved, n_rows, first_list, page, layer):
    u_rows, d_rows, refs = refs[:n_rows[0]], refs[n_rows[0]:sum(n_rows)], refs[sum(n_rows):]
    idx_all, gate_ref, g_ref, up_ref, w_ref = refs[:5]
    moved, whole, refs = refs[5:5 + n_moved], refs[5 + n_moved:5 + n_moved + n_alias], refs[5 + n_moved + n_alias:]
    (dg_ref, du_ref, dw_ref, og_ref, ou_ref, ow_ref,
     uds, rows, u0, c0, d0, h0, u1, c1, d1, h1, gacc, wacc, idx_s, seen, sem, tsem, *move_refs) = refs
    e = pl.program_id(0)
    ff = g_ref.shape[2]
    slots = 3
    both = ((u0, c0, d0, h0), (u1, c1, d1, h1))

    def table_copy(exp):
        slot = lax.rem(exp, slots)
        at = pl.multiple_of((first_list + exp) * page, PAGE)
        to = pl.multiple_of(slot * page, PAGE)
        return pltpu.make_async_copy(idx_all.at[pl.ds(at, page)], idx_s.at[pl.ds(to, page)], tsem.at[slot])

    def gather_row(at, r):
        rows[pl.ds(r * PITCH, 2 * parts), :] = uds[idx_s[at]].astype(jnp.float32)

    def column(first, count, k):
        return rows[pl.ds(first * PITCH + k, count, stride=PITCH), :]

    n_tok = uds.shape[0] - 8

    def row_copies(q):
        out = []
        for kind, arrays in enumerate((u_rows, d_rows)):
            run = n_tok // (SOURCES * len(arrays))
            for k, src in enumerate(arrays):
                place = uds.at[pl.ds((q * len(arrays) + k) * run, run), pl.ds(kind * parts, parts)]
                out.append(pltpu.make_async_copy(src.at[pl.ds(q * run, run)], place, sem.at[q]))
        return out

    def wait_rows(limit):
        def one(q, carry):
            @pl.when((q >= seen[0]) & (offsets[q] < limit))
            def _():
                for c in row_copies(q):
                    c.wait()
                seen[0] = q + 1

            return carry

        @pl.when(seen[0] < SOURCES)
        def _():
            lax.fori_loop(0, SOURCES, one, 0)

    @pl.when(e == 0)
    def _():
        for q in range(SOURCES):
            for c in row_copies(q):
                c.start()
        seen[0] = 0
        table_copy(0).start()
        table_copy(1).start()
        uds[pl.ds(n_tok, 8)] = jnp.zeros((8, 2 * parts, LANES), jnp.bfloat16)
        for ref in (*both[0], *both[1], gacc, wacc):
            clear(ref)
        table_copy(0).wait()
        wait_rows(WTILE)

        def first_rows(q, carry):
            for r in range(16):
                gather_row(q * 16 + r, q * 16 + r)
            return carry

        lax.fori_loop(0, WTILE // 16, first_rows, 0)

    if moved:
        move_step(e, n_exp, layer + 1, names, moved, whole, *move_refs)

    @pl.when(e + 1 < n_exp)
    def _():
        table_copy(e + 1).wait()

    @pl.when(e + 2 < n_exp)
    def _():
        table_copy(e + 2).start()

    here = lax.rem(e, slots) * page
    there = lax.rem(jnp.minimum(e + 1, n_exp - 1), slots) * page
    n_tiles = tiles[e]
    begin = begins[e]
    gate_rows = WTILE // LANES

    def compute(j, new, old):
        un, cn, dn, hn = new
        uo, co, do, ho = old
        gacc[...] += nn_dot(do[...], uo[...])
        wacc[...] += nn_dot(ho[...], co[...])
        nxt = jnp.where(j + 1 < n_tiles, here + (j + 1) * WTILE, there)
        gu = jnp.concatenate([g_ref[0, 0], up_ref[0, 0]], axis=0)
        for q in range(0, WTILE, CHUNK):
            part = slice(q, q + CHUNK)
            un[part] = jnp.concatenate([column(q, CHUNK, k) for k in range(parts)], axis=1).astype(jnp.bfloat16)
            for p in range(q, q + CHUNK, LANES):
                gate = spread_column(gate_ref[0, pl.ds(j * gate_rows + p // LANES, 1), :])
                for k in range(parts):
                    d = column(p, LANES, parts + k)
                    cn[p:p + LANES, k * LANES:(k + 1) * LANES] = (d * gate).astype(jnp.bfloat16)
            ab = nt_dot(gu, un[part])
            dh = nt_dot(w_ref[0, 0], cn[part])
            for r in range(q, q + CHUNK):
                gather_row(nxt + r, r)
            a, b = ab[:ff], ab[ff:]
            s = jax.nn.sigmoid(a)
            act = a * s
            hn[:, part] = (act * b).astype(jnp.bfloat16)
            dn[:ff, part] = (dh * b * (s * (1.0 + a * (1.0 - s)))).astype(jnp.bfloat16)
            dn[ff:, part] = (dh * act).astype(jnp.bfloat16)

    def tile(j, carry):
        odd = lax.rem(begin + j, 2)
        wait_rows(jnp.where((e == 0) & (j + 1 < n_tiles), (j + 2) * WTILE, page * SOURCES))

        @pl.when(odd == 0)
        def _():
            compute(j, both[0], both[1])

        @pl.when(odd == 1)
        def _():
            compute(j, both[1], both[0])

        @pl.when(j == 0)
        def _():
            dg = gacc[:ff].astype(jnp.bfloat16)
            du = gacc[ff:].astype(jnp.bfloat16)
            dw = wacc[...].astype(jnp.bfloat16)
            dg_ref[0, 0], du_ref[0, 0], dw_ref[0, 0] = dg, du, dw
            og_ref[0], ou_ref[0], ow_ref[0] = dg, du, dw
            gacc[...] = jnp.zeros_like(gacc)
            wacc[...] = jnp.zeros_like(wacc)

        return carry

    lax.fori_loop(0, n_tiles, tile, 0)


def move_step(e, n_steps, layer, names, arrived, whole, buf, in_sem, out_sem):
    per = buf.shape[2]

    def arrive(chunk):
        slot = lax.rem(chunk, 2)
        return [pltpu.make_async_copy(x.at[pl.ds(chunk * per, per)], buf.at[slot, k], in_sem.at[slot])
                for k, x in enumerate(arrived)]

    def leave(chunk):
        slot = lax.rem(chunk, 2)
        return [pltpu.make_async_copy(buf.at[slot, k, i], x.at[layer, names[chunk * per + i]], out_sem.at[slot])
                for k, x in enumerate(whole) for i in range(per)]

    def each(when, copies, act):
        @pl.when(when)
        def _():
            for c in copies:
                act(c)

    each(e >= 2, leave(jnp.maximum(e - 2, 0)), lambda c: c.wait())
    each(e < n_steps, arrive(jnp.minimum(e, n_steps - 1)), lambda c: c.start())
    each(e >= 1, arrive(jnp.maximum(e - 1, 0)), lambda c: c.wait())
    each(e >= 1, leave(jnp.maximum(e - 1, 0)), lambda c: c.start())
    each(e == n_steps, leave(n_steps - 1), lambda c: c.wait())


def weight_grads(layer, first, exps, tiles, offsets, rows, idx_all, gates, weights, full, moved=None):
    parts = rows[0][0].shape[1]
    n_tok = sum(x.shape[0] for x in rows[0])
    n_layers, n_local, ff, d_model = weights[0].shape
    n_exp = exps.shape[0]
    out_rows = gates.shape[1]
    page = out_rows * LANES
    tiles = jnp.concatenate([tiles, jnp.ones((1,), jnp.int32)])
    begins = jnp.cumsum(tiles) - tiles
    any_spec = pl.BlockSpec(memory_space=pl.ANY)
    mine = pl.BlockSpec((1, 1, ff, d_model), lambda e, exps, *_: (layer, exps[jnp.minimum(e, n_exp - 1)], 0, 0))
    done = pl.BlockSpec((1, 1, ff, d_model), lambda e, exps, *_: (layer, exps[jnp.maximum(e - 1, 0)], 0, 0))
    half = pl.BlockSpec((1, ff, d_model), lambda e, *_: (jnp.maximum(e - 1, 0), 0, 0))
    gate_spec = pl.BlockSpec((1, out_rows, LANES), lambda e, *_: (first + jnp.minimum(e, n_exp - 1), 0, 0))
    aliased = list(full) if full is not None else []
    tile_set = [pltpu.VMEM((WTILE, d_model), jnp.bfloat16)] * 2 + [pltpu.VMEM((2 * ff, WTILE), jnp.bfloat16),
                                                                 pltpu.VMEM((ff, WTILE), jnp.bfloat16)]
    arrived, names = moved if moved else ([], exps)
    scratch = []
    if moved:
        scratch = [pltpu.VMEM((2, 3, arrived[0].shape[0] // n_exp, ff, d_model), jnp.bfloat16), pltpu.SemaphoreType.DMA((2,)),
                   pltpu.SemaphoreType.DMA((2,))]
    outs = pl.pallas_call(
        functools.partial(weight_grad_body, parts=parts, n_exp=n_exp, n_alias=len(aliased), n_moved=len(arrived),
                          n_rows=[len(x) for x in rows], first_list=first, page=page, layer=layer),
        grid_spec=pltpu.PrefetchScalarGridSpec(
            num_scalar_prefetch=5,
            grid=(n_exp + 1,),
            in_specs=[any_spec] * (len(rows[0] + rows[1]) + 1) + [gate_spec] + [mine] * 3 + [any_spec] * (len(arrived) + len(aliased)),
            out_specs=[done] * 3 + [half] * 3,
            scratch_shapes=[pltpu.VMEM((n_tok + 8, 2 * parts, LANES), jnp.bfloat16)]
            + [pltpu.VMEM((WTILE * PITCH + 16, LANES), jnp.float32)] + tile_set * 2
            + [pltpu.VMEM((2 * ff, d_model), jnp.float32), pltpu.VMEM((ff, d_model), jnp.float32),
               pltpu.SMEM((3 * page,), jnp.int32), pltpu.SMEM((1,), jnp.int32), pltpu.SemaphoreType.DMA((SOURCES,)),
               pltpu.SemaphoreType.DMA((3,))] + scratch,
        ),
        out_shape=[jax.ShapeDtypeStruct((n_layers, n_local, ff, d_model), jnp.bfloat16)] * 3
        + [jax.ShapeDtypeStruct((n_exp, ff, d_model), jnp.bfloat16)] * 3,
        input_output_aliases={10 + len(rows[0] + rows[1] + arrived) + k: k for k in range(len(aliased))},
        compiler_params=pltpu.CompilerParams(dimension_semantics=("arbitrary",), vmem_limit_bytes=VMEM_LIMIT),
        cost_estimate=pl.CostEstimate(flops=6 * n_tok * n_exp * d_model * ff,
                                      bytes_accessed=n_tok * d_model * 4 + 9 * n_exp * ff * d_model * 2, transcendentals=0),
        name="weight_grads",
    )(exps, tiles, begins, offsets, names, *rows[0], *rows[1], idx_all, gates, *weights, *arrived, *aliased)
    return outs[:3], outs[3:]


def merge_body(exps, *refs, layers, n_exp):
    n_in = 3 * len(layers)
    wholes, (buf, in_sem, out_sem) = refs[n_in + 3:n_in + 6], refs[n_in + 6:]

    def arrive(g, k, q):
        return pltpu.make_async_copy(refs[3 * g + k].at[q], buf.at[g, k, q], in_sem.at[g, k, q])

    def leave(g, k, q):
        return pltpu.make_async_copy(buf.at[g, k, q], wholes[k].at[layers[g], exps[g * n_exp + q]], out_sem)

    def each(g, act):
        def one(q, carry):
            for k in range(3):
                act(g, k, q)
            return carry

        lax.fori_loop(0, n_exp, one, 0)

    def pass_on(*at):
        arrive(*at).wait()
        leave(*at).start()

    for act in (lambda *at: arrive(*at).start(), pass_on, lambda *at: leave(*at).wait()):
        for g in range(len(layers)):
            each(g, act)


def merge_lists(groups, full):
    layers, arrays, names = zip(*groups)
    n_exp, ff, d_model = arrays[0][0].shape
    flat = [x for group in arrays for x in group]
    any_spec = pl.BlockSpec(memory_space=pl.ANY)
    return pl.pallas_call(
        functools.partial(merge_body, layers=layers, n_exp=n_exp),
        grid_spec=pltpu.PrefetchScalarGridSpec(
            num_scalar_prefetch=1, grid=(1,), in_specs=[any_spec] * (len(flat) + 3), out_specs=[any_spec] * 3,
            scratch_shapes=[pltpu.VMEM((len(groups), 3, n_exp, ff, d_model), jnp.bfloat16),
                            pltpu.SemaphoreType.DMA((len(groups), 3, n_exp)), pltpu.SemaphoreType.DMA]),
        out_shape=[jax.ShapeDtypeStruct(x.shape, x.dtype) for x in full],
        input_output_aliases={len(flat) + 1 + k: k for k in range(3)},
        compiler_params=pltpu.CompilerParams(vmem_limit_bytes=VMEM_LIMIT),
        cost_estimate=pl.CostEstimate(flops=10**9, bytes_accessed=4 * len(flat) * flat[0].size, transcendentals=0),
        name="merge_lists",
    )(jnp.concatenate(names), *flat, *full)


def join_body(a, b, out, sem):
    n = a.shape[0]
    copies = [pltpu.make_async_copy(x, out.at[pl.ds(k * n, n)], sem.at[k]) for k, x in enumerate((a, b))]
    for c in copies:
        c.start()
    for c in copies:
        c.wait()


def join_rows(a, b):
    n, parts, _ = a.shape
    any_spec = pl.BlockSpec(memory_space=pl.ANY)
    return pl.pallas_call(
        join_body, in_specs=[any_spec] * 2, out_shape=jax.ShapeDtypeStruct((2 * n, parts, LANES), a.dtype),
        out_specs=pl.BlockSpec(memory_space=pltpu.VMEM), scratch_shapes=[pltpu.SemaphoreType.DMA((2,))], name="join_rows",
    )(a, b)


def route_tables(ids, gates, ep, n_local):
    n_src, top_k, tok = ids.shape
    n = n_src * top_k * tok
    local = ids - ep * n_local
    here = (local >= 0) & (local < n_local)
    group = jnp.where(here, local, n_local).reshape(-1)
    key, gate = lax.sort((group * n + jnp.arange(n, dtype=jnp.int32), gates.reshape(-1)), num_keys=1, is_stable=False)
    copy = key % n
    token = copy // (top_k * tok) * tok + copy % tok
    token = jnp.pad(token, (0, 2 * PAGE))
    gate = jnp.pad(gate, (0, 2 * PAGE)).reshape(-1, LANES)
    ids = jnp.arange(n_local, dtype=jnp.int32)
    hits = jnp.sum((group.reshape(n_src, -1, 1) == ids).astype(jnp.int32), axis=1)
    starts = jnp.sum(below(n_local) * jnp.sum(hits, axis=0), axis=1)
    ends = starts + jnp.sum(hits, axis=0)
    middle = starts + hits[0]
    bounds = jnp.pad(starts, (0, LANES - n_local), mode='edge')
    bounds = jnp.where(jnp.arange(LANES) < n_local, bounds, ends[-1])
    runs = [jnp.concatenate(x) for x in ((starts, middle), (middle, ends), (starts, ends))]
    return runs, token, gate, bounds


def deal_experts(bounds, n_local, n_lists):
    load = jnp.sum(bounds[:, 1:n_local + 1] - bounds[:, :n_local], axis=0)
    ids = jnp.arange(n_local, dtype=jnp.int32)
    mine = load.reshape(-1, 1)
    rank = jnp.sum((load > mine).astype(jnp.int32) + (load == mine).astype(jnp.int32) * below(n_local), axis=1)
    turn, which = jnp.arange(n_local // n_lists), jnp.arange(n_lists).reshape(-1, 1)
    want = n_lists * turn + jnp.where(turn % 2 == 0, which, n_lists - 1 - which)
    pick = (rank == jnp.expand_dims(want, 2)).astype(jnp.int32)
    tiles = jnp.maximum((jnp.sum(pick * load, axis=2) + WTILE - 1) // WTILE, 1)
    return jnp.sum(pick * ids, axis=2), tiles


def source_offsets(bounds, expert):
    lane = jnp.arange(bounds.shape[1], dtype=jnp.int32)
    counts = jnp.sum(bounds * ((lane == expert + 1).astype(jnp.int32) - (lane == expert).astype(jnp.int32)), axis=1)
    return jnp.sum(below(bounds.shape[0]) * counts, axis=1)


def after(x, *earlier):
    return lax.optimization_barrier((x, *earlier))[0]


def solution(mesh):
    ep_size = mesh.shape['ep']
    dp_size = mesh.shape['dp']
    tok_spec = P(('dp', 'ep'), None)
    route_spec = P(None, ('dp', 'ep'), None)
    whole_spec = P(None, None, None)
    expert_spec = P(None, 'ep', None, None)
    ep_pairs = [(i, 1 - i) for i in range(ep_size)]
    core_pairs = [(i, i ^ 1) for i in range(dp_size)]
    chip_pairs = [(i, i ^ (2 << i % 2)) for i in range(dp_size)]

    def device_body(tokens, d_out, expert_ids, gate_vals, w_mix, w_gate, w_up, w_down):
        n_layers = w_mix.shape[0]
        n_local = w_gate.shape[1]
        n_experts = n_local * ep_size
        tok, d_model = tokens.shape
        top_k = expert_ids.shape[2]
        parts = d_model // LANES
        cap = cdiv(CAP_FACTOR * tok * top_k, n_experts)
        ep_id = lax.axis_index('ep').astype(jnp.int32)
        dp_id = lax.axis_index('dp').astype(jnp.int32)
        weights = (jnp.swapaxes(w_gate, 2, 3), jnp.swapaxes(w_up, 2, 3), w_down)

        def swap(x):
            return lax.ppermute(x, 'ep', ep_pairs)

        def spread(x):
            return [lax.all_gather(y, 'dp', axis=0, tiled=True) for y in x]

        def trade(x, pairs):
            return [lax.ppermute(y, 'dp', pairs) for y in x]

        def slab(x):
            return x.reshape(tok, parts, LANES)

        def mixed(x, layer):
            return (x.astype(jnp.float32) + jnp.dot(x, w_mix[layer], preferred_element_type=jnp.float32)).astype(jnp.bfloat16)

        ids = jnp.swapaxes(expert_ids, 1, 2)
        gates = jnp.swapaxes(gate_vals, 1, 2)
        mine = jnp.stack([ids.astype(jnp.float32), gates])
        u = mixed(tokens, 0)
        u_slab = slab(u)
        theirs = swap(after(mine, u_slab))
        both = jnp.stack([mine, theirs], 2)
        top = n_layers - 1
        runs, tables, packed = [], [], []

        def add_tables(pair):
            run, token, gate, bounds = route_tables(pair[0].astype(jnp.int32), pair[1], ep_id, n_local)
            runs.append(run)
            tables.append((token, gate))
            spot = dp_id * (2 * tok) + token
            first = jnp.concatenate([spot.reshape(-1, LANES), jnp.pad(bounds.reshape(1, LANES), ((0, 7), (0, 0)))])
            packed.append(jnp.stack([first.astype(jnp.float32), jnp.pad(gate, ((0, 8), (0, 0)))]))

        add_tables(both[:, 0])

        x_in, u_slabs, u_others, xs = tokens, [u_slab], [swap(u_slab)], []
        d_slab = slab(d_out)
        d_other = swap(after(d_slab, u_others[0]))
        d_rows = spread([join_rows(d_slab, d_other)])
        for layer in range(n_layers):
            if layer:
                u = mixed(x_in, layer)
                u_slabs.append(slab(u))
                u_others.append(swap(u_slabs[layer]))
                add_tables(after(both[:, layer], u_slabs[layer]))
            xs.append(x_in)
            if layer < top:
                other, = token_kernel(layer, runs[layer][1], tables[layer], (u_slabs[layer], u_others[layer]), weights, (1,))
                sent = swap(other)
                own, = token_kernel(layer, runs[layer][0], tables[layer], (after(u_slabs[layer], other), u_others[layer]),
                                    weights, (0,))
                x_in = (u.astype(jnp.float32) + own + sent).astype(jnp.bfloat16)

        shared = lax.all_gather(jnp.stack(packed), 'dp', axis=0)
        starts = shared[:, :, 0, -8].astype(jnp.int32)
        core = dp_id % 2
        kind = (dp_id // 2 + dp_id // 4) % 2
        dealt = [deal_experts(starts[:, layer], n_local, 2 * PARTS) for layer in range(n_layers)]
        of_layer = [layer for layer in range(top) for _ in range(PARTS)] + [top]
        places = [PARTS * core + part for _ in range(top) for part in range(PARTS)] + [PARTS * core + kind]
        mine = [dealt[layer][0][place] for layer, place in zip(of_layer, places)]
        list_rows = cdiv(cdiv(dp_size * 2 * cap, LANES), 8) * 8 + 8
        idx_all, gate_all = merge_tables(shared, starts, jnp.concatenate(mine),
                                         jnp.concatenate([jnp.full_like(x, layer) for x, layer in zip(mine, of_layer)]),
                                         list_rows, dp_size * 2 * tok)
        offsets = [source_offsets(starts[:, layer], x[0]) for x, layer in zip(mine, of_layer)]
        idx_all = idx_all.reshape(-1)

        d_y, full, arrived = d_out, None, []
        d_mix = [None] * n_layers
        for layer in reversed(range(n_layers)):
            both_u = [u_slabs[layer], u_others[layer]]
            u_rows = spread(both_u if layer < top else [join_rows(*both_u)])
            slabs = (u_slabs[layer], u_others[layer], d_slab, d_other)
            own, other = token_kernel(layer, runs[layer][2], tables[layer], slabs, weights)
            d_u = (d_y.astype(jnp.float32) + own + swap(other)).astype(jnp.bfloat16)
            last = other
            if layer == top:
                y_own, last = token_kernel(top, runs[top][2], tables[top], (after(u_slabs[top], other), u_others[top]), weights)
            d_mix[layer] = jnp.einsum('td,te->de', xs[layer], d_u, preferred_element_type=jnp.float32).astype(jnp.bfloat16)
            d_y = (d_u.astype(jnp.float32)
                   + jnp.einsum('te,de->td', d_u, w_mix[layer], preferred_element_type=jnp.float32)).astype(jnp.bfloat16)
            lists, tiles = dealt[layer]
            theirs = PARTS * (1 - core)
            for part in range(PARTS if layer < top else 1):
                item = of_layer.index(layer) + part
                first = sum(x.shape[0] for x in mine[:item])
                full, done = weight_grads(layer, first, mine[item], after(tiles[places[item]], last), offsets[item],
                                          (u_rows, d_rows), idx_all, gate_all, weights, full, moved if part else None)
                got = trade(done, core_pairs)
                if layer < top:
                    arrived.insert(1 + 2 * part, (layer, got, lists[theirs + part]))
                    continue
                moved = got, lists[theirs + kind]
                far = trade(done, chip_pairs)
                arrived.append((layer, far, lists[PARTS * core + 1 - kind]))
                arrived.append((layer, trade(far, core_pairs), lists[theirs + 1 - kind]))
            if layer:
                d_slab = slab(d_y)
                d_other = swap(d_slab)
                d_rows = spread([join_rows(d_slab, d_other)])
                if layer == top:
                    layer_out = (u.astype(jnp.float32) + y_own + swap(after(last, d_other))).astype(jnp.bfloat16)
        full = merge_lists(arrived[-1:], merge_lists(arrived[:-1], full))
        d_mix = lax.psum(jnp.stack(d_mix), ('dp', 'ep'))
        return (layer_out, d_y, d_mix, jnp.swapaxes(full[0], 2, 3), jnp.swapaxes(full[1], 2, 3), full[2])

    return jax.shard_map(device_body, mesh=mesh,
                         in_specs=(tok_spec, tok_spec, route_spec, route_spec, whole_spec,
                                   expert_spec, expert_spec, expert_spec),
                         out_specs=(tok_spec, tok_spec, whole_spec, expert_spec, expert_spec, expert_spec),
                         check_vma=False)
```

```python
import functools
import math

import jax
import jax.numpy as jnp
from jax import lax
from jax.experimental import pallas as pl
from jax.experimental.pallas import tpu as pltpu
from jax.sharding import PartitionSpec as P


CAP_FACTOR = 3
LANES = 128
TILE = 96
HALF_TILE = 64
WTILE = 768
PARTS = 2
AHEAD = 3
SOURCES = 8
CHUNK = 256
PITCH = 9
BATCH = 16
SLOTS = 8
PAGE = 1024
VMEM_LIMIT = 62 * 2**20


def cdiv(a, b):
    return (a + b - 1) // b


def below(n):
    return jnp.tri(n, k=-1, dtype=jnp.int32)


def nt_dot(a, b):
    return lax.dot_general(a, b, (((1,), (1,)), ((), ())), preferred_element_type=jnp.float32)


def tn_dot(a, b):
    return lax.dot_general(a, b, (((0,), (0,)), ((), ())), preferred_element_type=jnp.float32)


def nn_dot(a, b):
    return lax.dot_general(a, b, (((1,), (0,)), ((), ())), preferred_element_type=jnp.float32)


def clear(ref):
    step = next(n for n in (64, 48, 32, 16, 8) if ref.shape[0] % n == 0)

    def one(q, carry):
        ref[pl.ds(pl.multiple_of(q * step, step), step), :] = jnp.zeros((step, ref.shape[1]), ref.dtype)
        return carry

    lax.fori_loop(0, ref.shape[0] // step, one, 0)


def add_rows(acc, vals_ref, idx, row, tile, pitch, width):
    for b in range(0, tile, BATCH):
        at = [pl.multiple_of(idx[row + b + r], 4) for r in range(BATCH)]
        vals = [acc[pl.ds(at[r], width), :] + vals_ref[pl.ds((b + r) * pitch, width), :] for r in range(BATCH)]
        for r in reversed(range(BATCH)):
            acc[pl.ds(at[r], width), :] = vals[r]


def spread_column(row):
    return jnp.broadcast_to(row, (LANES, LANES)).T


def tile_gates(gates, row):
    pair = gates[pl.ds(lax.div(row, LANES), 2), :]
    skip = lax.rem(row, LANES)
    pair = pltpu.roll(pair, lax.rem(LANES - skip, LANES), 1)
    lane = lax.broadcasted_iota(jnp.int32, (1, LANES), 1)
    return spread_column(jnp.where(lane < LANES - skip, pair[:1], pair[1:]))


def widen(src, dst, pitch, halves, tok):
    step = 32

    def one(q, carry):
        for r in range(step):
            dst[pl.ds((q * step + r) * pitch, pitch), :] = src[q * step + r].astype(jnp.float32)
        return carry

    lax.fori_loop(halves[0] * tok // step, (halves[-1] + 1) * tok // step, one, 0)


def write_sums(acc, outs, tok, parts, pitch, halves):
    step = min(32, tok)

    def copy_out(q, carry):
        r0 = pl.multiple_of(q * step, step)
        for k in range(parts):
            for out, half in zip(outs, halves):
                first = (half * tok + r0) * pitch + k
                out[pl.ds(r0, step), k * LANES:(k + 1) * LANES] = acc[pl.ds(first, step, stride=pitch), :]
        return carry

    lax.fori_loop(0, tok // step, copy_out, 0)


def expert_copies(weights, buf, sem, layer, e):
    slot = lax.rem(e, SLOTS)
    ff = weights[0].shape[2]
    return [pltpu.make_async_copy(w.at[layer, e], buf.at[slot, pl.ds(k * ff, ff)], sem.at[slot])
            for k, w in enumerate(weights)]


def run_tiles(step, weights, wbuf, wsem, runs, tile, layer, prepare):
    n_local = weights[0].shape[1]
    for e in range(SLOTS - 2):
        for c in expert_copies(weights, wbuf, wsem, layer, e):
            c.start()
    prepare()
    for c in expert_copies(weights, wbuf, wsem, layer, 0):
        c.wait()

    def length(e):
        return runs[n_local + e] - runs[e]

    def add_tiles(e, total):
        return total + jnp.maximum(lax.div(length(e) + tile - 1, tile), 1)

    def one(i, carry):
        (e, row, left), (e1, row1, n1), (e2, row2, n2), row3 = carry

        @pl.when(e != e1)
        def _():
            for c in expert_copies(weights, wbuf, wsem, layer, e):
                c.wait()

        @pl.when((e != e1) & (e + SLOTS - 3 < n_local))
        def _():
            for c in expert_copies(weights, wbuf, wsem, layer, e + SLOTS - 3):
                c.start()

        step(row, (lax.rem(e1, SLOTS), row1), (lax.rem(e2, SLOTS), row2, n2), row3)
        more = left > tile
        e_next = jnp.minimum(e + 1, n_local - 1)
        fresh = jnp.where(e + 1 < n_local, length(e_next), 0)
        ahead = (jnp.where(more, e, e_next), jnp.where(more, row + tile, runs[e_next]), jnp.where(more, left - tile, fresh))
        return ahead, (e, row, jnp.minimum(left, tile)), (e1, row1, n1), row2

    none = (0, 0, 0)
    lax.fori_loop(0, lax.fori_loop(0, n_local, add_tiles, 0) + 3, one, ((0, runs[0], length(0)), none, none, 0))


def token_body(runs, idx, gates, *refs, layer, tok, parts, tile, halves, backward):
    n_in = 4 if backward else 2
    sources, weights, outs, refs = refs[:n_in], refs[n_in:n_in + 3], refs[n_in + 3:n_in + 3 + len(halves)], refs[n_in + 3 + len(halves):]
    narrow, wide, rows, vt, acc, mid, wbuf, sem, wsem = refs
    ff = weights[0].shape[2]
    width = parts * n_in // 2
    pitch = width + 1

    def prepare():
        copies = [pltpu.make_async_copy(src, narrow.at[pl.ds(k % 2 * tok, tok), pl.ds(k // 2 * parts, parts)], sem.at[k])
                  for k, src in enumerate(sources) if k % 2 in halves]
        for c in copies:
            c.start()
        for ref in (acc, vt, rows, mid):
            clear(ref)
        for c in copies:
            c.wait()
        widen(narrow, wide, width, halves, tok)

    def column(k):
        return rows[pl.ds(k, tile, stride=pitch), :]

    def step(row, here, before, done):
        slot, row1 = here
        slot2, row2, n2 = before
        old = wbuf[slot2, :2 * ff] if backward else wbuf[slot2, 2 * ff:]
        v = tn_dot(mid[...], old).astype(jnp.bfloat16).astype(jnp.float32)
        u = jnp.concatenate([column(k) for k in range(parts)], axis=1).astype(jnp.bfloat16)
        ab = nt_dot(wbuf[slot, :2 * ff], u)
        if backward:
            gate = tile_gates(gates, row1)[:tile]
            c = jnp.concatenate([(column(parts + k) * gate).astype(jnp.bfloat16) for k in range(parts)], axis=1)
            dh = nt_dot(wbuf[slot, 2 * ff:], c)
        add_rows(acc, vt, idx, done, tile, parts + 1, parts)
        for r in range(tile):
            rows[pl.ds(pitch * r, width), :] = wide[pl.ds(pl.multiple_of(idx[row + r], width), width), :]
        live = lax.broadcasted_iota(jnp.int32, (tile, LANES), 0) < n2
        gate = tile_gates(gates, row2)[:tile]
        for k in range(parts):
            v_k = jnp.where(live, v[:, k * LANES:(k + 1) * LANES] * gate, 0.0)
            vt[pl.ds(k, tile, stride=parts + 1), :] = v_k
        a, b = ab[:ff], ab[ff:]
        s = jax.nn.sigmoid(a)
        act = a * s
        if backward:
            mid[:ff] = (dh * b * (s * (1.0 + a * (1.0 - s)))).astype(jnp.bfloat16)
            mid[ff:] = (dh * act).astype(jnp.bfloat16)
        else:
            mid[...] = (act * b).astype(jnp.bfloat16)

    run_tiles(step, weights, wbuf, wsem, runs, tile, layer, prepare)
    write_sums(acc, outs, tok, parts, width, halves)


def token_kernel(layer, runs, table, slabs, weights, halves=(0, 1)):
    idx, gates = table
    tok, parts, _ = slabs[0].shape
    _, n_local, ff, d_model = weights[0].shape
    backward = len(slabs) > 2
    tile = TILE if len(halves) == 2 else HALF_TILE
    width = parts * len(slabs) // 2
    rows_spec = pl.BlockSpec((tok, d_model), lambda i, *_: (0, 0))
    any_spec = pl.BlockSpec(memory_space=pl.ANY)
    tile_rows = cdiv(tile * (width + 1), 16) * 16
    work = (4 if backward else 3) * len(halves)
    return pl.pallas_call(
        functools.partial(token_body, layer=layer, tok=tok, parts=parts, tile=tile, halves=halves, backward=backward),
        grid_spec=pltpu.PrefetchScalarGridSpec(
            num_scalar_prefetch=2,
            grid=(1,),
            in_specs=[pl.BlockSpec(gates.shape, lambda i, *_: (0, 0))] + [any_spec] * (len(slabs) + 3),
            out_specs=[rows_spec] * len(halves),
            scratch_shapes=[pltpu.VMEM((2 * tok, width, LANES), jnp.bfloat16), pltpu.VMEM((2 * tok * width, LANES), jnp.float32),
                            pltpu.VMEM((tile_rows, LANES), jnp.float32), pltpu.VMEM((tile_rows, LANES), jnp.float32),
                            pltpu.VMEM((2 * tok * width, LANES), jnp.float32),
                            pltpu.VMEM((2 * ff if backward else ff, tile), jnp.bfloat16),
                            pltpu.VMEM((SLOTS, 3 * ff, d_model), jnp.bfloat16),
                            pltpu.SemaphoreType.DMA((len(slabs),)), pltpu.SemaphoreType.DMA((SLOTS,))],
        ),
        out_shape=[jax.ShapeDtypeStruct((tok, d_model), jnp.float32)] * len(halves),
        compiler_params=pltpu.CompilerParams(dimension_semantics=("arbitrary",), vmem_limit_bytes=VMEM_LIMIT),
        cost_estimate=pl.CostEstimate(flops=work * 2 * 8 * tok * d_model * ff * 4,
                                      bytes_accessed=3 * n_local * ff * d_model * 2, transcendentals=0),
        name="experts_backward" if backward else "experts_forward",
    )(runs, idx, gates, *slabs, *weights)


def merge_tables_body(st, exps, layers, table, idx_ref, gate_ref, buf, *, out_rows, pad_row):
    group = idx_ref.shape[0]

    def one(q, carry):
        item = pl.program_id(0) * group + q
        merge_expert(exps[item], layers[item], st, table, idx_ref.at[q], gate_ref.at[q], buf, out_rows, pad_row)
        return carry

    lax.fori_loop(0, group, one, 0)


def merge_expert(exp, layer, st, table, idx_out, gate_out, buf, out_rows, pad_row):
    src, n_layers = table.shape[:2]
    buf[0] = jnp.full(buf.shape[1:], float(pad_row), jnp.float32)
    buf[1] = jnp.zeros(buf.shape[1:], jnp.float32)
    row = lax.broadcasted_iota(jnp.int32, (8, LANES), 0)
    lane = lax.broadcasted_iota(jnp.int32, (8, LANES), 1)
    off = 0
    for d in range(src):
        at = (d * n_layers + layer) * LANES + exp
        first = st[at]
        count = st[at + 1] - first
        to = lax.rem(off, LANES) + LANES
        shift = to - lax.rem(first, LANES)
        over = lax.rem(shift, LANES)
        start = lax.div(off, LANES)
        place = row * LANES + lane
        take = (place >= to) & (place < to + count)
        for kind in range(2):
            x = table[d, layer, kind, pl.ds(lax.div(first, LANES), 8), :]
            x = pltpu.roll(pltpu.roll(x, over, 1), lax.div(shift, LANES), 0)
            x = jnp.where(lane >= over, x, pltpu.roll(x, 1, 0))
            old = buf[kind, pl.ds(start, 8), :]
            buf[kind, pl.ds(start, 8), :] = jnp.where(take, x, old)
        off = off + count
    idx_out[...] = buf[0, pl.ds(1, out_rows), :].astype(jnp.int32)
    gate_out[...] = buf[1, pl.ds(1, out_rows), :]


def merge_tables(shared, starts, exps, layers, out_rows, pad_row):
    n_items = exps.shape[0]
    group = math.gcd(n_items, 8)
    out = pl.BlockSpec((group, out_rows, LANES), lambda g, *_: (g, 0, 0))
    return pl.pallas_call(
        functools.partial(merge_tables_body, out_rows=out_rows, pad_row=pad_row),
        grid_spec=pltpu.PrefetchScalarGridSpec(
            num_scalar_prefetch=3,
            grid=(n_items // group,),
            in_specs=[pl.BlockSpec(shared.shape, lambda g, *_: (0,) * shared.ndim)],
            out_specs=[out] * 2,
            scratch_shapes=[pltpu.VMEM((2, out_rows + 16, LANES), jnp.float32)],
        ),
        out_shape=[jax.ShapeDtypeStruct((n_items, out_rows, LANES), jnp.int32),
                   jax.ShapeDtypeStruct((n_items, out_rows, LANES), jnp.float32)],
        compiler_params=pltpu.CompilerParams(dimension_semantics=("arbitrary",)),
        cost_estimate=pl.CostEstimate(flops=10**9, bytes_accessed=4 * shared.size, transcendentals=0),
        name="merge_tables",
    )(starts.reshape(-1), exps, layers, shared)


def weight_grad_body(exps, tiles, begins, offsets, names, *refs, parts, n_exp, n_alias, n_moved, n_rows, first_list, page, layer):
    u_rows, d_rows, refs = refs[:n_rows[0]], refs[n_rows[0]:sum(n_rows)], refs[sum(n_rows):]
    idx_all, gate_ref, g_ref, up_ref, w_ref = refs[:5]
    moved, whole, refs = refs[5:5 + n_moved], refs[5 + n_moved:5 + n_moved + n_alias], refs[5 + n_moved + n_alias:]
    (dg_ref, du_ref, dw_ref, og_ref, ou_ref, ow_ref,
     uds, rows, u0, c0, d0, h0, u1, c1, d1, h1, gacc, wacc, idx_s, seen, sem, tsem, *move_refs) = refs
    e = pl.program_id(0)
    ff = g_ref.shape[2]
    slots = 3
    both = ((u0, c0, d0, h0), (u1, c1, d1, h1))

    def table_copy(exp):
        slot = lax.rem(exp, slots)
        at = pl.multiple_of((first_list + exp) * page, PAGE)
        to = pl.multiple_of(slot * page, PAGE)
        return pltpu.make_async_copy(idx_all.at[pl.ds(at, page)], idx_s.at[pl.ds(to, page)], tsem.at[slot])

    def gather_row(at, r):
        rows[pl.ds(r * PITCH, 2 * parts), :] = uds[idx_s[at]].astype(jnp.float32)

    def column(first, count, k):
        return rows[pl.ds(first * PITCH + k, count, stride=PITCH), :]

    n_tok = uds.shape[0] - 8

    def row_copies(q):
        out = []
        for kind, arrays in enumerate((u_rows, d_rows)):
            run = n_tok // (SOURCES * len(arrays))
            for k, src in enumerate(arrays):
                place = uds.at[pl.ds((q * len(arrays) + k) * run, run), pl.ds(kind * parts, parts)]
                out.append(pltpu.make_async_copy(src.at[pl.ds(q * run, run)], place, sem.at[q]))
        return out

    def wait_rows(limit):
        def one(q, carry):
            @pl.when((q >= seen[0]) & (offsets[q] < limit))
            def _():
                for c in row_copies(q):
                    c.wait()
                seen[0] = q + 1

                @pl.when(q + AHEAD < SOURCES)
                def _():
                    for c in row_copies(q + AHEAD):
                        c.start()

            return carry

        @pl.when(seen[0] < SOURCES)
        def _():
            lax.fori_loop(0, SOURCES, one, 0)

    @pl.when(e == 0)
    def _():
        for q in range(AHEAD):
            for c in row_copies(q):
                c.start()
        seen[0] = 0
        table_copy(0).start()
        table_copy(1).start()
        uds[pl.ds(n_tok, 8)] = jnp.zeros((8, 2 * parts, LANES), jnp.bfloat16)
        for ref in (*both[0], *both[1], gacc, wacc):
            clear(ref)
        table_copy(0).wait()
        wait_rows(WTILE)

        def first_rows(q, carry):
            for r in range(16):
                gather_row(q * 16 + r, q * 16 + r)
            return carry

        lax.fori_loop(0, WTILE // 16, first_rows, 0)

    if moved:
        move_step(e, n_exp, layer + 1, names, moved, whole, *move_refs)

    @pl.when(e + 1 < n_exp)
    def _():
        table_copy(e + 1).wait()

    @pl.when(e + 2 < n_exp)
    def _():
        table_copy(e + 2).start()

    here = lax.rem(e, slots) * page
    there = lax.rem(jnp.minimum(e + 1, n_exp - 1), slots) * page
    n_tiles = tiles[e]
    begin = begins[e]
    gate_rows = WTILE // LANES

    def compute(j, new, old):
        un, cn, dn, hn = new
        uo, co, do, ho = old
        gacc[...] += nn_dot(do[...], uo[...])
        wacc[...] += nn_dot(ho[...], co[...])
        nxt = jnp.where(j + 1 < n_tiles, here + (j + 1) * WTILE, there)
        gu = jnp.concatenate([g_ref[0, 0], up_ref[0, 0]], axis=0)
        for q in range(0, WTILE, CHUNK):
            part = slice(q, q + CHUNK)
            un[part] = jnp.concatenate([column(q, CHUNK, k) for k in range(parts)], axis=1).astype(jnp.bfloat16)
            for p in range(q, q + CHUNK, LANES):
                gate = spread_column(gate_ref[0, pl.ds(j * gate_rows + p // LANES, 1), :])
                for k in range(parts):
                    d = column(p, LANES, parts + k)
                    cn[p:p + LANES, k * LANES:(k + 1) * LANES] = (d * gate).astype(jnp.bfloat16)
            ab = nt_dot(gu, un[part])
            dh = nt_dot(w_ref[0, 0], cn[part])
            for r in range(q, q + CHUNK):
                gather_row(nxt + r, r)
            a, b = ab[:ff], ab[ff:]
            s = jax.nn.sigmoid(a)
            act = a * s
            hn[:, part] = (act * b).astype(jnp.bfloat16)
            dn[:ff, part] = (dh * b * (s * (1.0 + a * (1.0 - s)))).astype(jnp.bfloat16)
            dn[ff:, part] = (dh * act).astype(jnp.bfloat16)

    def tile(j, carry):
        odd = lax.rem(begin + j, 2)
        wait_rows(jnp.where((e == 0) & (j + 1 < n_tiles), (j + 2) * WTILE, page * SOURCES))

        @pl.when(odd == 0)
        def _():
            compute(j, both[0], both[1])

        @pl.when(odd == 1)
        def _():
            compute(j, both[1], both[0])

        @pl.when(j == 0)
        def _():
            dg = gacc[:ff].astype(jnp.bfloat16)
            du = gacc[ff:].astype(jnp.bfloat16)
            dw = wacc[...].astype(jnp.bfloat16)
            dg_ref[0, 0], du_ref[0, 0], dw_ref[0, 0] = dg, du, dw
            og_ref[0], ou_ref[0], ow_ref[0] = dg, du, dw
            gacc[...] = jnp.zeros_like(gacc)
            wacc[...] = jnp.zeros_like(wacc)

        return carry

    lax.fori_loop(0, n_tiles, tile, 0)


def move_step(e, n_steps, layer, names, arrived, whole, buf, in_sem, out_sem):
    per = buf.shape[2]

    def arrive(chunk):
        slot = lax.rem(chunk, 2)
        return [pltpu.make_async_copy(x.at[pl.ds(chunk * per, per)], buf.at[slot, k], in_sem.at[slot])
                for k, x in enumerate(arrived)]

    def leave(chunk):
        slot = lax.rem(chunk, 2)
        return [pltpu.make_async_copy(buf.at[slot, k, i], x.at[layer, names[chunk * per + i]], out_sem.at[slot])
                for k, x in enumerate(whole) for i in range(per)]

    def each(when, copies, act):
        @pl.when(when)
        def _():
            for c in copies:
                act(c)

    each(e >= 2, leave(jnp.maximum(e - 2, 0)), lambda c: c.wait())
    each(e < n_steps, arrive(jnp.minimum(e, n_steps - 1)), lambda c: c.start())
    each(e >= 1, arrive(jnp.maximum(e - 1, 0)), lambda c: c.wait())
    each(e >= 1, leave(jnp.maximum(e - 1, 0)), lambda c: c.start())
    each(e == n_steps, leave(n_steps - 1), lambda c: c.wait())


def weight_grads(layer, first, exps, tiles, offsets, rows, idx_all, gates, weights, full, moved=None):
    parts = rows[0][0].shape[1]
    n_tok = sum(x.shape[0] for x in rows[0])
    n_layers, n_local, ff, d_model = weights[0].shape
    n_exp = exps.shape[0]
    out_rows = gates.shape[1]
    page = out_rows * LANES
    tiles = jnp.concatenate([tiles, jnp.ones((1,), jnp.int32)])
    begins = jnp.cumsum(tiles) - tiles
    any_spec = pl.BlockSpec(memory_space=pl.ANY)
    mine = pl.BlockSpec((1, 1, ff, d_model), lambda e, exps, *_: (layer, exps[jnp.minimum(e, n_exp - 1)], 0, 0))
    done = pl.BlockSpec((1, 1, ff, d_model), lambda e, exps, *_: (layer, exps[jnp.maximum(e - 1, 0)], 0, 0))
    half = pl.BlockSpec((1, ff, d_model), lambda e, *_: (jnp.maximum(e - 1, 0), 0, 0))
    gate_spec = pl.BlockSpec((1, out_rows, LANES), lambda e, *_: (first + jnp.minimum(e, n_exp - 1), 0, 0))
    aliased = list(full) if full is not None else []
    tile_set = [pltpu.VMEM((WTILE, d_model), jnp.bfloat16)] * 2 + [pltpu.VMEM((2 * ff, WTILE), jnp.bfloat16),
                                                                 pltpu.VMEM((ff, WTILE), jnp.bfloat16)]
    arrived, names = moved if moved else ([], exps)
    scratch = []
    if moved:
        scratch = [pltpu.VMEM((2, 3, arrived[0].shape[0] // n_exp, ff, d_model), jnp.bfloat16), pltpu.SemaphoreType.DMA((2,)),
                   pltpu.SemaphoreType.DMA((2,))]
    outs = pl.pallas_call(
        functools.partial(weight_grad_body, parts=parts, n_exp=n_exp, n_alias=len(aliased), n_moved=len(arrived),
                          n_rows=[len(x) for x in rows], first_list=first, page=page, layer=layer),
        grid_spec=pltpu.PrefetchScalarGridSpec(
            num_scalar_prefetch=5,
            grid=(n_exp + 1,),
            in_specs=[any_spec] * (len(rows[0] + rows[1]) + 1) + [gate_spec] + [mine] * 3 + [any_spec] * (len(arrived) + len(aliased)),
            out_specs=[done] * 3 + [half] * 3,
            scratch_shapes=[pltpu.VMEM((n_tok + 8, 2 * parts, LANES), jnp.bfloat16)]
            + [pltpu.VMEM((WTILE * PITCH + 16, LANES), jnp.float32)] + tile_set * 2
            + [pltpu.VMEM((2 * ff, d_model), jnp.float32), pltpu.VMEM((ff, d_model), jnp.float32),
               pltpu.SMEM((3 * page,), jnp.int32), pltpu.SMEM((1,), jnp.int32), pltpu.SemaphoreType.DMA((SOURCES,)),
               pltpu.SemaphoreType.DMA((3,))] + scratch,
        ),
        out_shape=[jax.ShapeDtypeStruct((n_layers, n_local, ff, d_model), jnp.bfloat16)] * 3
        + [jax.ShapeDtypeStruct((n_exp, ff, d_model), jnp.bfloat16)] * 3,
        input_output_aliases={10 + len(rows[0] + rows[1] + arrived) + k: k for k in range(len(aliased))},
        compiler_params=pltpu.CompilerParams(dimension_semantics=("arbitrary",), vmem_limit_bytes=VMEM_LIMIT),
        cost_estimate=pl.CostEstimate(flops=6 * n_tok * n_exp * d_model * ff,
                                      bytes_accessed=n_tok * d_model * 4 + 9 * n_exp * ff * d_model * 2, transcendentals=0),
        name="weight_grads",
    )(exps, tiles, begins, offsets, names, *rows[0], *rows[1], idx_all, gates, *weights, *arrived, *aliased)
    return outs[:3], outs[3:]


def merge_body(exps, *refs, layers, n_exp):
    n_in = 3 * len(layers)
    wholes, (buf, in_sem, out_sem) = refs[n_in + 3:n_in + 6], refs[n_in + 6:]

    def arrive(g, k, q):
        return pltpu.make_async_copy(refs[3 * g + k].at[q], buf.at[g, k, q], in_sem.at[g, k, q])

    def leave(g, k, q):
        return pltpu.make_async_copy(buf.at[g, k, q], wholes[k].at[layers[g], exps[g * n_exp + q]], out_sem)

    def each(g, act):
        def one(q, carry):
            for k in range(3):
                act(g, k, q)
            return carry

        lax.fori_loop(0, n_exp, one, 0)

    def pass_on(*at):
        arrive(*at).wait()
        leave(*at).start()

    for act in (lambda *at: arrive(*at).start(), pass_on, lambda *at: leave(*at).wait()):
        for g in range(len(layers)):
            each(g, act)


def merge_lists(groups, full):
    layers, arrays, names = zip(*groups)
    n_exp, ff, d_model = arrays[0][0].shape
    flat = [x for group in arrays for x in group]
    any_spec = pl.BlockSpec(memory_space=pl.ANY)
    return pl.pallas_call(
        functools.partial(merge_body, layers=layers, n_exp=n_exp),
        grid_spec=pltpu.PrefetchScalarGridSpec(
            num_scalar_prefetch=1, grid=(1,), in_specs=[any_spec] * (len(flat) + 3), out_specs=[any_spec] * 3,
            scratch_shapes=[pltpu.VMEM((len(groups), 3, n_exp, ff, d_model), jnp.bfloat16),
                            pltpu.SemaphoreType.DMA((len(groups), 3, n_exp)), pltpu.SemaphoreType.DMA]),
        out_shape=[jax.ShapeDtypeStruct(x.shape, x.dtype) for x in full],
        input_output_aliases={len(flat) + 1 + k: k for k in range(3)},
        compiler_params=pltpu.CompilerParams(vmem_limit_bytes=VMEM_LIMIT),
        cost_estimate=pl.CostEstimate(flops=10**9, bytes_accessed=4 * len(flat) * flat[0].size, transcendentals=0),
        name="merge_lists",
    )(jnp.concatenate(names), *flat, *full)


def join_body(a, b, out, sem):
    n = a.shape[0]
    copies = [pltpu.make_async_copy(x, out.at[pl.ds(k * n, n)], sem.at[k]) for k, x in enumerate((a, b))]
    for c in copies:
        c.start()
    for c in copies:
        c.wait()


def join_rows(a, b):
    n, parts, _ = a.shape
    any_spec = pl.BlockSpec(memory_space=pl.ANY)
    return pl.pallas_call(
        join_body, in_specs=[any_spec] * 2, out_shape=jax.ShapeDtypeStruct((2 * n, parts, LANES), a.dtype),
        out_specs=pl.BlockSpec(memory_space=pltpu.VMEM), scratch_shapes=[pltpu.SemaphoreType.DMA((2,))], name="join_rows",
    )(a, b)


def route_tables(ids, gates, ep, n_local):
    n_src, top_k, tok = ids.shape
    n = n_src * top_k * tok
    local = ids - ep * n_local
    here = (local >= 0) & (local < n_local)
    group = jnp.where(here, local, n_local).reshape(-1)
    key, gate = lax.sort((group * n + jnp.arange(n, dtype=jnp.int32), gates.reshape(-1)), num_keys=1, is_stable=False)
    copy = key % n
    token = copy // (top_k * tok) * tok + copy % tok
    token = jnp.pad(token, (0, 2 * PAGE))
    gate = jnp.pad(gate, (0, 2 * PAGE)).reshape(-1, LANES)
    ids = jnp.arange(n_local, dtype=jnp.int32)
    hits = jnp.sum((group.reshape(n_src, -1, 1) == ids).astype(jnp.int32), axis=1)
    starts = jnp.sum(below(n_local) * jnp.sum(hits, axis=0), axis=1)
    ends = starts + jnp.sum(hits, axis=0)
    middle = starts + hits[0]
    bounds = jnp.pad(starts, (0, LANES - n_local), mode='edge')
    bounds = jnp.where(jnp.arange(LANES) < n_local, bounds, ends[-1])
    runs = [jnp.concatenate(x) for x in ((starts, middle), (middle, ends), (starts, ends))]
    return runs, token, gate, bounds


def deal_experts(bounds, n_local, n_lists):
    load = jnp.sum(bounds[:, 1:n_local + 1] - bounds[:, :n_local], axis=0)
    ids = jnp.arange(n_local, dtype=jnp.int32)
    mine = load.reshape(-1, 1)
    rank = jnp.sum((load > mine).astype(jnp.int32) + (load == mine).astype(jnp.int32) * below(n_local), axis=1)
    turn, which = jnp.arange(n_local // n_lists), jnp.arange(n_lists).reshape(-1, 1)
    want = n_lists * turn + jnp.where(turn % 2 == 0, which, n_lists - 1 - which)
    pick = (rank == jnp.expand_dims(want, 2)).astype(jnp.int32)
    tiles = jnp.maximum((jnp.sum(pick * load, axis=2) + WTILE - 1) // WTILE, 1)
    return jnp.sum(pick * ids, axis=2), tiles


def source_offsets(bounds, expert):
    lane = jnp.arange(bounds.shape[1], dtype=jnp.int32)
    counts = jnp.sum(bounds * ((lane == expert + 1).astype(jnp.int32) - (lane == expert).astype(jnp.int32)), axis=1)
    return jnp.sum(below(bounds.shape[0]) * counts, axis=1)


def after(x, *earlier):
    return lax.optimization_barrier((x, *earlier))[0]


def solution(mesh):
    ep_size = mesh.shape['ep']
    dp_size = mesh.shape['dp']
    tok_spec = P(('dp', 'ep'), None)
    route_spec = P(None, ('dp', 'ep'), None)
    whole_spec = P(None, None, None)
    expert_spec = P(None, 'ep', None, None)
    ep_pairs = [(i, 1 - i) for i in range(ep_size)]
    core_pairs = [(i, i ^ 1) for i in range(dp_size)]
    chip_pairs = [(i, i ^ (2 << i % 2)) for i in range(dp_size)]

    def device_body(tokens, d_out, expert_ids, gate_vals, w_mix, w_gate, w_up, w_down):
        n_layers = w_mix.shape[0]
        n_local = w_gate.shape[1]
        n_experts = n_local * ep_size
        tok, d_model = tokens.shape
        top_k = expert_ids.shape[2]
        parts = d_model // LANES
        cap = cdiv(CAP_FACTOR * tok * top_k, n_experts)
        ep_id = lax.axis_index('ep').astype(jnp.int32)
        dp_id = lax.axis_index('dp').astype(jnp.int32)
        weights = (jnp.swapaxes(w_gate, 2, 3), jnp.swapaxes(w_up, 2, 3), w_down)

        def swap(x):
            return lax.ppermute(x, 'ep', ep_pairs)

        def spread(x):
            return [lax.all_gather(y, 'dp', axis=0, tiled=True) for y in x]

        def trade(x, pairs):
            return [lax.ppermute(y, 'dp', pairs) for y in x]

        def slab(x):
            return x.reshape(tok, parts, LANES)

        def mixed(x, layer):
            return (x.astype(jnp.float32) + jnp.dot(x, w_mix[layer], preferred_element_type=jnp.float32)).astype(jnp.bfloat16)

        ids = jnp.swapaxes(expert_ids, 1, 2)
        gates = jnp.swapaxes(gate_vals, 1, 2)
        mine = jnp.stack([ids.astype(jnp.float32), gates])
        u = mixed(tokens, 0)
        u_slab = slab(u)
        theirs = swap(after(mine, u_slab))
        both = jnp.stack([mine, theirs], 2)
        top = n_layers - 1
        runs, tables, packed = [], [], []

        def add_tables(pair):
            run, token, gate, bounds = route_tables(pair[0].astype(jnp.int32), pair[1], ep_id, n_local)
            runs.append(run)
            tables.append([(token * parts, gate), (token * (2 * parts), gate)])
            spot = dp_id * (2 * tok) + token
            first = jnp.concatenate([spot.reshape(-1, LANES), jnp.pad(bounds.reshape(1, LANES), ((0, 7), (0, 0)))])
            packed.append(jnp.stack([first.astype(jnp.float32), jnp.pad(gate, ((0, 8), (0, 0)))]))

        add_tables(both[:, 0])

        x_in, u_slabs, u_others, xs = tokens, [u_slab], [swap(u_slab)], []
        d_slab = slab(d_out)
        d_other = swap(after(d_slab, u_others[0]))
        d_rows = spread([join_rows(d_slab, d_other)])
        for layer in range(n_layers):
            if layer:
                u = mixed(x_in, layer)
                u_slabs.append(slab(u))
                u_others.append(swap(u_slabs[layer]))
                add_tables(after(both[:, layer], u_slabs[layer]))
            xs.append(x_in)
            if layer < top:
                other, = token_kernel(layer, runs[layer][1], tables[layer][0], (u_slabs[layer], u_others[layer]), weights, (1,))
                sent = swap(other)
                own, = token_kernel(layer, runs[layer][0], tables[layer][0], (after(u_slabs[layer], other), u_others[layer]),
                                    weights, (0,))
                x_in = (u.astype(jnp.float32) + own + sent).astype(jnp.bfloat16)

        shared = lax.all_gather(jnp.stack(packed), 'dp', axis=0)
        starts = shared[:, :, 0, -8].astype(jnp.int32)
        core = dp_id % 2
        kind = (dp_id // 2 + dp_id // 4) % 2
        dealt = [deal_experts(starts[:, layer], n_local, 2 * PARTS) for layer in range(n_layers)]
        of_layer = [layer for layer in range(top) for _ in range(PARTS)] + [top]
        places = [PARTS * core + part for _ in range(top) for part in range(PARTS)] + [PARTS * core + kind]
        mine = [dealt[layer][0][place] for layer, place in zip(of_layer, places)]
        list_rows = cdiv(cdiv(dp_size * 2 * cap, LANES), 8) * 8 + 8
        idx_all, gate_all = merge_tables(shared, starts, jnp.concatenate(mine),
                                         jnp.concatenate([jnp.full_like(x, layer) for x, layer in zip(mine, of_layer)]),
                                         list_rows, dp_size * 2 * tok)
        offsets = [source_offsets(starts[:, layer], x[0]) for x, layer in zip(mine, of_layer)]
        idx_all = idx_all.reshape(-1)

        d_y, full, arrived = d_out, None, []
        d_mix = [None] * n_layers
        for layer in reversed(range(n_layers)):
            both_u = [u_slabs[layer], u_others[layer]]
            u_rows = spread(both_u if layer < top else [join_rows(*both_u)])
            slabs = (u_slabs[layer], u_others[layer], d_slab, d_other)
            own, other = token_kernel(layer, runs[layer][2], tables[layer][1], slabs, weights)
            d_u = (d_y.astype(jnp.float32) + own + swap(other)).astype(jnp.bfloat16)
            last = other
            if layer == top:
                y_own, last = token_kernel(top, runs[top][2], tables[top][0], (after(u_slabs[top], other), u_others[top]), weights)
            d_mix[layer] = jnp.einsum('td,te->de', xs[layer], d_u, preferred_element_type=jnp.float32).astype(jnp.bfloat16)
            d_y = (d_u.astype(jnp.float32)
                   + jnp.einsum('te,de->td', d_u, w_mix[layer], preferred_element_type=jnp.float32)).astype(jnp.bfloat16)
            lists, tiles = dealt[layer]
            theirs = PARTS * (1 - core)
            for part in range(PARTS if layer < top else 1):
                item = of_layer.index(layer) + part
                first = sum(x.shape[0] for x in mine[:item])
                full, done = weight_grads(layer, first, mine[item], after(tiles[places[item]], last), offsets[item],
                                          (u_rows, d_rows), idx_all, gate_all, weights, full, moved if part else None)
                got = trade(done, core_pairs)
                if layer < top:
                    arrived.insert(1 + 2 * part, (layer, got, lists[theirs + part]))
                    continue
                moved = got, lists[theirs + kind]
                far = trade(done, chip_pairs)
                arrived.append((layer, far, lists[PARTS * core + 1 - kind]))
                arrived.append((layer, trade(far, core_pairs), lists[theirs + 1 - kind]))
            if layer:
                d_slab = slab(d_y)
                d_other = swap(d_slab)
                d_rows = spread([join_rows(d_slab, d_other)])
                if layer == top:
                    layer_out = (u.astype(jnp.float32) + y_own + swap(after(last, d_other))).astype(jnp.bfloat16)
        full = merge_lists(arrived[-1:], merge_lists(arrived[:-1], full))
        d_mix = lax.psum(jnp.stack(d_mix), ('dp', 'ep'))
        return (layer_out, d_y, d_mix, jnp.swapaxes(full[0], 2, 3), jnp.swapaxes(full[1], 2, 3), full[2])

    return jax.shard_map(device_body, mesh=mesh,
                         in_specs=(tok_spec, tok_spec, route_spec, route_spec, whole_spec,
                                   expert_spec, expert_spec, expert_spec),
                         out_specs=(tok_spec, tok_spec, whole_spec, expert_spec, expert_spec, expert_spec),
                         check_vma=False)
```
